32 devices in a mesh: shard: 4 (over y, x), ctx: 8 (over z, core).
Axes of the slice: x: 2, y: 2, z: 4, core: 2. Of those that a mesh axis runs over, the one named last changes fastest.
Arguments:
- tokens: bfloat16 [8, 1024, 1280], P('shard', 'ctx'), may hold values from -6 to 6
- cotangent: bfloat16 [8, 1024, 1280], P('shard', 'ctx'), may hold values from -6 to 6
- positions: int32 [8, 1024], P('shard'), may hold values from 0 to 1023, as said below
- lengths: int32 [8], P('shard'), may hold values from 256 to 1024, as said below
- attn_gain: bfloat16 [1280], P('shard'), may hold values from 0.5 to 1.5
- w_query: bfloat16 [1280, 1280], P('shard'), may hold values from -0.15625 to 0.15625
- w_key: bfloat16 [1280, 320], P('shard'), may hold values from -0.15625 to 0.15625
- w_value: bfloat16 [1280, 320], P('shard'), may hold values from -0.15625 to 0.15625
- w_out: bfloat16 [1280, 1280], P('shard'), may hold values from -3 to 3
- mlp_gain: bfloat16 [1280], P('shard'), may hold values from 0.5 to 1.5
- w_gate: bfloat16 [1280, 3584], P(None, 'shard'), may hold values from -0.15625 to 0.15625
- w_up: bfloat16 [1280, 3584], P(None, 'shard'), may hold values from -0.15625 to 0.15625
- w_down: bfloat16 [3584, 1280], P('shard'), may hold values from -0.09375 to 0.09375
Outputs:
- output: bfloat16 [8, 1024, 1280], P('shard', 'ctx')
- d_tokens: bfloat16 [8, 1024, 1280], P('shard', 'ctx')
- d_attn_gain: float32 [1280], P('shard')
- d_w_query: float32 [1280, 1280], P('shard')
- d_w_key: float32 [1280, 320], P('shard')
- d_w_value: float32 [1280, 320], P('shard')
- d_w_out: float32 [1280, 1280], P('shard')
- d_mlp_gain: float32 [1280], P('shard')
- d_w_gate: float32 [1280, 3584], P(None, 'shard')
- d_w_up: float32 [1280, 3584], P(None, 'shard')
- d_w_down: float32 [3584, 1280], P('shard')
The draws below stay inside these ranges and needn't reach their ends.
Inputs may be any that keep to these rules, and one draw needn't show every extreme that they name: In every sequence each position 0 to 1023 stands in exactly one slot; the 128 slots of one index of ctx hold two runs of 64 consecutive positions in rising order, run number a first and run number 2 * 8 - 1 - a second, with a drawn for each sequence and index. `lengths`: some sequence has length 1024 in every draw.
All inputs are finite; a program needn't handle non-finite values.
Results may differ from the reference program's by a relative error of at most 0.024.
Values may be sent and summed in bfloat16 or wider, within the bound.
A program may use at most 256 MiB of HBM per device.

```python
import math
import jax
import jax.numpy as jnp
from jax import lax

D = 1280
HQ = 20
HK = 5
HD = 64
FF = 3584
CH = 128
SEQ = 1024
SEQS = 8
HALF = 64
GROUP = 4


def draw_positions(key, part):
    rank_count = SEQ // CH
    seq_keys = jax.random.split(key, SEQS)
    orders = jax.vmap(lambda seq_key: jax.random.permutation(seq_key, rank_count))(seq_keys)
    offsets = jnp.arange(HALF, dtype=jnp.int32)
    first_run = orders[:, :, None] * HALF + offsets
    second_run = (2 * rank_count - 1 - orders)[:, :, None] * HALF + offsets
    return jnp.concatenate([first_run, second_run], axis=2).reshape(SEQS, SEQ).astype(jnp.int32)


def draw_lengths(key, part):
    length_key = jax.random.fold_in(key, 11)
    pick_key = jax.random.fold_in(key, 23)
    drawn = jax.random.randint(length_key, (SEQS,), SEQ // 4, SEQ + 1)
    longest = jax.random.randint(pick_key, (), 0, SEQS)
    return jnp.where(jnp.arange(SEQS) == longest, SEQ, drawn).astype(jnp.int32)


def block_scale(key, extent, cuts, low, largest):
    def one(position, parts):
        draws = jax.random.uniform(jax.random.fold_in(jax.random.fold_in(key, 6), position), (parts,), jnp.float32, low / len(cuts), largest / len(cuts))
        return jnp.repeat(jnp.exp(draws), extent[position] // parts).reshape((-1,) + (1,) * (len(extent) - position - 1))

    factor_of = one(*cuts[0])
    for cut in cuts[1:]:
        factor_of = factor_of * one(*cut)
    return factor_of


def bell_draw(own_key, extent, width, bound, cuts=(), held_as=jnp.bfloat16):
    values = jax.random.normal(own_key, extent, jnp.float32) * width
    if len(cuts) > 0:
        values = block_scale(own_key, extent, cuts, -0.22, 0.18) * values
    return jnp.clip(values, min=-bound, max=bound).astype(held_as)


def setup_inputs(seed: int = 0) -> dict:
    seeds = jax.random.split(jax.random.key(seed), 14)
    return {
        "tokens": bell_draw(seeds[0], (SEQS, SEQ, D), 1.0, 6.0, ((0, 4), (1, 8))),
        "cotangent": bell_draw(seeds[1], (SEQS, SEQ, D), 1.0, 6.0, ((0, 4), (1, 8))),
        "positions": draw_positions(jax.random.fold_in(seeds[13], 71), 0),
        "lengths": draw_lengths(jax.random.fold_in(seeds[13], 71), 0),
        "attn_gain": jnp.clip(1.0 + 0.1 * jax.random.normal(seeds[4], (D,), jnp.float32), 0.5, 1.5).astype(jnp.bfloat16),
        "w_query": bell_draw(seeds[5], (D, HQ * HD), D ** -0.5, 0.15625, ((0, 4),)),
        "w_key": bell_draw(seeds[6], (D, HK * HD), D ** -0.5, 0.15625, ((0, 4),)),
        "w_value": bell_draw(seeds[7], (D, HK * HD), D ** -0.5, 0.15625, ((0, 4),)),
        "w_out": bell_draw(seeds[8], (HQ * HD, D), 4 ** -0.5, 3.0, ((0, 4),)),
        "mlp_gain": jnp.clip(1.0 + 0.1 * jax.random.normal(seeds[9], (D,), jnp.float32), 0.5, 1.5).astype(jnp.bfloat16),
        "w_gate": bell_draw(seeds[10], (D, FF), D ** -0.5, 0.15625, ((1, 4),)),
        "w_up": bell_draw(seeds[11], (D, FF), D ** -0.5, 0.15625, ((1, 4),)),
        "w_down": bell_draw(seeds[12], (FF, D), FF ** -0.5, 0.09375, ((0, 4),)),
    }


EPSILON = 1e-05
NEGATIVE = -1e+30
ROPE_BASE = 10000.0
PRECISE = lax.Precision.HIGHEST

@jax.custom_vjp
def low(v):
    return lax.optimization_barrier(v.astype(jnp.bfloat16)).astype(jnp.float32)

@jax.custom_vjp
def low_back(v):
    return v

def low_keep(v):
    return (low(v), None)

def low_pass(kept, grad):
    return (grad,)

def back_keep(v):
    return (v, None)

def back_low(kept, grad):
    return (low(grad),)
low.defvjp(low_keep, low_pass)
low_back.defvjp(back_keep, back_low)

def rope_parts(places):
    half_dim = HD // 2
    frequency = ROPE_BASE ** (-jnp.arange(half_dim, dtype=jnp.float32) * 2.0 / HD)
    angles = places.astype(jnp.float32)[..., None] * frequency
    return (jnp.cos(angles), jnp.sin(angles))

def rotate(values, cosine, sine_part):
    half_dim = values.shape[-1] // 2
    first_half = values[..., :half_dim]
    second_half = values[..., half_dim:]
    cosine_b = cosine[..., None, :]
    sine_b = sine_part[..., None, :]
    return jnp.concatenate([first_half * cosine_b - second_half * sine_b, second_half * cosine_b + first_half * sine_b], -1)

def rms_norm(hidden, gain_vec):
    inv_scale = lax.rsqrt(lax.optimization_barrier(jnp.mean(hidden * hidden, -1, keepdims=True)) + EPSILON)
    return hidden * inv_scale * gain_vec

def matmul(left_side, right_side):
    return jnp.dot(left_side, right_side, precision=PRECISE, preferred_element_type=jnp.float32)

def attention(query_rot, key_rot, value_low, places, seq_lengths):
    batch_size = query_rot.shape[0]
    block_rows = math.gcd(SEQ, 512)
    block_count = SEQ // block_rows
    factor = 1.0 / math.sqrt(HD)
    query_blocks = jnp.moveaxis(query_rot.reshape(batch_size, block_count, block_rows, HK, GROUP, HD), 1, 0)
    place_blocks = jnp.moveaxis(places.reshape(batch_size, block_count, block_rows), 1, 0)
    key_ok = places < seq_lengths[:, None]

    def one_block(block_item):
        query_part, query_places = block_item
        scores = jnp.einsum('bqhgd,bkhd->bhgqk', query_part, key_rot, precision=PRECISE) * factor
        scores = low_back(scores)
        allowed = (places[:, None, :] <= query_places[:, :, None]) & key_ok[:, None, :]
        masked = jnp.where(allowed[:, None, None], scores, NEGATIVE)
        row_max = lax.optimization_barrier(jnp.max(masked, -1, keepdims=True))
        exp_scores = jnp.exp(masked - row_max)
        softmax = exp_scores / lax.optimization_barrier(jnp.sum(exp_scores, -1, keepdims=True))
        return jnp.einsum('bhgqk,bkhd->bqhgd', low(softmax), value_low, precision=PRECISE)
    blocks_out = lax.map(jax.checkpoint(one_block), (query_blocks, place_blocks))
    return jnp.moveaxis(blocks_out, 0, 1).reshape(batch_size, SEQ, HQ * HD)

def layer(inputs, attn_gain, w_query, w_key, w_value, w_out, mlp_gain, w_gate, w_up, w_down, places, seq_lengths):
    batch_size = inputs.shape[0]
    row_count = batch_size * SEQ
    hidden = inputs.reshape(row_count, D)
    norm_one = low(rms_norm(hidden, attn_gain))
    queries = low_back(matmul(norm_one, w_query))
    key_proj = low_back(matmul(norm_one, w_key))
    value_low = low(low_back(matmul(norm_one, w_value)))
    cosine, sine_part = rope_parts(places.reshape(row_count))
    query_rot = low(rotate(queries.reshape(row_count, HQ, HD), cosine, sine_part))
    key_rot = low(rotate(key_proj.reshape(row_count, HK, HD), cosine, sine_part))
    mixed_heads = attention(query_rot.reshape(batch_size, SEQ, HK, GROUP, HD), key_rot.reshape(batch_size, SEQ, HK, HD), value_low.reshape(batch_size, SEQ, HK, HD), places, seq_lengths)
    attended = low(low_back(mixed_heads.reshape(row_count, HQ * HD)))
    middle = hidden + low_back(matmul(attended, w_out))
    norm_two = low(rms_norm(middle, mlp_gain))
    gate_proj = low_back(matmul(norm_two, w_gate))
    up_proj = low_back(matmul(norm_two, w_up))
    inner_act = low(jax.nn.silu(gate_proj) * up_proj)
    result = middle + low_back(matmul(inner_act, w_down))
    return result.reshape(batch_size, SEQ, D)

def reference(tokens, cotangent, positions, lengths, attn_gain, w_query, w_key, w_value, w_out, mlp_gain, w_gate, w_up, w_down):
    weights = tuple((weight.astype(jnp.float32) for weight in (attn_gain, w_query, w_key, w_value, w_out, mlp_gain, w_gate, w_up, w_down)))
    group_size = math.gcd(SEQS, max(1, 4096 // SEQ))
    step_count = SEQS // group_size

    def one_group(running, batch_item):
        inputs, cot_part, places, seq_lengths = batch_item
        valid_rows = (places < seq_lengths[:, None]).astype(jnp.float32)

        def apply_layer(inputs_f, *params):
            return layer(inputs_f, *params, places, seq_lengths)
        result, pullback = jax.vjp(apply_layer, inputs.astype(jnp.float32), *weights)
        gradients = pullback(cot_part.astype(jnp.float32) * valid_rows[..., None])
        running = tuple((carried + gradient for carried, gradient in zip(running, gradients[1:])))
        return (running, (result.astype(jnp.bfloat16), gradients[0].astype(jnp.bfloat16)))
    initial = tuple((jnp.zeros(weight.shape, jnp.float32) for weight in weights))
    stacked = (tokens.reshape(step_count, group_size, SEQ, D), cotangent.reshape(step_count, group_size, SEQ, D), positions.reshape(step_count, group_size, SEQ), lengths.reshape(step_count, group_size))
    totals, (outputs, d_inputs) = lax.scan(one_group, initial, stacked)
    return (outputs.reshape(SEQS, SEQ, D), d_inputs.reshape(SEQS, SEQ, D), totals[0], totals[1], totals[2], totals[3], totals[4], totals[5], totals[6], totals[7], totals[8])
```

```python
import math

import jax
import jax.numpy as jnp
from jax import lax
from jax.sharding import Mesh
from jax.sharding import PartitionSpec as P

HQ = 20
HK = 5
HD = 64


EPSILON = 1e-05
NEGATIVE = -1e30
ROPE_BASE = 10000.0


def rope_parts(places):
    half_dim = HD // 2
    frequency = ROPE_BASE ** (-jnp.arange(half_dim, dtype=jnp.float32) * 2.0 / HD)
    angles = places.astype(jnp.float32)[..., None] * frequency
    return (jnp.cos(angles), jnp.sin(angles))


def rotate(values, cosine, sine_part):
    half_dim = values.shape[-1] // 2
    first_half = values[..., :half_dim]
    second_half = values[..., half_dim:]
    cosine_b = cosine[..., None, :]
    sine_b = sine_part[..., None, :]
    return jnp.concatenate(
        [
            first_half * cosine_b - second_half * sine_b,
            second_half * cosine_b + first_half * sine_b,
        ],
        -1,
    )


def row_norm(hidden, gain_vec):
    inv_scale = lax.rsqrt(jnp.mean(hidden * hidden, -1, keepdims=True) + EPSILON)
    return (hidden * inv_scale * gain_vec, inv_scale)


def norm_back(grad_norm, hidden, inv_scale, gain_vec):
    scaled = grad_norm * gain_vec
    grad_gain = jnp.sum(grad_norm * hidden * inv_scale, 0)
    grad_hidden = inv_scale * scaled - hidden * inv_scale**3 * jnp.mean(
        scaled * hidden, -1, keepdims=True
    )
    return (grad_hidden, grad_gain)


def product(left_side, right_side):
    return jnp.dot(left_side, right_side, preferred_element_type=jnp.float32)


def product_tn(left_side, right_side):
    return jnp.einsum("ra,rb->ab", left_side, right_side, preferred_element_type=jnp.float32)


def product_nt(left_side, right_side):
    return jnp.einsum("ra,ba->rb", left_side, right_side, preferred_element_type=jnp.float32)


def gate_back(grad_inner, gate_proj, up_proj):
    sigmoid_gate = jax.nn.sigmoid(gate_proj)
    grad_gate = (
        grad_inner * up_proj * sigmoid_gate * (1.0 + gate_proj * (1.0 - sigmoid_gate))
    ).astype(jnp.bfloat16)
    grad_up = (grad_inner * gate_proj * sigmoid_gate).astype(jnp.bfloat16)
    return (grad_gate, grad_up)


def block_scores(query_rot, key_piece, query_places, key_places, seq_lengths):
    micro_count, span_rows = (key_piece.shape[0], key_piece.shape[1])
    key_heads = key_piece.reshape(micro_count, span_rows, HK, HD)
    scores = jnp.einsum(
        "mqhgd,mkhd->mhgqk", query_rot, key_heads, preferred_element_type=jnp.float32
    ) * (1.0 / math.sqrt(HD))
    allowed = (key_places[:, None, :] <= query_places[:, :, None]) & (
        key_places < seq_lengths[:, None]
    )[:, None, :]
    return (scores, allowed[:, None, None])


def over_blocks(span_rows, block_rows, step_fn, carried):
    sub_rows = math.gcd(span_rows, block_rows)

    def one_step(fold_state, block_index):
        return (step_fn(fold_state, block_index * sub_rows, sub_rows), None)

    final_state, unused = lax.scan(one_step, carried, jnp.arange(span_rows // sub_rows))
    return final_state


def per_device(
    tokens,
    cotangent,
    positions,
    lengths,
    attn_gain,
    w_query,
    w_key,
    w_value,
    w_out,
    mlp_gain,
    w_gate,
    w_up,
    w_down,
):
    micro_count, stretch_len, model_width = tokens.shape
    ctx_count = lax.axis_size("line") * lax.axis_size("core")
    full_len = stretch_len * ctx_count
    row_count = micro_count * stretch_len
    query_width = HQ * HD
    kv_width = HK * HD
    group_size = HQ // HK
    factor = 1.0 / math.sqrt(HD)
    block_rows = stretch_len * math.gcd(ctx_count, max(1, 512 // stretch_len))
    rank_ctx = lax.axis_index("line") * lax.axis_size("core") + lax.axis_index("core")
    query_places = lax.dynamic_slice_in_dim(positions, rank_ctx * stretch_len, stretch_len, 1)
    valid_rows = (query_places < lengths[:, None]).astype(jnp.float32).reshape(row_count, 1)
    cosine, sine_part = rope_parts(query_places.reshape(row_count))
    gain_one, gain_two = (
        lax.all_gather(attn_gain, "shard", axis=0, tiled=True),
        lax.all_gather(mlp_gain, "shard", axis=0, tiled=True),
    )
    qkv_local = jnp.concatenate([w_query, w_key, w_value], axis=1)
    qkv_all = lax.all_gather(qkv_local, "shard", axis=0, tiled=True)
    query_all = qkv_all[:, :query_width]
    key_all = qkv_all[:, query_width : query_width + kv_width]
    value_all = qkv_all[:, query_width + kv_width :]
    out_all = lax.all_gather(w_out, "shard", axis=0, tiled=True)
    grad_out = cotangent.reshape(row_count, model_width).astype(jnp.float32) * valid_rows
    grad_low = grad_out.astype(jnp.bfloat16)
    grad_low_all = lax.all_gather(grad_low, "shard", axis=0, tiled=True)
    hidden = tokens.reshape(row_count, model_width).astype(jnp.float32)
    normed_one, inv_one = row_norm(hidden, gain_one.astype(jnp.float32))
    norm_one = normed_one.astype(jnp.bfloat16)
    qkv = product(norm_one, qkv_all)
    queries = qkv[:, :query_width]
    key_proj = qkv[:, query_width : query_width + kv_width]
    value_low = (
        qkv[:, query_width + kv_width :]
        .astype(jnp.bfloat16)
        .reshape(micro_count, stretch_len, kv_width)
    )
    query_rot = (
        rotate(queries.reshape(row_count, HQ, HD), cosine, sine_part)
        .astype(jnp.bfloat16)
        .reshape(micro_count, stretch_len, HK, group_size, HD)
    )
    key_rot = (
        rotate(key_proj.reshape(row_count, HK, HD), cosine, sine_part)
        .astype(jnp.bfloat16)
        .reshape(micro_count, stretch_len, kv_width)
    )

    def attend_rows(fold_state, key_piece, value_piece, first_row):
        run_max, run_sum, run_acc = fold_state
        span_rows = key_piece.shape[1]
        key_places = lax.dynamic_slice_in_dim(positions, first_row, span_rows, 1)
        scores, allowed = block_scores(query_rot, key_piece, query_places, key_places, lengths)
        masked = jnp.where(allowed, scores, NEGATIVE)
        new_max = jnp.maximum(run_max, jnp.max(masked, -1))
        weights = jnp.where(allowed, jnp.exp(masked - new_max[..., None]), 0.0)
        factor_old = jnp.exp(run_max - new_max)
        new_sum = run_sum * factor_old + jnp.sum(weights, -1)
        update = jnp.einsum(
            "mhgqk,mkhd->mqhgd",
            weights.astype(jnp.bfloat16),
            value_piece.reshape(micro_count, span_rows, HK, HD),
            preferred_element_type=jnp.float32,
        )
        rescale = jnp.transpose(factor_old, (0, 3, 1, 2))[..., None]
        return (new_max, new_sum, run_acc * rescale + update)

    initial = (
        jnp.full((micro_count, HK, group_size, stretch_len), NEGATIVE, jnp.float32),
        jnp.zeros((micro_count, HK, group_size, stretch_len), jnp.float32),
        jnp.zeros((micro_count, stretch_len, HK, group_size, HD), jnp.float32),
    )
    key_piece = lax.all_gather(key_rot, ("line", "core"), axis=1, tiled=True)
    value_piece = lax.all_gather(value_low, ("line", "core"), axis=1, tiled=True)

    def step_fn(inner_state, offset, sub_rows):
        key_sub = lax.dynamic_slice_in_dim(key_piece, offset, sub_rows, 1)
        value_sub = lax.dynamic_slice_in_dim(value_piece, offset, sub_rows, 1)
        return attend_rows(inner_state, key_sub, value_sub, offset)

    run_max, run_sum, run_acc = over_blocks(key_piece.shape[1], block_rows, step_fn, initial)
    log_sum = run_max + jnp.log(run_sum)
    attended = run_acc / jnp.transpose(run_sum, (0, 3, 1, 2))[..., None]
    attn_low = attended.reshape(row_count, query_width).astype(jnp.bfloat16)
    middle = hidden + product(attn_low, out_all)
    gain_two_f = gain_two.astype(jnp.float32)
    normed_two, inv_two = row_norm(middle, gain_two_f)
    norm_two = normed_two.astype(jnp.bfloat16)
    norm_two_all = lax.all_gather(norm_two, "shard", axis=0, tiled=True)
    gate_proj = product(norm_two_all, w_gate)
    up_proj = product(norm_two_all, w_up)
    inner_act = (jax.nn.silu(gate_proj) * up_proj).astype(jnp.bfloat16)
    grad_inner = product_nt(grad_low_all, w_down)
    grad_gate, grad_up = gate_back(grad_inner, gate_proj, up_proj)
    grad_norm_two = lax.psum_scatter(
        (product_nt(grad_gate, w_gate) + product_nt(grad_up, w_up)).astype(jnp.bfloat16),
        "shard",
        scatter_dimension=0,
        tiled=True,
    ).astype(jnp.float32)
    mlp_out = lax.psum_scatter(
        product(inner_act, w_down).astype(jnp.bfloat16), "shard", scatter_dimension=0, tiled=True
    ).astype(jnp.float32)
    result = (middle + mlp_out).astype(jnp.bfloat16).reshape(micro_count, stretch_len, model_width)
    grad_wdown = product_tn(inner_act, grad_low_all).astype(jnp.bfloat16)
    grad_wgate = product_tn(norm_two_all, grad_gate).astype(jnp.bfloat16)
    grad_wup = product_tn(norm_two_all, grad_up).astype(jnp.bfloat16)

    def over_ctx(part):
        share = lax.psum_scatter(part, "core", scatter_dimension=0, tiled=True)
        share = lax.psum(share, "line")
        return lax.all_gather(share, "core", axis=0, tiled=True)

    total_wdown, total_wgate, total_wup = over_ctx(grad_wdown), over_ctx(grad_wgate), over_ctx(grad_wup)
    grad_mid_norm, grad_gain_two = norm_back(grad_norm_two, middle, inv_two, gain_two_f)
    grad_middle = grad_out + grad_mid_norm
    grad_proj = grad_middle.astype(jnp.bfloat16)
    grad_wout = product_tn(attn_low, grad_proj)
    grad_attn = (
        product_nt(grad_proj, out_all)
        .astype(jnp.bfloat16)
        .reshape(micro_count, stretch_len, HK, group_size, HD)
    )
    row_delta = jnp.transpose(jnp.sum(grad_attn.astype(jnp.float32) * attended, -1), (0, 2, 3, 1))
    key_full, value_full = key_piece, value_piece

    def grad_block(key_piece, value_piece, first_row):
        span_rows = key_piece.shape[1]
        key_places = lax.dynamic_slice_in_dim(positions, first_row, span_rows, 1)
        scores, allowed = block_scores(query_rot, key_piece, query_places, key_places, lengths)
        softmax = jnp.where(allowed, jnp.exp(scores - log_sum[..., None]), 0.0)
        grad_soft = jnp.einsum(
            "mqhgd,mkhd->mhgqk",
            grad_attn,
            value_piece.reshape(micro_count, span_rows, HK, HD),
            preferred_element_type=jnp.float32,
        )
        grad_score = (softmax * (grad_soft - row_delta[..., None])).astype(jnp.bfloat16)
        return (softmax, grad_score)

    def query_step(grad_acc, offset, sub_rows):
        key_piece = lax.dynamic_slice_in_dim(key_full, offset, sub_rows, 1)
        value_piece = lax.dynamic_slice_in_dim(value_full, offset, sub_rows, 1)
        softmax, grad_score = grad_block(key_piece, value_piece, offset)
        return grad_acc + jnp.einsum(
            "mhgqk,mkhd->mqhgd",
            grad_score,
            key_piece.reshape(micro_count, sub_rows, HK, HD),
            preferred_element_type=jnp.float32,
        )

    grad_qrot = (
        over_blocks(
            full_len,
            block_rows,
            query_step,
            jnp.zeros((micro_count, stretch_len, HK, group_size, HD), jnp.float32),
        )
        * factor
    )
    span_rows = stretch_len * ctx_count
    sub_rows = math.gcd(span_rows, block_rows)

    def one_piece(block_index):
        offset = block_index * sub_rows
        key_piece = lax.dynamic_slice_in_dim(key_full, offset, sub_rows, 1)
        value_piece = lax.dynamic_slice_in_dim(value_full, offset, sub_rows, 1)
        softmax, grad_score = grad_block(key_piece, value_piece, offset)
        grad_val = jnp.einsum(
            "mhgqk,mqhgd->kmhd",
            softmax.astype(jnp.bfloat16),
            grad_attn,
            preferred_element_type=jnp.float32,
        )
        grad_key = (
            jnp.einsum(
                "mhgqk,mqhgd->kmhd", grad_score, query_rot, preferred_element_type=jnp.float32
            )
            * factor
        )
        return jnp.concatenate(
            [
                grad_key.reshape(sub_rows, micro_count, kv_width),
                grad_val.reshape(sub_rows, micro_count, kv_width),
            ],
            -1,
        )

    stacked = lax.map(one_piece, jnp.arange(span_rows // sub_rows))
    grad_kv = lax.psum_scatter(
        stacked.reshape(span_rows, micro_count, 2 * kv_width).astype(jnp.bfloat16),
        ("line", "core"),
        scatter_dimension=0,
        tiled=True,
    ).astype(jnp.float32)
    grad_kv = jnp.transpose(grad_kv, (1, 0, 2)).reshape(row_count, 2 * kv_width)
    grad_queries = (
        rotate(grad_qrot.reshape(row_count, HQ, HD), cosine, -sine_part)
        .reshape(row_count, query_width)
        .astype(jnp.bfloat16)
    )
    grad_keys = (
        rotate(grad_kv[:, :kv_width].reshape(row_count, HK, HD), cosine, -sine_part)
        .reshape(row_count, kv_width)
        .astype(jnp.bfloat16)
    )
    grad_values = grad_kv[:, kv_width:].astype(jnp.bfloat16)
    grad_qkv = jnp.concatenate([grad_queries, grad_keys, grad_values], axis=1)
    grad_wqkv = product_tn(norm_one, grad_qkv).astype(jnp.bfloat16)
    grad_norm_one = product_nt(grad_qkv, qkv_all)
    grad_hidden, grad_gain_one = norm_back(
        grad_norm_one, hidden, inv_one, gain_one.astype(jnp.float32)
    )
    grad_input = (
        (grad_middle + grad_hidden)
        .astype(jnp.bfloat16)
        .reshape(micro_count, stretch_len, model_width)
    )

    def over_all(part):
        share = lax.psum_scatter(part, "shard", scatter_dimension=0, tiled=True)
        return over_ctx(share)

    total_wout = over_all(grad_wout.astype(jnp.bfloat16))
    total_wqkv = over_all(grad_wqkv)
    gains = jnp.stack([grad_gain_one, grad_gain_two], axis=1).astype(jnp.bfloat16)
    gains = lax.psum(gains, ("shard", "line", "core")).astype(jnp.float32)
    span = attn_gain.shape[0]
    gains = lax.dynamic_slice_in_dim(gains, lax.axis_index("shard") * span, span, 0)
    f32 = jnp.float32
    return (
        result,
        grad_input,
        gains[:, 0],
        total_wqkv[:, :query_width].astype(f32),
        total_wqkv[:, query_width : query_width + kv_width].astype(f32),
        total_wqkv[:, query_width + kv_width :].astype(f32),
        total_wout.astype(f32),
        gains[:, 1],
        total_wgate.astype(f32),
        total_wup.astype(f32),
        total_wdown.astype(f32),
    )


def solution(mesh):
    shards, ctx = mesh.devices.shape
    inner = Mesh(mesh.devices.reshape(shards, ctx // 2, 2), ("shard", "line", "core"))
    where = ("line", "core")
    return jax.shard_map(
        per_device,
        mesh=inner,
        in_specs=(
            P("shard", where, None),
            P("shard", where, None),
            P("shard", None),
            P("shard"),
            P("shard"),
            P("shard", None),
            P("shard", None),
            P("shard", None),
            P("shard", None),
            P("shard"),
            P(None, "shard"),
            P(None, "shard"),
            P("shard", None),
        ),
        out_specs=(
            P("shard", where, None),
            P("shard", where, None),
            P("shard"),
            P("shard", None),
            P("shard", None),
            P("shard", None),
            P("shard", None),
            P("shard"),
            P(None, "shard"),
            P(None, "shard"),
            P("shard", None),
        ),
        check_vma=False,
    )
```

```python
import math

import jax
import jax.numpy as jnp
from jax import lax
from jax.experimental import pallas as pl
from jax.experimental.pallas import tpu as pltpu
from jax.sharding import Mesh
from jax.sharding import PartitionSpec as P

HQ = 20
HK = 5
HD = 64
GROUP = HQ // HK
EPSILON = 1e-05
NEGATIVE = -1e30
ROPE_BASE = 10000.0
BF = jnp.bfloat16
F32 = jnp.float32
BY_MESH = pl.DeviceIdType.MESH
VMEM_LIMIT = 67043328


def nn(a, b):
    return lax.dot_general(a, b, (((1,), (0,)), ((), ())), preferred_element_type=F32)


def nt(a, b):
    return lax.dot_general(a, b, (((1,), (1,)), ((), ())), preferred_element_type=F32)


def tn(a, b):
    return lax.dot_general(a, b, (((0,), (0,)), ((), ())), preferred_element_type=F32)


def lanes_of(rows):
    return lax.broadcasted_iota(jnp.int32, (rows, 128), 1)


def swap_halves(block, lane):
    left = pltpu.roll(block, 96, 1)
    right = pltpu.roll(block, 32, 1)
    return jnp.where(lane % 64 < 32, left, right)


def add_rows(target, parts, rows, step):
    def body(index, carry):
        span = pl.ds(pl.multiple_of(index * step, step), step)
        total = parts[0][span, :].astype(F32)
        for part in parts[1:]:
            total = total + part[span, :].astype(F32)
        target[span, :] = total.astype(target.dtype)
        return carry

    lax.fori_loop(0, rows // step, body, 0)


def backward_kernel(
    sizes,
    gm_ref,
    attn_ref,
    attn_t_ref,
    qp_ref,
    n1_t_ref,
    x_ref,
    gain_ref,
    cos_ref,
    sin_ref,
    gg_ref,
    wo_hbm,
    wq_hbm,
    wkv_hbm,
    pt_hbm,
    kv_hbm,
    dw_hbm,
    out_dw,
    out_wo,
    out_wq,
    out_wkv,
    out_gain,
    out_dx,
    w_buf,
    wkv_buf,
    pt_buf,
    kv_buf,
    dproj,
    dop,
    delta,
    dkv,
    dkv_x,
    dkv_z,
    dq,
    dkv_own,
    own,
    got_x,
    got_r,
    got_t,
    g_buf,
    g_kv,
    o_x,
    o_z,
    o_r,
    o_t,
    q_x,
    q_z,
    q_r,
    q_t,
    k_x,
    k_z,
    k_r,
    k_t,
    gn_own,
    gn_x,
    gn_z,
    gn_r,
    gn_t,
    load_sem,
    pt_sem,
    kv_sem,
    core_sem,
    up_send,
    r_recv,
    t_recv,
    down_send,
    sib_send,
    sib_recv,
    local_sem,
    dkv_core,
    dkv_send,
    dkv_recv,
    g_core,
    g_send,
    g_recv,
    a_up,
    a_r,
    a_t,
    a_down,
    a_sib_send,
    a_sib_recv,
    a_local,
):
    shards, line, keys, rows, width, feed = sizes
    s_id, l_id, c_id = lax.axis_index("shard"), lax.axis_index("line"), lax.axis_index("core")
    sibling = (s_id, l_id, 1 - c_id)
    in_low = l_id < line // 2
    toward = jnp.where(in_low, 1, -1)
    inner = (s_id, l_id + toward, c_id)
    has_outer = (l_id > 0) & (l_id < line - 1)
    is_mid = (l_id == line // 2 - 1) | (l_id == line // 2)
    outer = (s_id, jnp.where(has_outer, l_id - toward, l_id + toward), c_id)
    peers = [(lax.rem(s_id + k, shards), l_id, c_id) for k in range(1, shards)]
    mates = [(s_id, lax.rem(l_id + k, line), c_id) for k in range(1, line)]

    def remote(src, dst, send, recv, to):
        return pltpu.make_async_remote_copy(
            src, dst, send, recv, device_id=to, device_id_type=BY_MESH
        )

    barrier = pltpu.get_barrier_semaphore()
    for other in [sibling] + peers + mates:
        pl.semaphore_signal(barrier, inc=1, device_id=other, device_id_type=BY_MESH)
    pl.semaphore_wait(barrier, 1 + len(peers) + len(mates))

    half = width // 2
    chunk = half // 4
    chunks = 12
    slab = 16
    part = width // shards
    own_rows = part // 2
    blocks = keys // 1024
    hlf = pl.ds(pl.multiple_of(c_id * half, 16), half)
    oth = pl.ds(pl.multiple_of((1 - c_id) * half, 16), half)

    core_copy = [
        remote(dw_hbm.at[k, oth], got_x.at[k], core_sem.at[k], core_sem.at[3 + k], sibling)
        for k in range(3)
    ]
    own_load = [
        pltpu.make_async_copy(dw_hbm.at[k, hlf], own.at[k], load_sem.at[k]) for k in range(3)
    ]
    load_wo = pltpu.make_async_copy(wo_hbm, w_buf, load_sem.at[3])
    load_wkv = pltpu.make_async_copy(wkv_hbm, wkv_buf, load_sem.at[4])
    load_wq = pltpu.make_async_copy(wq_hbm, w_buf, load_sem.at[5])
    load_wo.start()
    for k in range(3):
        own_load[k].start()
        core_copy[k].start()
    load_wkv.start()

    total_steps = 2 * HK * blocks

    def pt_copy(step, slot):
        pair, block = step // blocks, step % blocks
        span = pl.ds(pl.multiple_of(block * 1024, 1024), 1024)
        return pltpu.make_async_copy(pt_hbm.at[pair, span], pt_buf.at[slot], pt_sem.at[slot])

    def kv_copy(step, slot):
        pair, block = step // blocks, step % blocks
        span = pl.ds(pl.multiple_of(block * 1024, 1024), 1024)
        return pltpu.make_async_copy(kv_hbm.at[pair, span], kv_buf.at[slot], kv_sem.at[slot])

    pt_copy(0, 0).start()
    kv_copy(0, 0).start()

    def spot(index):
        array, piece = index // 4, index % 4
        return array, pl.ds(pl.multiple_of(piece * chunk, 16), chunk)

    def up(index):
        array, span = spot(index)
        mine, extra, came = own.at[array, span], got_x.at[array, span], got_r.at[array, span]

        @pl.when(index % 4 == 0)
        def _():
            pltpu.make_async_copy(
                dw_hbm.at[array, hlf], own.at[array], load_sem.at[array]
            ).wait()
            remote(
                dw_hbm.at[array, oth],
                got_x.at[array],
                core_sem.at[array],
                core_sem.at[3 + array],
                sibling,
            ).wait()

        @pl.when(has_outer)
        def _():
            remote(mine, came, up_send.at[index], r_recv.at[index], inner).wait_recv()
            add_rows(mine, [mine, extra, came], chunk, slab)

        @pl.when(jnp.logical_not(has_outer))
        def _():
            add_rows(mine, [mine, extra], chunk, slab)

        @pl.when(is_mid)
        def _():
            remote(
                mine, got_t.at[array, span], up_send.at[index], t_recv.at[index], inner
            ).start()

        @pl.when(jnp.logical_not(is_mid))
        def _():
            remote(mine, came, up_send.at[index], r_recv.at[index], inner).start()

    def out_span(index, core):
        array, piece = index // 4, index % 4
        return out_dw.at[array, pl.ds(pl.multiple_of(core * half + piece * chunk, 16), chunk)]

    def down(index):
        array, span = spot(index)
        mine, total = own.at[array, span], got_t.at[array, span]
        remote(mine, total, up_send.at[index], t_recv.at[index], inner).wait_recv()

        @pl.when(is_mid)
        def _():
            add_rows(total, [mine, total], chunk, slab)

        @pl.when(has_outer)
        def _():
            remote(total, total, down_send.at[index], t_recv.at[index], outer).start()

        remote(
            total, out_span(index, c_id), sib_send.at[index], sib_recv.at[index], sibling
        ).start()
        pltpu.make_async_copy(total, out_span(index, c_id), local_sem.at[index]).start()

    def settle(index):
        array, span = spot(index)
        mine, total = own.at[array, span], got_t.at[array, span]
        remote(mine, total, up_send.at[index], t_recv.at[index], inner).wait_send()

        @pl.when(has_outer)
        def _():
            remote(total, total, down_send.at[index], t_recv.at[index], outer).wait_send()

        last = remote(
            total, out_span(index, 1 - c_id), sib_send.at[index], sib_recv.at[index], sibling
        )
        last.wait()
        pltpu.make_async_copy(total, out_span(index, c_id), local_sem.at[index]).wait()

    def ring(step):
        @pl.when((step >= 0) & (step < chunks))
        def _():
            up(step)

        @pl.when((step >= 3) & (step < chunks + 3) & is_mid)
        def _():
            down(step - 3)

        @pl.when((step >= 6) & (step < chunks + 6) & jnp.logical_not(is_mid))
        def _():
            down(step - 6)

    def core_part(grad, cols, box, slot):
        far = pl.ds(pl.multiple_of((1 - c_id) * own_rows, 16), own_rows)
        return remote(
            grad.at[:, far, :], box, g_core.at[slot], g_core.at[3 + slot], sibling
        )

    def scatter_part(grad, box, zone, slot):
        core_part(grad, None, box, slot).wait()
        near = pl.ds(pl.multiple_of(c_id * own_rows, 16), own_rows)

        def body(s, carry):
            add_rows(box.at[s], [grad.at[s, near], box.at[s]], own_rows, slab)
            return carry

        lax.fori_loop(0, shards, body, 0)
        for k in range(1, shards):
            scatter_copy(box, zone, slot, k).start()

    def scatter_copy(box, zone, slot, k):
        return remote(
            box.at[lax.rem(s_id + k, shards)],
            zone.at[k - 1],
            g_send.at[slot, k - 1],
            g_recv.at[slot, k - 1],
            peers[k - 1],
        )

    def gather_part(box, zone, slot):
        for k in range(1, shards):
            scatter_copy(box, zone, slot, k).wait()
        add_rows(
            box.at[s_id],
            [box.at[s_id]] + [zone.at[k] for k in range(shards - 1)],
            own_rows,
            slab,
        )

    def line_up(mine, came, total, slot, count):
        @pl.when(has_outer)
        def _():
            remote(mine, came, a_up.at[slot], a_r.at[slot], inner).wait_recv()
            add_rows(mine, [mine, came], count, slab if mine.dtype == BF else 8)

        @pl.when(is_mid)
        def _():
            remote(mine, total, a_up.at[slot], a_t.at[slot], inner).start()

        @pl.when(jnp.logical_not(is_mid))
        def _():
            remote(mine, came, a_up.at[slot], a_r.at[slot], inner).start()

    def line_down(mine, total, slot, count, near, far):
        remote(mine, total, a_up.at[slot], a_t.at[slot], inner).wait()

        @pl.when(is_mid)
        def _():
            add_rows(total, [mine, total], count, slab if mine.dtype == BF else 8)

        @pl.when(has_outer)
        def _():
            remote(total, total, a_down.at[slot], a_t.at[slot], outer).start()

        if far is not None:
            remote(total, near, a_sib_send.at[slot], a_sib_recv.at[slot], sibling).start()
        pltpu.make_async_copy(total, near, a_local.at[slot]).start()

    def line_settle(total, slot, near, far):
        @pl.when(has_outer)
        def _():
            remote(total, total, a_down.at[slot], a_t.at[slot], outer).wait_send()

        if far is not None:
            remote(total, far, a_sib_send.at[slot], a_sib_recv.at[slot], sibling).wait()
        pltpu.make_async_copy(total, near, a_local.at[slot]).wait()

    lane = lanes_of(128)
    dproj[...] = gm_ref[...].astype(BF)
    load_wo.wait()

    def spread(head, carry):
        block = nt(
            dproj[...], w_buf[pl.ds(pl.multiple_of(head * 256, 256), 256), :]
        ).astype(BF)
        for seq in range(2):
            for two in range(2):
                piece = block[seq * 128 : seq * 128 + 128, two * 128 : two * 128 + 128].astype(
                    F32
                )
                place = seq * HK + head
                first = jnp.where(lane >= 64, pltpu.roll(piece, 64, 1), 0.0)
                dop[place, pl.ds(two * 256, 128), :] = first.astype(BF)
                dop[place, pl.ds(two * 256 + 128, 128), :] = jnp.where(
                    lane >= 64, piece, 0.0
                ).astype(BF)
                value = attn_ref[
                    pl.ds(seq * 128, 128),
                    pl.ds(pl.multiple_of(head * 256 + two * 128, 128), 128),
                ].astype(F32)
                product = jnp.transpose(piece * value)
                delta[place, :, pl.ds(two * 256, 128)] = jnp.sum(
                    product[:64], 0, keepdims=True
                )
                delta[place, :, pl.ds(two * 256 + 128, 128)] = jnp.sum(
                    product[64:], 0, keepdims=True
                )
        return carry

    lax.fori_loop(0, HK, spread, 0)
    load_wq.start()
    ring(0)

    def weight_grad(left, right, grad, count):
        def body(s, carry):
            grad[s] = nn(
                left[pl.ds(pl.multiple_of(s * part, 16), part), :], right[...]
            ).astype(BF)
            return carry

        lax.fori_loop(0, count, body, 0)

    weight_grad(attn_t_ref, dproj, g_buf, shards)
    core_part(g_buf, None, o_x, 0).start()
    ring(1)

    cosine, sine = cos_ref, sin_ref

    def attend(step, carry):
        slot = lax.rem(step, 2)
        pair, block = step // blocks, step % blocks

        @pl.when(step + 1 < total_steps)
        def _():
            pt_copy(step + 1, 1 - slot).start()
            kv_copy(step + 1, 1 - slot).start()

        pt_copy(step, slot).wait()
        kv_copy(step, slot).wait()
        keyval = kv_buf[slot]
        soft = pt_buf[slot]
        grad_soft = nt(keyval, dop[pair])
        score = (soft.astype(F32) * (grad_soft - delta[pair])).astype(BF)
        both = (nn(score, qp_ref[pair]) + nn(soft, dop[pair])).astype(BF)
        for sub in range(8):
            dkv[pair, block * 4 + sub // 2, sub % 2] = both[sub * 128 : sub * 128 + 128]
        query = tn(keyval, score)[:64] * (1.0 / math.sqrt(HD))
        seq, head = pair // HK, pair % HK
        for two in range(2):
            piece = jnp.transpose(
                jnp.concatenate(
                    [
                        query[:, two * 256 : two * 256 + 128],
                        query[:, two * 256 + 128 : two * 256 + 256],
                    ],
                    0,
                )
            )
            where = (
                pl.ds(pl.multiple_of(seq * 128, 128), 128),
                pl.ds(pl.multiple_of(head * 256 + two * 128, 128), 128),
            )
            if blocks == 1:
                cos = cosine[where[0], :]
                sin = sine[where[0], :]
                dq[where] = (piece * cos - swap_halves(piece, lane) * sin).astype(BF)
            else:
                dq[where] = jnp.where(block == 0, piece, dq[where].astype(F32) + piece).astype(
                    dq.dtype
                )

        @pl.when(lax.rem(step, 2 * blocks) == 2 * blocks - 1)
        def _():
            ring(2 + step // (2 * blocks))

        return carry

    def dkv_core_copy(seq):
        return remote(
            dkv.at[pl.ds(seq * HK, HK), :, 1 - c_id],
            dkv_x.at[pl.ds(seq * HK, HK)],
            dkv_core.at[seq],
            dkv_core.at[2 + seq],
            sibling,
        )

    def dkv_copy(seq, k):
        return remote(
            dkv_x.at[pl.ds(seq * HK, HK), lax.rem(l_id + k, line)],
            dkv_z.at[seq, k - 1],
            dkv_send.at[seq, k - 1],
            dkv_recv.at[seq, k - 1],
            mates[k - 1],
        )

    def dkv_scatter(seq):
        dkv_core_copy(seq).wait()

        def body(index, carry):
            head, place = seq * HK + index // line, index % line
            dkv_x[head, place] = (
                dkv_x[head, place].astype(F32) + dkv[head, place, c_id].astype(F32)
            ).astype(BF)
            return carry

        lax.fori_loop(0, HK * line, body, 0)
        for k in range(1, line):
            dkv_copy(seq, k).start()

    def dkv_gather(seq):
        for k in range(1, line):
            dkv_copy(seq, k).wait()
        cos = jnp.where(lane < 64, cosine[pl.ds(seq * 128, 128), :], 1.0)
        sin = jnp.where(lane < 64, sine[pl.ds(seq * 128, 128), :], 0.0)
        for head in range(HK):
            total = dkv_x[seq * HK + head, l_id].astype(F32)
            for k in range(line - 1):
                total = total + dkv_z[seq, k, head].astype(F32)
            dkv_own[pl.ds(seq * 128, 128), pl.ds(head * 128, 128)] = (
                total * cos - swap_halves(total, lane) * sin
            ).astype(BF)

    lax.fori_loop(0, HK * blocks, attend, 0)
    dkv_core_copy(0).start()
    scatter_part(g_buf, o_x, o_z, 0)
    lax.fori_loop(HK * blocks, total_steps, attend, 0)
    dkv_core_copy(1).start()
    dkv_scatter(0)
    if blocks > 1:
        for two in range(width // 128):
            for seq in range(2):
                where = (pl.ds(seq * 128, 128), pl.ds(two * 128, 128))
                piece = dq[where].astype(F32)
                cos = cosine[where[0], :]
                sin = sine[where[0], :]
                dq[where] = (piece * cos - swap_halves(piece, lane) * sin).astype(dq.dtype)
    dkv_scatter(1)
    weight_grad(n1_t_ref, dq, g_buf, shards)
    core_part(g_buf, None, q_x, 1).start()
    ring(7)
    scatter_part(g_buf, q_x, q_z, 1)
    gather_part(o_x, o_z, 0)
    line_up(o_x.at[s_id], o_r, o_t, 0, own_rows)
    load_wq.wait()
    load_wkv.wait()
    back = nt(dq[...], w_buf[...])
    dkv_gather(0)
    dkv_gather(1)
    weight_grad(n1_t_ref, dkv_own, g_kv, shards)
    core_part(g_kv, None, k_x, 2).start()
    ring(8)
    back = back + nt(dkv_own[...], wkv_buf[...])
    scatter_part(g_kv, k_x, k_z, 2)
    hidden = x_ref[...].astype(F32)
    scale = lax.rsqrt(jnp.mean(hidden * hidden, -1, keepdims=True) + EPSILON)
    scaled = back * gain_ref[...]
    gn_own[0:1, :] = jnp.sum(back * hidden * scale, 0, keepdims=True)
    gn_own[1:2, :] = gg_ref[...]
    gn_own[2:8, :] = jnp.zeros((6, width), F32)
    gain_core = remote(gn_own, gn_x, g_core.at[6], g_core.at[7], sibling)
    gain_core.start()
    out_dx[...] = (
        gm_ref[...]
        + scale * scaled
        - hidden * (scale * scale * scale) * jnp.mean(scaled * hidden, -1, keepdims=True)
    ).astype(BF)
    ring(9)
    gather_part(q_x, q_z, 1)
    line_up(q_x.at[s_id], q_r, q_t, 1, own_rows)
    gain_core.wait()
    gn_own[...] = gn_own[...] + gn_x[...]

    def gain_copy(k):
        return remote(
            gn_own, gn_z.at[k - 1], g_send.at[3, k - 1], g_recv.at[3, k - 1], peers[k - 1]
        )

    for k in range(1, shards):
        gain_copy(k).start()
    ring(10)
    gather_part(k_x, k_z, 2)
    line_up(k_x.at[s_id], k_r, k_t, 2, own_rows)
    for k in range(1, shards):
        gain_copy(k).wait()
    total = gn_own[...]
    for k in range(shards - 1):
        total = total + gn_z[k]
    gn_x[...] = total
    line_up(gn_x, gn_r, gn_t, 3, 8)
    ring(11)

    def tail(step, carry):
        ring(step)
        return carry

    lax.fori_loop(12, chunks + 3, tail, 0)
    near = pl.ds(pl.multiple_of(c_id * own_rows, 16), own_rows)
    far = pl.ds(pl.multiple_of((1 - c_id) * own_rows, 16), own_rows)
    jobs = [
        (o_x.at[s_id], o_t, 0, own_rows, out_wo.at[near], out_wo.at[far]),
        (q_x.at[s_id], q_t, 1, own_rows, out_wq.at[near], out_wq.at[far]),
        (k_x.at[s_id], k_t, 2, own_rows, out_wkv.at[near], out_wkv.at[far]),
        (gn_x, gn_t, 3, 8, out_gain, None),
    ]
    for mine, tot, slot, count, to, other in jobs:
        line_down(mine, tot, slot, count, to, other)
    lax.fori_loop(chunks + 3, chunks + 6, tail, 0)
    for mine, tot, slot, count, to, other in jobs:
        line_settle(tot, slot, to, other)

    def last(index, carry):
        settle(index)
        return carry

    lax.fori_loop(0, chunks, last, 0)


def backward_call(
    shards, line, gm, attn, attn_t, qp, n1_t, x, gain, cos, sin, gg, wo, wq, wkv, pt, kv, dw
):
    rows, width = gm.shape
    keys = kv.shape[1]
    feed = dw.shape[2]
    part = width // shards
    own_rows = part // 2
    kv_width = 2 * HK * HD
    sizes = (shards, line, keys, rows, width, feed)
    dma = pltpu.SemaphoreType.DMA
    v = pltpu.VMEM
    vm = pl.BlockSpec(memory_space=pltpu.VMEM)
    hbm = pl.BlockSpec(memory_space=pltpu.HBM)
    blocks = keys // 1024
    half = width // 2

    def boxes(cols):
        return [
            v((shards, own_rows, cols), BF),
            v((shards - 1, own_rows, cols), BF),
            v((own_rows, cols), BF),
            v((own_rows, cols), BF),
        ]

    scratch = [
        v((width, width), BF),
        v((width, kv_width), BF),
        v((2, 1024, 512), BF),
        v((2, 1024, 128), BF),
        v((rows, width), BF),
        v((2 * HK, 512, 128), BF),
        v((2 * HK, 1, 512), F32),
        v((2 * HK, line, 2, 128, 128), BF),
        v((2 * HK, line, 128, 128), BF),
        v((2, line - 1, HK, 128, 128), BF),
        v((rows, width), BF if blocks == 1 else F32),
        v((rows, kv_width), BF),
        v((3, half, feed), BF),
        v((3, half, feed), BF),
        v((3, half, feed), BF),
        v((3, half, feed), BF),
        v((shards, part, width), BF),
        v((shards, part, kv_width), BF),
        *boxes(width),
        *boxes(width),
        *boxes(kv_width),
        v((8, width), F32),
        v((8, width), F32),
        v((shards - 1, 8, width), F32),
        v((8, width), F32),
        v((8, width), F32),
        dma((6,)),
        dma((2,)),
        dma((2,)),
        dma((6,)),
        *[dma((12,)) for _ in range(7)],
        dma((4,)),
        dma((2, line - 1)),
        dma((2, line - 1)),
        dma((8,)),
        dma((4, shards - 1)),
        dma((4, shards - 1)),
        *[dma((4,)) for _ in range(7)],
    ]
    return pl.pallas_call(
        lambda *refs: backward_kernel(sizes, *refs),
        out_shape=(
            jax.ShapeDtypeStruct((3, width, feed), BF),
            jax.ShapeDtypeStruct((part, width), BF),
            jax.ShapeDtypeStruct((part, width), BF),
            jax.ShapeDtypeStruct((part, kv_width), BF),
            jax.ShapeDtypeStruct((8, width), F32),
            jax.ShapeDtypeStruct((rows, width), BF),
        ),
        in_specs=[vm] * 10 + [hbm] * 6,
        out_specs=(hbm, hbm, hbm, hbm, hbm, vm),
        scratch_shapes=scratch,
        compiler_params=pltpu.CompilerParams(
            collective_id=3, has_side_effects=True, vmem_limit_bytes=VMEM_LIMIT
        ),
        name="backward",
    )(gm, attn, attn_t, qp, n1_t, x, gain, cos, sin, gg, wo, wq, wkv, pt, kv, dw)


def attend_kernel(qp_ref, kv_ref, bias_ref, pt_ref, out_ref):
    blocks = kv_ref.shape[1] // 1024

    def scores(block):
        span = pl.ds(pl.multiple_of(block * 1024, 1024), 1024)
        bias = bias_ref[0, span, :]
        return nt(kv_ref[0, span, :], qp_ref[0]) + jnp.concatenate([bias] * GROUP, 1)

    if blocks == 1:
        value = scores(0)
        top = jnp.max(value, 0, keepdims=True)
        weight = jnp.exp(value - top)
        soft = (weight * (1.0 / jnp.sum(weight, 0, keepdims=True))).astype(BF)
        pt_ref[0] = soft
        mixed = tn(kv_ref[0], soft)[HD:]
    else:

        def first(block, carry):
            top, total = carry
            value = scores(block)
            new = jnp.maximum(top, jnp.max(value, 0, keepdims=True))
            total = total * jnp.exp(top - new) + jnp.sum(jnp.exp(value - new), 0, keepdims=True)
            return new, total

        top, total = lax.fori_loop(
            0,
            blocks,
            first,
            (jnp.full((1, 512), NEGATIVE, F32), jnp.zeros((1, 512), F32)),
        )
        inverse = 1.0 / total

        def second(block, mixed):
            soft = (jnp.exp(scores(block) - top) * inverse).astype(BF)
            span = pl.ds(pl.multiple_of(block * 1024, 1024), 1024)
            pt_ref[0, span, :] = soft
            return mixed + tn(kv_ref[0, span, :], soft)[HD:]

        mixed = lax.fori_loop(0, blocks, second, jnp.zeros((HD, 512), F32))
    for two in range(2):
        pair = jnp.concatenate(
            [mixed[:, two * 256 : two * 256 + 128], mixed[:, two * 256 + 128 : two * 256 + 256]], 0
        )
        out_ref[:, two * 128 : two * 128 + 128] = jnp.transpose(pair).astype(BF)


def attend_call(qp, kv, bias):
    keys = kv.shape[1]
    rows = 256
    return pl.pallas_call(
        attend_kernel,
        grid=(2, HK),
        out_shape=(
            jax.ShapeDtypeStruct((2 * HK, keys, 512), BF),
            jax.ShapeDtypeStruct((rows, HQ * HD), BF),
        ),
        in_specs=[
            pl.BlockSpec((1, 512, 128), lambda m, h: (m * HK + h, 0, 0)),
            pl.BlockSpec((1, keys, 128), lambda m, h: (m * HK + h, 0, 0)),
            pl.BlockSpec((1, keys, 128), lambda m, h: (m, 0, 0)),
        ],
        out_specs=(
            pl.BlockSpec((1, keys, 512), lambda m, h: (m * HK + h, 0, 0)),
            pl.BlockSpec((128, 256), lambda m, h: (m, h)),
        ),
        compiler_params=pltpu.CompilerParams(vmem_limit_bytes=VMEM_LIMIT),
        name="attend",
    )(qp, kv, bias)


def rope_parts(places):
    half_dim = HD // 2
    frequency = ROPE_BASE ** (-jnp.arange(half_dim, dtype=F32) * 2.0 / HD)
    angles = places.astype(F32)[..., None] * frequency
    return (jnp.cos(angles), jnp.sin(angles))


def rotate_wide(values, cosine, sine, keys_only):
    rows, cols = values.shape
    tiles = values.reshape(rows, cols // 128, 128)
    lane = jnp.arange(128)
    left = jnp.roll(tiles, -32, 2)
    right = jnp.roll(tiles, 32, 2)
    swapped = jnp.where(lane % 64 < 32, left, right)
    if keys_only:
        cosine = jnp.where(lane < 64, cosine, 1.0)
        sine = jnp.where(lane < 64, sine, 0.0)
    return (tiles * cosine[:, None, :] + swapped * sine[:, None, :]).reshape(rows, cols)


def row_norm(hidden, gain_vec):
    inv_scale = lax.rsqrt(jnp.mean(hidden * hidden, -1, keepdims=True) + EPSILON)
    return (hidden * inv_scale * gain_vec, inv_scale)


def norm_back(grad_norm, hidden, inv_scale, gain_vec):
    scaled = grad_norm * gain_vec
    grad_gain = jnp.sum(grad_norm * hidden * inv_scale, 0)
    grad_hidden = inv_scale * scaled - hidden * inv_scale**3 * jnp.mean(
        scaled * hidden, -1, keepdims=True
    )
    return (grad_hidden, grad_gain)


def gate_back(grad_inner, gate_proj, up_proj):
    sigmoid_gate = jax.nn.sigmoid(gate_proj)
    grad_gate = (
        grad_inner * up_proj * sigmoid_gate * (1.0 + gate_proj * (1.0 - sigmoid_gate))
    ).astype(BF)
    grad_up = (grad_inner * gate_proj * sigmoid_gate).astype(BF)
    return (grad_gate, grad_up)


def per_device(
    tokens,
    cotangent,
    positions,
    lengths,
    attn_gain,
    w_query,
    w_key,
    w_value,
    w_out,
    mlp_gain,
    w_gate,
    w_up,
    w_down,
):
    seqs, stretch, width = tokens.shape
    shards, line = lax.axis_size("shard"), lax.axis_size("line")
    rows = seqs * stretch
    where_ctx = ("line", "core")
    rank = lax.axis_index("line") * 2 + lax.axis_index("core")
    places = lax.dynamic_slice_in_dim(positions, rank * stretch, stretch, 1)
    valid = (places < lengths[:, None]).astype(F32).reshape(rows, 1)
    cosine, sine = rope_parts(places.reshape(rows))
    cos_wide = jnp.concatenate([cosine] * 4, 1)
    sin_wide = jnp.concatenate([-sine, sine, -sine, sine], 1)
    allowed = (positions[:, :, None] <= places[:, None, :]) & (
        positions < lengths[:, None]
    )[:, :, None]
    bias = jnp.where(allowed, 0.0, NEGATIVE).astype(F32)
    gains = lax.all_gather(jnp.stack([attn_gain, mlp_gain]), "shard", axis=1, tiled=True)
    gain_one, gain_two = gains[0].astype(F32), gains[1].astype(F32)
    w_kv = jnp.stack(
        [w_key.reshape(-1, HK, HD), w_value.reshape(-1, HK, HD)], 2
    ).reshape(-1, 2 * HK * HD)
    qkv_local = jnp.concatenate([w_query, w_kv], axis=1)
    qkv_all = lax.all_gather(qkv_local, "shard", axis=0, tiled=True)
    out_all = lax.all_gather(w_out, "shard", axis=0, tiled=True)
    grad_out = cotangent.reshape(rows, width).astype(F32) * valid
    grad_low = grad_out.astype(BF)
    grad_low_all = lax.all_gather(grad_low, "shard", axis=0, tiled=True)
    hidden = tokens.reshape(rows, width).astype(F32)
    normed_one, inv_one = row_norm(hidden, gain_one)
    norm_one = normed_one.astype(BF)
    wq_all, wkv_all = qkv_all[:, :width], qkv_all[:, width:]
    queries = rotate_wide(nn(norm_one, wq_all), cos_wide, sin_wide, False).astype(BF)
    keyval = rotate_wide(nn(norm_one, wkv_all), cos_wide, sin_wide, True).astype(BF)
    packed_q = jnp.transpose(
        queries.reshape(seqs, stretch, HK, GROUP, HD), (0, 2, 3, 1, 4)
    ).reshape(seqs * HK, GROUP * stretch, HD) * BF(1.0 / math.sqrt(HD))
    packed_q = jnp.pad(packed_q, ((0, 0), (0, 0), (0, 128 - HD)))
    packed_kv = jnp.transpose(keyval.reshape(seqs, stretch, HK, 128), (0, 2, 1, 3))
    packed_kv = lax.all_gather(packed_kv, where_ctx, axis=2, tiled=True)
    packed_kv = packed_kv.reshape(seqs * HK, -1, 128)
    soft, attn = attend_call(packed_q, packed_kv, bias)
    middle = hidden + nn(attn, out_all)
    normed_two, inv_two = row_norm(middle, gain_two)
    norm_two = normed_two.astype(BF)
    norm_two_all = lax.all_gather(norm_two, "shard", axis=0, tiled=True)
    gate_proj = nn(norm_two_all, w_gate)
    up_proj = nn(norm_two_all, w_up)
    inner_act = (jax.nn.silu(gate_proj) * up_proj).astype(BF)
    grad_inner = nt(grad_low_all, w_down)
    grad_gate, grad_up = gate_back(grad_inner, gate_proj, up_proj)
    grad_norm_two = lax.psum_scatter(
        (nt(grad_gate, w_gate) + nt(grad_up, w_up)).astype(BF),
        "shard",
        scatter_dimension=0,
        tiled=True,
    ).astype(F32)
    mlp_out = lax.psum_scatter(
        nn(inner_act, w_down).astype(BF), "shard", scatter_dimension=0, tiled=True
    ).astype(F32)
    result = (middle + mlp_out).astype(BF).reshape(seqs, stretch, width)
    feed_grads = jnp.stack(
        [
            tn(norm_two_all, grad_gate).astype(BF),
            tn(norm_two_all, grad_up).astype(BF),
            tn(grad_low_all, inner_act).astype(BF),
        ]
    )
    grad_mid_norm, grad_gain_two = norm_back(grad_norm_two, middle, inv_two, gain_two)
    grad_middle = grad_out + grad_mid_norm
    sum_feed, sum_out, sum_query, sum_kv, sum_gain, grad_input = backward_call(
        shards,
        line,
        grad_middle,
        attn,
        attn.T,
        packed_q,
        norm_one.T,
        tokens.reshape(rows, width),
        gain_one[None],
        cos_wide,
        sin_wide,
        grad_gain_two[None],
        out_all,
        wq_all,
        wkv_all,
        soft,
        packed_kv,
        feed_grads,
    )
    sum_kv = sum_kv.reshape(-1, HK, 2, HD)
    span = attn_gain.shape[0]
    sum_gain = lax.dynamic_slice_in_dim(sum_gain, lax.axis_index("shard") * span, span, 1)
    return (
        result,
        grad_input.reshape(seqs, stretch, width),
        sum_gain[0],
        sum_query.astype(F32),
        sum_kv[:, :, 0].reshape(-1, HK * HD).astype(F32),
        sum_kv[:, :, 1].reshape(-1, HK * HD).astype(F32),
        sum_out.astype(F32),
        sum_gain[1],
        sum_feed[0].astype(F32),
        sum_feed[1].astype(F32),
        sum_feed[2].T.astype(F32),
    )


def solution(mesh):
    shards, ctx = mesh.devices.shape
    inner = Mesh(mesh.devices.reshape(shards, ctx // 2, 2), ("shard", "line", "core"))
    where = ("line", "core")
    return jax.shard_map(
        per_device,
        mesh=inner,
        in_specs=(
            P("shard", where, None),
            P("shard", where, None),
            P("shard", None),
            P("shard"),
            P("shard"),
            P("shard", None),
            P("shard", None),
            P("shard", None),
            P("shard", None),
            P("shard"),
            P(None, "shard"),
            P(None, "shard"),
            P("shard", None),
        ),
        out_specs=(
            P("shard", where, None),
            P("shard", where, None),
            P("shard"),
            P("shard", None),
            P("shard", None),
            P("shard", None),
            P("shard", None),
            P("shard"),
            P(None, "shard"),
            P(None, "shard"),
            P("shard", None),
        ),
        check_vma=False,
    )
```

```python
import math

import jax
import jax.numpy as jnp
from jax import lax
from jax.experimental import pallas as pl
from jax.experimental.pallas import tpu as pltpu
from jax.sharding import Mesh
from jax.sharding import PartitionSpec as P

HQ = 20
HK = 5
HD = 64
GROUP = HQ // HK
EPSILON = 1e-05
NEGATIVE = -1e30
ROPE_BASE = 10000.0
BF = jnp.bfloat16
F32 = jnp.float32
BY_MESH = pl.DeviceIdType.MESH
VMEM_LIMIT = 67043328


def nn(a, b):
    return lax.dot_general(a, b, (((1,), (0,)), ((), ())), preferred_element_type=F32)


def nt(a, b):
    return lax.dot_general(a, b, (((1,), (1,)), ((), ())), preferred_element_type=F32)


def tn(a, b):
    return lax.dot_general(a, b, (((0,), (0,)), ((), ())), preferred_element_type=F32)


def lanes_of(rows):
    return lax.broadcasted_iota(jnp.int32, (rows, 128), 1)


def swap_halves(block, lane):
    left = pltpu.roll(block, 96, 1)
    right = pltpu.roll(block, 32, 1)
    return jnp.where(lane % 64 < 32, left, right)


def peer_of(s_id, shards, k, back):
    if shards == 4:
        if isinstance(k, int):
            return [s_id, s_id + 1 - 2 * (s_id % 2), (s_id + 2) % 4, 3 - s_id][k]
        return jnp.where(
            k == 0,
            s_id,
            jnp.where(
                k == 1, s_id + 1 - 2 * (s_id % 2), jnp.where(k == 2, (s_id + 2) % 4, 3 - s_id)
            ),
        )
    return (s_id + (shards - k if back else k)) % shards


def feed_kernel(
    sizes,
    n2_ref,
    mid_ref,
    g_ref,
    gain_ref,
    g_hbm,
    wg_hbm,
    wu_hbm,
    wd_hbm,
    out_gm,
    out_gg,
    out_parts,
    out_dw,
    n2_all,
    g_all,
    wg,
    wu,
    wd,
    inner,
    dgate,
    dup,
    back,
    zone,
    part_stage,
    dw_stage,
    load_sem,
    n2_send,
    n2_recv,
    back_send,
    back_recv,
    part_sem,
    dw_sem,
):
    shards, rows, width, feed = sizes
    s_id, l_id, c_id = lax.axis_index("shard"), lax.axis_index("line"), lax.axis_index("core")

    def remote(src, dst, send, recv, shard):
        return pltpu.make_async_remote_copy(
            src,
            dst,
            send,
            recv,
            device_id=(shard, l_id, c_id),
            device_id_type=BY_MESH,
        )

    barrier = pltpu.get_barrier_semaphore()
    for k in range(1, shards):
        pl.semaphore_signal(
            barrier,
            inc=1,
            device_id=(peer_of(s_id, shards, k, False), l_id, c_id),
            device_id_type=BY_MESH,
        )
    pl.semaphore_wait(barrier, shards - 1)

    def n2_copy(k):
        return remote(
            n2_ref,
            n2_all.at[s_id],
            n2_send.at[k],
            n2_recv.at[k],
            peer_of(s_id, shards, k, False),
        )

    for k in range(1, shards):
        n2_copy(k).start()
    loads = [
        pltpu.make_async_copy(src, dst, load_sem.at[i])
        for i, (src, dst) in enumerate(
            ((wg_hbm, wg), (wu_hbm, wu), (g_hbm, g_all), (wd_hbm, wd))
        )
    ]
    for load in loads:
        load.start()
    n2_all[s_id] = n2_ref[...]
    for load in loads:
        load.wait()

    def back_copy(k):
        return remote(
            back.at[peer_of(s_id, shards, k, True)],
            zone.at[k - 1],
            back_send.at[k],
            back_recv.at[k],
            peer_of(s_id, shards, k, True),
        )

    def block(step, carry):
        k = step
        source = peer_of(s_id, shards, k, True)

        @pl.when(k > 0)
        def _():
            remote(n2_ref, n2_all.at[source], n2_send.at[k], n2_recv.at[k], source).wait_recv()

        normed, grad = n2_all[source], g_all[source]
        gate, upper = nn(normed, wg[...]), nn(normed, wu[...])
        grad_inner = nt(grad, wd[...])
        sig = 1.0 / (1.0 + jnp.exp(-gate))
        act = gate * sig
        inner[source] = (act * upper).astype(BF)
        dgate[source] = (grad_inner * upper * sig * (1.0 + gate * (1.0 - sig))).astype(BF)
        dup[source] = (grad_inner * act).astype(BF)
        back[source] = (nt(dgate[source], wg[...]) + nt(dup[source], wu[...])).astype(BF)

        @pl.when(k > 0)
        def _():
            back_copy(k).start()

        return carry

    lax.fori_loop(0, shards, block, 0)

    def part_copy(k, slot):
        return pltpu.make_async_copy(part_stage.at[slot], out_parts.at[k], part_sem.at[slot])

    def project(k, carry):
        slot = k % 2

        @pl.when(k >= 2)
        def _():
            part_copy(k - 2, slot).wait()

        part_stage[slot] = nn(inner[k], wd[...]).astype(BF)
        part_copy(k, slot).start()
        return carry

    def dw_copy(tile, slot):
        span = pl.ds(pl.multiple_of(tile * 256, 256), 256)
        return pltpu.make_async_copy(dw_stage.at[slot], out_dw.at[:, span, :], dw_sem.at[slot])

    def weight(tile, carry):
        slot = tile % 2

        @pl.when(tile >= 2)
        def _():
            dw_copy(tile - 2, slot).wait()

        span = pl.ds(pl.multiple_of(tile * 256, 256), 256)
        left = jnp.zeros((256, feed), F32)
        right = jnp.zeros((256, feed), F32)
        low = jnp.zeros((256, feed), F32)
        for k in range(shards):
            n2_t = jnp.transpose(n2_all[k, :, span])
            left = left + nn(n2_t, dgate[k])
            right = right + nn(n2_t, dup[k])
            low = low + nn(jnp.transpose(g_all[k, :, span]), inner[k])
        dw_stage[slot, 0] = left.astype(BF)
        dw_stage[slot, 1] = right.astype(BF)
        dw_stage[slot, 2] = low.astype(BF)
        dw_copy(tile, slot).start()
        return carry

    tiles = width // 256
    lax.fori_loop(0, tiles, weight, 0)
    lax.fori_loop(0, shards, project, 0)
    total = back[s_id].astype(F32)
    for k in range(1, shards):
        back_copy(k).wait()
        total = total + zone[k - 1].astype(F32)
    hidden = mid_ref[...]
    scale = lax.rsqrt(jnp.mean(hidden * hidden, -1, keepdims=True) + EPSILON)
    scaled = total * gain_ref[...]
    out_gg[...] = jnp.sum(total * hidden * scale, 0, keepdims=True)
    out_gm[...] = (
        g_ref[...].astype(F32)
        + scale * scaled
        - hidden * (scale * scale * scale) * jnp.mean(scaled * hidden, -1, keepdims=True)
    )
    for k in range(1, shards):
        n2_copy(k).wait_send()
    for last in (2, 1):
        part_copy(shards - last, (shards - last) % 2).wait()
        dw_copy(tiles - last, (tiles - last) % 2).wait()


def feed_call(shards, n2, middle, grad, gain, grad_all, w_gate, w_up, w_down):
    rows, width = n2.shape
    feed = w_gate.shape[1]
    dma = pltpu.SemaphoreType.DMA
    v = pltpu.VMEM
    vm = pl.BlockSpec(memory_space=pltpu.VMEM)
    hbm = pl.BlockSpec(memory_space=pltpu.HBM)
    return pl.pallas_call(
        lambda *refs: feed_kernel((shards, rows, width, feed), *refs),
        out_shape=(
            jax.ShapeDtypeStruct((rows, width), F32),
            jax.ShapeDtypeStruct((1, width), F32),
            jax.ShapeDtypeStruct((shards, rows, width), BF),
            jax.ShapeDtypeStruct((3, width, feed), BF),
        ),
        in_specs=[vm] * 4 + [hbm] * 4,
        out_specs=(vm, vm, hbm, hbm),
        scratch_shapes=[
            v((shards, rows, width), BF),
            v((shards, rows, width), BF),
            v((width, feed), BF),
            v((width, feed), BF),
            v((feed, width), BF),
            v((shards, rows, feed), BF),
            v((shards, rows, feed), BF),
            v((shards, rows, feed), BF),
            v((shards, rows, width), BF),
            v((shards - 1, rows, width), BF),
            v((2, rows, width), BF),
            v((2, 3, 256, feed), BF),
            dma((4,)),
            dma((shards,)),
            dma((shards,)),
            dma((shards,)),
            dma((shards,)),
            dma((2,)),
            dma((2,)),
        ],
        compiler_params=pltpu.CompilerParams(
            collective_id=2, has_side_effects=True, vmem_limit_bytes=VMEM_LIMIT
        ),
        name="feed",
    )(n2, middle, grad, gain, grad_all, w_gate, w_up, w_down)


def add_rows(target, parts, rows, step):
    def body(index, carry):
        span = pl.ds(pl.multiple_of(index * step, step), step)
        total = parts[0][span, :].astype(F32)
        for part in parts[1:]:
            total = total + part[span, :].astype(F32)
        target[span, :] = total.astype(target.dtype)
        return carry

    lax.fori_loop(0, rows // step, body, 0)


def backward_kernel(
    sizes,
    gm_ref,
    attn_ref,
    attn_t_ref,
    qp_ref,
    n1_t_ref,
    x_ref,
    gain_ref,
    cos_ref,
    sin_ref,
    gg_ref,
    mid_ref,
    parts_hbm,
    wo_hbm,
    wq_hbm,
    wkv_hbm,
    pt_hbm,
    kv_hbm,
    dw_hbm,
    out_dw,
    out_wo,
    out_wq,
    out_wkv,
    out_gain,
    out_dx,
    out_result,
    p_zone,
    w_buf,
    wkv_buf,
    pt_buf,
    kv_buf,
    dproj,
    dop,
    delta,
    dkv,
    dkv_x,
    dkv_z,
    dq,
    dkv_own,
    own,
    got_x,
    got_r,
    got_t,
    g_buf,
    o_x,
    o_z,
    o_r,
    o_t,
    q_x,
    q_z,
    q_r,
    q_t,
    k_x,
    k_z,
    k_r,
    k_t,
    gn_own,
    gn_x,
    gn_z,
    gn_r,
    gn_t,
    load_sem,
    pt_sem,
    kv_sem,
    core_sem,
    up_send,
    r_recv,
    t_recv,
    down_send,
    sib_send,
    sib_recv,
    local_sem,
    dkv_core,
    dkv_send,
    dkv_recv,
    g_core,
    g_send,
    g_recv,
    a_up,
    a_r,
    a_t,
    a_down,
    a_sib_send,
    a_sib_recv,
    a_local,
    p_send,
    p_recv,
):
    shards, line, keys, rows, width, feed = sizes
    s_id, l_id, c_id = lax.axis_index("shard"), lax.axis_index("line"), lax.axis_index("core")
    sibling = (s_id, l_id, 1 - c_id)
    in_low = l_id < line // 2
    toward = jnp.where(in_low, 1, -1)
    inner = (s_id, l_id + toward, c_id)
    has_outer = (l_id > 0) & (l_id < line - 1)
    is_mid = (l_id == line // 2 - 1) | (l_id == line // 2)
    outer = (s_id, jnp.where(has_outer, l_id - toward, l_id + toward), c_id)
    peers = [(peer_of(s_id, shards, k, False), l_id, c_id) for k in range(1, shards)]
    mates = [(s_id, lax.rem(l_id + k, line), c_id) for k in range(1, line)]

    def remote(src, dst, send, recv, to):
        return pltpu.make_async_remote_copy(
            src, dst, send, recv, device_id=to, device_id_type=BY_MESH
        )

    barrier = pltpu.get_barrier_semaphore()
    for other in [sibling] + peers + mates:
        pl.semaphore_signal(barrier, inc=1, device_id=other, device_id_type=BY_MESH)
    pl.semaphore_wait(barrier, 1 + len(peers) + len(mates))

    half = width // 2
    chunk = half // 4
    chunks = 12
    slab = 16
    part = width // shards
    own_rows = part // 2
    blocks = keys // 1024
    hlf = pl.ds(pl.multiple_of(c_id * half, 16), half)
    oth = pl.ds(pl.multiple_of((1 - c_id) * half, 16), half)

    core_copy = [
        remote(dw_hbm.at[k, oth], got_x.at[k], core_sem.at[k], core_sem.at[3 + k], sibling)
        for k in range(3)
    ]
    own_load = [
        pltpu.make_async_copy(dw_hbm.at[k, hlf], own.at[k], load_sem.at[k]) for k in range(3)
    ]
    load_wo = pltpu.make_async_copy(wo_hbm, w_buf, load_sem.at[3])
    load_wkv = pltpu.make_async_copy(wkv_hbm, wkv_buf, load_sem.at[4])
    load_wq = pltpu.make_async_copy(wq_hbm, w_buf, load_sem.at[5])
    load_wo.start()

    def part_copy(k):
        return remote(
            parts_hbm.at[peer_of(s_id, shards, k, False)],
            p_zone.at[k - 1],
            p_send.at[k - 1],
            p_recv.at[k - 1],
            peers[k - 1],
        )

    for k in range(3):
        own_load[k].start()
        core_copy[k].start()
    load_wkv.start()

    total_steps = 2 * HK * blocks

    def pt_copy(step, slot):
        pair, block = step // blocks, step % blocks
        span = pl.ds(pl.multiple_of(block * 1024, 1024), 1024)
        return pltpu.make_async_copy(pt_hbm.at[pair, span], pt_buf.at[slot], pt_sem.at[slot])

    def kv_copy(step, slot):
        pair, block = step // blocks, step % blocks
        span = pl.ds(pl.multiple_of(block * 1024, 1024), 1024)
        return pltpu.make_async_copy(kv_hbm.at[pair, span], kv_buf.at[slot], kv_sem.at[slot])

    pt_copy(0, 0).start()
    kv_copy(0, 0).start()

    def spot(index):
        array, piece = index // 4, index % 4
        return array, pl.ds(pl.multiple_of(piece * chunk, 16), chunk)

    def up(index):
        array, span = spot(index)
        mine, extra, came = own.at[array, span], got_x.at[array, span], got_r.at[array, span]

        @pl.when(index % 4 == 0)
        def _():
            pltpu.make_async_copy(
                dw_hbm.at[array, hlf], own.at[array], load_sem.at[array]
            ).wait()
            remote(
                dw_hbm.at[array, oth],
                got_x.at[array],
                core_sem.at[array],
                core_sem.at[3 + array],
                sibling,
            ).wait()

        @pl.when(has_outer)
        def _():
            remote(mine, came, up_send.at[index], r_recv.at[index], inner).wait_recv()
            add_rows(mine, [mine, extra, came], chunk, slab)

        @pl.when(jnp.logical_not(has_outer))
        def _():
            add_rows(mine, [mine, extra], chunk, slab)

        @pl.when(is_mid)
        def _():
            remote(
                mine, got_t.at[array, span], up_send.at[index], t_recv.at[index], inner
            ).start()

        @pl.when(jnp.logical_not(is_mid))
        def _():
            remote(mine, came, up_send.at[index], r_recv.at[index], inner).start()

    def out_span(index, core):
        array, piece = index // 4, index % 4
        return out_dw.at[array, pl.ds(pl.multiple_of(core * half + piece * chunk, 16), chunk)]

    def down(index):
        array, span = spot(index)
        mine, total = own.at[array, span], got_t.at[array, span]
        remote(mine, total, up_send.at[index], t_recv.at[index], inner).wait_recv()

        @pl.when(is_mid)
        def _():
            add_rows(total, [mine, total], chunk, slab)

        @pl.when(has_outer)
        def _():
            remote(total, total, down_send.at[index], t_recv.at[index], outer).start()

        remote(
            total, out_span(index, c_id), sib_send.at[index], sib_recv.at[index], sibling
        ).start()
        pltpu.make_async_copy(total, out_span(index, c_id), local_sem.at[index]).start()

    def settle(index):
        array, span = spot(index)
        mine, total = own.at[array, span], got_t.at[array, span]
        remote(mine, total, up_send.at[index], t_recv.at[index], inner).wait_send()

        @pl.when(has_outer)
        def _():
            remote(total, total, down_send.at[index], t_recv.at[index], outer).wait_send()

        last = remote(
            total, out_span(index, 1 - c_id), sib_send.at[index], sib_recv.at[index], sibling
        )
        last.wait()
        pltpu.make_async_copy(total, out_span(index, c_id), local_sem.at[index]).wait()

    def ring(step):
        @pl.when((step >= 0) & (step < chunks))
        def _():
            up(step)

        @pl.when((step >= 3) & (step < chunks + 3) & is_mid)
        def _():
            down(step - 3)

        @pl.when((step >= 6) & (step < chunks + 6) & jnp.logical_not(is_mid))
        def _():
            down(step - 6)

    def core_part(grad, cols, box, slot):
        far = pl.ds(pl.multiple_of((1 - c_id) * own_rows, 16), own_rows)
        return remote(
            grad.at[:, far, :], box, g_core.at[slot], g_core.at[3 + slot], sibling
        )

    def scatter_part(grad, box, zone, slot):
        core_part(grad, None, box, slot).wait()
        near = pl.ds(pl.multiple_of(c_id * own_rows, 16), own_rows)

        def body(s, carry):
            add_rows(box.at[s], [grad.at[s, near], box.at[s]], own_rows, slab)
            return carry

        lax.fori_loop(0, shards, body, 0)
        for k in range(1, shards):
            scatter_copy(box, zone, slot, k).start()

    def scatter_copy(box, zone, slot, k):
        return remote(
            box.at[peer_of(s_id, shards, k, False)],
            zone.at[k - 1],
            g_send.at[slot, k - 1],
            g_recv.at[slot, k - 1],
            peers[k - 1],
        )

    def gather_part(box, zone, slot):
        for k in range(1, shards):
            scatter_copy(box, zone, slot, k).wait()
        add_rows(
            box.at[s_id],
            [box.at[s_id]] + [zone.at[k] for k in range(shards - 1)],
            own_rows,
            slab,
        )

    def line_up(mine, came, total, slot, count):
        @pl.when(has_outer)
        def _():
            remote(mine, came, a_up.at[slot], a_r.at[slot], inner).wait_recv()
            add_rows(mine, [mine, came], count, slab if mine.dtype == BF else 8)

        @pl.when(is_mid)
        def _():
            remote(mine, total, a_up.at[slot], a_t.at[slot], inner).start()

        @pl.when(jnp.logical_not(is_mid))
        def _():
            remote(mine, came, a_up.at[slot], a_r.at[slot], inner).start()

    def line_down(mine, total, slot, count, near, far):
        remote(mine, total, a_up.at[slot], a_t.at[slot], inner).wait()

        @pl.when(is_mid)
        def _():
            add_rows(total, [mine, total], count, slab if mine.dtype == BF else 8)

        @pl.when(has_outer)
        def _():
            remote(total, total, a_down.at[slot], a_t.at[slot], outer).start()

        if far is not None:
            remote(total, near, a_sib_send.at[slot], a_sib_recv.at[slot], sibling).start()
        pltpu.make_async_copy(total, near, a_local.at[slot]).start()

    def line_settle(total, slot, near, far):
        @pl.when(has_outer)
        def _():
            remote(total, total, a_down.at[slot], a_t.at[slot], outer).wait_send()

        if far is not None:
            remote(total, far, a_sib_send.at[slot], a_sib_recv.at[slot], sibling).wait()
        pltpu.make_async_copy(total, near, a_local.at[slot]).wait()

    lane = lanes_of(128)
    dproj[...] = gm_ref[...].astype(BF)
    load_wo.wait()

    def spread(head, carry):
        block = nt(
            dproj[...], w_buf[pl.ds(pl.multiple_of(head * 256, 256), 256), :]
        ).astype(BF)
        for seq in range(2):
            for two in range(2):
                piece = block[seq * 128 : seq * 128 + 128, two * 128 : two * 128 + 128].astype(
                    F32
                )
                place = seq * HK + head
                first = jnp.where(lane >= 64, pltpu.roll(piece, 64, 1), 0.0)
                dop[place, pl.ds(two * 256, 128), :] = first.astype(BF)
                dop[place, pl.ds(two * 256 + 128, 128), :] = jnp.where(
                    lane >= 64, piece, 0.0
                ).astype(BF)
                value = attn_ref[
                    pl.ds(seq * 128, 128),
                    pl.ds(pl.multiple_of(head * 256 + two * 128, 128), 128),
                ].astype(F32)
                product = jnp.transpose(piece * value)
                delta[place, :, pl.ds(two * 256, 128)] = jnp.sum(
                    product[:64], 0, keepdims=True
                )
                delta[place, :, pl.ds(two * 256 + 128, 128)] = jnp.sum(
                    product[64:], 0, keepdims=True
                )
        return carry

    lax.fori_loop(0, HK, spread, 0)
    load_wq.start()
    ring(0)

    def weight_grad(left, right, grad, count):
        def body(s, carry):
            grad[s] = nn(
                left[pl.ds(pl.multiple_of(s * part, 16), part), :], right[...]
            ).astype(BF)
            return carry

        lax.fori_loop(0, count, body, 0)

    weight_grad(attn_t_ref, dproj, g_buf, shards)
    core_part(g_buf, None, o_x, 0).start()
    ring(1)

    cosine, sine = cos_ref, sin_ref

    def attend(step, carry):
        slot = lax.rem(step, 2)
        pair, block = step // blocks, step % blocks

        @pl.when(step + 1 < total_steps)
        def _():
            pt_copy(step + 1, 1 - slot).start()
            kv_copy(step + 1, 1 - slot).start()

        pt_copy(step, slot).wait()
        kv_copy(step, slot).wait()
        keyval = kv_buf[slot]
        soft = pt_buf[slot]
        grad_soft = nt(keyval, dop[pair])
        score = (soft.astype(F32) * (grad_soft - delta[pair])).astype(BF)
        both = (nn(score, qp_ref[pair]) + nn(soft, dop[pair])).astype(BF)
        for sub in range(8):
            dkv[pair, block * 4 + sub // 2, sub % 2] = both[sub * 128 : sub * 128 + 128]
        query = tn(keyval, score)[:64] * (1.0 / math.sqrt(HD))
        seq, head = pair // HK, pair % HK
        for two in range(2):
            piece = jnp.transpose(
                jnp.concatenate(
                    [
                        query[:, two * 256 : two * 256 + 128],
                        query[:, two * 256 + 128 : two * 256 + 256],
                    ],
                    0,
                )
            )
            where = (
                pl.ds(pl.multiple_of(seq * 128, 128), 128),
                pl.ds(pl.multiple_of(head * 256 + two * 128, 128), 128),
            )
            if blocks == 1:
                cos = cosine[where[0], :]
                sin = sine[where[0], :]
                dq[where] = (piece * cos - swap_halves(piece, lane) * sin).astype(BF)
            else:
                dq[where] = jnp.where(block == 0, piece, dq[where].astype(F32) + piece).astype(
                    dq.dtype
                )

        @pl.when(lax.rem(step, 2 * blocks) == 2 * blocks - 1)
        def _():
            ring(2 + step // (2 * blocks))

        return carry

    def dkv_core_copy(seq):
        return remote(
            dkv.at[pl.ds(seq * HK, HK), :, 1 - c_id],
            dkv_x.at[pl.ds(seq * HK, HK)],
            dkv_core.at[seq],
            dkv_core.at[2 + seq],
            sibling,
        )

    def dkv_copy(seq, k):
        return remote(
            dkv_x.at[pl.ds(seq * HK, HK), lax.rem(l_id + k, line)],
            dkv_z.at[seq, k - 1],
            dkv_send.at[seq, k - 1],
            dkv_recv.at[seq, k - 1],
            mates[k - 1],
        )

    def dkv_scatter(seq):
        dkv_core_copy(seq).wait()

        def body(index, carry):
            head, place = seq * HK + index // line, index % line
            dkv_x[head, place] = (
                dkv_x[head, place].astype(F32) + dkv[head, place, c_id].astype(F32)
            ).astype(BF)
            return carry

        lax.fori_loop(0, HK * line, body, 0)
        for k in range(1, line):
            dkv_copy(seq, k).start()

    def dkv_gather(seq):
        for k in range(1, line):
            dkv_copy(seq, k).wait()
        cos = jnp.where(lane < 64, cosine[pl.ds(seq * 128, 128), :], 1.0)
        sin = jnp.where(lane < 64, sine[pl.ds(seq * 128, 128), :], 0.0)
        for head in range(HK):
            total = dkv_x[seq * HK + head, l_id].astype(F32)
            for k in range(line - 1):
                total = total + dkv_z[seq, k, head].astype(F32)
            dkv_own[pl.ds(seq * 128, 128), pl.ds(head * 128, 128)] = (
                total * cos - swap_halves(total, lane) * sin
            ).astype(BF)

    for k in range(1, shards):
        part_copy(k).start()
    lax.fori_loop(0, HK * blocks, attend, 0)
    dkv_core_copy(0).start()
    scatter_part(g_buf, o_x, o_z, 0)
    lax.fori_loop(HK * blocks, total_steps, attend, 0)
    dkv_core_copy(1).start()
    dkv_scatter(0)
    if blocks > 1:
        for two in range(width // 128):
            for seq in range(2):
                where = (pl.ds(seq * 128, 128), pl.ds(two * 128, 128))
                piece = dq[where].astype(F32)
                cos = cosine[where[0], :]
                sin = sine[where[0], :]
                dq[where] = (piece * cos - swap_halves(piece, lane) * sin).astype(dq.dtype)
    dkv_scatter(1)
    weight_grad(n1_t_ref, dq, g_buf, shards)
    core_part(g_buf, None, q_x, 1).start()
    ring(7)
    scatter_part(g_buf, q_x, q_z, 1)
    gather_part(o_x, o_z, 0)
    line_up(o_x.at[s_id], o_r, o_t, 0, own_rows)
    load_wq.wait()
    load_wkv.wait()
    back = nt(dq[...], w_buf[...])
    dkv_gather(0)
    dkv_gather(1)
    g_kv = g_buf.at[:, :, pl.ds(0, 2 * HK * HD)]
    weight_grad(n1_t_ref, dkv_own, g_kv, shards)
    core_part(g_kv, None, k_x, 2).start()
    ring(8)
    back = back + nt(dkv_own[...], wkv_buf[...])
    scatter_part(g_kv, k_x, k_z, 2)
    hidden = x_ref[...].astype(F32)
    scale = lax.rsqrt(jnp.mean(hidden * hidden, -1, keepdims=True) + EPSILON)
    scaled = back * gain_ref[...]
    gn_own[0:1, :] = jnp.sum(back * hidden * scale, 0, keepdims=True)
    gn_own[1:2, :] = gg_ref[...]
    gn_own[2:8, :] = jnp.zeros((6, width), F32)
    gain_core = remote(gn_own, gn_x, g_core.at[6], g_core.at[7], sibling)
    gain_core.start()
    out_dx[...] = (
        gm_ref[...]
        + scale * scaled
        - hidden * (scale * scale * scale) * jnp.mean(scaled * hidden, -1, keepdims=True)
    ).astype(BF)
    ring(9)
    for k in range(1, shards):
        part_copy(k).wait()
    result = mid_ref[...]
    for first in range(0, shards, 4):
        stage = [
            pltpu.make_async_copy(
                parts_hbm.at[s_id] if k == 0 else p_zone.at[k - 1],
                w_buf.at[pl.ds((k - first) * rows, rows)],
                load_sem.at[k - first],
            )
            for k in range(first, min(shards, first + 4))
        ]
        for copy in stage:
            copy.start()
        for k, copy in enumerate(stage):
            copy.wait()
            result = result + w_buf[k * rows : (k + 1) * rows, :].astype(F32)
    out_result[...] = result.astype(BF)
    gather_part(q_x, q_z, 1)
    line_up(q_x.at[s_id], q_r, q_t, 1, own_rows)
    gain_core.wait()
    gn_own[...] = gn_own[...] + gn_x[...]

    def gain_copy(k):
        return remote(
            gn_own, gn_z.at[k - 1], g_send.at[3, k - 1], g_recv.at[3, k - 1], peers[k - 1]
        )

    for k in range(1, shards):
        gain_copy(k).start()
    ring(10)
    gather_part(k_x, k_z, 2)
    line_up(k_x.at[s_id], k_r, k_t, 2, own_rows)
    for k in range(1, shards):
        gain_copy(k).wait()
    total = gn_own[...]
    for k in range(shards - 1):
        total = total + gn_z[k]
    gn_x[...] = total
    line_up(gn_x, gn_r, gn_t, 3, 8)
    ring(11)

    def tail(step, carry):
        ring(step)
        return carry

    lax.fori_loop(12, chunks + 3, tail, 0)
    near = pl.ds(pl.multiple_of(c_id * own_rows, 16), own_rows)
    far = pl.ds(pl.multiple_of((1 - c_id) * own_rows, 16), own_rows)
    jobs = [
        (o_x.at[s_id], o_t, 0, own_rows, out_wo.at[near], out_wo.at[far]),
        (q_x.at[s_id], q_t, 1, own_rows, out_wq.at[near], out_wq.at[far]),
        (k_x.at[s_id], k_t, 2, own_rows, out_wkv.at[near], out_wkv.at[far]),
        (gn_x, gn_t, 3, 8, out_gain, None),
    ]
    for mine, tot, slot, count, to, other in jobs:
        line_down(mine, tot, slot, count, to, other)
    lax.fori_loop(chunks + 3, chunks + 6, tail, 0)
    for mine, tot, slot, count, to, other in jobs:
        line_settle(tot, slot, to, other)

    def last(index, carry):
        settle(index)
        return carry

    lax.fori_loop(0, chunks, last, 0)


def backward_call(
    shards, line, gm, attn, attn_t, qp, n1_t, x, gain, cos, sin, gg, middle, parts, wo, wq, wkv, pt, kv, dw
):
    rows, width = gm.shape
    keys = kv.shape[1]
    feed = dw.shape[2]
    part = width // shards
    own_rows = part // 2
    kv_width = 2 * HK * HD
    sizes = (shards, line, keys, rows, width, feed)
    dma = pltpu.SemaphoreType.DMA
    v = pltpu.VMEM
    vm = pl.BlockSpec(memory_space=pltpu.VMEM)
    hbm = pl.BlockSpec(memory_space=pltpu.HBM)
    blocks = keys // 1024
    half = width // 2

    def boxes(cols):
        return [
            v((shards, own_rows, cols), BF),
            v((shards - 1, own_rows, cols), BF),
            v((own_rows, cols), BF),
            v((own_rows, cols), BF),
        ]

    scratch = [
        v((width, width), BF),
        v((width, kv_width), BF),
        v((2, 1024, 512), BF),
        v((2, 1024, 128), BF),
        v((rows, width), BF),
        v((2 * HK, 512, 128), BF),
        v((2 * HK, 1, 512), F32),
        v((2 * HK, line, 2, 128, 128), BF),
        v((2 * HK, line, 128, 128), BF),
        v((2, line - 1, HK, 128, 128), BF),
        v((rows, width), BF if blocks == 1 else F32),
        v((rows, kv_width), BF),
        v((3, half, feed), BF),
        v((3, half, feed), BF),
        v((3, half, feed), BF),
        v((3, half, feed), BF),
        v((shards, part, width), BF),
        *boxes(width),
        *boxes(width),
        *boxes(kv_width),
        v((8, width), F32),
        v((8, width), F32),
        v((shards - 1, 8, width), F32),
        v((8, width), F32),
        v((8, width), F32),
        dma((6,)),
        dma((2,)),
        dma((2,)),
        dma((6,)),
        *[dma((12,)) for _ in range(7)],
        dma((4,)),
        dma((2, line - 1)),
        dma((2, line - 1)),
        dma((8,)),
        dma((4, shards - 1)),
        dma((4, shards - 1)),
        *[dma((4,)) for _ in range(7)],
        dma((shards - 1,)),
        dma((shards - 1,)),
    ]
    return pl.pallas_call(
        lambda *refs: backward_kernel(sizes, *refs),
        out_shape=(
            jax.ShapeDtypeStruct((3, width, feed), BF),
            jax.ShapeDtypeStruct((part, width), BF),
            jax.ShapeDtypeStruct((part, width), BF),
            jax.ShapeDtypeStruct((part, kv_width), BF),
            jax.ShapeDtypeStruct((8, width), F32),
            jax.ShapeDtypeStruct((rows, width), BF),
            jax.ShapeDtypeStruct((rows, width), BF),
            jax.ShapeDtypeStruct((shards - 1, rows, width), BF),
        ),
        in_specs=[vm] * 11 + [hbm] * 7,
        out_specs=(hbm, hbm, hbm, hbm, hbm, vm, vm, hbm),
        scratch_shapes=scratch,
        compiler_params=pltpu.CompilerParams(
            collective_id=3, has_side_effects=True, vmem_limit_bytes=VMEM_LIMIT
        ),
        name="backward",
    )(gm, attn, attn_t, qp, n1_t, x, gain, cos, sin, gg, middle, parts, wo, wq, wkv, pt, kv, dw)


class Spread:
    def __init__(self, env, block, source, sems, shared):
        self.env, self.block, self.source, self.shared = env, block, source, shared
        self.send, self.recv, self.sib_send, self.sib_recv = sems
        self.relay = env.shards == 4

    def copy(self, k):
        env = self.env
        return env.remote(
            self.source,
            self.block(env.s_id, env.c_id, 0, 2),
            self.send.at[k],
            self.recv.at[k],
            env.peer(k),
        )

    def passing(self, k):
        env = self.env
        piece = self.block(env.origin(k), env.c_id, k - 1, 1)
        return env.remote(
            piece, piece, self.send.at[2 + k], self.recv.at[2 + k], env.peer(3 - k)
        )

    def direct(self):
        return range(1, 3 if self.relay else self.env.shards)

    def start(self):
        for k in self.direct():
            self.copy(k).start()

    def sib_copy(self, k):
        piece = self.block(self.env.origin(k), self.env.c_id, 0, 2)
        return self.env.remote(
            piece, piece, self.sib_send.at[k], self.sib_recv.at[k], self.env.sibling
        )

    def forward(self):
        for k in self.direct():
            self.copy(k).wait_recv()
            if self.relay:
                self.passing(k).start()
            if self.shared:
                self.sib_copy(k).start()

    def collect(self):
        if self.relay:
            for k in (1, 2):
                self.passing(k).wait_recv()
            if self.shared:
                self.sib_copy(3).start()

    def finish(self):
        if self.shared:
            for k in range(1, self.env.shards):
                self.sib_copy(k).wait_recv()

    def settle(self):
        for k in self.direct():
            self.copy(k).wait_send()
            if self.relay:
                self.passing(k).wait_send()
        if self.shared:
            for k in range(1, self.env.shards):
                self.sib_copy(k).wait_send()


class Env:
    def __init__(self, shards, line):
        self.shards, self.line = shards, line
        self.s_id = lax.axis_index("shard")
        self.l_id = lax.axis_index("line")
        self.c_id = lax.axis_index("core")
        self.sibling = (self.s_id, self.l_id, 1 - self.c_id)

    def remote(self, src, dst, send, recv, to):
        return pltpu.make_async_remote_copy(
            src, dst, send, recv, device_id=to, device_id_type=BY_MESH
        )

    def peer(self, k):
        return (peer_of(self.s_id, self.shards, k, False), self.l_id, self.c_id)

    def origin(self, k):
        return peer_of(self.s_id, self.shards, k, True)

    def mate(self, k):
        return (self.s_id, lax.rem(self.l_id + k, self.line), self.c_id)

    def barrier(self, others):
        barrier = pltpu.get_barrier_semaphore()
        for other in others:
            pl.semaphore_signal(barrier, inc=1, device_id=other, device_id_type=BY_MESH)
        pl.semaphore_wait(barrier, len(others))


def front_kernel(
    sizes,
    x_ref,
    gains_ref,
    wq_ref,
    wkv_ref,
    wo_ref,
    g_ref,
    bias_ref,
    cos_ref,
    sin_ref,
    out_attn,
    out_attn_t,
    out_n1_t,
    out_qp,
    out_mid,
    out_n2,
    out_gains,
    out_wq,
    out_wkv,
    out_wo,
    out_kv,
    out_pt,
    out_g,
    wq_all,
    wkv_all,
    wo_all,
    kv_all,
    norm,
    gain_zone,
    pt_stage,
    gain_send,
    gain_recv,
    wq_s,
    wq_r,
    wq_ss,
    wq_sr,
    wkv_s,
    wkv_r,
    wkv_ss,
    wkv_sr,
    wo_s,
    wo_r,
    wo_ss,
    wo_sr,
    g_s,
    g_r,
    kv_send,
    kv_recv,
    kv_sib_send,
    kv_sib_recv,
    pt_sem,
    out_sem,
):
    shards, line, keys, rows, width = sizes
    env = Env(shards, line)
    s_id, l_id, c_id = env.s_id, env.l_id, env.c_id
    part = width // shards
    hp = part // 2
    quarter = hp // 2
    blocks = keys // 1024
    env.barrier(
        [env.sibling]
        + [env.peer(k) for k in range(1, shards)]
        + [env.mate(k) for k in range(1, line)]
    )

    def rows_of(ref):
        def block(s, core, first, count):
            start = s * part + core * hp + first * quarter
            return ref.at[pl.ds(pl.multiple_of(start, 16), count * quarter)]

        return block

    def g_rows(s, core, first, count):
        start = s * rows + first * (rows // 2)
        return out_g.at[pl.ds(pl.multiple_of(start, 16), count * (rows // 2))]

    mine = pl.ds(pl.multiple_of(c_id * hp, 16), hp)
    own = pl.ds(pl.multiple_of(s_id * part, 16), part)
    kv_gather = Spread(
        env, rows_of(wkv_all), wkv_ref.at[mine], (wkv_s, wkv_r, wkv_ss, wkv_sr), True
    )
    q_gather = Spread(env, rows_of(wq_all), wq_ref.at[mine], (wq_s, wq_r, wq_ss, wq_sr), True)
    o_gather = Spread(env, rows_of(wo_all), wo_ref.at[mine], (wo_s, wo_r, wo_ss, wo_sr), True)
    grad_gather = Spread(env, g_rows, g_ref, (g_s, g_r, None, None), False)

    def gain_copy(k):
        return env.remote(
            gains_ref, gain_zone.at[s_id], gain_send.at[k], gain_recv.at[k], env.peer(k)
        )

    for k in range(1, shards):
        gain_copy(k).start()
    kv_gather.start()
    q_gather.start()
    locals_ = [
        pltpu.make_async_copy(wkv_ref, wkv_all.at[own], out_sem.at[0]),
        pltpu.make_async_copy(wq_ref, wq_all.at[own], out_sem.at[1]),
        pltpu.make_async_copy(wo_ref, wo_all.at[own], out_sem.at[2]),
        pltpu.make_async_copy(
            g_ref, out_g.at[pl.ds(pl.multiple_of(s_id * rows, 16), rows)], out_sem.at[3]
        ),
    ]
    for copy in locals_:
        copy.start()
    gain_zone[s_id] = gains_ref[...]
    hidden = x_ref[...].astype(F32)
    scale = lax.rsqrt(jnp.mean(hidden * hidden, -1, keepdims=True) + EPSILON)
    for k in range(1, shards):
        gain_copy(k).wait()
    out_gains[...] = jnp.concatenate([gain_zone[s] for s in range(shards)], 1)
    norm[...] = (hidden * scale * out_gains[0:1, :]).astype(BF)
    for tile in range(width // 128):
        piece = norm[:, tile * 128 : tile * 128 + 128].astype(F32)
        out_n1_t[tile * 128 : tile * 128 + 128, :] = jnp.transpose(piece).astype(BF)
    kv_gather.forward()
    q_gather.forward()
    o_gather.start()
    kv_gather.collect()
    q_gather.collect()
    grad_gather.start()
    for copy in locals_:
        copy.wait()
    kv_gather.finish()

    lane = lanes_of(128)
    place = l_id * 2 + c_id

    def make_kv(head, carry):
        block = nn(norm[...], wkv_all[:, pl.ds(pl.multiple_of(head * 128, 128), 128)])
        for seq in range(2):
            piece = block[seq * 128 : seq * 128 + 128]
            cos = jnp.where(lane < 64, cos_ref[pl.ds(seq * 128, 128), :], 1.0)
            sin = jnp.where(lane < 64, sin_ref[pl.ds(seq * 128, 128), :], 0.0)
            kv_all[seq * HK + head, place] = (piece * cos + swap_halves(piece, lane) * sin).astype(
                BF
            )
        return carry

    lax.fori_loop(0, HK, make_kv, 0)

    def kv_slice(seq, l, c):
        return kv_all.at[pl.ds(seq * HK, HK), l * 2 + c]

    def kv_copy(seq, k):
        piece = kv_slice(seq, l_id, c_id)
        return env.remote(
            piece, piece, kv_send.at[seq, k - 1], kv_recv.at[seq, k - 1], env.mate(k)
        )

    def kv_sib(seq, k):
        piece = kv_slice(seq, lax.rem(l_id + line - k, line), c_id)
        return env.remote(
            piece, piece, kv_sib_send.at[seq, k], kv_sib_recv.at[seq, k], env.sibling
        )

    for seq in range(2):
        for k in range(1, line):
            kv_copy(seq, k).start()
        kv_sib(seq, 0).start()

    q_gather.finish()

    def make_q(head, carry):
        block = nn(norm[...], wq_all[:, pl.ds(pl.multiple_of(head * 256, 256), 256)])
        for seq in range(2):
            cos = cos_ref[pl.ds(seq * 128, 128), :]
            sin = sin_ref[pl.ds(seq * 128, 128), :]
            for two in range(2):
                piece = block[seq * 128 : seq * 128 + 128, two * 128 : two * 128 + 128]
                piece = piece * cos + swap_halves(piece, lane) * sin
                piece = piece.astype(BF).astype(F32) * (1.0 / math.sqrt(HD))
                pair = seq * HK + head
                out_qp[pair, pl.ds(two * 256, 128), :] = jnp.where(lane < 64, piece, 0.0).astype(
                    BF
                )
                out_qp[pair, pl.ds(two * 256 + 128, 128), :] = jnp.where(
                    lane < 64, pltpu.roll(piece, 64, 1), 0.0
                ).astype(BF)
        return carry

    lax.fori_loop(0, HK, make_q, 0)
    o_gather.forward()

    def pt_copy(pair, block, slot):
        span = pl.ds(pl.multiple_of(block * 1024, 1024), 1024)
        return pltpu.make_async_copy(pt_stage.at[slot], out_pt.at[pair, span], pt_sem.at[slot])

    def keys_of(pair, block):
        if blocks == 1:
            return kv_all[pair].reshape(1024, 128)
        return kv_all[pair, pl.ds(block * 8, 8)].reshape(1024, 128)

    def scores(pair, block):
        span = pl.ds(pl.multiple_of(block * 1024, 1024), 1024)
        bias = bias_ref[pair // HK, span, :]
        return nt(keys_of(pair, block), out_qp[pair]) + jnp.concatenate([bias] * GROUP, 1)

    def attend(pair, carry):
        if blocks == 1:
            slot = lax.rem(pair, 2)

            @pl.when(pair >= 2)
            def _():
                pt_copy(pair - 2, 0, slot).wait()

            value = scores(pair, 0)
            top = jnp.max(value, 0, keepdims=True)
            weight = jnp.exp(value - top)
            inverse = 1.0 / jnp.sum(weight, 0, keepdims=True)
            soft = (weight * inverse).astype(BF)
            pt_stage[slot] = soft
            pt_copy(pair, 0, slot).start()
            mixed = tn(keys_of(pair, 0), soft)[HD:]
        else:

            def first(block, state):
                top, total = state
                value = scores(pair, block)
                new = jnp.maximum(top, jnp.max(value, 0, keepdims=True))
                total = total * jnp.exp(top - new) + jnp.sum(
                    jnp.exp(value - new), 0, keepdims=True
                )
                return new, total

            top, total = lax.fori_loop(
                0,
                blocks,
                first,
                (jnp.full((1, 512), NEGATIVE, F32), jnp.zeros((1, 512), F32)),
            )
            inverse = 1.0 / total

            def second(block, mixed):
                pt_stage[0] = (jnp.exp(scores(pair, block) - top) * inverse).astype(BF)
                copy = pt_copy(pair, block, 0)
                copy.start()
                mixed = mixed + tn(keys_of(pair, block), pt_stage[0])[HD:]
                copy.wait()
                return mixed

            mixed = lax.fori_loop(0, blocks, second, jnp.zeros((HD, 512), F32))
        seq, head = pair // HK, pair % HK
        for two in range(2):
            both = jnp.concatenate(
                [
                    mixed[:, two * 256 : two * 256 + 128],
                    mixed[:, two * 256 + 128 : two * 256 + 256],
                ],
                0,
            )
            tokens_ = pl.ds(pl.multiple_of(seq * 128, 128), 128)
            cols = pl.ds(pl.multiple_of(head * 256 + two * 128, 128), 128)
            out_attn_t[cols, tokens_] = both.astype(BF)
            out_attn[tokens_, cols] = jnp.transpose(both).astype(BF)
        return carry

    for seq in range(2):
        for k in range(1, line):
            kv_copy(seq, k).wait()
            kv_sib(seq, k).start()
        if seq == 0:
            o_gather.collect()
        for k in range(line):
            kv_sib(seq, k).wait()
        lax.fori_loop(seq * HK, seq * HK + HK, attend, 0)
    outs = [
        pltpu.make_async_copy(wkv_all, out_wkv, out_sem.at[0]),
        pltpu.make_async_copy(wq_all, out_wq, out_sem.at[1]),
        pltpu.make_async_copy(kv_all, out_kv, out_sem.at[2]),
    ]
    for copy in outs:
        copy.start()
    o_gather.finish()
    outs.append(pltpu.make_async_copy(wo_all, out_wo, out_sem.at[3]))
    outs[3].start()
    grad_gather.forward()

    def project(tile, carry):
        cols = pl.ds(pl.multiple_of(tile * 256, 256), 256)
        out_mid[:, cols] = x_ref[:, cols].astype(F32) + nn(out_attn[...], wo_all[:, cols])
        return carry

    lax.fori_loop(0, width // 256, project, 0)
    middle = out_mid[...]
    scale_two = lax.rsqrt(jnp.mean(middle * middle, -1, keepdims=True) + EPSILON)
    out_n2[...] = (middle * scale_two * out_gains[1:2, :]).astype(BF)
    if blocks == 1:
        pt_copy(2 * HK - 2, 0, 0).wait()
        pt_copy(2 * HK - 1, 0, 1).wait()
    grad_gather.collect()
    for gather in (kv_gather, q_gather, o_gather, grad_gather):
        gather.settle()
    for copy in outs:
        copy.wait()


def front_call(shards, line, keys, x, gains, wq, wkv, wo, grad, bias, cos, sin):
    rows, width = x.shape
    kv_width = wkv.shape[1]
    dma = pltpu.SemaphoreType.DMA
    v = pltpu.VMEM
    vm = pl.BlockSpec(memory_space=pltpu.VMEM)
    hbm = pl.BlockSpec(memory_space=pltpu.HBM)
    part = width // shards
    shape = jax.ShapeDtypeStruct
    hops = max(5, shards)
    return pl.pallas_call(
        lambda *refs: front_kernel((shards, line, keys, rows, width), *refs),
        out_shape=(
            shape((rows, width), BF),
            shape((width, rows), BF),
            shape((width, rows), BF),
            shape((2 * HK, 512, 128), BF),
            shape((rows, width), F32),
            shape((rows, width), BF),
            shape((8, width), F32),
            shape((width, width), BF),
            shape((width, kv_width), BF),
            shape((width, width), BF),
            shape((2 * HK, 2 * line, 128, 128), BF),
            shape((2 * HK, keys, 512), BF),
            shape((shards * rows, width), BF),
        ),
        in_specs=[vm] * 9,
        out_specs=(*[vm] * 7, *[hbm] * 6),
        scratch_shapes=[
            v((width, width), BF),
            v((width, kv_width), BF),
            v((width, width), BF),
            v((2 * HK, 2 * line, 128, 128), BF),
            v((rows, width), BF),
            v((shards, 8, part), F32),
            v((2, 1024, 512), BF),
            dma((shards,)),
            dma((shards,)),
            *[dma((hops,)) for _ in range(12)],
            dma((hops,)),
            dma((hops,)),
            dma((2, line)),
            dma((2, line)),
            dma((2, line)),
            dma((2, line)),
            dma((2,)),
            dma((4,)),
        ],
        compiler_params=pltpu.CompilerParams(
            collective_id=1, has_side_effects=True, vmem_limit_bytes=VMEM_LIMIT
        ),
        name="front",
    )(x, gains, wq, wkv, wo, grad, bias, cos, sin)


def rope_parts(places):
    half_dim = HD // 2
    frequency = ROPE_BASE ** (-jnp.arange(half_dim, dtype=F32) * 2.0 / HD)
    angles = places.astype(F32)[..., None] * frequency
    return (jnp.cos(angles), jnp.sin(angles))


def per_device(
    tokens,
    cotangent,
    positions,
    lengths,
    attn_gain,
    w_query,
    w_key,
    w_value,
    w_out,
    mlp_gain,
    w_gate,
    w_up,
    w_down,
):
    seqs, stretch, width = tokens.shape
    shards, line = lax.axis_size("shard"), lax.axis_size("line")
    rows = seqs * stretch
    rank = lax.axis_index("line") * 2 + lax.axis_index("core")
    places = lax.dynamic_slice_in_dim(positions, rank * stretch, stretch, 1)
    valid = (places < lengths[:, None]).astype(F32).reshape(rows, 1)
    cosine, sine = rope_parts(places.reshape(rows))
    cos_wide = jnp.concatenate([cosine] * 4, 1)
    sin_wide = jnp.concatenate([-sine, sine, -sine, sine], 1)
    allowed = (positions[:, :, None] <= places[:, None, :]) & (
        positions < lengths[:, None]
    )[:, :, None]
    bias = jnp.where(allowed, 0.0, NEGATIVE).astype(F32)
    w_kv = jnp.stack(
        [w_key.reshape(-1, HK, HD), w_value.reshape(-1, HK, HD)], 2
    ).reshape(-1, 2 * HK * HD)
    grad_out = cotangent.reshape(rows, width).astype(F32) * valid
    grad_low = grad_out.astype(BF)
    span = attn_gain.shape[0]
    gains = jnp.concatenate(
        [attn_gain[None].astype(F32), mlp_gain[None].astype(F32), jnp.zeros((6, span), F32)], 0
    )
    x = tokens.reshape(rows, width)
    (
        attn,
        attn_t,
        norm_t,
        packed_q,
        middle,
        norm_two,
        gains,
        wq_all,
        wkv_all,
        out_all,
        packed_kv,
        soft,
        grad_low_all,
    ) = front_call(
        shards,
        line,
        positions.shape[1],
        x,
        gains,
        w_query,
        w_kv,
        w_out,
        grad_low,
        bias,
        cos_wide,
        sin_wide,
    )
    packed_kv = packed_kv.reshape(seqs * HK, -1, 128)
    gain_one, gain_two = gains[0:1], gains[1:2]
    grad_middle, grad_gain_two, parts, feed_grads = feed_call(
        shards,
        norm_two,
        middle,
        grad_low,
        gain_two,
        grad_low_all.reshape(shards, rows, width),
        w_gate,
        w_up,
        w_down,
    )
    sum_feed, sum_out, sum_query, sum_kv, sum_gain, grad_input, result, _ = backward_call(
        shards,
        line,
        grad_middle,
        attn,
        attn_t,
        packed_q,
        norm_t,
        x,
        gain_one,
        cos_wide,
        sin_wide,
        grad_gain_two,
        middle,
        parts,
        out_all,
        wq_all,
        wkv_all,
        soft,
        packed_kv,
        feed_grads,
    )
    sum_kv = sum_kv.reshape(-1, HK, 2, HD)
    sum_gain = lax.dynamic_slice_in_dim(sum_gain, lax.axis_index("shard") * span, span, 1)
    return (
        result.reshape(seqs, stretch, width),
        grad_input.reshape(seqs, stretch, width),
        sum_gain[0],
        sum_query.astype(F32),
        sum_kv[:, :, 0].reshape(-1, HK * HD).astype(F32),
        sum_kv[:, :, 1].reshape(-1, HK * HD).astype(F32),
        sum_out.astype(F32),
        sum_gain[1],
        sum_feed[0].astype(F32),
        sum_feed[1].astype(F32),
        sum_feed[2].T.astype(F32),
    )


def solution(mesh):
    shards, ctx = mesh.devices.shape
    inner = Mesh(mesh.devices.reshape(shards, ctx // 2, 2), ("shard", "line", "core"))
    where = ("line", "core")
    return jax.shard_map(
        per_device,
        mesh=inner,
        in_specs=(
            P("shard", where, None),
            P("shard", where, None),
            P("shard", None),
            P("shard"),
            P("shard"),
            P("shard", None),
            P("shard", None),
            P("shard", None),
            P("shard", None),
            P("shard"),
            P(None, "shard"),
            P(None, "shard"),
            P("shard", None),
        ),
        out_specs=(
            P("shard", where, None),
            P("shard", where, None),
            P("shard"),
            P("shard", None),
            P("shard", None),
            P("shard", None),
            P("shard", None),
            P("shard"),
            P(None, "shard"),
            P(None, "shard"),
            P("shard", None),
        ),
        check_vma=False,
    )
```

```python
import math

import jax
import jax.numpy as jnp
from jax import lax
from jax.experimental import pallas as pl
from jax.experimental.pallas import tpu as pltpu
from jax.sharding import Mesh
from jax.sharding import PartitionSpec as P

HQ = 20
HK = 5
HD = 64
GROUP = HQ // HK
EPSILON = 1e-05
NEGATIVE = -1e30
ROPE_BASE = 10000.0
BF = jnp.bfloat16
F32 = jnp.float32
BY_MESH = pl.DeviceIdType.MESH
VMEM_LIMIT = 67043328


def nn(a, b):
    return lax.dot_general(a, b, (((1,), (0,)), ((), ())), preferred_element_type=F32)


def nt(a, b):
    return lax.dot_general(a, b, (((1,), (1,)), ((), ())), preferred_element_type=F32)


def tn(a, b):
    return lax.dot_general(a, b, (((0,), (0,)), ((), ())), preferred_element_type=F32)


def lanes_of(rows):
    return lax.broadcasted_iota(jnp.int32, (rows, 128), 1)


def swap_halves(block, lane):
    left = pltpu.roll(block, 96, 1)
    right = pltpu.roll(block, 32, 1)
    return jnp.where(lane % 64 < 32, left, right)


def peer_of(s_id, shards, k, back):
    if shards == 4:
        if isinstance(k, int):
            return [s_id, s_id + 1 - 2 * (s_id % 2), (s_id + 2) % 4, 3 - s_id][k]
        return jnp.where(
            k == 0,
            s_id,
            jnp.where(
                k == 1, s_id + 1 - 2 * (s_id % 2), jnp.where(k == 2, (s_id + 2) % 4, 3 - s_id)
            ),
        )
    return (s_id + (shards - k if back else k)) % shards


class Spread:
    def __init__(self, env, block, source, sems, shared):
        self.env, self.block, self.source, self.shared = env, block, source, shared
        self.send, self.recv, self.sib_send, self.sib_recv = sems
        self.relay = env.shards == 4

    def copy(self, k):
        env = self.env
        return env.remote(
            self.source,
            self.block(env.s_id, env.c_id, 0, 2),
            self.send.at[k],
            self.recv.at[k],
            env.peer(k),
        )

    def passing(self, k):
        env = self.env
        piece = self.block(env.origin(k), env.c_id, k - 1, 1)
        return env.remote(
            piece, piece, self.send.at[2 + k], self.recv.at[2 + k], env.peer(3 - k)
        )

    def direct(self):
        return range(1, 3 if self.relay else self.env.shards)

    def start(self):
        for k in self.direct():
            self.copy(k).start()

    def sib_copy(self, k):
        piece = self.block(self.env.origin(k), self.env.c_id, 0, 2)
        return self.env.remote(
            piece, piece, self.sib_send.at[k], self.sib_recv.at[k], self.env.sibling
        )

    def forward(self):
        for k in self.direct():
            self.copy(k).wait_recv()
            if self.relay:
                self.passing(k).start()
            if self.shared:
                self.sib_copy(k).start()

    def collect(self):
        if self.relay:
            for k in (1, 2):
                self.passing(k).wait_recv()
            if self.shared:
                self.sib_copy(3).start()

    def finish(self):
        if self.shared:
            for k in range(1, self.env.shards):
                self.sib_copy(k).wait_recv()

    def settle(self):
        for k in self.direct():
            self.copy(k).wait_send()
            if self.relay:
                self.passing(k).wait_send()
        if self.shared:
            for k in range(1, self.env.shards):
                self.sib_copy(k).wait_send()


class Env:
    def __init__(self, shards, line):
        self.shards, self.line = shards, line
        self.s_id = lax.axis_index("shard")
        self.l_id = lax.axis_index("line")
        self.c_id = lax.axis_index("core")
        self.sibling = (self.s_id, self.l_id, 1 - self.c_id)

    def remote(self, src, dst, send, recv, to):
        return pltpu.make_async_remote_copy(
            src, dst, send, recv, device_id=to, device_id_type=BY_MESH
        )

    def peer(self, k):
        return (peer_of(self.s_id, self.shards, k, False), self.l_id, self.c_id)

    def origin(self, k):
        return peer_of(self.s_id, self.shards, k, True)

    def mate(self, k):
        return (self.s_id, lax.rem(self.l_id + k, self.line), self.c_id)

    def barrier(self, others):
        barrier = pltpu.get_barrier_semaphore()
        for other in others:
            pl.semaphore_signal(barrier, inc=1, device_id=other, device_id_type=BY_MESH)
        pl.semaphore_wait(barrier, len(others))


def front_kernel(
    sizes,
    info_ref,
    keys_ref,
    freq_ref,
    gain_one_ref,
    gain_two_ref,
    x_hbm,
    g_hbm,
    wq_ref,
    wkv_ref,
    wo_ref,
    out_attn,
    out_attn_t,
    out_n1_t,
    out_qp,
    out_mid,
    out_n2,
    out_gains,
    cos_ref,
    sin_ref,
    out_wq,
    out_wkv,
    out_wo,
    out_kv,
    out_pt,
    out_g,
    wq_all,
    wkv_all,
    wo_all,
    kv_all,
    norm,
    x_ref,
    g_ref,
    bias_ref,
    gains_ref,
    gain_zone,
    pt_stage,
    gain_send,
    gain_recv,
    wq_s,
    wq_r,
    wq_ss,
    wq_sr,
    wkv_s,
    wkv_r,
    wkv_ss,
    wkv_sr,
    wo_s,
    wo_r,
    wo_ss,
    wo_sr,
    g_s,
    g_r,
    kv_send,
    kv_recv,
    kv_sib_send,
    kv_sib_recv,
    pt_sem,
    out_sem,
):
    shards, line, keys, rows, width = sizes
    env = Env(shards, line)
    s_id, l_id, c_id = env.s_id, env.l_id, env.c_id
    part = width // shards
    hp = part // 2
    quarter = hp // 2
    blocks = keys // 1024
    load_x = pltpu.make_async_copy(x_hbm, x_ref, out_sem.at[4])
    load_g = pltpu.make_async_copy(g_hbm, g_ref, out_sem.at[5])
    load_x.start()
    load_g.start()
    gains_ref[0:1, :] = gain_one_ref[...].astype(F32)
    gains_ref[1:2, :] = gain_two_ref[...].astype(F32)
    gains_ref[2:8, :] = jnp.zeros((6, part), F32)
    env.barrier(
        [env.sibling]
        + [env.peer(k) for k in range(1, shards)]
        + [env.mate(k) for k in range(1, line)]
    )

    def rows_of(ref):
        def block(s, core, first, count):
            start = s * part + core * hp + first * quarter
            return ref.at[pl.ds(pl.multiple_of(start, 16), count * quarter)]

        return block

    def g_rows(s, core, first, count):
        start = s * rows + first * (rows // 2)
        return out_g.at[pl.ds(pl.multiple_of(start, 16), count * (rows // 2))]

    mine = pl.ds(pl.multiple_of(c_id * hp, 16), hp)
    own = pl.ds(pl.multiple_of(s_id * part, 16), part)
    kv_gather = Spread(
        env, rows_of(wkv_all), wkv_ref.at[mine], (wkv_s, wkv_r, wkv_ss, wkv_sr), True
    )
    q_gather = Spread(env, rows_of(wq_all), wq_ref.at[mine], (wq_s, wq_r, wq_ss, wq_sr), True)
    o_gather = Spread(env, rows_of(wo_all), wo_ref.at[mine], (wo_s, wo_r, wo_ss, wo_sr), True)
    grad_gather = Spread(env, g_rows, g_ref, (g_s, g_r, None, None), False)

    def gain_copy(k):
        return env.remote(
            gains_ref, gain_zone.at[s_id], gain_send.at[k], gain_recv.at[k], env.peer(k)
        )

    for k in range(1, shards):
        gain_copy(k).start()
    kv_gather.start()
    locals_ = [
        pltpu.make_async_copy(wkv_ref, wkv_all.at[own], out_sem.at[0]),
        pltpu.make_async_copy(wq_ref, wq_all.at[own], out_sem.at[1]),
        pltpu.make_async_copy(wo_ref, wo_all.at[own], out_sem.at[2]),
    ]
    for copy in locals_:
        copy.start()
    gain_zone[s_id] = gains_ref[...]
    lane = lanes_of(128)
    info = jnp.transpose(info_ref[...])
    for seq in range(2):
        angle = info[:, seq : seq + 1] * freq_ref[...]
        cos_ref[seq * 128 : seq * 128 + 128, :] = jnp.cos(angle)
        sine = jnp.sin(angle)
        sin_ref[seq * 128 : seq * 128 + 128, :] = jnp.where(lane % 64 < 32, -sine, sine)
    load_x.wait()
    hidden = x_ref[...].astype(F32)
    scale = lax.rsqrt(jnp.mean(hidden * hidden, -1, keepdims=True) + EPSILON)
    for k in range(1, shards):
        gain_copy(k).wait()
    out_gains[...] = jnp.concatenate([gain_zone[s] for s in range(shards)], 1)
    norm[...] = (hidden * scale * out_gains[0:1, :]).astype(BF)
    kv_gather.forward()
    q_gather.start()
    for copy in locals_:
        copy.wait()
    kv_gather.collect()
    kv_gather.finish()

    place = l_id * 2 + c_id

    def make_kv(head, carry):
        block = nn(norm[...], wkv_all[:, pl.ds(pl.multiple_of(head * 128, 128), 128)])
        for seq in range(2):
            piece = block[seq * 128 : seq * 128 + 128]
            cos = jnp.where(lane < 64, cos_ref[pl.ds(seq * 128, 128), :], 1.0)
            sin = jnp.where(lane < 64, sin_ref[pl.ds(seq * 128, 128), :], 0.0)
            kv_all[seq * HK + head, place] = (piece * cos + swap_halves(piece, lane) * sin).astype(
                BF
            )
        return carry

    lax.fori_loop(0, HK, make_kv, 0)

    def kv_slice(seq, l, c):
        return kv_all.at[pl.ds(seq * HK, HK), l * 2 + c]

    def kv_move(seq, way, src):
        piece = kv_slice(seq, src, c_id)
        to = (s_id, lax.rem(l_id + (1 if way == 0 else line - 1), line), c_id)
        return env.remote(
            piece, piece, kv_send.at[seq, way * line + src], kv_recv.at[seq, src], to
        )

    def kv_sib(seq, src):
        piece = kv_slice(seq, src, c_id)
        return env.remote(
            piece, piece, kv_sib_send.at[seq, src], kv_sib_recv.at[seq, src], env.sibling
        )

    def kv_onward(seq, way, src):
        @pl.when((l_id < line - 1) if way == 0 else (l_id > 0))
        def _():
            kv_move(seq, way, src).start()

    def kv_start(seq):
        for way in range(2):
            kv_onward(seq, way, l_id)
        kv_sib(seq, l_id).start()

    def kv_step(seq, far):
        for way in range(2):
            src = l_id - far if way == 0 else l_id + far

            @pl.when((src >= 0) & (src < line))
            def _():
                kv_move(seq, way, src).wait_recv()
                kv_onward(seq, way, src)
                kv_sib(seq, src).start()

    def kv_finish(seq):
        for src in range(line):
            kv_sib(seq, src).wait()

    def kv_settle(seq):
        for src in range(line):

            @pl.when((l_id < line - 1) & (src <= l_id))
            def _():
                kv_move(seq, 0, src).wait_send()

            @pl.when((l_id > 0) & (src >= l_id))
            def _():
                kv_move(seq, 1, src).wait_send()

    kv_start(0)
    load_g.wait()
    for seq in range(2):
        rows_ = pl.ds(seq * 128, 128)
        g_ref[rows_, :] = (g_ref[rows_, :].astype(F32) * info[:, 2 + seq : 3 + seq]).astype(BF)
        key_at = jnp.transpose(keys_ref[seq])
        for tile in range(keys // 128):
            bias_ref[seq, tile * 128 : tile * 128 + 128, :] = jnp.where(
                key_at[:, tile : tile + 1] <= info_ref[seq : seq + 1, :], 0.0, NEGATIVE
            )
    keep_g = pltpu.make_async_copy(
        g_ref, out_g.at[pl.ds(pl.multiple_of(s_id * rows, 16), rows)], out_sem.at[4]
    )
    keep_g.start()
    for tile in range(width // 128):
        piece = norm[:, tile * 128 : tile * 128 + 128].astype(F32)
        out_n1_t[tile * 128 : tile * 128 + 128, :] = jnp.transpose(piece).astype(BF)
    q_gather.forward()
    o_gather.start()
    kv_step(0, 1)
    if line == 2:
        kv_start(1)
    else:
        kv_step(0, 2)
        kv_start(1)
    q_gather.collect()
    q_gather.finish()

    def make_q(head, carry):
        block = nn(norm[...], wq_all[:, pl.ds(pl.multiple_of(head * 256, 256), 256)])
        for seq in range(2):
            cos = cos_ref[pl.ds(seq * 128, 128), :]
            sin = sin_ref[pl.ds(seq * 128, 128), :]
            for two in range(2):
                piece = block[seq * 128 : seq * 128 + 128, two * 128 : two * 128 + 128]
                piece = piece * cos + swap_halves(piece, lane) * sin
                piece = piece.astype(BF).astype(F32) * (1.0 / math.sqrt(HD))
                pair = seq * HK + head
                out_qp[pair, pl.ds(two * 256, 128), :] = jnp.where(lane < 64, piece, 0.0).astype(
                    BF
                )
                out_qp[pair, pl.ds(two * 256 + 128, 128), :] = jnp.where(
                    lane < 64, pltpu.roll(piece, 64, 1), 0.0
                ).astype(BF)
        return carry

    lax.fori_loop(0, HK, make_q, 0)

    def pt_copy(pair, block, slot):
        span = pl.ds(pl.multiple_of(block * 1024, 1024), 1024)
        return pltpu.make_async_copy(pt_stage.at[slot], out_pt.at[pair, span], pt_sem.at[slot])

    def keys_of(pair, block):
        if blocks == 1:
            return kv_all[pair].reshape(1024, 128)
        return kv_all[pair, pl.ds(block * 8, 8)].reshape(1024, 128)

    def scores(pair, block):
        span = pl.ds(pl.multiple_of(block * 1024, 1024), 1024)
        bias = bias_ref[pair // HK, span, :]
        return nt(keys_of(pair, block), out_qp[pair]) + jnp.concatenate([bias] * GROUP, 1)

    def attend(pair, carry):
        if blocks == 1:
            slot = lax.rem(pair, 2)

            @pl.when(pair >= 2)
            def _():
                pt_copy(pair - 2, 0, slot).wait()

            value = scores(pair, 0)
            top = jnp.max(value, 0, keepdims=True)
            weight = jnp.exp(value - top)
            inverse = 1.0 / jnp.sum(weight, 0, keepdims=True)
            soft = (weight * inverse).astype(BF)
            pt_stage[slot] = soft
            pt_copy(pair, 0, slot).start()
            mixed = tn(keys_of(pair, 0), soft)[HD:]
        else:

            def first(block, state):
                top, total = state
                value = scores(pair, block)
                new = jnp.maximum(top, jnp.max(value, 0, keepdims=True))
                total = total * jnp.exp(top - new) + jnp.sum(
                    jnp.exp(value - new), 0, keepdims=True
                )
                return new, total

            top, total = lax.fori_loop(
                0,
                blocks,
                first,
                (jnp.full((1, 512), NEGATIVE, F32), jnp.zeros((1, 512), F32)),
            )
            inverse = 1.0 / total

            def second(block, mixed):
                pt_stage[0] = (jnp.exp(scores(pair, block) - top) * inverse).astype(BF)
                copy = pt_copy(pair, block, 0)
                copy.start()
                mixed = mixed + tn(keys_of(pair, block), pt_stage[0])[HD:]
                copy.wait()
                return mixed

            mixed = lax.fori_loop(0, blocks, second, jnp.zeros((HD, 512), F32))
        seq, head = pair // HK, pair % HK
        for two in range(2):
            both = jnp.concatenate(
                [
                    mixed[:, two * 256 : two * 256 + 128],
                    mixed[:, two * 256 + 128 : two * 256 + 256],
                ],
                0,
            )
            tokens_ = pl.ds(pl.multiple_of(seq * 128, 128), 128)
            cols = pl.ds(pl.multiple_of(head * 256 + two * 128, 128), 128)
            out_attn_t[cols, tokens_] = both.astype(BF)
            out_attn[tokens_, cols] = jnp.transpose(both).astype(BF)
        return carry

    for far in range(3, line):
        kv_step(0, far)
    o_gather.forward()
    grad_gather.start()
    kv_step(1, 1)
    kv_finish(0)
    lax.fori_loop(0, 2, attend, 0)
    if line > 2:
        kv_step(1, 2)
    lax.fori_loop(2, HK, attend, 0)
    for far in range(3, line):
        kv_step(1, far)
    o_gather.collect()
    kv_finish(1)
    lax.fori_loop(HK, 2 * HK - 2, attend, 0)
    grad_gather.forward()
    lax.fori_loop(2 * HK - 2, 2 * HK, attend, 0)
    outs = [
        pltpu.make_async_copy(wkv_all, out_wkv, out_sem.at[0]),
        pltpu.make_async_copy(wq_all, out_wq, out_sem.at[1]),
        pltpu.make_async_copy(kv_all, out_kv, out_sem.at[2]),
    ]
    for copy in outs:
        copy.start()
    o_gather.finish()
    outs.append(pltpu.make_async_copy(wo_all, out_wo, out_sem.at[3]))
    outs[3].start()

    def project(tile, carry):
        cols = pl.ds(pl.multiple_of(tile * 256, 256), 256)
        out_mid[:, cols] = x_ref[:, cols].astype(F32) + nn(out_attn[...], wo_all[:, cols])
        return carry

    lax.fori_loop(0, width // 256, project, 0)
    middle = out_mid[...]
    scale_two = lax.rsqrt(jnp.mean(middle * middle, -1, keepdims=True) + EPSILON)
    out_n2[...] = (middle * scale_two * out_gains[1:2, :]).astype(BF)
    if blocks == 1:
        pt_copy(2 * HK - 2, 0, 0).wait()
        pt_copy(2 * HK - 1, 0, 1).wait()
    grad_gather.collect()
    for gather in (kv_gather, q_gather, o_gather, grad_gather):
        gather.settle()
    kv_settle(0)
    kv_settle(1)
    keep_g.wait()
    for copy in outs:
        copy.wait()


def front_call(shards, line, *arrays):
    info, keys_at, x, wkv = arrays[0], arrays[1], arrays[5], arrays[8]
    rows, width = x.shape
    keys = keys_at.shape[1] * 128
    kv_width = wkv.shape[1]
    dma = pltpu.SemaphoreType.DMA
    v = pltpu.VMEM
    vm = pl.BlockSpec(memory_space=pltpu.VMEM)
    hbm = pl.BlockSpec(memory_space=pltpu.HBM)
    part = width // shards
    shape = jax.ShapeDtypeStruct
    hops = max(5, shards)
    return pl.pallas_call(
        lambda *refs: front_kernel((shards, line, keys, rows, width), *refs),
        out_shape=(
            shape((rows, width), BF),
            shape((width, rows), BF),
            shape((width, rows), BF),
            shape((2 * HK, 512, 128), BF),
            shape((rows, width), F32),
            shape((rows, width), BF),
            shape((8, width), F32),
            shape((rows, 128), F32),
            shape((rows, 128), F32),
            shape((width, width), BF),
            shape((width, kv_width), BF),
            shape((width, width), BF),
            shape((2 * HK, 2 * line, 128, 128), BF),
            shape((2 * HK, keys, 512), BF),
            shape((shards * rows, width), BF),
        ),
        in_specs=[vm] * 5 + [hbm] * 5,
        out_specs=(*[vm] * 9, *[hbm] * 6),
        scratch_shapes=[
            v((width, width), BF),
            v((width, kv_width), BF),
            v((width, width), BF),
            v((2 * HK, 2 * line, 128, 128), BF),
            v((rows, width), BF),
            v((rows, width), BF),
            v((rows, width), BF),
            v((2, keys, 128), F32),
            v((8, part), F32),
            v((shards, 8, part), F32),
            v((2, 1024, 512), BF),
            dma((shards,)),
            dma((shards,)),
            *[dma((hops,)) for _ in range(12)],
            dma((hops,)),
            dma((hops,)),
            dma((2, 2 * line)),
            dma((2, line)),
            dma((2, line)),
            dma((2, line)),
            dma((2,)),
            dma((6,)),
        ],
        compiler_params=pltpu.CompilerParams(
            collective_id=1, has_side_effects=True, vmem_limit_bytes=VMEM_LIMIT
        ),
        name="front",
    )(*arrays)


def feed_kernel(
    sizes,
    n2_ref,
    g_hbm,
    wg_hbm,
    wu_hbm,
    wd_hbm,
    out_parts,
    out_back,
    out_n2_t,
    out_inner_t,
    out_dgate,
    out_dup,
    n2_all,
    g_all,
    wg,
    wu,
    wd,
    inner,
    dgate,
    dup,
    stage,
    part_stage,
    n2_t,
    inner_t,
    load_sem,
    n2_send,
    n2_recv,
    part_sem,
    back_sem,
    out_sem,
):
    shards, rows, width, feed = sizes
    env = Env(shards, 1)
    s_id = env.s_id
    env.barrier([env.peer(k) for k in range(1, shards)])

    def n2_rows(s, core, first, count):
        return n2_all.at[s, pl.ds(first * (rows // 2), count * (rows // 2))]

    gather = Spread(env, n2_rows, n2_ref, (n2_send, n2_recv, None, None), False)
    gather.start()
    loads = [
        pltpu.make_async_copy(src, dst, load_sem.at[i])
        for i, (src, dst) in enumerate(
            ((wg_hbm, wg), (wu_hbm, wu), (g_hbm, g_all), (wd_hbm, wd))
        )
    ]
    for load in loads:
        load.start()
    n2_all[s_id] = n2_ref[...]
    loads[0].wait()
    loads[1].wait()

    def back_copy(k, slot):
        return pltpu.make_async_copy(
            stage.at[slot], out_back.at[peer_of(s_id, shards, k, True)], back_sem.at[slot]
        )

    def part_copy(k, slot):
        return pltpu.make_async_copy(
            part_stage.at[slot], out_parts.at[peer_of(s_id, shards, k, True)], part_sem.at[slot]
        )

    def outs(k):
        source = peer_of(s_id, shards, k, True)
        cols = pl.ds(pl.multiple_of(source * rows, 128), rows)
        return [
            pltpu.make_async_copy(n2_t.at[k], out_n2_t.at[:, cols], out_sem.at[k, 0]),
            pltpu.make_async_copy(inner_t.at[k], out_inner_t.at[:, cols], out_sem.at[k, 1]),
            pltpu.make_async_copy(dgate.at[source], out_dgate.at[source], out_sem.at[k, 2]),
            pltpu.make_async_copy(dup.at[source], out_dup.at[source], out_sem.at[k, 3]),
        ]

    def project(k):
        slot = lax.rem(k, 2)

        @pl.when(k >= 2)
        def _():
            part_copy(k - 2, slot).wait()

        part_stage[slot] = nn(inner[peer_of(s_id, shards, k, True)], wd[...]).astype(BF)
        part_copy(k, slot).start()

    def block(k, carry):
        source = peer_of(s_id, shards, k, True)
        slot = lax.rem(k, 2)
        if gather.relay:

            @pl.when(k == 1)
            def _():
                gather.forward()

            @pl.when(k == 3)
            def _():
                gather.passing(1).wait_recv()
                gather.passing(2).wait_recv()

        else:

            @pl.when(k > 0)
            def _():
                gather.copy(k).wait_recv()

        normed = n2_all[source]
        gate, upper = nn(normed, wg[...]), nn(normed, wu[...])

        @pl.when(k == 0)
        def _():
            loads[2].wait()
            loads[3].wait()

        grad = g_all[source]
        grad_inner = nt(grad, wd[...])
        sig = 1.0 / (1.0 + jnp.exp(-gate))
        act = gate * sig
        inner[source] = (act * upper).astype(BF)
        dgate[source] = (grad_inner * upper * sig * (1.0 + gate * (1.0 - sig))).astype(BF)
        dup[source] = (grad_inner * act).astype(BF)

        @pl.when(k >= 2)
        def _():
            back_copy(k - 2, slot).wait()

        stage[slot] = (nt(dgate[source], wg[...]) + nt(dup[source], wu[...])).astype(BF)
        back_copy(k, slot).start()
        n2_t[k] = jnp.transpose(normed)
        inner_t[k] = jnp.transpose(inner[source])
        for copy in outs(k):
            copy.start()

        @pl.when(k > 0)
        def _():
            project(k - 1)

        return carry

    lax.fori_loop(0, shards, block, 0)
    project(shards - 1)
    for k in range(shards):
        for copy in outs(k):
            copy.wait()
    gather.settle()
    for last in (2, 1):
        part_copy(shards - last, (shards - last) % 2).wait()
        back_copy(shards - last, (shards - last) % 2).wait()


def feed_call(shards, n2, grad_all, w_gate, w_up, w_down):
    rows, width = n2.shape
    feed = w_gate.shape[1]
    dma = pltpu.SemaphoreType.DMA
    v = pltpu.VMEM
    vm = pl.BlockSpec(memory_space=pltpu.VMEM)
    hbm = pl.BlockSpec(memory_space=pltpu.HBM)
    shape = jax.ShapeDtypeStruct
    hops = max(5, shards)
    return pl.pallas_call(
        lambda *refs: feed_kernel((shards, rows, width, feed), *refs),
        out_shape=(
            shape((shards, rows, width), BF),
            shape((shards, rows, width), BF),
            shape((width, shards * rows), BF),
            shape((feed, shards * rows), BF),
            shape((shards, rows, feed), BF),
            shape((shards, rows, feed), BF),
        ),
        in_specs=[vm] + [hbm] * 4,
        out_specs=tuple([hbm] * 6),
        scratch_shapes=[
            v((shards, rows, width), BF),
            v((shards, rows, width), BF),
            v((width, feed), BF),
            v((width, feed), BF),
            v((feed, width), BF),
            v((shards, rows, feed), BF),
            v((shards, rows, feed), BF),
            v((shards, rows, feed), BF),
            v((2, rows, width), BF),
            v((2, rows, width), BF),
            v((shards, width, rows), BF),
            v((shards, feed, rows), BF),
            dma((4,)),
            dma((hops,)),
            dma((hops,)),
            dma((2,)),
            dma((2,)),
            dma((shards, 4)),
        ],
        compiler_params=pltpu.CompilerParams(
            collective_id=2, has_side_effects=True, vmem_limit_bytes=VMEM_LIMIT
        ),
        name="feed",
    )(n2, grad_all, w_gate, w_up, w_down)


def add_rows(target, parts, rows, step):
    def body(index, carry):
        span = pl.ds(pl.multiple_of(index * step, step), step)
        total = parts[0][span, :].astype(F32)
        for part in parts[1:]:
            total = total + part[span, :].astype(F32)
        target[span, :] = total.astype(target.dtype)
        return carry

    lax.fori_loop(0, rows // step, body, 0)


def backward_kernel(
    sizes,
    gains_ref,
    cos_ref,
    sin_ref,
    attn_hbm,
    attn_t_hbm,
    qp_hbm,
    n1_t_hbm,
    x_hbm,
    mid_hbm,
    parts_hbm,
    back_hbm,
    n2_t_hbm,
    g_hbm,
    inner_t_hbm,
    dgate_hbm,
    dup_hbm,
    wo_hbm,
    wq_hbm,
    wkv_hbm,
    pt_hbm,
    kv_hbm,
    out_gate,
    out_up,
    out_dn,
    out_wo,
    out_wq,
    out_wkv,
    out_gain,
    out_dx,
    out_result,
    p_zone,
    b_zone,
    w_buf,
    gm,
    mid_ref,
    dkv_x,
    dkv_z,
    own_gu,
    got_gu_x,
    got_gu_r,
    got_gu_t,
    own_dn,
    got_dn_x,
    got_dn_r,
    got_dn_t,
    o_x,
    o_z,
    o_r,
    o_t,
    q_x,
    q_z,
    q_r,
    q_t,
    k_x,
    k_z,
    k_r,
    k_t,
    gn_own,
    gn_x,
    gn_z,
    gn_r,
    gn_t,
    load_sem,
    pt_sem,
    kv_sem,
    core_sem,
    up_send,
    r_recv,
    t_recv,
    down_send,
    sib_send,
    sib_recv,
    local_sem,
    dkv_core,
    dkv_send,
    dkv_recv,
    g_core,
    g_send,
    g_recv,
    a_up,
    a_r,
    a_t,
    a_down,
    a_sib_send,
    a_sib_recv,
    a_local,
    p_send,
    p_recv,
    b_send,
    b_recv,
    late_sem,
):
    shards, line, keys, rows, width, feed = sizes
    env = Env(shards, line)
    s_id, l_id, c_id = env.s_id, env.l_id, env.c_id
    sibling, remote = env.sibling, env.remote
    toward = jnp.where(l_id < line // 2, 1, -1)
    inner_to = (s_id, l_id + toward, c_id)
    has_outer = (l_id > 0) & (l_id < line - 1)
    is_mid = (l_id == line // 2 - 1) | (l_id == line // 2)
    outer_to = (s_id, jnp.where(has_outer, l_id - toward, l_id + toward), c_id)
    peers = [env.peer(k) for k in range(1, shards)]
    mates = [env.mate(k) for k in range(1, line)]
    env.barrier([sibling] + peers + mates)

    half = width // 2
    chunks = 12
    slab = 16
    part = width // shards
    own_rows = part // 2
    blocks = keys // 1024
    tokens = shards * rows
    hops = line == 4
    near_half = pl.ds(pl.multiple_of(c_id * half, 128), half)
    far_half = pl.ds(pl.multiple_of((1 - c_id) * half, 128), half)

    def back_copy(k):
        return remote(
            back_hbm.at[peer_of(s_id, shards, k, False)],
            b_zone.at[k - 1],
            b_send.at[k - 1],
            b_recv.at[k - 1],
            peers[k - 1],
        )

    def part_copy(k):
        return remote(
            parts_hbm.at[peer_of(s_id, shards, k, False)],
            p_zone.at[k - 1],
            p_send.at[k - 1],
            p_recv.at[k - 1],
            peers[k - 1],
        )

    for k in range(1, shards):
        back_copy(k).start()

    def local(src, dst, sem):
        return pltpu.make_async_copy(src, dst, sem)

    def views(index, where):
        if where != "dn":
            rows_ = half // 4
            array, piece = (0 if where == "gate" else 1), index % 4
            array_of = out_gate if where == "gate" else out_up
            span = pl.ds(pl.multiple_of(piece * rows_, 16), rows_)
            bufs = [ref.at[array, span] for ref in (own_gu, got_gu_x, got_gu_r, got_gu_t)]

            def out(core):
                start = core * half + piece * rows_
                return array_of.at[pl.ds(pl.multiple_of(start, 16), rows_)]

            return rows_, bufs, out
        rows_ = feed // 4
        span = pl.ds(pl.multiple_of((index - 8) * rows_, 16), rows_)
        bufs = [ref.at[span] for ref in (own_dn, got_dn_x, got_dn_r, got_dn_t)]

        def out(core):
            return out_dn.at[span, pl.ds(pl.multiple_of(core * half, 128), half)]

        return rows_, bufs, out

    def split(action):
        def run(index):
            if isinstance(index, int):
                if 0 <= index < chunks:
                    action(index, ("gate", "up", "dn")[index // 4])
                return
            for number, where in enumerate(("gate", "up", "dn")):

                @pl.when(index // 4 == number)
                def _():
                    action(index, where)

        return run

    def up_end(index, where):
        count, (mine, extra, came, total), _ = views(index, where)
        add_rows(mine, [mine, extra], count, slab)
        send_up(index, mine, came, total)

    def up_inner(index, where):
        count, (mine, extra, came, total), _ = views(index, where)
        remote(mine, came, up_send.at[index], r_recv.at[index], inner_to).wait_recv()
        add_rows(mine, [mine, extra, came], count, slab)
        send_up(index, mine, came, total)

    def send_up(index, mine, came, total):
        @pl.when(is_mid)
        def _():
            remote(mine, total, up_send.at[index], t_recv.at[index], inner_to).start()

        @pl.when(jnp.logical_not(is_mid))
        def _():
            remote(mine, came, up_send.at[index], r_recv.at[index], inner_to).start()

    def down(index, where):
        count, (mine, _, _, total), out = views(index, where)
        remote(mine, total, up_send.at[index], t_recv.at[index], inner_to).wait_recv()

        @pl.when(is_mid)
        def _():
            add_rows(total, [mine, total], count, slab)

        @pl.when(has_outer)
        def _():
            remote(total, total, down_send.at[index], t_recv.at[index], outer_to).start()

        remote(total, out(c_id), sib_send.at[index], sib_recv.at[index], sibling).start()
        local(total, out(c_id), local_sem.at[index]).start()

    def settle(index, where):
        _, (mine, _, _, total), out = views(index, where)
        remote(mine, total, up_send.at[index], t_recv.at[index], inner_to).wait_send()

        @pl.when(has_outer)
        def _():
            remote(total, total, down_send.at[index], t_recv.at[index], outer_to).wait_send()

        remote(total, out(1 - c_id), sib_send.at[index], sib_recv.at[index], sibling).wait()
        local(total, out(c_id), local_sem.at[index]).wait()

    up_end, up_inner, down, settle = [split(f) for f in (up_end, up_inner, down, settle)]

    def ends_up(first, last):
        @pl.when(jnp.logical_not(has_outer))
        def _():
            for index in range(first, last):
                up_end(index)

    def ring(step, lag=2):
        @pl.when((step < chunks) & has_outer)
        def _():
            up_inner(step)

        @pl.when((step >= lag) & (step < chunks + lag) & is_mid)
        def _():
            down(step - lag)

    def ring_down(index):
        @pl.when(is_mid)
        def _():
            down(index)

    def ends_down(first, last):
        @pl.when(jnp.logical_not(is_mid))
        def _():
            for index in range(first, last):
                down(index)

    def core_send(array, src):
        dst = got_gu_x.at[array] if array < 2 else got_dn_x
        return remote(src, dst, core_sem.at[array], core_sem.at[3 + array], sibling)

    load_wo = local(wo_hbm, w_buf, late_sem.at[3])

    load_mid = local(mid_hbm, mid_ref, late_sem.at[0])

    def feed_grads(g_v, g_own, dgate_v, dup_v, wide_t, near_t, inner_t, far_gu, far_dn):
        loads = [
            local(src, dst, load_sem.at[i])
            for i, (src, dst) in enumerate(
                (
                    (n2_t_hbm.at[far_half], wide_t),
                    (dgate_hbm, dgate_v),
                    (dup_hbm, dup_v),
                    (inner_t_hbm, inner_t),
                    (g_hbm, g_v),
                )
            )
        ]
        load_near = local(n2_t_hbm.at[near_half], near_t, late_sem.at[1])
        load_own = local(g_hbm.at[s_id], g_own, late_sem.at[2])
        loads[0].start()
        loads[1].start()
        load_near.start()
        for load in loads[2:]:
            load.start()
        load_own.start()
        load_mid.start()
        load_wo.start()

        def flat(ref):
            return ref[...].reshape(tokens, ref.shape[2])

        loads[0].wait()
        loads[1].wait()
        far_gu[0] = nn(wide_t[...], flat(dgate_v)).astype(BF)
        core_send(0, far_gu.at[0]).start()
        load_near.wait()
        own_gu[0] = nn(near_t[...], flat(dgate_v)).astype(BF)
        core_send(0, far_gu.at[0]).wait()
        ends_up(0, 4)
        loads[2].wait()
        far_gu[1] = nn(wide_t[...], flat(dup_v)).astype(BF)
        core_send(1, far_gu.at[1]).start()
        own_gu[1] = nn(near_t[...], flat(dup_v)).astype(BF)
        core_send(1, far_gu.at[1]).wait()
        ends_up(4, 7)
        loads[3].wait()
        loads[4].wait()
        far_dn[...] = nn(inner_t[...], g_v[:, :, far_half].reshape(tokens, half)).astype(BF)
        core_send(2, far_dn).start()
        own_dn[...] = nn(inner_t[...], g_v[:, :, near_half].reshape(tokens, half)).astype(BF)
        ring(0)
        core_send(2, far_dn).wait()
        ring(1)
        own_back = local(back_hbm.at[s_id], g_v.at[0], load_sem.at[shards - 1])
        own_back.start()
        stage = []
        for k in range(1, shards):
            back_copy(k).wait()
            stage.append(local(b_zone.at[k - 1], g_v.at[k], load_sem.at[k - 1]))
            stage[-1].start()
        own_back.wait()
        total = g_v[0].astype(F32)
        for k in range(1, shards):
            stage[k - 1].wait()
            total = total + g_v[k].astype(F32)
        load_mid.wait()
        load_own.wait()
        hidden = mid_ref[...]
        scale = lax.rsqrt(jnp.mean(hidden * hidden, -1, keepdims=True) + EPSILON)
        scaled = total * gains_ref[1:2, :]
        gn_own[1:2, :] = jnp.sum(total * hidden * scale, 0, keepdims=True)
        gm[...] = (
            g_own[...].astype(F32)
            + scale * scaled
            - hidden * (scale * scale * scale) * jnp.mean(scaled * hidden, -1, keepdims=True)
        )

    v = pltpu.VMEM
    pl.run_scoped(
        feed_grads,
        v((shards, rows, width), BF),
        v((rows, width), BF),
        v((shards, rows, feed), BF),
        v((shards, rows, feed), BF),
        v((half, tokens), BF),
        v((half, tokens), BF),
        v((feed, tokens), BF),
        v((2, half, feed), BF),
        v((feed, half), BF),
    )

    def attention(
        wkv_buf,
        pt_buf,
        kv_buf,
        dproj,
        dop,
        delta,
        dkv,
        dq,
        dkv_own,
        g_buf,
        attn_ref,
        attn_t_ref,
        qp_ref,
        n1_t_ref,
        x_ref,
    ):
        load_wkv = local(wkv_hbm, wkv_buf, late_sem.at[0])
        load_wq = local(wq_hbm, w_buf, late_sem.at[3])
        early = [
            local(src, dst, late_sem.at[4 + i])
            for i, (src, dst) in enumerate(
                (
                    (attn_hbm, attn_ref),
                    (attn_t_hbm, attn_t_ref),
                    (qp_hbm, qp_ref),
                    (n1_t_hbm, n1_t_ref),
                    (x_hbm, x_ref),
                )
            )
        ]
        for load in early:
            load.start()
        load_wkv.start()
        total_steps = 2 * HK * blocks

        def pt_copy(step, slot):
            pair, block = step // blocks, step % blocks
            span = pl.ds(pl.multiple_of(block * 1024, 1024), 1024)
            return local(pt_hbm.at[pair, span], pt_buf.at[slot], pt_sem.at[slot])

        def kv_copy(step, slot):
            pair, block = step // blocks, step % blocks
            span = pl.ds(pl.multiple_of(block * 1024, 1024), 1024)
            return local(kv_hbm.at[pair, span], kv_buf.at[slot], kv_sem.at[slot])

        pt_copy(0, 0).start()
        kv_copy(0, 0).start()

        def core_part(grad, box, slot):
            far = pl.ds(pl.multiple_of((1 - c_id) * own_rows, 16), own_rows)
            return remote(grad.at[:, far, :], box, g_core.at[slot], g_core.at[3 + slot], sibling)

        def scatter_part(grad, box, zone, slot):
            core_part(grad, box, slot).wait()
            near = pl.ds(pl.multiple_of(c_id * own_rows, 16), own_rows)

            def body(s, carry):
                add_rows(box.at[s], [grad.at[s, near], box.at[s]], own_rows, slab)
                return carry

            lax.fori_loop(0, shards, body, 0)
            for k in range(1, shards):
                scatter_copy(box, zone, slot, k).start()

        def scatter_copy(box, zone, slot, k):
            return remote(
                box.at[peer_of(s_id, shards, k, False)],
                zone.at[k - 1],
                g_send.at[slot, k - 1],
                g_recv.at[slot, k - 1],
                peers[k - 1],
            )

        def gather_part(box, zone, slot):
            for k in range(1, shards):
                scatter_copy(box, zone, slot, k).wait()
            add_rows(
                box.at[s_id],
                [box.at[s_id]] + [zone.at[k] for k in range(shards - 1)],
                own_rows,
                slab,
            )

        def line_up(mine, came, total, slot, count):
            @pl.when(has_outer)
            def _():
                remote(mine, came, a_up.at[slot], a_r.at[slot], inner_to).wait_recv()
                add_rows(mine, [mine, came], count, slab if mine.dtype == BF else 8)

            @pl.when(is_mid)
            def _():
                remote(mine, total, a_up.at[slot], a_t.at[slot], inner_to).start()

            @pl.when(jnp.logical_not(is_mid))
            def _():
                remote(mine, came, a_up.at[slot], a_r.at[slot], inner_to).start()

        def line_down(mine, total, slot, count, near, far):
            remote(mine, total, a_up.at[slot], a_t.at[slot], inner_to).wait()

            @pl.when(is_mid)
            def _():
                add_rows(total, [mine, total], count, slab if mine.dtype == BF else 8)

            @pl.when(has_outer)
            def _():
                remote(total, total, a_down.at[slot], a_t.at[slot], outer_to).start()

            if far is not None:
                remote(total, near, a_sib_send.at[slot], a_sib_recv.at[slot], sibling).start()
            local(total, near, a_local.at[slot]).start()

        def line_settle(total, slot, near, far):
            @pl.when(has_outer)
            def _():
                remote(total, total, a_down.at[slot], a_t.at[slot], outer_to).wait_send()

            if far is not None:
                remote(total, far, a_sib_send.at[slot], a_sib_recv.at[slot], sibling).wait()
            local(total, near, a_local.at[slot]).wait()

        lane = lanes_of(128)
        dproj[...] = gm[...].astype(BF)
        load_wo.wait()
        early[0].wait()

        def spread(head, carry):
            block = nt(
                dproj[...], w_buf[pl.ds(pl.multiple_of(head * 256, 256), 256), :]
            ).astype(BF)
            for seq in range(2):
                for two in range(2):
                    piece = block[
                        seq * 128 : seq * 128 + 128, two * 128 : two * 128 + 128
                    ].astype(F32)
                    place = seq * HK + head
                    first = jnp.where(lane >= 64, pltpu.roll(piece, 64, 1), 0.0)
                    dop[place, pl.ds(two * 256, 128), :] = first.astype(BF)
                    dop[place, pl.ds(two * 256 + 128, 128), :] = jnp.where(
                        lane >= 64, piece, 0.0
                    ).astype(BF)
                    value = attn_ref[
                        pl.ds(seq * 128, 128),
                        pl.ds(pl.multiple_of(head * 256 + two * 128, 128), 128),
                    ].astype(F32)
                    product = jnp.transpose(piece * value)
                    delta[place, :, pl.ds(two * 256, 128)] = jnp.sum(
                        product[:64], 0, keepdims=True
                    )
                    delta[place, :, pl.ds(two * 256 + 128, 128)] = jnp.sum(
                        product[64:], 0, keepdims=True
                    )
            return carry

        lax.fori_loop(0, HK, spread, 0)
        load_wq.start()
        ring(2)

        def weight_grad(left, right, grad, count):
            def body(s, carry):
                grad[s] = nn(
                    left[pl.ds(pl.multiple_of(s * part, 16), part), :], right[...]
                ).astype(BF)
                return carry

            lax.fori_loop(0, count, body, 0)

        early[1].wait()
        weight_grad(attn_t_ref, dproj, g_buf, shards)
        for load in early[2:]:
            load.wait()
        core_part(g_buf, o_x, 0).start()
        cosine, sine = cos_ref, sin_ref

        def attend(step, carry):
            slot = lax.rem(step, 2)
            pair, block = step // blocks, step % blocks

            @pl.when(step + 1 < total_steps)
            def _():
                pt_copy(step + 1, 1 - slot).start()
                kv_copy(step + 1, 1 - slot).start()

            pt_copy(step, slot).wait()
            kv_copy(step, slot).wait()
            keyval = kv_buf[slot]
            soft = pt_buf[slot]
            grad_soft = nt(keyval, dop[pair])
            score = (soft.astype(F32) * (grad_soft - delta[pair])).astype(BF)
            both = (nn(score, qp_ref[pair]) + nn(soft, dop[pair])).astype(BF)
            for sub in range(8):
                dkv[pair, block * 4 + sub // 2, sub % 2] = both[sub * 128 : sub * 128 + 128]
            query = tn(keyval, score)[:64] * (1.0 / math.sqrt(HD))
            seq, head = pair // HK, pair % HK
            for two in range(2):
                piece = jnp.transpose(
                    jnp.concatenate(
                        [
                            query[:, two * 256 : two * 256 + 128],
                            query[:, two * 256 + 128 : two * 256 + 256],
                        ],
                        0,
                    )
                )
                where = (
                    pl.ds(pl.multiple_of(seq * 128, 128), 128),
                    pl.ds(pl.multiple_of(head * 256 + two * 128, 128), 128),
                )
                if blocks == 1:
                    cos = cosine[where[0], :]
                    sin = sine[where[0], :]
                    dq[where] = (piece * cos - swap_halves(piece, lane) * sin).astype(BF)
                else:
                    dq[where] = jnp.where(
                        block == 0, piece, dq[where].astype(F32) + piece
                    ).astype(dq.dtype)
            return carry

        def dkv_core_copy(seq):
            return remote(
                dkv.at[pl.ds(seq * HK, HK), :, 1 - c_id],
                dkv_x.at[pl.ds(seq * HK, HK)],
                dkv_core.at[seq],
                dkv_core.at[2 + seq],
                sibling,
            )

        def dkv_copy(seq, k):
            return remote(
                dkv_x.at[pl.ds(seq * HK, HK), lax.rem(l_id + k, line)],
                dkv_z.at[seq, k - 1],
                dkv_send.at[seq, k - 1],
                dkv_recv.at[seq, k - 1],
                mates[k - 1],
            )

        def dkv_scatter(seq):
            dkv_core_copy(seq).wait()

            def body(index, carry):
                head, place = seq * HK + index // line, index % line
                dkv_x[head, place] = (
                    dkv_x[head, place].astype(F32) + dkv[head, place, c_id].astype(F32)
                ).astype(BF)
                return carry

            lax.fori_loop(0, HK * line, body, 0)
            if not hops:
                for k in range(1, line):
                    dkv_copy(seq, k).start()
                return

            @pl.when(l_id == 0)
            def _():
                for dest in range(line - 1, 0, -1):
                    dkv_hop(seq, 0, dest).start()

            @pl.when(l_id == line - 1)
            def _():
                for dest in range(line - 1):
                    dkv_hop(seq, 1, dest).start()

        def dkv_hop(seq, way, dest):
            to = (s_id, lax.rem(l_id + (1 if way == 0 else line - 1), line), c_id)
            return remote(
                dkv_x.at[pl.ds(seq * HK, HK), dest],
                dkv_z.at[seq, way, dest],
                dkv_send.at[seq, way * line + dest],
                dkv_recv.at[seq, way * line + dest],
                to,
            )

        def dkv_hops(seq):
            if not hops:
                return
            low = l_id < line // 2
            for first in (True, False):
                for step in range(1, line):
                    for way, dest in ((0, line - step), (1, step - 1)):
                        ahead = (
                            (l_id > 0) & (l_id < dest)
                            if way == 0
                            else (l_id < line - 1) & (l_id > dest)
                        )
                        turn_now = low if first == (way == 0) else jnp.logical_not(low)

                        @pl.when(ahead & turn_now)
                        def _():
                            dkv_hop(seq, way, dest).wait_recv()
                            dkv_take(seq, way, dest)
                            dkv_hop(seq, way, dest).start()

        def dkv_take(seq, way, dest):
            def body(head, carry):
                dkv_x[seq * HK + head, dest] = (
                    dkv_x[seq * HK + head, dest].astype(F32)
                    + dkv_z[seq, way, dest, head].astype(F32)
                ).astype(BF)
                return carry

            lax.fori_loop(0, HK, body, 0)

        def dkv_arrive(seq):
            if not hops:
                for k in range(1, line):
                    dkv_copy(seq, k).wait()
                return
            for dest in range(line):

                @pl.when(l_id < dest)
                def _():
                    dkv_hop(seq, 0, dest).wait_send()

                @pl.when(l_id > dest)
                def _():
                    dkv_hop(seq, 1, dest).wait_send()

                @pl.when((l_id == dest) & (l_id > 0))
                def _():
                    dkv_hop(seq, 0, dest).wait_recv()

                @pl.when((l_id == dest) & (l_id < line - 1))
                def _():
                    dkv_hop(seq, 1, dest).wait_recv()

        def dkv_parts(seq, head, total):
            if not hops:
                for k in range(line - 1):
                    total = total + dkv_z[seq, k, head].astype(F32)
                return total
            left = jnp.where(l_id > 0, dkv_z[seq, 0, l_id, head].astype(F32), 0.0)
            right = jnp.where(l_id < line - 1, dkv_z[seq, 1, l_id, head].astype(F32), 0.0)
            return total + left + right

        def dkv_gather(seq):
            dkv_arrive(seq)
            cos = jnp.where(lane < 64, cosine[pl.ds(seq * 128, 128), :], 1.0)
            sin = jnp.where(lane < 64, sine[pl.ds(seq * 128, 128), :], 0.0)
            for head in range(HK):
                total = dkv_x[seq * HK + head, l_id].astype(F32)
                total = dkv_parts(seq, head, total)
                dkv_own[pl.ds(seq * 128, 128), pl.ds(head * 128, 128)] = (
                    total * cos - swap_halves(total, lane) * sin
                ).astype(BF)

        near = c_id * own_rows
        far = (1 - c_id) * own_rows
        pieces = 2 if own_rows % 32 == 0 else 1

        def jobs_of(box, came, total, out, slot):
            count = own_rows // pieces
            result = []
            for piece in range(pieces):
                span = pl.ds(piece * count, count)
                result.append(
                    (
                        box.at[s_id, span],
                        came.at[span],
                        total.at[span],
                        slot + piece,
                        count,
                        out.at[pl.ds(pl.multiple_of(near + piece * count, 16), count)],
                        out.at[pl.ds(pl.multiple_of(far + piece * count, 16), count)],
                    )
                )
            return result

        o_jobs = jobs_of(o_x, o_r, o_t, out_wo, 0)
        q_jobs = jobs_of(q_x, q_r, q_t, out_wq, 2)
        k_jobs = jobs_of(k_x, k_r, k_t, out_wkv, 4)
        gain_job = [(gn_x, gn_r, gn_t, 6, 8, out_gain, None)]
        jobs = o_jobs + q_jobs + gain_job + k_jobs

        def first_up(some):
            @pl.when(jnp.logical_not(has_outer))
            def _():
                for mine, came, total, slot, count, _, _ in some:
                    line_up(mine, came, total, slot, count)

        def job_up(job):
            mine, came, total, slot, count, _, _ = job

            @pl.when(has_outer)
            def _():
                line_up(mine, came, total, slot, count)

        def job_down(job):
            mine, _, total, slot, count, to, other = job
            line_down(mine, total, slot, count, to, other)

        lax.fori_loop(0, 2 * blocks, attend, 0)
        scatter_part(g_buf, o_x, o_z, 0)
        ring(3)
        lax.fori_loop(2 * blocks, HK * blocks, attend, 0)
        dkv_core_copy(0).start()
        ring(4)
        lax.fori_loop(HK * blocks, (HK + 2) * blocks, attend, 0)
        dkv_scatter(0)
        lax.fori_loop((HK + 2) * blocks, total_steps, attend, 0)
        dkv_core_copy(1).start()
        if blocks > 1:
            for two in range(width // 128):
                for seq in range(2):
                    where = (pl.ds(seq * 128, 128), pl.ds(two * 128, 128))
                    piece = dq[where].astype(F32)
                    cos = cosine[where[0], :]
                    sin = sine[where[0], :]
                    dq[where] = (piece * cos - swap_halves(piece, lane) * sin).astype(dq.dtype)
        ring(5)
        weight_grad(n1_t_ref, dq, g_buf, shards)
        core_part(g_buf, q_x, 1).start()
        dkv_scatter(1)
        ends_up(7, chunks)
        ring(6)
        ring_down(5)
        dkv_hops(0)
        scatter_part(g_buf, q_x, q_z, 1)
        gather_part(o_x, o_z, 0)
        first_up(o_jobs)
        dkv_hops(1)
        ring_down(6)
        load_wq.wait()
        load_wkv.wait()
        back = nt(dq[...], w_buf[...])
        ends_down(0, 3)
        dkv_gather(0)
        dkv_gather(1)
        g_kv = g_buf.at[:, :, pl.ds(0, 2 * HK * HD)]
        weight_grad(n1_t_ref, dkv_own, g_kv, shards)
        core_part(g_kv, k_x, 2).start()
        back = back + nt(dkv_own[...], wkv_buf[...])
        scatter_part(g_kv, k_x, k_z, 2)
        ring(7, 8)
        hidden = x_ref[...].astype(F32)
        scale = lax.rsqrt(jnp.mean(hidden * hidden, -1, keepdims=True) + EPSILON)
        scaled = back * gains_ref[0:1, :]
        gn_own[0:1, :] = jnp.sum(back * hidden * scale, 0, keepdims=True)
        gn_own[2:8, :] = jnp.zeros((6, width), F32)
        gain_core = remote(gn_own, gn_x, g_core.at[6], g_core.at[7], sibling)
        gain_core.start()
        out_dx[...] = (
            gm[...]
            + scale * scaled
            - hidden * (scale * scale * scale) * jnp.mean(scaled * hidden, -1, keepdims=True)
        ).astype(BF)
        gain_core.wait()
        gn_own[...] = gn_own[...] + gn_x[...]

        def gain_copy(k):
            return remote(
                gn_own, gn_z.at[k - 1], g_send.at[3, k - 1], g_recv.at[3, k - 1], peers[k - 1]
            )

        for k in range(1, shards):
            gain_copy(k).start()
        for k in range(1, shards):
            part_copy(k).start()

        def gather_gain():
            for k in range(1, shards):
                gain_copy(k).wait()
            total = gn_own[...]
            for k in range(shards - 1):
                total = total + gn_z[k]
            gn_x[...] = total

        @pl.when(jnp.logical_not(has_outer))
        def _():
            gather_part(q_x, q_z, 1)
            for mine, came, total, slot, count, _, _ in q_jobs:
                line_up(mine, came, total, slot, count)
            gather_gain()
            gather_part(k_x, k_z, 2)
            for mine, came, total, slot, count, _, _ in gain_job + k_jobs:
                line_up(mine, came, total, slot, count)

        @pl.when(has_outer)
        def _():
            ring(8, 1)
            ring(9, 1)
            gather_part(q_x, q_z, 1)
            ring(10, 1)
            gather_gain()
            gather_part(k_x, k_z, 2)
            ring(11, 1)

        ends_down(3, 8)
        todo = list(jobs)
        done = [todo.pop(0)]
        job_up(done[-1])
        ring(chunks, 1)
        ends_down(8, chunks)
        for job in todo:
            job_up(job)
            done.append(job)
            job_down(done.pop(0))
        for job in done:
            job_down(job)
        for k in range(1, shards):
            part_copy(k).wait()
        result = mid_ref[...]
        for first in range(0, shards, 4):
            stage = [
                local(
                    parts_hbm.at[s_id] if k == 0 else p_zone.at[k - 1],
                    w_buf.at[pl.ds((k - first) * rows, rows)],
                    load_sem.at[k - first],
                )
                for k in range(first, min(shards, first + 4))
            ]
            for copy in stage:
                copy.start()
            for k, copy in enumerate(stage):
                copy.wait()
                result = result + w_buf[k * rows : (k + 1) * rows, :].astype(F32)
        out_result[...] = result.astype(BF)
        for _, _, total, slot, _, to, other in jobs:
            line_settle(total, slot, to, other)

    pl.run_scoped(
        attention,
        v((width, 2 * HK * HD), BF),
        v((2, 1024, 512), BF),
        v((2, 1024, 128), BF),
        v((rows, width), BF),
        v((2 * HK, 512, 128), BF),
        v((2 * HK, 1, 512), F32),
        v((2 * HK, line, 2, 128, 128), BF),
        v((rows, width), BF if blocks == 1 else F32),
        v((rows, 2 * HK * HD), BF),
        v((shards, part, width), BF),
        v((rows, width), BF),
        v((width, rows), BF),
        v((2 * HK, 512, 128), BF),
        v((width, rows), BF),
        v((rows, width), BF),
    )

    def last(index, carry):
        settle(index)
        return carry

    lax.fori_loop(0, chunks, last, 0)


def backward_call(shards, line, *arrays):
    x, kv, gate = arrays[7], arrays[-1], arrays[14]
    rows, width = x.shape
    keys = kv.shape[1]
    feed = gate.shape[2]
    part = width // shards
    own_rows = part // 2
    kv_width = 2 * HK * HD
    sizes = (shards, line, keys, rows, width, feed)
    dma = pltpu.SemaphoreType.DMA
    v = pltpu.VMEM
    vm = pl.BlockSpec(memory_space=pltpu.VMEM)
    hbm = pl.BlockSpec(memory_space=pltpu.HBM)
    half = width // 2
    shape = jax.ShapeDtypeStruct

    def boxes(cols):
        return [
            v((shards, own_rows, cols), BF),
            v((shards - 1, own_rows, cols), BF),
            v((own_rows, cols), BF),
            v((own_rows, cols), BF),
        ]

    scratch = [
        v((width, width), BF),
        v((rows, width), F32),
        v((rows, width), F32),
        v((2 * HK, line, 128, 128), BF),
        v((2, 2, 4, HK, 128, 128) if line == 4 else (2, line - 1, HK, 128, 128), BF),
        *[v((2, half, feed), BF) for _ in range(4)],
        *[v((feed, half), BF) for _ in range(4)],
        *boxes(width),
        *boxes(width),
        *boxes(kv_width),
        v((8, width), F32),
        v((8, width), F32),
        v((shards - 1, 8, width), F32),
        v((8, width), F32),
        v((8, width), F32),
        dma((max(6, shards),)),
        dma((2,)),
        dma((2,)),
        dma((6,)),
        *[dma((12,)) for _ in range(7)],
        dma((4,)),
        dma((2, 2 * line)),
        dma((2, 2 * line)),
        dma((8,)),
        dma((4, shards - 1)),
        dma((4, shards - 1)),
        *[dma((7,)) for _ in range(7)],
        *[dma((shards - 1,)) for _ in range(4)],
        dma((9,)),
    ]
    return pl.pallas_call(
        lambda *refs: backward_kernel(sizes, *refs),
        out_shape=(
            shape((width, feed), BF),
            shape((width, feed), BF),
            shape((feed, width), BF),
            shape((part, width), BF),
            shape((part, width), BF),
            shape((part, kv_width), BF),
            shape((8, width), F32),
            shape((rows, width), BF),
            shape((rows, width), BF),
            shape((shards - 1, rows, width), BF),
            shape((shards - 1, rows, width), BF),
        ),
        in_specs=[vm] * 3 + [hbm] * 18,
        out_specs=(*[hbm] * 7, vm, vm, hbm, hbm),
        scratch_shapes=scratch,
        compiler_params=pltpu.CompilerParams(
            collective_id=3, has_side_effects=True, vmem_limit_bytes=VMEM_LIMIT
        ),
        name="backward",
    )(*arrays)


def per_device(
    tokens,
    cotangent,
    positions,
    lengths,
    attn_gain,
    w_query,
    w_key,
    w_value,
    w_out,
    mlp_gain,
    w_gate,
    w_up,
    w_down,
):
    seqs, stretch, width = tokens.shape
    shards, line = lax.axis_size("shard"), lax.axis_size("line")
    rows = seqs * stretch
    rank = lax.axis_index("line") * 2 + lax.axis_index("core")
    places = lax.dynamic_slice_in_dim(positions, rank * stretch, stretch, 1)
    valid = (places < lengths[:, None]).astype(F32)
    info = jnp.concatenate([places.astype(F32), valid, jnp.zeros((4, stretch), F32)], 0)
    keys_at = jnp.where(positions < lengths[:, None], positions, 1 << 24).astype(F32)
    frequency = ROPE_BASE ** (-jnp.arange(HD // 2, dtype=F32) * 2.0 / HD)
    frequency = jnp.concatenate([frequency] * 4)[None]
    w_kv = jnp.stack(
        [w_key.reshape(-1, HK, HD), w_value.reshape(-1, HK, HD)], 2
    ).reshape(-1, 2 * HK * HD)
    span = attn_gain.shape[0]
    x = tokens.reshape(rows, width)
    (
        attn,
        attn_t,
        norm_t,
        packed_q,
        middle,
        norm_two,
        gains,
        cos_wide,
        sin_wide,
        wq_all,
        wkv_all,
        out_all,
        packed_kv,
        soft,
        grad_low_all,
    ) = front_call(
        shards,
        line,
        info,
        keys_at.reshape(seqs, -1, 128),
        frequency,
        attn_gain[None],
        mlp_gain[None],
        x,
        cotangent.reshape(rows, width),
        w_query,
        w_kv,
        w_out,
    )
    packed_kv = packed_kv.reshape(seqs * HK, -1, 128)
    grad_low_all = grad_low_all.reshape(shards, rows, width)
    parts, back, norm_all_t, inner_t, grad_gate, grad_up = feed_call(
        shards, norm_two, grad_low_all, w_gate, w_up, w_down
    )
    sum_gate, sum_up, sum_down, sum_out, sum_query, sum_kv, sum_gain, grad_input, result, _, _ = (
        backward_call(
            shards,
            line,
            gains,
            cos_wide,
            sin_wide,
            attn,
            attn_t,
            packed_q,
            norm_t,
            x,
            middle,
            parts,
            back,
            norm_all_t,
            grad_low_all,
            inner_t,
            grad_gate,
            grad_up,
            out_all,
            wq_all,
            wkv_all,
            soft,
            packed_kv,
        )
    )
    sum_kv = sum_kv.reshape(-1, HK, 2, HD)
    sum_gain = lax.dynamic_slice_in_dim(sum_gain, lax.axis_index("shard") * span, span, 1)
    return (
        result.reshape(seqs, stretch, width),
        grad_input.reshape(seqs, stretch, width),
        sum_gain[0],
        sum_query.astype(F32),
        sum_kv[:, :, 0].reshape(-1, HK * HD).astype(F32),
        sum_kv[:, :, 1].reshape(-1, HK * HD).astype(F32),
        sum_out.astype(F32),
        sum_gain[1],
        sum_gate.astype(F32),
        sum_up.astype(F32),
        sum_down.astype(F32),
    )


def solution(mesh):
    shards, ctx = mesh.devices.shape
    inner = Mesh(mesh.devices.reshape(shards, ctx // 2, 2), ("shard", "line", "core"))
    where = ("line", "core")
    return jax.shard_map(
        per_device,
        mesh=inner,
        in_specs=(
            P("shard", where, None),
            P("shard", where, None),
            P("shard", None),
            P("shard"),
            P("shard"),
            P("shard", None),
            P("shard", None),
            P("shard", None),
            P("shard", None),
            P("shard"),
            P(None, "shard"),
            P(None, "shard"),
            P("shard", None),
        ),
        out_specs=(
            P("shard", where, None),
            P("shard", where, None),
            P("shard"),
            P("shard", None),
            P("shard", None),
            P("shard", None),
            P("shard", None),
            P("shard"),
            P(None, "shard"),
            P(None, "shard"),
            P("shard", None),
        ),
        check_vma=False,
    )
```

```python
import math

import jax
import jax.numpy as jnp
import numpy as np
from jax import lax
from jax.experimental import pallas as pl
from jax.experimental.pallas import tpu as pltpu
from jax.sharding import Mesh
from jax.sharding import PartitionSpec as P

HQ = 20
HK = 5
HD = 64
GROUP = HQ // HK
EPSILON = 1e-05
NEGATIVE = -1e30
ROPE_BASE = 10000.0
BF = jnp.bfloat16
F32 = jnp.float32
BY_MESH = pl.DeviceIdType.MESH
VMEM_LIMIT = 67043328


def nn(a, b):
    return lax.dot_general(a, b, (((1,), (0,)), ((), ())), preferred_element_type=F32)


def nt(a, b):
    return lax.dot_general(a, b, (((1,), (1,)), ((), ())), preferred_element_type=F32)


def tn(a, b):
    return lax.dot_general(a, b, (((0,), (0,)), ((), ())), preferred_element_type=F32)


def lanes_of(rows):
    return lax.broadcasted_iota(jnp.int32, (rows, 128), 1)


def swap_halves(block, lane):
    left = pltpu.roll(block, 96, 1)
    right = pltpu.roll(block, 32, 1)
    return jnp.where(lane % 64 < 32, left, right)


def peer_of(s_id, shards, k, back):
    if shards == 4:
        if isinstance(k, int):
            return [s_id, s_id + 1 - 2 * (s_id % 2), (s_id + 2) % 4, 3 - s_id][k]
        return jnp.where(
            k == 0,
            s_id,
            jnp.where(
                k == 1, s_id + 1 - 2 * (s_id % 2), jnp.where(k == 2, (s_id + 2) % 4, 3 - s_id)
            ),
        )
    return (s_id + (shards - k if back else k)) % shards


class Spread:
    def __init__(self, env, block, source, sems, shared):
        self.env, self.block, self.source, self.shared = env, block, source, shared
        self.send, self.recv, self.sib_send, self.sib_recv = sems
        self.relay = env.shards == 4

    def copy(self, k):
        env = self.env
        return env.remote(
            self.source,
            self.block(env.s_id, env.c_id, 0, 2),
            self.send.at[k],
            self.recv.at[k],
            env.peer(k),
        )

    def passing(self, k):
        env = self.env
        piece = self.block(env.origin(k), env.c_id, k - 1, 1)
        return env.remote(
            piece, piece, self.send.at[2 + k], self.recv.at[2 + k], env.peer(3 - k)
        )

    def direct(self):
        return range(1, 3 if self.relay else self.env.shards)

    def start(self):
        for k in self.direct():
            self.copy(k).start()

    def sib_copy(self, k):
        piece = self.block(self.env.origin(k), self.env.c_id, 0, 2)
        return self.env.remote(
            piece, piece, self.sib_send.at[k], self.sib_recv.at[k], self.env.sibling
        )

    def forward(self):
        for k in self.direct():
            self.copy(k).wait_recv()
            if self.relay:
                self.passing(k).start()
            if self.shared:
                self.sib_copy(k).start()

    def collect(self):
        if self.relay:
            for k in (1, 2):
                self.passing(k).wait_recv()
            if self.shared:
                self.sib_copy(3).start()

    def finish(self):
        if self.shared:
            for k in range(1, self.env.shards):
                self.sib_copy(k).wait_recv()

    def settle(self):
        for k in self.direct():
            self.copy(k).wait_send()
            if self.relay:
                self.passing(k).wait_send()
        if self.shared:
            for k in range(1, self.env.shards):
                self.sib_copy(k).wait_send()


class Env:
    def __init__(self, shards, line):
        self.shards, self.line = shards, line
        self.s_id = lax.axis_index("shard")
        self.l_id = lax.axis_index("line")
        self.c_id = lax.axis_index("core")
        self.sibling = (self.s_id, self.l_id, 1 - self.c_id)

    def remote(self, src, dst, send, recv, to):
        return pltpu.make_async_remote_copy(
            src, dst, send, recv, device_id=to, device_id_type=BY_MESH
        )

    def peer(self, k):
        return (peer_of(self.s_id, self.shards, k, False), self.l_id, self.c_id)

    def origin(self, k):
        return peer_of(self.s_id, self.shards, k, True)

    def mate(self, k):
        return (self.s_id, lax.rem(self.l_id + k, self.line), self.c_id)

    def barrier(self, others):
        barrier = pltpu.get_barrier_semaphore()
        for other in others:
            pl.semaphore_signal(barrier, inc=1, device_id=other, device_id_type=BY_MESH)
        pl.semaphore_wait(barrier, len(others))


def front_kernel(
    sizes,
    positions_ref,
    lengths_ref,
    freq_ref,
    gains_in,
    wk_ref,
    wv_ref,
    x_hbm,
    g_hbm,
    wq_ref,
    wo_ref,
    wg_hbm,
    wu_hbm,
    wd_hbm,
    out_gains,
    cos_ref,
    sin_ref,
    out_wq,
    out_wkv,
    out_wo,
    out_kv,
    out_pt,
    out_g,
    keep_attn,
    keep_attn_t,
    keep_n1_t,
    keep_qp,
    keep_mid,
    out_parts,
    out_back,
    out_n2_t,
    out_inner_t,
    out_dgate,
    out_dup,
    wq_all,
    wkv_all,
    wo_all,
    kv_all,
    n2_all,
    g_all,
    wg,
    wu,
    wd,
    out_attn,
    out_attn_t,
    out_n1_t,
    out_qp,
    out_mid,
    norm,
    x_ref,
    bias_ref,
    pt_stage,
    gains_ref,
    gain_zone,
    gain_send,
    gain_recv,
    wq_s,
    wq_r,
    wq_ss,
    wq_sr,
    wkv_s,
    wkv_r,
    wkv_ss,
    wkv_sr,
    wo_s,
    wo_r,
    wo_ss,
    wo_sr,
    g_s,
    g_r,
    n2_send,
    n2_recv,
    kv_send,
    kv_recv,
    kv_sib_send,
    kv_sib_recv,
    pt_sem,
    in_sem,
    load_sem,
    keep_sem,
    part_sem,
    back_sem,
    out_sem,
):
    shards, line, keys, rows, width, feed = sizes
    env = Env(shards, line)
    s_id, l_id, c_id = env.s_id, env.l_id, env.c_id
    part = width // shards
    hp = part // 2
    quarter = hp // 2
    blocks = keys // 1024
    load_g = pltpu.make_async_copy(g_hbm, g_all.at[s_id], in_sem.at[0])
    load_g.start()
    loads = [
        pltpu.make_async_copy(src, dst, load_sem.at[i])
        for i, (src, dst) in enumerate(((wg_hbm, wg), (wu_hbm, wu), (wd_hbm, wd)))
    ]
    for head in range(HK):
        both = jnp.concatenate(
            [ref[:, head * HD : head * HD + HD].astype(F32) for ref in (wk_ref, wv_ref)], 1
        )
        wkv_all[pl.ds(pl.multiple_of(s_id * part, 16), part), head * 128 : head * 128 + 128] = (
            both.astype(BF)
        )
    gains_ref[0:2, :] = gains_in[...].astype(F32)
    gains_ref[2:8, :] = jnp.zeros((6, part), F32)
    env.barrier(
        [env.sibling]
        + [env.peer(k) for k in range(1, shards)]
        + [env.mate(k) for k in range(1, line)]
    )

    def tokens_of(ref):
        def block(s, core, first, count):
            return ref.at[s, pl.ds(first * (rows // 2), count * (rows // 2))]

        return block

    grad_gather = Spread(env, tokens_of(g_all), g_all.at[s_id], (g_s, g_r, None, None), False)
    n2_gather = Spread(
        env, tokens_of(n2_all), n2_all.at[s_id], (n2_send, n2_recv, None, None), False
    )

    def rows_of(ref):
        def block(s, core, first, count):
            start = s * part + core * hp + first * quarter
            return ref.at[pl.ds(pl.multiple_of(start, 16), count * quarter)]

        return block


    mine = pl.ds(pl.multiple_of(c_id * hp, 16), hp)
    own = pl.ds(pl.multiple_of(s_id * part, 16), part)
    kv_mine = pl.ds(pl.multiple_of(s_id * part + c_id * hp, 16), hp)
    kv_gather = Spread(
        env, rows_of(wkv_all), wkv_all.at[kv_mine], (wkv_s, wkv_r, wkv_ss, wkv_sr), True
    )
    q_gather = Spread(env, rows_of(wq_all), wq_ref.at[mine], (wq_s, wq_r, wq_ss, wq_sr), True)
    o_gather = Spread(env, rows_of(wo_all), wo_ref.at[mine], (wo_s, wo_r, wo_ss, wo_sr), True)
    outs = [
        pltpu.make_async_copy(src, dst, keep_sem.at[i])
        for i, (src, dst) in enumerate(
            (
                (wkv_all, out_wkv),
                (wq_all, out_wq),
                (kv_all, out_kv),
                (wo_all, out_wo),
                (out_attn, keep_attn),
                (out_attn_t, keep_attn_t),
                (out_n1_t, keep_n1_t),
                (out_qp, keep_qp),
                (out_mid, keep_mid),
            )
        )
    ]

    def attention_part():
        load_x = pltpu.make_async_copy(x_hbm, x_ref, in_sem.at[3])
        load_x.start()
        def gain_copy(k):
            return env.remote(
                gains_ref, gain_zone.at[s_id], gain_send.at[k], gain_recv.at[k], env.peer(k)
            )

        for k in range(1, shards):
            gain_copy(k).start()
        kv_gather.start()
        locals_ = [
            pltpu.make_async_copy(wq_ref, wq_all.at[own], in_sem.at[1]),
            pltpu.make_async_copy(wo_ref, wo_all.at[own], in_sem.at[2]),
        ]
        for copy in locals_:
            copy.start()
        gain_zone[s_id] = gains_ref[...]
        lane = lanes_of(128)
        place = pl.ds(pl.multiple_of((l_id * 2 + c_id) * 128, 128), 128)
        spots = positions_ref[:, place].astype(F32)
        good = [
            jnp.where(positions_ref[seq : seq + 1, place] < lengths_ref[seq], 1.0, 0.0).astype(F32)
            for seq in range(2)
        ]
        info = jnp.transpose(jnp.concatenate([spots] + good + [jnp.zeros((4, 128), F32)], 0))
        for seq in range(2):
            angle = info[:, seq : seq + 1] * freq_ref[...]
            cos_ref[seq * 128 : seq * 128 + 128, :] = jnp.cos(angle)
            sine = jnp.sin(angle)
            sin_ref[seq * 128 : seq * 128 + 128, :] = jnp.where(lane % 64 < 32, -sine, sine)
        load_x.wait()
        hidden = x_ref[...].astype(F32)
        scale = lax.rsqrt(jnp.mean(hidden * hidden, -1, keepdims=True) + EPSILON)
        for k in range(1, shards):
            gain_copy(k).wait()
        out_gains[...] = jnp.concatenate([gain_zone[s] for s in range(shards)], 1)
        norm[...] = (hidden * scale * out_gains[0:1, :]).astype(BF)
        kv_gather.forward()
        q_gather.start()
        for copy in locals_:
            copy.wait()
        kv_gather.collect()
        kv_gather.finish()

        spot = l_id * 2 + c_id

        def make_kv(head, carry):
            block = nn(norm[...], wkv_all[:, pl.ds(pl.multiple_of(head * 128, 128), 128)])
            for seq in range(2):
                piece = block[seq * 128 : seq * 128 + 128]
                cos = jnp.where(lane < 64, cos_ref[pl.ds(seq * 128, 128), :], 1.0)
                sin = jnp.where(lane < 64, sin_ref[pl.ds(seq * 128, 128), :], 0.0)
                kv_all[seq * HK + head, spot] = (piece * cos + swap_halves(piece, lane) * sin).astype(
                    BF
                )
            return carry

        lax.fori_loop(0, HK, make_kv, 0)

        def kv_slice(seq, l, c):
            return kv_all.at[pl.ds(seq * HK, HK), l * 2 + c]

        def kv_move(seq, way, src):
            piece = kv_slice(seq, src, c_id)
            to = (s_id, lax.rem(l_id + (1 if way == 0 else line - 1), line), c_id)
            return env.remote(
                piece, piece, kv_send.at[seq, way * line + src], kv_recv.at[seq, src], to
            )

        def kv_sib(seq, src):
            piece = kv_slice(seq, src, c_id)
            return env.remote(
                piece, piece, kv_sib_send.at[seq, src], kv_sib_recv.at[seq, src], env.sibling
            )

        def kv_onward(seq, way, src):
            @pl.when((l_id < line - 1) if way == 0 else (l_id > 0))
            def _():
                kv_move(seq, way, src).start()

        def kv_start(seq):
            for way in range(2):
                kv_onward(seq, way, l_id)
            kv_sib(seq, l_id).start()

        def kv_step(seq, far):
            for way in range(2):
                src = l_id - far if way == 0 else l_id + far

                @pl.when((src >= 0) & (src < line))
                def _():
                    kv_move(seq, way, src).wait_recv()
                    kv_onward(seq, way, src)
                    kv_sib(seq, src).start()

        def kv_finish(seq):
            for src in range(line):
                kv_sib(seq, src).wait()

        def kv_settle(seq):
            for src in range(line):

                @pl.when((l_id < line - 1) & (src <= l_id))
                def _():
                    kv_move(seq, 0, src).wait_send()

                @pl.when((l_id > 0) & (src >= l_id))
                def _():
                    kv_move(seq, 1, src).wait_send()

        kv_start(0)
        for load in loads:
            load.start()
        load_g.wait()
        for seq in range(2):
            rows_ = pl.ds(seq * 128, 128)
            g_all[s_id, rows_, :] = (
                g_all[s_id, rows_, :].astype(F32) * info[:, 2 + seq : 3 + seq]
            ).astype(BF)
            for group in range(keys // 1024):
                some = jnp.concatenate(
                    [
                        positions_ref[seq : seq + 1, (group * 8 + t) * 128 : (group * 8 + t + 1) * 128]
                        for t in range(8)
                    ],
                    0,
                )
                some = jnp.where(some < lengths_ref[seq], some, 1 << 24)
                key_at = jnp.transpose(some.astype(F32))
                for t in range(8):
                    first = (group * 8 + t) * 128
                    bias_ref[seq, first : first + 128, :] = jnp.where(
                        key_at[:, t : t + 1] <= spots[seq : seq + 1, :], 0.0, NEGATIVE
                    )
        for tile in range(width // 128):
            piece = norm[:, tile * 128 : tile * 128 + 128].astype(F32)
            out_n1_t[tile * 128 : tile * 128 + 128, :] = jnp.transpose(piece).astype(BF)
        q_gather.forward()
        o_gather.start()
        kv_step(0, 1)
        if line == 2:
            kv_start(1)
        else:
            kv_step(0, 2)
            kv_start(1)
        q_gather.collect()
        q_gather.finish()

        def make_q(head, carry):
            block = nn(norm[...], wq_all[:, pl.ds(pl.multiple_of(head * 256, 256), 256)])
            for seq in range(2):
                cos = cos_ref[pl.ds(seq * 128, 128), :]
                sin = sin_ref[pl.ds(seq * 128, 128), :]
                for two in range(2):
                    piece = block[seq * 128 : seq * 128 + 128, two * 128 : two * 128 + 128]
                    piece = piece * cos + swap_halves(piece, lane) * sin
                    piece = piece.astype(BF).astype(F32) * (1.0 / math.sqrt(HD))
                    pair = seq * HK + head
                    out_qp[pair, pl.ds(two * 256, 128), :] = jnp.where(lane < 64, piece, 0.0).astype(
                        BF
                    )
                    out_qp[pair, pl.ds(two * 256 + 128, 128), :] = jnp.where(
                        lane < 64, pltpu.roll(piece, 64, 1), 0.0
                    ).astype(BF)
            return carry

        lax.fori_loop(0, HK, make_q, 0)

        def pt_copy(pair, block, slot):
            span = pl.ds(pl.multiple_of(block * 1024, 1024), 1024)
            return pltpu.make_async_copy(pt_stage.at[slot], out_pt.at[pair, span], pt_sem.at[slot])

        def keys_of(pair, block):
            if blocks == 1:
                return kv_all[pair].reshape(1024, 128)
            return kv_all[pair, pl.ds(block * 8, 8)].reshape(1024, 128)

        def scores(pair, block):
            span = pl.ds(pl.multiple_of(block * 1024, 1024), 1024)
            bias = bias_ref[pair // HK, span, :]
            return nt(keys_of(pair, block), out_qp[pair]) + jnp.concatenate([bias] * GROUP, 1)

        def attend(pair, carry):
            if blocks == 1:
                slot = lax.rem(pair, 2)

                @pl.when(pair >= 2)
                def _():
                    pt_copy(pair - 2, 0, slot).wait()

                value = scores(pair, 0)
                top = jnp.max(value, 0, keepdims=True)
                weight = jnp.exp(value - top)
                inverse = 1.0 / jnp.sum(weight, 0, keepdims=True)
                soft = (weight * inverse).astype(BF)
                pt_stage[slot] = soft
                pt_copy(pair, 0, slot).start()
                mixed = tn(keys_of(pair, 0), soft)[HD:]
            else:

                def first(block, state):
                    top, total = state
                    value = scores(pair, block)
                    new = jnp.maximum(top, jnp.max(value, 0, keepdims=True))
                    total = total * jnp.exp(top - new) + jnp.sum(
                        jnp.exp(value - new), 0, keepdims=True
                    )
                    return new, total

                top, total = lax.fori_loop(
                    0,
                    blocks,
                    first,
                    (jnp.full((1, 512), NEGATIVE, F32), jnp.zeros((1, 512), F32)),
                )
                inverse = 1.0 / total

                def second(block, mixed):
                    pt_stage[0] = (jnp.exp(scores(pair, block) - top) * inverse).astype(BF)
                    copy = pt_copy(pair, block, 0)
                    copy.start()
                    mixed = mixed + tn(keys_of(pair, block), pt_stage[0])[HD:]
                    copy.wait()
                    return mixed

                mixed = lax.fori_loop(0, blocks, second, jnp.zeros((HD, 512), F32))
            seq, head = pair // HK, pair % HK
            for two in range(2):
                both = jnp.concatenate(
                    [
                        mixed[:, two * 256 : two * 256 + 128],
                        mixed[:, two * 256 + 128 : two * 256 + 256],
                    ],
                    0,
                )
                tokens_ = pl.ds(pl.multiple_of(seq * 128, 128), 128)
                cols = pl.ds(pl.multiple_of(head * 256 + two * 128, 128), 128)
                out_attn_t[cols, tokens_] = both.astype(BF)
                out_attn[tokens_, cols] = jnp.transpose(both).astype(BF)
            return carry

        for far in range(3, line):
            kv_step(0, far)
        o_gather.forward()
        grad_gather.start()
        kv_step(1, 1)
        kv_finish(0)
        lax.fori_loop(0, 2, attend, 0)
        if line > 2:
            kv_step(1, 2)
        lax.fori_loop(2, HK, attend, 0)
        for far in range(3, line):
            kv_step(1, far)
        o_gather.collect()
        kv_finish(1)
        lax.fori_loop(HK, 2 * HK, attend, 0)
        o_gather.finish()

        def project(tile, carry):
            cols = pl.ds(pl.multiple_of(tile * 256, 256), 256)
            out_mid[:, cols] = x_ref[:, cols].astype(F32) + nn(out_attn[...], wo_all[:, cols])
            return carry

        lax.fori_loop(0, width // 256, project, 0)
        middle = out_mid[...]
        scale_two = lax.rsqrt(jnp.mean(middle * middle, -1, keepdims=True) + EPSILON)
        n2_all[s_id] = (middle * scale_two * out_gains[1:2, :]).astype(BF)
        n2_gather.start()
        grad_gather.forward()
        for copy in outs:
            copy.start()
        if blocks == 1:
            pt_copy(2 * HK - 2, 0, 0).wait()
            pt_copy(2 * HK - 1, 0, 1).wait()

        def finish():
            for gather in (kv_gather, q_gather, o_gather):
                gather.settle()
            kv_settle(0)
            kv_settle(1)
            for copy in outs:
                copy.wait()

        finishing.append(finish)

    v = pltpu.VMEM
    finishing = []
    attention_part()

    def feed_part(inner, dgate, dup, stage, part_stage, n2_t, inner_t):
        def back_copy(k, slot):
            return pltpu.make_async_copy(
                stage.at[slot], out_back.at[peer_of(s_id, shards, k, True)], back_sem.at[slot]
            )

        def part_copy(k, slot):
            return pltpu.make_async_copy(
                part_stage.at[slot], out_parts.at[peer_of(s_id, shards, k, True)], part_sem.at[slot]
            )

        def outs(k):
            source = peer_of(s_id, shards, k, True)
            cols = pl.ds(pl.multiple_of(source * rows, 128), rows)
            return [
                pltpu.make_async_copy(n2_t.at[k], out_n2_t.at[:, cols], out_sem.at[k, 0]),
                pltpu.make_async_copy(inner_t.at[k], out_inner_t.at[:, cols], out_sem.at[k, 1]),
                pltpu.make_async_copy(dgate.at[source], out_dgate.at[source], out_sem.at[k, 2]),
                pltpu.make_async_copy(dup.at[source], out_dup.at[source], out_sem.at[k, 3]),
                pltpu.make_async_copy(g_all.at[source], out_g.at[source], out_sem.at[k, 4]),
            ]

        def project(k):
            slot = lax.rem(k, 2)

            @pl.when(k >= 2)
            def _():
                part_copy(k - 2, slot).wait()

            part_stage[slot] = nn(inner[peer_of(s_id, shards, k, True)], wd[...]).astype(BF)
            part_copy(k, slot).start()

        def block(k, carry):
            source = peer_of(s_id, shards, k, True)
            slot = lax.rem(k, 2)
            if n2_gather.relay:

                @pl.when(k == 1)
                def _():
                    n2_gather.forward()

                @pl.when(k == 3)
                def _():
                    n2_gather.collect()
                    grad_gather.collect()

            else:

                @pl.when(k > 0)
                def _():
                    n2_gather.copy(k).wait_recv()

            normed = n2_all[source]
            gate, upper = nn(normed, wg[...]), nn(normed, wu[...])

            @pl.when(k == 0)
            def _():
                loads[2].wait()

            grad = g_all[source]
            grad_inner = nt(grad, wd[...])
            sig = 1.0 / (1.0 + jnp.exp(-gate))
            act = gate * sig
            inner[source] = (act * upper).astype(BF)
            dgate[source] = (grad_inner * upper * sig * (1.0 + gate * (1.0 - sig))).astype(BF)
            dup[source] = (grad_inner * act).astype(BF)

            @pl.when(k >= 2)
            def _():
                back_copy(k - 2, slot).wait()

            stage[slot] = (nt(dgate[source], wg[...]) + nt(dup[source], wu[...])).astype(BF)
            back_copy(k, slot).start()
            n2_t[k] = jnp.transpose(normed)
            inner_t[k] = jnp.transpose(inner[source])
            for copy in outs(k):
                copy.start()

            @pl.when(k > 0)
            def _():
                project(k - 1)

            return carry

        loads[0].wait()
        loads[1].wait()
        lax.fori_loop(0, shards, block, 0)
        project(shards - 1)
        for k in range(shards):
            for copy in outs(k):
                copy.wait()
        n2_gather.settle()
        grad_gather.settle()
        for last in (2, 1):
            part_copy(shards - last, (shards - last) % 2).wait()
            back_copy(shards - last, (shards - last) % 2).wait()

    pl.run_scoped(
        feed_part,
        v((shards, rows, feed), BF),
        v((shards, rows, feed), BF),
        v((shards, rows, feed), BF),
        v((2, rows, width), BF),
        v((2, rows, width), BF),
        v((shards, width, rows), BF),
        v((shards, feed, rows), BF),
    )
    finishing[0]()


def front_call(shards, line, *arrays):
    positions, x, w_gate = arrays[0], arrays[6], arrays[10]
    rows, width = x.shape
    keys = positions.shape[1]
    feed = w_gate.shape[1]
    kv_width = 2 * HK * HD
    dma = pltpu.SemaphoreType.DMA
    v = pltpu.VMEM
    vm = pl.BlockSpec(memory_space=pltpu.VMEM)
    sm = pl.BlockSpec(memory_space=pltpu.SMEM)
    hbm = pl.BlockSpec(memory_space=pltpu.HBM)
    part = width // shards
    shape = jax.ShapeDtypeStruct
    hops = max(5, shards)
    return pl.pallas_call(
        lambda *refs: front_kernel((shards, line, keys, rows, width, feed), *refs),
        out_shape=(
            shape((8, width), F32),
            shape((rows, 128), F32),
            shape((rows, 128), F32),
            shape((width, width), BF),
            shape((width, kv_width), BF),
            shape((width, width), BF),
            shape((2 * HK, 2 * line, 128, 128), BF),
            shape((2 * HK, keys, 512), BF),
            shape((shards, rows, width), BF),
            shape((rows, width), BF),
            shape((width, rows), BF),
            shape((width, rows), BF),
            shape((2 * HK, 512, 128), BF),
            shape((rows, width), F32),
            shape((shards, rows, width), BF),
            shape((shards, rows, width), BF),
            shape((width, shards * rows), BF),
            shape((feed, shards * rows), BF),
            shape((shards, rows, feed), BF),
            shape((shards, rows, feed), BF),
        ),
        in_specs=[vm, sm, vm, vm, vm, vm] + [hbm] * 7,
        out_specs=(*[vm] * 3, *[hbm] * 17),
        scratch_shapes=[
            v((width, width), BF),
            v((width, kv_width), BF),
            v((width, width), BF),
            v((2 * HK, 2 * line, 128, 128), BF),
            v((shards, rows, width), BF),
            v((shards, rows, width), BF),
            v((width, feed), BF),
            v((width, feed), BF),
            v((feed, width), BF),
            v((rows, width), BF),
            v((width, rows), BF),
            v((width, rows), BF),
            v((2 * HK, 512, 128), BF),
            v((rows, width), F32),
            v((rows, width), BF),
            v((rows, width), BF),
            v((2, keys, 128), F32),
            v((2, 1024, 512), BF),
            v((8, part), F32),
            v((shards, 8, part), F32),
            dma((shards,)),
            dma((shards,)),
            *[dma((hops,)) for _ in range(16)],
            dma((2, 2 * line)),
            dma((2, line)),
            dma((2, line)),
            dma((2, line)),
            dma((2,)),
            dma((4,)),
            dma((3,)),
            dma((9,)),
            dma((2,)),
            dma((2,)),
            dma((shards, 5)),
        ],
        compiler_params=pltpu.CompilerParams(
            collective_id=1, has_side_effects=True, vmem_limit_bytes=VMEM_LIMIT
        ),
        name="front",
    )(*arrays)


def widen_kernel(count, *refs):
    src, dst = refs[:count], refs[count : 2 * count]
    narrow = refs[2 * count : 3 * count]
    wide = refs[3 * count : 4 * count]
    load_sem, store_sem = refs[4 * count :]
    for i in range(count):
        pltpu.make_async_copy(src[i], narrow[i], load_sem.at[i]).start()

    def piece(i, part, parts):
        rows = narrow[i].shape[0] // parts
        span = pl.ds(part * rows, rows)
        held = wide[i] if dst[i].dtype == F32 else narrow[i]
        return span, pltpu.make_async_copy(held.at[span], dst[i].at[span], store_sem.at[i, part])

    for i in range(count):
        pltpu.make_async_copy(src[i], narrow[i], load_sem.at[i]).wait()
        for part in range(4):
            span, copy = piece(i, part, 4)
            if dst[i].dtype == F32:
                wide[i][span, :] = narrow[i][span, :].astype(F32)
            copy.start()
    for i in range(count):
        for part in range(4):
            piece(i, part, 4)[1].wait()


def widen_call(arrays, types):
    v = pltpu.VMEM
    hbm = pl.BlockSpec(memory_space=pltpu.HBM)
    count = len(arrays)
    return pl.pallas_call(
        lambda *refs: widen_kernel(count, *refs),
        out_shape=tuple(jax.ShapeDtypeStruct(a.shape, t) for a, t in zip(arrays, types)),
        in_specs=[hbm] * count,
        out_specs=tuple([hbm] * count),
        scratch_shapes=[
            *[v(a.shape, a.dtype) for a in arrays],
            *[v(a.shape if t == F32 else (16, 128), F32) for a, t in zip(arrays, types)],
            pltpu.SemaphoreType.DMA((count,)),
            pltpu.SemaphoreType.DMA((count, 4)),
        ],
        compiler_params=pltpu.CompilerParams(vmem_limit_bytes=VMEM_LIMIT),
        name="widen",
    )(*arrays)


def add_rows(target, parts, rows, step):
    def body(index, carry):
        span = pl.ds(pl.multiple_of(index * step, step), step)
        total = parts[0][span, :].astype(F32)
        for part in parts[1:]:
            total = total + part[span, :].astype(F32)
        target[span, :] = total.astype(target.dtype)
        return carry

    lax.fori_loop(0, rows // step, body, 0)


def backward_kernel(
    sizes,
    gains_ref,
    cos_ref,
    sin_ref,
    attn_hbm,
    attn_t_hbm,
    qp_hbm,
    n1_t_hbm,
    x_hbm,
    mid_hbm,
    parts_hbm,
    back_hbm,
    n2_t_hbm,
    g_hbm,
    inner_t_hbm,
    dgate_hbm,
    dup_hbm,
    wo_hbm,
    wq_hbm,
    wkv_hbm,
    pt_hbm,
    kv_hbm,
    out_gate,
    out_up,
    out_dn,
    out_wo,
    out_wq,
    out_wk,
    out_wv,
    out_gain,
    out_dx,
    out_result,
    p_zone,
    b_zone,
    w_buf,
    gm,
    mid_ref,
    dkv_x,
    dkv_z,
    own_gu,
    got_gu_x,
    got_gu_r,
    got_gu_t,
    own_dn,
    got_dn_x,
    got_dn_r,
    got_dn_t,
    o_x,
    o_z,
    o_r,
    o_t,
    q_x,
    q_z,
    q_r,
    q_t,
    k_x,
    k_z,
    k_r,
    k_t,
    gn_own,
    gn_x,
    gn_z,
    gn_r,
    gn_t,
    k_nat,
    gn_out,
    load_sem,
    pt_sem,
    kv_sem,
    core_sem,
    up_send,
    r_recv,
    t_recv,
    down_send,
    sib_send,
    sib_recv,
    local_sem,
    dkv_core,
    dkv_send,
    dkv_recv,
    g_core,
    g_send,
    g_recv,
    a_up,
    a_r,
    a_t,
    a_down,
    a_sib_send,
    a_sib_recv,
    a_local,
    p_send,
    p_recv,
    b_send,
    b_recv,
    late_sem,
):
    shards, line, keys, rows, width, feed = sizes
    env = Env(shards, line)
    s_id, l_id, c_id = env.s_id, env.l_id, env.c_id
    sibling, remote = env.sibling, env.remote
    toward = jnp.where(l_id < line // 2, 1, -1)
    inner_to = (s_id, l_id + toward, c_id)
    has_outer = (l_id > 0) & (l_id < line - 1)
    is_mid = (l_id == line // 2 - 1) | (l_id == line // 2)
    outer_to = (s_id, jnp.where(has_outer, l_id - toward, l_id + toward), c_id)
    peers = [env.peer(k) for k in range(1, shards)]
    mates = [env.mate(k) for k in range(1, line)]
    env.barrier([sibling] + peers + mates)

    half = width // 2
    wide_pieces = 8
    down_pieces = 8 if feed % 128 == 0 else 4
    chunks = 2 * wide_pieces + down_pieces
    turns = 12
    slab = 16
    part = width // shards
    own_rows = part // 2
    blocks = keys // 1024
    tokens = shards * rows
    hops = line == 4
    near_half = pl.ds(pl.multiple_of(c_id * half, 128), half)
    far_half = pl.ds(pl.multiple_of((1 - c_id) * half, 128), half)

    def back_copy(k):
        return remote(
            back_hbm.at[peer_of(s_id, shards, k, False)],
            b_zone.at[k - 1],
            b_send.at[k - 1],
            b_recv.at[k - 1],
            peers[k - 1],
        )

    def part_copy(k):
        return remote(
            parts_hbm.at[peer_of(s_id, shards, k, False)],
            p_zone.at[k - 1],
            p_send.at[k - 1],
            p_recv.at[k - 1],
            peers[k - 1],
        )

    for k in range(1, shards):
        back_copy(k).start()

    def local(src, dst, sem):
        return pltpu.make_async_copy(src, dst, sem)

    def views(index, where):
        if where != "dn":
            rows_ = half // wide_pieces
            array, piece = (0 if where == "gate" else 1), index % wide_pieces
            array_of = out_gate if where == "gate" else out_up
            span = pl.ds(pl.multiple_of(piece * rows_, 16), rows_)
            bufs = [ref.at[array, span] for ref in (own_gu, got_gu_x, got_gu_r, got_gu_t)]

            def out(core):
                start = core * half + piece * rows_
                return array_of.at[pl.ds(pl.multiple_of(start, 16), rows_)]

            return rows_, bufs, out
        rows_ = feed // down_pieces
        span = pl.ds(pl.multiple_of((index - 2 * wide_pieces) * rows_, 16), rows_)
        bufs = [ref.at[span] for ref in (own_dn, got_dn_x, got_dn_r, got_dn_t)]

        def out(core):
            return out_dn.at[span, pl.ds(pl.multiple_of(core * half, 128), half)]

        return rows_, bufs, out

    def split(action):
        def run(index):
            if isinstance(index, int):
                if 0 <= index < chunks:
                    action(index, ("gate", "up", "dn")[min(2, index // wide_pieces)])
                return
            for number, where in enumerate(("gate", "up", "dn")):

                @pl.when(jnp.minimum(index // wide_pieces, 2) == number)
                def _():
                    action(index, where)

        return run

    def up_end(index, where):
        count, (mine, extra, came, total), _ = views(index, where)
        add_rows(mine, [mine, extra], count, slab)
        send_up(index, mine, came, total)

    def up_inner(index, where):
        count, (mine, extra, came, total), _ = views(index, where)
        remote(mine, came, up_send.at[index], r_recv.at[index], inner_to).wait_recv()
        add_rows(mine, [mine, extra, came], count, slab)
        send_up(index, mine, came, total)

    def send_up(index, mine, came, total):
        @pl.when(is_mid)
        def _():
            remote(mine, total, up_send.at[index], t_recv.at[index], inner_to).start()

        @pl.when(jnp.logical_not(is_mid))
        def _():
            remote(mine, came, up_send.at[index], r_recv.at[index], inner_to).start()

    def down(index, where):
        count, (mine, _, _, total), out = views(index, where)
        remote(mine, total, up_send.at[index], t_recv.at[index], inner_to).wait_recv()

        @pl.when(is_mid)
        def _():
            add_rows(total, [mine, total], count, slab)

        @pl.when(has_outer)
        def _():
            remote(total, total, down_send.at[index], t_recv.at[index], outer_to).start()

        remote(total, out(c_id), sib_send.at[index], sib_recv.at[index], sibling).start()
        local(total, out(c_id), local_sem.at[index]).start()

    def settle(index, where):
        _, (mine, _, _, total), out = views(index, where)
        remote(mine, total, up_send.at[index], t_recv.at[index], inner_to).wait_send()

        @pl.when(has_outer)
        def _():
            remote(total, total, down_send.at[index], t_recv.at[index], outer_to).wait_send()

        remote(total, out(1 - c_id), sib_send.at[index], sib_recv.at[index], sibling).wait()
        local(total, out(c_id), local_sem.at[index]).wait()

    up_end, up_inner, down, settle = [split(f) for f in (up_end, up_inner, down, settle)]

    def of_turns(first, last):
        return min(2 * first, chunks), min(2 * last, chunks)

    def run_all(action, first, last):
        if last > first:

            def body(index, carry):
                action(index)
                return carry

            lax.fori_loop(first, last, body, 0)

    def ends_up(first, last):
        @pl.when(jnp.logical_not(has_outer))
        def _():
            run_all(up_end, *of_turns(first, last))

    def ring(turn, lag=2):
        for step in (2 * turn, 2 * turn + 1):
            if step < chunks:

                @pl.when(has_outer)
                def _():
                    up_inner(step)

            if 0 <= step - 2 * lag < chunks:

                @pl.when(is_mid)
                def _():
                    down(step - 2 * lag)

    def ring_down(turn):
        @pl.when(is_mid)
        def _():
            run_all(down, *of_turns(turn, turn + 1))

    def ends_down(first, last):
        @pl.when(jnp.logical_not(is_mid))
        def _():
            run_all(down, *of_turns(first, last))

    def core_send(array, src):
        dst = got_gu_x.at[array] if array < 2 else got_dn_x
        return remote(src, dst, core_sem.at[array], core_sem.at[3 + array], sibling)

    load_wo = local(wo_hbm, w_buf, late_sem.at[3])

    load_mid = local(mid_hbm, mid_ref, late_sem.at[0])

    def feed_grads(g_v, g_own, dgate_v, dup_v, wide_t, near_t, inner_t, far_gu, far_dn):
        loads = [
            local(src, dst, load_sem.at[i])
            for i, (src, dst) in enumerate(
                (
                    (n2_t_hbm.at[far_half], wide_t),
                    (dgate_hbm, dgate_v),
                    (dup_hbm, dup_v),
                    (inner_t_hbm, inner_t),
                    (g_hbm, g_v),
                )
            )
        ]
        load_near = local(n2_t_hbm.at[near_half], near_t, late_sem.at[1])
        load_own = local(g_hbm.at[s_id], g_own, late_sem.at[2])
        loads[0].start()
        loads[1].start()
        load_near.start()
        for load in loads[2:]:
            load.start()
        load_own.start()
        load_mid.start()
        load_wo.start()

        def flat(ref):
            return ref[...].reshape(tokens, ref.shape[2])

        loads[0].wait()
        loads[1].wait()
        far_gu[0] = nn(wide_t[...], flat(dgate_v)).astype(BF)
        core_send(0, far_gu.at[0]).start()
        load_near.wait()
        own_gu[0] = nn(near_t[...], flat(dgate_v)).astype(BF)
        core_send(0, far_gu.at[0]).wait()
        ends_up(0, 4)
        loads[2].wait()
        far_gu[1] = nn(wide_t[...], flat(dup_v)).astype(BF)
        core_send(1, far_gu.at[1]).start()
        own_gu[1] = nn(near_t[...], flat(dup_v)).astype(BF)
        core_send(1, far_gu.at[1]).wait()
        ends_up(4, 7)
        loads[3].wait()
        loads[4].wait()
        far_dn[...] = nn(inner_t[...], g_v[:, :, far_half].reshape(tokens, half)).astype(BF)
        core_send(2, far_dn).start()
        own_dn[...] = nn(inner_t[...], g_v[:, :, near_half].reshape(tokens, half)).astype(BF)
        ring(0)
        core_send(2, far_dn).wait()
        ring(1)
        own_back = local(back_hbm.at[s_id], g_v.at[0], load_sem.at[shards - 1])
        own_back.start()
        stage = []
        for k in range(1, shards):
            if k == shards - 1:
                ring(2)
            back_copy(k).wait()
            stage.append(local(b_zone.at[k - 1], g_v.at[k], load_sem.at[k - 1]))
            stage[-1].start()
        own_back.wait()
        total = g_v[0].astype(F32)
        for k in range(1, shards):
            stage[k - 1].wait()
            total = total + g_v[k].astype(F32)
        load_mid.wait()
        load_own.wait()
        hidden = mid_ref[...]
        scale = lax.rsqrt(jnp.mean(hidden * hidden, -1, keepdims=True) + EPSILON)
        scaled = total * gains_ref[1:2, :]
        gn_own[1:2, :] = jnp.sum(total * hidden * scale, 0, keepdims=True)
        gm[...] = (
            g_own[...].astype(F32)
            + scale * scaled
            - hidden * (scale * scale * scale) * jnp.mean(scaled * hidden, -1, keepdims=True)
        )

    v = pltpu.VMEM
    pl.run_scoped(
        feed_grads,
        v((shards, rows, width), BF),
        v((rows, width), BF),
        v((shards, rows, feed), BF),
        v((shards, rows, feed), BF),
        v((half, tokens), BF),
        v((half, tokens), BF),
        v((feed, tokens), BF),
        v((2, half, feed), BF),
        v((feed, half), BF),
    )

    def attention(
        wkv_buf,
        pt_buf,
        kv_buf,
        dproj,
        dop,
        delta,
        dkv,
        dq,
        dkv_own,
        g_buf,
        attn_ref,
        attn_t_ref,
        qp_ref,
        n1_t_ref,
        x_ref,
    ):
        load_wkv = local(wkv_hbm, wkv_buf, late_sem.at[0])
        load_wq = local(wq_hbm, w_buf, late_sem.at[3])
        early = [
            local(src, dst, late_sem.at[4 + i])
            for i, (src, dst) in enumerate(
                (
                    (attn_hbm, attn_ref),
                    (attn_t_hbm, attn_t_ref),
                    (qp_hbm, qp_ref),
                    (n1_t_hbm, n1_t_ref),
                    (x_hbm, x_ref),
                )
            )
        ]
        for load in early:
            load.start()
        load_wkv.start()
        total_steps = 2 * HK * blocks

        def pt_copy(step, slot):
            pair, block = step // blocks, step % blocks
            span = pl.ds(pl.multiple_of(block * 1024, 1024), 1024)
            return local(pt_hbm.at[pair, span], pt_buf.at[slot], pt_sem.at[slot])

        def kv_copy(step, slot):
            pair, block = step // blocks, step % blocks
            span = pl.ds(pl.multiple_of(block * 1024, 1024), 1024)
            return local(kv_hbm.at[pair, span], kv_buf.at[slot], kv_sem.at[slot])

        pt_copy(0, 0).start()
        kv_copy(0, 0).start()

        def core_part(grad, box, slot):
            far = pl.ds(pl.multiple_of((1 - c_id) * own_rows, 16), own_rows)
            return remote(grad.at[:, far, :], box, g_core.at[slot], g_core.at[3 + slot], sibling)

        def scatter_part(grad, box, zone, slot):
            core_part(grad, box, slot).wait()
            near = pl.ds(pl.multiple_of(c_id * own_rows, 16), own_rows)

            def body(s, carry):
                add_rows(box.at[s], [grad.at[s, near], box.at[s]], own_rows, slab)
                return carry

            lax.fori_loop(0, shards, body, 0)
            for k in range(1, shards):
                scatter_copy(box, zone, slot, k).start()

        def scatter_copy(box, zone, slot, k):
            return remote(
                box.at[peer_of(s_id, shards, k, False)],
                zone.at[k - 1],
                g_send.at[slot, k - 1],
                g_recv.at[slot, k - 1],
                peers[k - 1],
            )

        def gather_part(box, zone, slot):
            for k in range(1, shards):
                scatter_copy(box, zone, slot, k).wait()
            add_rows(
                box.at[s_id],
                [box.at[s_id]] + [zone.at[k] for k in range(shards - 1)],
                own_rows,
                slab,
            )

        def line_up(mine, came, total, slot, count):
            @pl.when(has_outer)
            def _():
                remote(mine, came, a_up.at[slot], a_r.at[slot], inner_to).wait_recv()
                add_rows(mine, [mine, came], count, slab if mine.dtype == BF else 8)

            @pl.when(is_mid)
            def _():
                remote(mine, total, a_up.at[slot], a_t.at[slot], inner_to).start()

            @pl.when(jnp.logical_not(is_mid))
            def _():
                remote(mine, came, a_up.at[slot], a_r.at[slot], inner_to).start()

        def line_down(mine, total, slot, count, ready, outs):
            remote(mine, total, a_up.at[slot], a_t.at[slot], inner_to).wait()

            @pl.when(is_mid)
            def _():
                add_rows(total, [mine, total], count, slab if mine.dtype == BF else 8)

            @pl.when(has_outer)
            def _():
                remote(total, total, a_down.at[slot], a_t.at[slot], outer_to).start()

            if ready is not None:
                ready()
            for src, near, far, box in outs:
                if far is not None:
                    remote(src, near, a_sib_send.at[box], a_sib_recv.at[box], sibling).start()
                local(src, near, a_local.at[box]).start()

        def line_settle(total, slot, outs):
            @pl.when(has_outer)
            def _():
                remote(total, total, a_down.at[slot], a_t.at[slot], outer_to).wait_send()

            for src, near, far, box in outs:
                if far is not None:
                    remote(src, far, a_sib_send.at[box], a_sib_recv.at[box], sibling).wait()
                local(src, near, a_local.at[box]).wait()

        lane = lanes_of(128)
        dproj[...] = gm[...].astype(BF)
        load_wo.wait()
        early[0].wait()

        def spread(head, carry):
            block = nt(
                dproj[...], w_buf[pl.ds(pl.multiple_of(head * 256, 256), 256), :]
            ).astype(BF)
            for seq in range(2):
                for two in range(2):
                    piece = block[
                        seq * 128 : seq * 128 + 128, two * 128 : two * 128 + 128
                    ].astype(F32)
                    place = seq * HK + head
                    first = jnp.where(lane >= 64, pltpu.roll(piece, 64, 1), 0.0)
                    dop[place, pl.ds(two * 256, 128), :] = first.astype(BF)
                    dop[place, pl.ds(two * 256 + 128, 128), :] = jnp.where(
                        lane >= 64, piece, 0.0
                    ).astype(BF)
                    value = attn_ref[
                        pl.ds(seq * 128, 128),
                        pl.ds(pl.multiple_of(head * 256 + two * 128, 128), 128),
                    ].astype(F32)
                    product = jnp.transpose(piece * value)
                    delta[place, :, pl.ds(two * 256, 128)] = jnp.sum(
                        product[:64], 0, keepdims=True
                    )
                    delta[place, :, pl.ds(two * 256 + 128, 128)] = jnp.sum(
                        product[64:], 0, keepdims=True
                    )
            return carry

        lax.fori_loop(0, HK, spread, 0)
        load_wq.start()
        ring(3)

        def weight_grad(left, right, grad, count):
            def body(s, carry):
                grad[s] = nn(
                    left[pl.ds(pl.multiple_of(s * part, 16), part), :], right[...]
                ).astype(BF)
                return carry

            lax.fori_loop(0, count, body, 0)

        early[1].wait()
        weight_grad(attn_t_ref, dproj, g_buf, shards)
        for load in early[2:]:
            load.wait()
        core_part(g_buf, o_x, 0).start()
        cosine, sine = cos_ref, sin_ref

        def attend(step, carry):
            slot = lax.rem(step, 2)
            pair, block = step // blocks, step % blocks

            @pl.when(step + 1 < total_steps)
            def _():
                pt_copy(step + 1, 1 - slot).start()
                kv_copy(step + 1, 1 - slot).start()

            pt_copy(step, slot).wait()
            kv_copy(step, slot).wait()
            keyval = kv_buf[slot]
            soft = pt_buf[slot]
            grad_soft = nt(keyval, dop[pair])
            score = (soft.astype(F32) * (grad_soft - delta[pair])).astype(BF)
            both = (nn(score, qp_ref[pair]) + nn(soft, dop[pair])).astype(BF)
            for sub in range(8):
                dkv[pair, block * 4 + sub // 2, sub % 2] = both[sub * 128 : sub * 128 + 128]
            query = tn(keyval, score)[:64] * (1.0 / math.sqrt(HD))
            seq, head = pair // HK, pair % HK
            for two in range(2):
                piece = jnp.transpose(
                    jnp.concatenate(
                        [
                            query[:, two * 256 : two * 256 + 128],
                            query[:, two * 256 + 128 : two * 256 + 256],
                        ],
                        0,
                    )
                )
                where = (
                    pl.ds(pl.multiple_of(seq * 128, 128), 128),
                    pl.ds(pl.multiple_of(head * 256 + two * 128, 128), 128),
                )
                if blocks == 1:
                    cos = cosine[where[0], :]
                    sin = sine[where[0], :]
                    dq[where] = (piece * cos - swap_halves(piece, lane) * sin).astype(BF)
                else:
                    dq[where] = jnp.where(
                        block == 0, piece, dq[where].astype(F32) + piece
                    ).astype(dq.dtype)
            return carry

        def dkv_core_copy(seq):
            return remote(
                dkv.at[pl.ds(seq * HK, HK), :, 1 - c_id],
                dkv_x.at[pl.ds(seq * HK, HK)],
                dkv_core.at[seq],
                dkv_core.at[2 + seq],
                sibling,
            )

        def dkv_copy(seq, k):
            return remote(
                dkv_x.at[pl.ds(seq * HK, HK), lax.rem(l_id + k, line)],
                dkv_z.at[seq, k - 1],
                dkv_send.at[seq, k - 1],
                dkv_recv.at[seq, k - 1],
                mates[k - 1],
            )

        def dkv_scatter(seq):
            dkv_core_copy(seq).wait()

            def body(index, carry):
                head, place = seq * HK + index // line, index % line
                dkv_x[head, place] = (
                    dkv_x[head, place].astype(F32) + dkv[head, place, c_id].astype(F32)
                ).astype(BF)
                return carry

            lax.fori_loop(0, HK * line, body, 0)
            if not hops:
                for k in range(1, line):
                    dkv_copy(seq, k).start()
                return

            @pl.when(l_id == 0)
            def _():
                for dest in range(line - 1, 0, -1):
                    dkv_hop(seq, 0, dest).start()

            @pl.when(l_id == line - 1)
            def _():
                for dest in range(line - 1):
                    dkv_hop(seq, 1, dest).start()

        def dkv_hop(seq, way, dest):
            to = (s_id, lax.rem(l_id + (1 if way == 0 else line - 1), line), c_id)
            return remote(
                dkv_x.at[pl.ds(seq * HK, HK), dest],
                dkv_z.at[seq, way, dest],
                dkv_send.at[seq, way * line + dest],
                dkv_recv.at[seq, way * line + dest],
                to,
            )

        def dkv_hops(seq):
            if not hops:
                return
            low = l_id < line // 2
            for first in (True, False):
                for step in range(1, line):
                    for way, dest in ((0, line - step), (1, step - 1)):
                        ahead = (
                            (l_id > 0) & (l_id < dest)
                            if way == 0
                            else (l_id < line - 1) & (l_id > dest)
                        )
                        turn_now = low if first == (way == 0) else jnp.logical_not(low)

                        @pl.when(ahead & turn_now)
                        def _():
                            dkv_hop(seq, way, dest).wait_recv()
                            dkv_take(seq, way, dest)
                            dkv_hop(seq, way, dest).start()

        def dkv_take(seq, way, dest):
            def body(head, carry):
                dkv_x[seq * HK + head, dest] = (
                    dkv_x[seq * HK + head, dest].astype(F32)
                    + dkv_z[seq, way, dest, head].astype(F32)
                ).astype(BF)
                return carry

            lax.fori_loop(0, HK, body, 0)

        def dkv_arrive(seq):
            if not hops:
                for k in range(1, line):
                    dkv_copy(seq, k).wait()
                return
            for dest in range(line):

                @pl.when(l_id < dest)
                def _():
                    dkv_hop(seq, 0, dest).wait_send()

                @pl.when(l_id > dest)
                def _():
                    dkv_hop(seq, 1, dest).wait_send()

                @pl.when((l_id == dest) & (l_id > 0))
                def _():
                    dkv_hop(seq, 0, dest).wait_recv()

                @pl.when((l_id == dest) & (l_id < line - 1))
                def _():
                    dkv_hop(seq, 1, dest).wait_recv()

        def dkv_parts(seq, head, total):
            if not hops:
                for k in range(line - 1):
                    total = total + dkv_z[seq, k, head].astype(F32)
                return total
            left = jnp.where(l_id > 0, dkv_z[seq, 0, l_id, head].astype(F32), 0.0)
            right = jnp.where(l_id < line - 1, dkv_z[seq, 1, l_id, head].astype(F32), 0.0)
            return total + left + right

        def dkv_gather(seq):
            dkv_arrive(seq)
            cos = jnp.where(lane < 64, cosine[pl.ds(seq * 128, 128), :], 1.0)
            sin = jnp.where(lane < 64, sine[pl.ds(seq * 128, 128), :], 0.0)
            for head in range(HK):
                total = dkv_x[seq * HK + head, l_id].astype(F32)
                total = dkv_parts(seq, head, total)
                dkv_own[pl.ds(seq * 128, 128), pl.ds(head * 128, 128)] = (
                    total * cos - swap_halves(total, lane) * sin
                ).astype(BF)

        near = c_id * own_rows
        far = (1 - c_id) * own_rows
        pieces = 2 if own_rows % 32 == 0 else 1

        def jobs_of(box, came, total, slot, outs_of):
            count = own_rows // pieces
            result = []
            for piece in range(pieces):
                span = pl.ds(piece * count, count)

                def rows_at(out, start, piece=piece):
                    return out.at[pl.ds(pl.multiple_of(start + piece * count, 16), count)]

                ready, outs = outs_of(total.at[span], span, slot + piece, rows_at)
                result.append(
                    (box.at[s_id, span], came.at[span], total.at[span], slot + piece, count)
                    + (ready, outs)
                )
            return result

        def plain(out):
            def outs_of(total, span, slot, rows_at):
                return None, [(total, rows_at(out, near), rows_at(out, far), slot)]

            return outs_of

        def unpacked(total, span, slot, rows_at):
            def ready():
                value = total[...].astype(F32)
                for half_, first in ((0, 0), (1, HD)):
                    k_nat[half_, span, :] = jnp.concatenate(
                        [
                            value[:, head * 128 + first : head * 128 + first + HD]
                            for head in range(HK)
                        ],
                        1,
                    ).astype(BF)

            outs = [
                (k_nat.at[half_, span], rows_at(out, near), rows_at(out, far), slot + 3 * half_)
                for half_, out in ((0, out_wk), (1, out_wv))
            ]
            return ready, outs

        def own_gain():
            value = gn_t[...]
            chosen = value[:, 0:part]
            for s in range(1, shards):
                chosen = jnp.where(s_id == s, value[:, s * part : (s + 1) * part], chosen)
            gn_out[...] = chosen

        o_jobs = jobs_of(o_x, o_r, o_t, 0, plain(out_wo))
        q_jobs = jobs_of(q_x, q_r, q_t, 2, plain(out_wq))
        k_jobs = jobs_of(k_x, k_r, k_t, 4, unpacked)
        gain_job = [(gn_x, gn_r, gn_t, 6, 8, own_gain, [(gn_out, out_gain, None, 6)])]
        jobs = o_jobs + q_jobs + gain_job + k_jobs

        def first_up(some):
            @pl.when(jnp.logical_not(has_outer))
            def _():
                for mine, came, total, slot, count, _, _ in some:
                    line_up(mine, came, total, slot, count)

        def job_up(job):
            mine, came, total, slot, count, _, _ = job

            @pl.when(has_outer)
            def _():
                line_up(mine, came, total, slot, count)

        def job_down(job):
            mine, _, total, slot, count, ready, outs = job
            line_down(mine, total, slot, count, ready, outs)

        lax.fori_loop(0, 2 * blocks, attend, 0)
        ring(4)
        scatter_part(g_buf, o_x, o_z, 0)
        lax.fori_loop(2 * blocks, HK * blocks, attend, 0)
        dkv_core_copy(0).start()
        ring(5)
        lax.fori_loop(HK * blocks, (HK + 2) * blocks, attend, 0)
        dkv_scatter(0)
        lax.fori_loop((HK + 2) * blocks, total_steps, attend, 0)
        dkv_core_copy(1).start()
        if blocks > 1:
            for two in range(width // 128):
                for seq in range(2):
                    where = (pl.ds(seq * 128, 128), pl.ds(two * 128, 128))
                    piece = dq[where].astype(F32)
                    cos = cosine[where[0], :]
                    sin = sine[where[0], :]
                    dq[where] = (piece * cos - swap_halves(piece, lane) * sin).astype(dq.dtype)
        ring(6)
        weight_grad(n1_t_ref, dq, g_buf, shards)
        core_part(g_buf, q_x, 1).start()
        dkv_scatter(1)
        ends_up(7, turns)
        ring_down(5)
        dkv_hops(0)
        scatter_part(g_buf, q_x, q_z, 1)
        gather_part(o_x, o_z, 0)
        first_up(o_jobs)
        dkv_hops(1)
        ring_down(6)
        load_wq.wait()
        load_wkv.wait()
        back = nt(dq[...], w_buf[...])
        ends_down(0, 3)
        ring(7, 8)
        dkv_gather(0)
        dkv_gather(1)
        g_kv = g_buf.at[:, :, pl.ds(0, 2 * HK * HD)]
        weight_grad(n1_t_ref, dkv_own, g_kv, shards)
        core_part(g_kv, k_x, 2).start()
        back = back + nt(dkv_own[...], wkv_buf[...])
        scatter_part(g_kv, k_x, k_z, 2)
        ring(8, 1)
        hidden = x_ref[...].astype(F32)
        scale = lax.rsqrt(jnp.mean(hidden * hidden, -1, keepdims=True) + EPSILON)
        scaled = back * gains_ref[0:1, :]
        gn_own[0:1, :] = jnp.sum(back * hidden * scale, 0, keepdims=True)
        gn_own[2:8, :] = jnp.zeros((6, width), F32)
        gain_core = remote(gn_own, gn_x, g_core.at[6], g_core.at[7], sibling)
        gain_core.start()
        x_ref[...] = (
            gm[...]
            + scale * scaled
            - hidden * (scale * scale * scale) * jnp.mean(scaled * hidden, -1, keepdims=True)
        ).astype(BF)
        keep_dx = local(x_ref, out_dx, late_sem.at[1])
        keep_dx.start()
        gain_core.wait()
        gn_own[...] = gn_own[...] + gn_x[...]

        def gain_copy(k):
            return remote(
                gn_own, gn_z.at[k - 1], g_send.at[3, k - 1], g_recv.at[3, k - 1], peers[k - 1]
            )

        for k in range(1, shards):
            gain_copy(k).start()
        for k in range(1, shards):
            part_copy(k).start()

        def gather_gain():
            for k in range(1, shards):
                gain_copy(k).wait()
            total = gn_own[...]
            for k in range(shards - 1):
                total = total + gn_z[k]
            gn_x[...] = total

        @pl.when(jnp.logical_not(has_outer))
        def _():
            gather_part(q_x, q_z, 1)
            for mine, came, total, slot, count, _, _ in q_jobs:
                line_up(mine, came, total, slot, count)
            gather_gain()
            gather_part(k_x, k_z, 2)
            for mine, came, total, slot, count, _, _ in gain_job + k_jobs:
                line_up(mine, came, total, slot, count)

        @pl.when(has_outer)
        def _():
            ring(9, 1)
            gather_part(q_x, q_z, 1)
            ring(10, 1)
            gather_gain()
            gather_part(k_x, k_z, 2)
            ring(11, 1)

        ends_down(3, 8)
        def finish_result():
            for k in range(1, shards):
                part_copy(k).wait()
            result = mid_ref[...]
            for first in range(0, shards, 4):
                stage = [
                    local(
                        parts_hbm.at[s_id] if k == 0 else p_zone.at[k - 1],
                        w_buf.at[pl.ds((k - first) * rows, rows)],
                        load_sem.at[k - first],
                    )
                    for k in range(first, min(shards, first + 4))
                ]
                for copy in stage:
                    copy.start()
                for k, copy in enumerate(stage):
                    copy.wait()
                    result = result + w_buf[k * rows : (k + 1) * rows, :].astype(F32)
            dproj[...] = result.astype(BF)
            local(dproj, out_result, late_sem.at[2]).start()

        todo = list(jobs)
        done = [todo.pop(0)]
        job_up(done[-1])
        ring(turns, 1)
        ends_down(8, turns)

        @pl.when(jnp.logical_not(has_outer))
        def _():
            finish_result()

        for job in todo:
            job_up(job)
            done.append(job)
            job_down(done.pop(0))
        for job in done:
            job_down(job)

        @pl.when(has_outer)
        def _():
            finish_result()

        for _, _, total, slot, _, _, outs in jobs:
            line_settle(total, slot, outs)
        keep_dx.wait()
        local(dproj, out_result, late_sem.at[2]).wait()

    pl.run_scoped(
        attention,
        v((width, 2 * HK * HD), BF),
        v((2, 1024, 512), BF),
        v((2, 1024, 128), BF),
        v((rows, width), BF),
        v((2 * HK, 512, 128), BF),
        v((2 * HK, 1, 512), F32),
        v((2 * HK, line, 2, 128, 128), BF),
        v((rows, width), BF if blocks == 1 else F32),
        v((rows, 2 * HK * HD), BF),
        v((shards, part, width), BF),
        v((rows, width), BF),
        v((width, rows), BF),
        v((2 * HK, 512, 128), BF),
        v((width, rows), BF),
        v((rows, width), BF),
    )

    def last(index, carry):
        settle(index)
        return carry

    lax.fori_loop(0, chunks, last, 0)


def backward_call(shards, line, *arrays):
    x, kv, gate = arrays[7], arrays[-1], arrays[14]
    rows, width = x.shape
    keys = kv.shape[1]
    feed = gate.shape[2]
    part = width // shards
    own_rows = part // 2
    kv_width = 2 * HK * HD
    sizes = (shards, line, keys, rows, width, feed)
    dma = pltpu.SemaphoreType.DMA
    v = pltpu.VMEM
    vm = pl.BlockSpec(memory_space=pltpu.VMEM)
    hbm = pl.BlockSpec(memory_space=pltpu.HBM)
    half = width // 2
    shape = jax.ShapeDtypeStruct

    def boxes(cols):
        return [
            v((shards, own_rows, cols), BF),
            v((shards - 1, own_rows, cols), BF),
            v((own_rows, cols), BF),
            v((own_rows, cols), BF),
        ]

    scratch = [
        v((width, width), BF),
        v((rows, width), F32),
        v((rows, width), F32),
        v((2 * HK, line, 128, 128), BF),
        v((2, 2, 4, HK, 128, 128) if line == 4 else (2, line - 1, HK, 128, 128), BF),
        *[v((2, half, feed), BF) for _ in range(4)],
        *[v((feed, half), BF) for _ in range(4)],
        *boxes(width),
        *boxes(width),
        *boxes(kv_width),
        v((8, width), F32),
        v((8, width), F32),
        v((shards - 1, 8, width), F32),
        v((8, width), F32),
        v((8, width), F32),
        v((2, own_rows, HK * HD), BF),
        v((8, part), F32),
        dma((max(6, shards),)),
        dma((2,)),
        dma((2,)),
        dma((6,)),
        *[dma((24,)) for _ in range(7)],
        dma((4,)),
        dma((2, 2 * line)),
        dma((2, 2 * line)),
        dma((8,)),
        dma((4, shards - 1)),
        dma((4, shards - 1)),
        *[dma((9,)) for _ in range(7)],
        *[dma((shards - 1,)) for _ in range(4)],
        dma((9,)),
    ]
    return pl.pallas_call(
        lambda *refs: backward_kernel(sizes, *refs),
        out_shape=(
            shape((width, feed), BF),
            shape((width, feed), BF),
            shape((feed, width), BF),
            shape((part, width), BF),
            shape((part, width), BF),
            shape((part, HK * HD), BF),
            shape((part, HK * HD), BF),
            shape((8, part), F32),
            shape((rows, width), BF),
            shape((rows, width), BF),
            shape((shards - 1, rows, width), BF),
            shape((shards - 1, rows, width), BF),
        ),
        in_specs=[vm] * 3 + [hbm] * 18,
        out_specs=tuple([hbm] * 12),
        scratch_shapes=scratch,
        compiler_params=pltpu.CompilerParams(
            collective_id=3, has_side_effects=True, vmem_limit_bytes=VMEM_LIMIT
        ),
        name="backward",
    )(*arrays)


def per_device(
    tokens,
    cotangent,
    positions,
    lengths,
    attn_gain,
    w_query,
    w_key,
    w_value,
    w_out,
    mlp_gain,
    w_gate,
    w_up,
    w_down,
):
    seqs, stretch, width = tokens.shape
    shards, line = lax.axis_size("shard"), lax.axis_size("line")
    rows = seqs * stretch
    frequency = ROPE_BASE ** (-np.arange(HD // 2, dtype=np.float32) * 2.0 / HD)
    frequency = np.tile(frequency, 4)[None].astype(np.float32)
    x = tokens.reshape(rows, width)
    (
        gains,
        cos_wide,
        sin_wide,
        wq_all,
        wkv_all,
        out_all,
        packed_kv,
        soft,
        grad_all,
        attn,
        attn_t,
        norm_t,
        packed_q,
        middle,
        parts,
        back,
        norm_all_t,
        inner_t,
        grad_gate,
        grad_up,
    ) = front_call(
        shards,
        line,
        positions,
        lengths,
        frequency,
        jnp.stack([attn_gain, mlp_gain]),
        w_key,
        w_value,
        x,
        cotangent.reshape(rows, width),
        w_query,
        w_out,
        w_gate,
        w_up,
        w_down,
    )
    (
        sum_gate,
        sum_up,
        sum_down,
        sum_out,
        sum_query,
        sum_key,
        sum_value,
        sum_gain,
        grad_input,
        result,
        _,
        _,
    ) = backward_call(
        shards,
        line,
        gains,
        cos_wide,
        sin_wide,
        attn,
        attn_t,
        packed_q,
        norm_t,
        x,
        middle,
        parts,
        back,
        norm_all_t,
        grad_all,
        inner_t,
        grad_gate,
        grad_up,
        out_all,
        wq_all,
        wkv_all,
        soft,
        packed_kv.reshape(seqs * HK, -1, 128),
    )
    arrays = [sum_gate, sum_up, sum_down, sum_query, sum_out, sum_key, sum_value]
    arrays = widen_call(arrays + [grad_input, result], [F32] * 7 + [BF] * 2)
    sum_gate, sum_up, sum_down, sum_query, sum_out, sum_key, sum_value = arrays[:7]
    grad_input, result = arrays[7:]
    return (
        result.reshape(seqs, stretch, width),
        grad_input.reshape(seqs, stretch, width),
        sum_gain[0],
        sum_query,
        sum_key,
        sum_value,
        sum_out,
        sum_gain[1],
        sum_gate,
        sum_up,
        sum_down,
    )


def solution(mesh):
    shards, ctx = mesh.devices.shape
    inner = Mesh(mesh.devices.reshape(shards, ctx // 2, 2), ("shard", "line", "core"))
    where = ("line", "core")
    return jax.shard_map(
        per_device,
        mesh=inner,
        in_specs=(
            P("shard", where, None),
            P("shard", where, None),
            P("shard", None),
            P("shard"),
            P("shard"),
            P("shard", None),
            P("shard", None),
            P("shard", None),
            P("shard", None),
            P("shard"),
            P(None, "shard"),
            P(None, "shard"),
            P("shard", None),
        ),
        out_specs=(
            P("shard", where, None),
            P("shard", where, None),
            P("shard"),
            P("shard", None),
            P("shard", None),
            P("shard", None),
            P("shard", None),
            P("shard"),
            P(None, "shard"),
            P(None, "shard"),
            P("shard", None),
        ),
        check_vma=False,
    )
```

```python
import math

import jax
import jax.numpy as jnp
import numpy as np
from jax import lax
from jax.experimental import pallas as pl
from jax.experimental.pallas import tpu as pltpu
from jax.sharding import Mesh
from jax.sharding import PartitionSpec as P

HQ = 20
HK = 5
HD = 64
GROUP = HQ // HK
EPSILON = 1e-05
NEGATIVE = -1e30
ROPE_BASE = 10000.0
BF = jnp.bfloat16
F32 = jnp.float32
BY_MESH = pl.DeviceIdType.MESH
VMEM_LIMIT = 67043328


def nn(a, b):
    return lax.dot_general(a, b, (((1,), (0,)), ((), ())), preferred_element_type=F32)


def nt(a, b):
    return lax.dot_general(a, b, (((1,), (1,)), ((), ())), preferred_element_type=F32)


def tn(a, b):
    return lax.dot_general(a, b, (((0,), (0,)), ((), ())), preferred_element_type=F32)


def lanes_of(rows):
    return lax.broadcasted_iota(jnp.int32, (rows, 128), 1)


def swap_halves(block, lane):
    left = pltpu.roll(block, 96, 1)
    right = pltpu.roll(block, 32, 1)
    return jnp.where(lane % 64 < 32, left, right)


def peer_of(s_id, shards, k, back):
    if shards == 4:
        if isinstance(k, int):
            return [s_id, s_id + 1 - 2 * (s_id % 2), (s_id + 2) % 4, 3 - s_id][k]
        return jnp.where(
            k == 0,
            s_id,
            jnp.where(
                k == 1, s_id + 1 - 2 * (s_id % 2), jnp.where(k == 2, (s_id + 2) % 4, 3 - s_id)
            ),
        )
    return (s_id + (shards - k if back else k)) % shards


class Spread:
    def __init__(self, env, block, source, sems, shared):
        self.env, self.block, self.source, self.shared = env, block, source, shared
        self.send, self.recv, self.sib_send, self.sib_recv = sems
        self.relay = env.shards == 4

    def copy(self, k):
        env = self.env
        return env.remote(
            self.source,
            self.block(env.s_id, env.c_id, 0, 2),
            self.send.at[k],
            self.recv.at[k],
            env.peer(k),
        )

    def passing(self, k):
        env = self.env
        piece = self.block(env.origin(k), env.c_id, k - 1, 1)
        return env.remote(
            piece, piece, self.send.at[2 + k], self.recv.at[2 + k], env.peer(3 - k)
        )

    def direct(self):
        return range(1, 3 if self.relay else self.env.shards)

    def start(self):
        for k in self.direct():
            self.copy(k).start()

    def sib_copy(self, k):
        piece = self.block(self.env.origin(k), self.env.c_id, 0, 2)
        return self.env.remote(
            piece, piece, self.sib_send.at[k], self.sib_recv.at[k], self.env.sibling
        )

    def forward(self):
        for k in self.direct():
            self.copy(k).wait_recv()
            if self.relay:
                self.passing(k).start()
            if self.shared:
                self.sib_copy(k).start()

    def collect(self):
        if self.relay:
            for k in (1, 2):
                self.passing(k).wait_recv()
            if self.shared:
                self.sib_copy(3).start()

    def finish(self):
        if self.shared:
            for k in range(1, self.env.shards):
                self.sib_copy(k).wait_recv()

    def settle(self):
        for k in self.direct():
            self.copy(k).wait_send()
            if self.relay:
                self.passing(k).wait_send()
        if self.shared:
            for k in range(1, self.env.shards):
                self.sib_copy(k).wait_send()


class Env:
    def __init__(self, shards, line):
        self.shards, self.line = shards, line
        self.s_id = lax.axis_index("shard")
        self.l_id = lax.axis_index("line")
        self.c_id = lax.axis_index("core")
        self.sibling = (self.s_id, self.l_id, 1 - self.c_id)

    def remote(self, src, dst, send, recv, to):
        return pltpu.make_async_remote_copy(
            src, dst, send, recv, device_id=to, device_id_type=BY_MESH
        )

    def peer(self, k):
        return (peer_of(self.s_id, self.shards, k, False), self.l_id, self.c_id)

    def origin(self, k):
        return peer_of(self.s_id, self.shards, k, True)

    def mate(self, k):
        return (self.s_id, lax.rem(self.l_id + k, self.line), self.c_id)

    def barrier(self, others):
        barrier = pltpu.get_barrier_semaphore()
        for other in others:
            pl.semaphore_signal(barrier, inc=1, device_id=other, device_id_type=BY_MESH)
        pl.semaphore_wait(barrier, len(others))


def front_kernel(
    sizes,
    positions_ref,
    lengths_ref,
    freq_ref,
    gain_one_ref,
    gain_two_ref,
    wk_ref,
    wv_ref,
    x_hbm,
    g_hbm,
    wq_ref,
    wo_ref,
    wg_hbm,
    wu_hbm,
    wd_hbm,
    out_gains,
    cos_ref,
    sin_ref,
    out_wq,
    out_wkv,
    out_wo,
    out_kv,
    out_pt,
    out_g,
    keep_attn,
    keep_attn_t,
    keep_n1_t,
    keep_qp,
    keep_mid,
    out_inner,
    out_back,
    out_n2_t,
    out_inner_t,
    out_dgate,
    out_dup,
    wq_all,
    wkv_all,
    wo_all,
    kv_all,
    n2_all,
    g_all,
    wg,
    wu,
    wd,
    out_attn,
    out_attn_t,
    out_n1_t,
    out_qp,
    out_mid,
    norm,
    x_ref,
    bias_ref,
    pt_stage,
    gains_ref,
    gain_zone,
    gain_send,
    gain_recv,
    wq_s,
    wq_r,
    wq_ss,
    wq_sr,
    wkv_s,
    wkv_r,
    wkv_ss,
    wkv_sr,
    wo_s,
    wo_r,
    wo_ss,
    wo_sr,
    g_s,
    g_r,
    n2_send,
    n2_recv,
    kv_send,
    kv_recv,
    kv_sib_send,
    kv_sib_recv,
    pt_sem,
    in_sem,
    load_sem,
    keep_sem,
    part_sem,
    back_sem,
    out_sem,
):
    shards, line, keys, rows, width, feed = sizes
    env = Env(shards, line)
    s_id, l_id, c_id = env.s_id, env.l_id, env.c_id
    part = width // shards
    hp = part // 2
    quarter = hp // 2
    blocks = keys // 1024
    load_g = pltpu.make_async_copy(g_hbm, g_all.at[s_id], in_sem.at[0])
    load_g.start()
    loads = [
        pltpu.make_async_copy(src, dst, load_sem.at[i])
        for i, (src, dst) in enumerate(((wg_hbm, wg), (wu_hbm, wu), (wd_hbm, wd)))
    ]
    for head in range(HK):
        both = jnp.concatenate(
            [ref[:, head * HD : head * HD + HD].astype(F32) for ref in (wk_ref, wv_ref)], 1
        )
        wkv_all[pl.ds(pl.multiple_of(s_id * part, 16), part), head * 128 : head * 128 + 128] = (
            both.astype(BF)
        )
    gains_ref[0:1, :] = gain_one_ref[...].astype(F32).reshape(1, part)
    gains_ref[1:2, :] = gain_two_ref[...].astype(F32).reshape(1, part)
    gains_ref[2:8, :] = jnp.zeros((6, part), F32)
    env.barrier(
        [env.sibling]
        + [env.peer(k) for k in range(1, shards)]
        + [env.mate(k) for k in range(1, line)]
    )

    def tokens_of(ref):
        def block(s, core, first, count):
            return ref.at[s, pl.ds(first * (rows // 2), count * (rows // 2))]

        return block

    grad_gather = Spread(env, tokens_of(g_all), g_all.at[s_id], (g_s, g_r, None, None), False)
    n2_gather = Spread(
        env, tokens_of(n2_all), n2_all.at[s_id], (n2_send, n2_recv, None, None), False
    )

    def rows_of(ref):
        def block(s, core, first, count):
            start = s * part + core * hp + first * quarter
            return ref.at[pl.ds(pl.multiple_of(start, 16), count * quarter)]

        return block


    mine = pl.ds(pl.multiple_of(c_id * hp, 16), hp)
    own = pl.ds(pl.multiple_of(s_id * part, 16), part)
    kv_mine = pl.ds(pl.multiple_of(s_id * part + c_id * hp, 16), hp)
    kv_gather = Spread(
        env, rows_of(wkv_all), wkv_all.at[kv_mine], (wkv_s, wkv_r, wkv_ss, wkv_sr), True
    )
    q_gather = Spread(env, rows_of(wq_all), wq_ref.at[mine], (wq_s, wq_r, wq_ss, wq_sr), True)
    o_gather = Spread(env, rows_of(wo_all), wo_ref.at[mine], (wo_s, wo_r, wo_ss, wo_sr), True)
    outs = [
        pltpu.make_async_copy(src, dst, keep_sem.at[i])
        for i, (src, dst) in enumerate(
            (
                (wkv_all, out_wkv),
                (wq_all, out_wq),
                (kv_all, out_kv),
                (wo_all, out_wo),
                (out_attn, keep_attn),
                (out_attn_t, keep_attn_t),
                (out_n1_t, keep_n1_t),
                (out_qp, keep_qp),
                (out_mid, keep_mid),
            )
        )
    ]

    def attention_part():
        load_x = pltpu.make_async_copy(x_hbm, x_ref, in_sem.at[3])
        load_x.start()
        def gain_copy(k):
            return env.remote(
                gains_ref, gain_zone.at[s_id], gain_send.at[k], gain_recv.at[k], env.peer(k)
            )

        for k in range(1, shards):
            gain_copy(k).start()
        kv_gather.start()
        locals_ = [
            pltpu.make_async_copy(wq_ref, wq_all.at[own], in_sem.at[1]),
            pltpu.make_async_copy(wo_ref, wo_all.at[own], in_sem.at[2]),
        ]
        for copy in locals_:
            copy.start()
        gain_zone[s_id] = gains_ref[...]
        lane = lanes_of(128)
        place = pl.ds(pl.multiple_of((l_id * 2 + c_id) * 128, 128), 128)
        spots = positions_ref[:, place].astype(F32)
        good = [
            jnp.where(positions_ref[seq : seq + 1, place] < lengths_ref[seq], 1.0, 0.0).astype(F32)
            for seq in range(2)
        ]
        info = jnp.transpose(jnp.concatenate([spots] + good + [jnp.zeros((4, 128), F32)], 0))
        for seq in range(2):
            angle = info[:, seq : seq + 1] * freq_ref[...]
            cos_ref[seq * 128 : seq * 128 + 128, :] = jnp.cos(angle)
            sine = jnp.sin(angle)
            sin_ref[seq * 128 : seq * 128 + 128, :] = jnp.where(lane % 64 < 32, -sine, sine)
        load_x.wait()
        hidden = x_ref[...].astype(F32)
        scale = lax.rsqrt(jnp.mean(hidden * hidden, -1, keepdims=True) + EPSILON)
        for k in range(1, shards):
            gain_copy(k).wait()
        out_gains[...] = jnp.concatenate([gain_zone[s] for s in range(shards)], 1)
        norm[...] = (hidden * scale * out_gains[0:1, :]).astype(BF)
        kv_gather.forward()
        q_gather.start()
        for copy in locals_:
            copy.wait()
        kv_gather.collect()
        kv_gather.finish()

        spot = l_id * 2 + c_id

        def make_kv(head, carry):
            block = nn(norm[...], wkv_all[:, pl.ds(pl.multiple_of(head * 128, 128), 128)])
            for seq in range(2):
                piece = block[seq * 128 : seq * 128 + 128]
                cos = jnp.where(lane < 64, cos_ref[pl.ds(seq * 128, 128), :], 1.0)
                sin = jnp.where(lane < 64, sin_ref[pl.ds(seq * 128, 128), :], 0.0)
                kv_all[seq * HK + head, spot] = (piece * cos + swap_halves(piece, lane) * sin).astype(
                    BF
                )
            return carry

        lax.fori_loop(0, HK, make_kv, 0)

        def kv_slice(seq, l, c):
            return kv_all.at[pl.ds(seq * HK, HK), l * 2 + c]

        def kv_move(seq, way, src):
            piece = kv_slice(seq, src, c_id)
            to = (s_id, lax.rem(l_id + (1 if way == 0 else line - 1), line), c_id)
            return env.remote(
                piece, piece, kv_send.at[seq, way * line + src], kv_recv.at[seq, src], to
            )

        def kv_sib(seq, src):
            piece = kv_slice(seq, src, c_id)
            return env.remote(
                piece, piece, kv_sib_send.at[seq, src], kv_sib_recv.at[seq, src], env.sibling
            )

        def kv_onward(seq, way, src):
            @pl.when((l_id < line - 1) if way == 0 else (l_id > 0))
            def _():
                kv_move(seq, way, src).start()

        def kv_start(seq):
            for way in range(2):
                kv_onward(seq, way, l_id)
            kv_sib(seq, l_id).start()

        def kv_step(seq, far):
            for way in range(2):
                src = l_id - far if way == 0 else l_id + far

                @pl.when((src >= 0) & (src < line))
                def _():
                    kv_move(seq, way, src).wait_recv()
                    kv_onward(seq, way, src)
                    kv_sib(seq, src).start()

        def kv_finish(seq):
            for src in range(line):
                kv_sib(seq, src).wait()

        def kv_settle(seq):
            for src in range(line):

                @pl.when((l_id < line - 1) & (src <= l_id))
                def _():
                    kv_move(seq, 0, src).wait_send()

                @pl.when((l_id > 0) & (src >= l_id))
                def _():
                    kv_move(seq, 1, src).wait_send()

        kv_start(0)
        for load in loads:
            load.start()
        load_g.wait()
        for seq in range(2):
            rows_ = pl.ds(seq * 128, 128)
            g_all[s_id, rows_, :] = (
                g_all[s_id, rows_, :].astype(F32) * info[:, 2 + seq : 3 + seq]
            ).astype(BF)
            for group in range(keys // 1024):
                some = jnp.concatenate(
                    [
                        positions_ref[seq : seq + 1, (group * 8 + t) * 128 : (group * 8 + t + 1) * 128]
                        for t in range(8)
                    ],
                    0,
                )
                some = jnp.where(some < lengths_ref[seq], some, 1 << 24)
                key_at = jnp.transpose(some.astype(F32))
                for t in range(8):
                    first = (group * 8 + t) * 128
                    bias_ref[seq, first : first + 128, :] = jnp.where(
                        key_at[:, t : t + 1] <= spots[seq : seq + 1, :], 0.0, NEGATIVE
                    )
        for tile in range(width // 128):
            piece = norm[:, tile * 128 : tile * 128 + 128].astype(F32)
            out_n1_t[tile * 128 : tile * 128 + 128, :] = jnp.transpose(piece).astype(BF)
        q_gather.forward()
        o_gather.start()
        kv_step(0, 1)
        if line == 2:
            kv_start(1)
        else:
            kv_step(0, 2)
            kv_start(1)
        q_gather.collect()
        q_gather.finish()

        def make_q(head, carry):
            block = nn(norm[...], wq_all[:, pl.ds(pl.multiple_of(head * 256, 256), 256)])
            for seq in range(2):
                cos = cos_ref[pl.ds(seq * 128, 128), :]
                sin = sin_ref[pl.ds(seq * 128, 128), :]
                for two in range(2):
                    piece = block[seq * 128 : seq * 128 + 128, two * 128 : two * 128 + 128]
                    piece = piece * cos + swap_halves(piece, lane) * sin
                    piece = piece.astype(BF).astype(F32) * (1.0 / math.sqrt(HD))
                    pair = seq * HK + head
                    out_qp[pair, pl.ds(two * 256, 128), :] = jnp.where(lane < 64, piece, 0.0).astype(
                        BF
                    )
                    out_qp[pair, pl.ds(two * 256 + 128, 128), :] = jnp.where(
                        lane < 64, pltpu.roll(piece, 64, 1), 0.0
                    ).astype(BF)
            return carry

        lax.fori_loop(0, HK, make_q, 0)

        def pt_copy(pair, block, slot):
            span = pl.ds(pl.multiple_of(block * 1024, 1024), 1024)
            return pltpu.make_async_copy(pt_stage.at[slot], out_pt.at[pair, span], pt_sem.at[slot])

        def keys_of(pair, block):
            if blocks == 1:
                return kv_all[pair].reshape(1024, 128)
            return kv_all[pair, pl.ds(block * 8, 8)].reshape(1024, 128)

        def scores(pair, block):
            span = pl.ds(pl.multiple_of(block * 1024, 1024), 1024)
            bias = bias_ref[pair // HK, span, :]
            return nt(keys_of(pair, block), out_qp[pair]) + jnp.concatenate([bias] * GROUP, 1)

        def attend(pair, carry):
            if blocks == 1:
                slot = lax.rem(pair, 2)

                @pl.when(pair >= 2)
                def _():
                    pt_copy(pair - 2, 0, slot).wait()

                value = scores(pair, 0)
                top = jnp.max(value, 0, keepdims=True)
                weight = jnp.exp(value - top)
                inverse = 1.0 / jnp.sum(weight, 0, keepdims=True)
                soft = (weight * inverse).astype(BF)
                pt_stage[slot] = soft
                pt_copy(pair, 0, slot).start()
                mixed = tn(keys_of(pair, 0), soft)[HD:]
            else:

                def first(block, state):
                    top, total = state
                    value = scores(pair, block)
                    new = jnp.maximum(top, jnp.max(value, 0, keepdims=True))
                    total = total * jnp.exp(top - new) + jnp.sum(
                        jnp.exp(value - new), 0, keepdims=True
                    )
                    return new, total

                top, total = lax.fori_loop(
                    0,
                    blocks,
                    first,
                    (jnp.full((1, 512), NEGATIVE, F32), jnp.zeros((1, 512), F32)),
                )
                inverse = 1.0 / total

                def second(block, mixed):
                    pt_stage[0] = (jnp.exp(scores(pair, block) - top) * inverse).astype(BF)
                    copy = pt_copy(pair, block, 0)
                    copy.start()
                    mixed = mixed + tn(keys_of(pair, block), pt_stage[0])[HD:]
                    copy.wait()
                    return mixed

                mixed = lax.fori_loop(0, blocks, second, jnp.zeros((HD, 512), F32))
            seq, head = pair // HK, pair % HK
            for two in range(2):
                both = jnp.concatenate(
                    [
                        mixed[:, two * 256 : two * 256 + 128],
                        mixed[:, two * 256 + 128 : two * 256 + 256],
                    ],
                    0,
                )
                tokens_ = pl.ds(pl.multiple_of(seq * 128, 128), 128)
                cols = pl.ds(pl.multiple_of(head * 256 + two * 128, 128), 128)
                out_attn_t[cols, tokens_] = both.astype(BF)
                out_attn[tokens_, cols] = jnp.transpose(both).astype(BF)
            return carry

        for far in range(3, line):
            kv_step(0, far)
        o_gather.forward()
        grad_gather.start()
        kv_step(1, 1)
        kv_finish(0)
        lax.fori_loop(0, 2, attend, 0)
        if line > 2:
            kv_step(1, 2)
        lax.fori_loop(2, HK, attend, 0)
        for far in range(3, line):
            kv_step(1, far)
        o_gather.collect()
        kv_finish(1)
        lax.fori_loop(HK, 2 * HK, attend, 0)
        o_gather.finish()

        def project(tile, carry):
            cols = pl.ds(pl.multiple_of(tile * 256, 256), 256)
            out_mid[:, cols] = x_ref[:, cols].astype(F32) + nn(out_attn[...], wo_all[:, cols])
            return carry

        lax.fori_loop(0, width // 256, project, 0)
        middle = out_mid[...]
        scale_two = lax.rsqrt(jnp.mean(middle * middle, -1, keepdims=True) + EPSILON)
        n2_all[s_id] = (middle * scale_two * out_gains[1:2, :]).astype(BF)
        n2_gather.start()
        grad_gather.forward()
        for copy in outs:
            copy.start()
        if blocks == 1:
            pt_copy(2 * HK - 2, 0, 0).wait()
            pt_copy(2 * HK - 1, 0, 1).wait()

        def finish():
            for gather in (kv_gather, q_gather, o_gather):
                gather.settle()
            kv_settle(0)
            kv_settle(1)
            for copy in outs:
                copy.wait()

        finishing.append(finish)

    v = pltpu.VMEM
    finishing = []
    attention_part()

    def feed_part(inner, dgate, dup, stage, grads, n2_t, inner_t):
        def back_copy(k, slot):
            return pltpu.make_async_copy(
                stage.at[slot], out_back.at[peer_of(s_id, shards, k, True)], back_sem.at[slot]
            )

        def outs(k):
            source = peer_of(s_id, shards, k, True)
            cols = pl.ds(pl.multiple_of(source * rows, 128), rows)
            return [
                pltpu.make_async_copy(n2_t.at[k], out_n2_t.at[:, cols], out_sem.at[k, 0]),
                pltpu.make_async_copy(inner_t.at[k], out_inner_t.at[:, cols], out_sem.at[k, 1]),
                pltpu.make_async_copy(dgate.at[source], out_dgate.at[source], out_sem.at[k, 2]),
                pltpu.make_async_copy(dup.at[source], out_dup.at[source], out_sem.at[k, 3]),
                pltpu.make_async_copy(g_all.at[source], out_g.at[source], out_sem.at[k, 4]),
                pltpu.make_async_copy(inner.at[source], out_inner.at[source], out_sem.at[k, 5]),
            ]

        def block(k, carry):
            source = peer_of(s_id, shards, k, True)
            slot = lax.rem(k, 2)
            if n2_gather.relay:

                @pl.when(k == 0)
                def _():
                    loads[2].wait()

                @pl.when(k == 3)
                def _():
                    grad_gather.collect()

                def grad_of(other, carry):
                    grads[other] = nt(g_all[peer_of(s_id, shards, other, True)], wd[...])
                    return carry

                first = jnp.where(k == 0, 0, jnp.where(k == 1, 1, 3))
                last = jnp.where(k == 0, 1, jnp.where(k == 3, 4, 3))
                lax.fori_loop(first, last, grad_of, 0)

                @pl.when(k == 1)
                def _():
                    n2_gather.forward()

                @pl.when(k == 3)
                def _():
                    n2_gather.collect()

            else:

                @pl.when(k == 0)
                def _():
                    loads[2].wait()

                @pl.when(k > 0)
                def _():
                    n2_gather.copy(k).wait_recv()

                grads[0] = nt(g_all[source], wd[...])

            normed = n2_all[source]
            n2_t[k] = jnp.transpose(normed)
            copies = outs(k)
            copies[0].start()
            copies[4].start()
            gate, upper = nn(normed, wg[...]), nn(normed, wu[...])
            grad_inner = grads[k if n2_gather.relay else 0]
            sig = 1.0 / (1.0 + jnp.exp(-gate))
            act = gate * sig
            inner[source] = (act * upper).astype(BF)
            dgate[source] = (grad_inner * upper * sig * (1.0 + gate * (1.0 - sig))).astype(BF)
            dup[source] = (grad_inner * act).astype(BF)
            for index in (2, 3, 5):
                copies[index].start()
            inner_t[k] = jnp.transpose(inner[source])
            copies[1].start()

            @pl.when(k >= 2)
            def _():
                back_copy(k - 2, slot).wait()

            stage[slot] = (nt(dgate[source], wg[...]) + nt(dup[source], wu[...])).astype(BF)
            back_copy(k, slot).start()
            return carry

        loads[0].wait()
        loads[1].wait()
        lax.fori_loop(0, shards, block, 0)
        for k in range(shards):
            for copy in outs(k):
                copy.wait()
        n2_gather.settle()
        grad_gather.settle()
        for last in (2, 1):
            back_copy(shards - last, (shards - last) % 2).wait()

    pl.run_scoped(
        feed_part,
        v((shards, rows, feed), BF),
        v((shards, rows, feed), BF),
        v((shards, rows, feed), BF),
        v((2, rows, width), BF),
        v((shards if shards == 4 else 1, rows, feed), F32),
        v((shards, width, rows), BF),
        v((shards, feed, rows), BF),
    )
    finishing[0]()


def front_call(shards, line, *arrays):
    positions, x, w_gate = arrays[0], arrays[7], arrays[11]
    rows, width = x.shape
    keys = positions.shape[1]
    feed = w_gate.shape[1]
    kv_width = 2 * HK * HD
    dma = pltpu.SemaphoreType.DMA
    v = pltpu.VMEM
    vm = pl.BlockSpec(memory_space=pltpu.VMEM)
    sm = pl.BlockSpec(memory_space=pltpu.SMEM)
    hbm = pl.BlockSpec(memory_space=pltpu.HBM)
    part = width // shards
    shape = jax.ShapeDtypeStruct
    hops = max(5, shards)
    return pl.pallas_call(
        lambda *refs: front_kernel((shards, line, keys, rows, width, feed), *refs),
        out_shape=(
            shape((8, width), F32),
            shape((rows, 128), F32),
            shape((rows, 128), F32),
            shape((width, width), BF),
            shape((width, kv_width), BF),
            shape((width, width), BF),
            shape((2 * HK, 2 * line, 128, 128), BF),
            shape((2 * HK, keys, 512), BF),
            shape((shards, rows, width), BF),
            shape((rows, width), BF),
            shape((width, rows), BF),
            shape((width, rows), BF),
            shape((2 * HK, 512, 128), BF),
            shape((rows, width), F32),
            shape((shards, rows, feed), BF),
            shape((shards, rows, width), BF),
            shape((width, shards * rows), BF),
            shape((feed, shards * rows), BF),
            shape((shards, rows, feed), BF),
            shape((shards, rows, feed), BF),
        ),
        in_specs=[vm, sm, vm, vm, vm, vm, vm] + [hbm] * 7,
        out_specs=(*[vm] * 3, *[hbm] * 17),
        scratch_shapes=[
            v((width, width), BF),
            v((width, kv_width), BF),
            v((width, width), BF),
            v((2 * HK, 2 * line, 128, 128), BF),
            v((shards, rows, width), BF),
            v((shards, rows, width), BF),
            v((width, feed), BF),
            v((width, feed), BF),
            v((feed, width), BF),
            v((rows, width), BF),
            v((width, rows), BF),
            v((width, rows), BF),
            v((2 * HK, 512, 128), BF),
            v((rows, width), F32),
            v((rows, width), BF),
            v((rows, width), BF),
            v((2, keys, 128), F32),
            v((2, 1024, 512), BF),
            v((8, part), F32),
            v((shards, 8, part), F32),
            dma((shards,)),
            dma((shards,)),
            *[dma((hops,)) for _ in range(16)],
            dma((2, 2 * line)),
            dma((2, line)),
            dma((2, line)),
            dma((2, line)),
            dma((2,)),
            dma((4,)),
            dma((3,)),
            dma((9,)),
            dma((2,)),
            dma((2,)),
            dma((shards, 6)),
        ],
        compiler_params=pltpu.CompilerParams(
            collective_id=1, has_side_effects=True, vmem_limit_bytes=VMEM_LIMIT
        ),
        name="front",
    )(*arrays)


def widen_kernel(count, gain_ref, *refs):
    src, dst = refs[:count], refs[count : 2 * count]
    out_one, out_two = refs[2 * count : 2 * count + 2]
    refs = refs[2 * count + 2 :]
    narrow, wide = refs[:count], refs[count : 2 * count]
    load_sem, store_sem = refs[2 * count :]
    out_one[...] = gain_ref[0:1, :].reshape(out_one.shape)
    out_two[...] = gain_ref[1:2, :].reshape(out_two.shape)
    for i in range(count):
        pltpu.make_async_copy(src[i], narrow[i], load_sem.at[i]).start()

    def piece(i, part, parts):
        rows = narrow[i].shape[0] // parts
        span = pl.ds(part * rows, rows)
        held = wide[i] if dst[i].dtype == F32 else narrow[i]
        return span, pltpu.make_async_copy(held.at[span], dst[i].at[span], store_sem.at[i])

    for i in range(count):
        pltpu.make_async_copy(src[i], narrow[i], load_sem.at[i]).wait()
        for part in range(4):
            span, copy = piece(i, part, 4)
            if dst[i].dtype == F32:
                wide[i][span, :] = narrow[i][span, :].astype(F32)
            copy.start()
    for i in range(count):
        piece(i, 0, 1)[1].wait()


def widen_call(gains, arrays, types):
    v = pltpu.VMEM
    hbm = pl.BlockSpec(memory_space=pltpu.HBM)
    vm = pl.BlockSpec(memory_space=pltpu.VMEM)
    count = len(arrays)
    return pl.pallas_call(
        lambda *refs: widen_kernel(count, *refs),
        out_shape=tuple(jax.ShapeDtypeStruct(a.shape, t) for a, t in zip(arrays, types))
        + (jax.ShapeDtypeStruct(gains.shape[1:], F32),) * 2,
        in_specs=[vm] + [hbm] * count,
        out_specs=tuple([hbm] * count) + (vm, vm),
        scratch_shapes=[
            *[v(a.shape, a.dtype) for a in arrays],
            *[v(a.shape if t == F32 else (16, 128), F32) for a, t in zip(arrays, types)],
            pltpu.SemaphoreType.DMA((count,)),
            pltpu.SemaphoreType.DMA((count,)),
        ],
        compiler_params=pltpu.CompilerParams(vmem_limit_bytes=VMEM_LIMIT),
        name="widen",
    )(gains, *arrays)


def add_rows(target, parts, rows, step):
    def body(index, carry):
        span = pl.ds(pl.multiple_of(index * step, step), step)
        total = parts[0][span, :].astype(F32)
        for part in parts[1:]:
            total = total + part[span, :].astype(F32)
        target[span, :] = total.astype(target.dtype)
        return carry

    lax.fori_loop(0, rows // step, body, 0)


def backward_kernel(
    sizes,
    gains_ref,
    cos_ref,
    sin_ref,
    attn_hbm,
    attn_t_hbm,
    qp_hbm,
    n1_t_hbm,
    x_hbm,
    mid_hbm,
    inner_hbm,
    wd_hbm,
    back_hbm,
    n2_t_hbm,
    g_hbm,
    inner_t_hbm,
    dgate_hbm,
    dup_hbm,
    wo_hbm,
    wq_hbm,
    wkv_hbm,
    pt_hbm,
    kv_hbm,
    out_gate,
    out_up,
    out_dn,
    out_wo,
    out_wq,
    out_wk,
    out_wv,
    out_gain,
    out_dx,
    out_result,
    parts_hbm,
    p_zone,
    b_zone,
    w_buf,
    gm,
    mid_ref,
    dkv_x,
    dkv_z,
    own_gu,
    got_gu_x,
    got_gu_r,
    got_gu_t,
    own_dn,
    got_dn_x,
    got_dn_r,
    got_dn_t,
    o_x,
    o_z,
    o_r,
    o_t,
    q_x,
    q_z,
    q_r,
    q_t,
    k_x,
    k_z,
    k_r,
    k_t,
    gn_own,
    gn_x,
    gn_z,
    gn_r,
    gn_t,
    k_nat,
    gn_out,
    load_sem,
    pt_sem,
    kv_sem,
    core_sem,
    up_send,
    r_recv,
    t_recv,
    down_send,
    sib_send,
    sib_recv,
    local_sem,
    dkv_core,
    dkv_send,
    dkv_recv,
    g_core,
    g_send,
    g_recv,
    a_up,
    a_r,
    a_t,
    a_down,
    a_sib_send,
    a_sib_recv,
    a_local,
    p_send,
    p_recv,
    b_send,
    b_recv,
    late_sem,
):
    shards, line, keys, rows, width, feed = sizes
    env = Env(shards, line)
    s_id, l_id, c_id = env.s_id, env.l_id, env.c_id
    sibling, remote = env.sibling, env.remote
    toward = jnp.where(l_id < line // 2, 1, -1)
    inner_to = (s_id, l_id + toward, c_id)
    has_outer = (l_id > 0) & (l_id < line - 1)
    is_mid = (l_id == line // 2 - 1) | (l_id == line // 2)
    outer_to = (s_id, jnp.where(has_outer, l_id - toward, l_id + toward), c_id)
    peers = [env.peer(k) for k in range(1, shards)]
    mates = [env.mate(k) for k in range(1, line)]
    half = width // 2
    wide_pieces = 8
    down_pieces = 8 if feed % 128 == 0 else 4
    chunks = 2 * wide_pieces + down_pieces
    turns = 12
    slab = 16
    part = width // shards
    own_rows = part // 2
    blocks = keys // 1024
    tokens = shards * rows
    hops = line == 4
    near_half = pl.ds(pl.multiple_of(c_id * half, 128), half)
    far_half = pl.ds(pl.multiple_of((1 - c_id) * half, 128), half)

    def back_copy(k):
        return remote(
            back_hbm.at[peer_of(s_id, shards, k, False)],
            b_zone.at[k - 1],
            b_send.at[k - 1],
            b_recv.at[k - 1],
            peers[k - 1],
        )

    def part_copy(k):
        return remote(
            parts_hbm.at[peer_of(s_id, shards, k, False)],
            p_zone.at[k - 1],
            p_send.at[0],
            p_recv.at[0],
            peers[k - 1],
        )

    def local(src, dst, sem):
        return pltpu.make_async_copy(src, dst, sem)

    def views(index, where):
        if where != "dn":
            rows_ = half // wide_pieces
            array, piece = (0 if where == "gate" else 1), index % wide_pieces
            array_of = out_gate if where == "gate" else out_up
            span = pl.ds(pl.multiple_of(piece * rows_, 16), rows_)
            bufs = [ref.at[array, span] for ref in (own_gu, got_gu_x, got_gu_r, got_gu_t)]

            def out(core):
                start = core * half + piece * rows_
                return array_of.at[pl.ds(pl.multiple_of(start, 16), rows_)]

            return rows_, bufs, out, array
        rows_ = feed // down_pieces
        span = pl.ds(pl.multiple_of((index - 2 * wide_pieces) * rows_, 16), rows_)
        bufs = [ref.at[span] for ref in (own_dn, got_dn_x, got_dn_r, got_dn_t)]

        def out(core):
            return out_dn.at[span, pl.ds(pl.multiple_of(core * half, 128), half)]

        return rows_, bufs, out, 2

    def split(action):
        def run(index):
            if isinstance(index, int):
                if 0 <= index < chunks:
                    action(index, ("gate", "up", "dn")[min(2, index // wide_pieces)])
                return
            for number, where in enumerate(("gate", "up", "dn")):

                @pl.when(jnp.minimum(index // wide_pieces, 2) == number)
                def _():
                    action(index, where)

        return run

    def up_end(index, where):
        count, (mine, extra, came, total), _, array = views(index, where)
        add_rows(mine, [mine, extra], count, slab)
        send_up(index, mine, came, total, array)

    def up_inner(index, where):
        count, (mine, extra, came, total), _, array = views(index, where)
        remote(mine, came, up_send.at[array], r_recv.at[index], inner_to).wait_recv()
        add_rows(mine, [mine, extra, came], count, slab)
        send_up(index, mine, came, total, array)

    def send_up(index, mine, came, total, array):
        @pl.when(is_mid)
        def _():
            remote(mine, total, up_send.at[array], t_recv.at[index], inner_to).start()

        @pl.when(jnp.logical_not(is_mid))
        def _():
            remote(mine, came, up_send.at[array], r_recv.at[index], inner_to).start()

    def down(index, where):
        count, (mine, _, _, total), out, array = views(index, where)
        remote(mine, total, up_send.at[array], t_recv.at[index], inner_to).wait_recv()

        @pl.when(is_mid)
        def _():
            add_rows(total, [mine, total], count, slab)

        @pl.when(has_outer)
        def _():
            remote(total, total, down_send.at[array], t_recv.at[index], outer_to).start()

        remote(total, out(c_id), sib_send.at[array], sib_recv.at[array], sibling).start()
        local(total, out(c_id), local_sem.at[array]).start()

    def settle(array):
        if array < 2:
            mine, total = own_gu.at[array], got_gu_t.at[array]
            out_of = (out_gate, out_up)[array]
            outs = [
                out_of.at[pl.ds(pl.multiple_of(core * half, 16), half)]
                for core in (c_id, 1 - c_id)
            ]
        else:
            mine, total = own_dn, got_dn_t
            outs = [
                out_dn.at[:, pl.ds(pl.multiple_of(core * half, 128), half)]
                for core in (c_id, 1 - c_id)
            ]
        remote(mine, total, up_send.at[array], t_recv.at[0], inner_to).wait_send()

        @pl.when(has_outer)
        def _():
            remote(total, total, down_send.at[array], t_recv.at[0], outer_to).wait_send()

        remote(total, outs[1], sib_send.at[array], sib_recv.at[array], sibling).wait()
        local(total, outs[0], local_sem.at[array]).wait()

    up_end, up_inner, down = [split(f) for f in (up_end, up_inner, down)]

    def of_turns(first, last):
        return min(2 * first, chunks), min(2 * last, chunks)

    def run_all(action, first, last):
        if last > first:

            def body(index, carry):
                action(index)
                return carry

            lax.fori_loop(first, last, body, 0)

    def ends_up(first, last):
        @pl.when(jnp.logical_not(has_outer))
        def _():
            run_all(up_end, *of_turns(first, last))

    def ring(turn, lag=2):
        for step in (2 * turn, 2 * turn + 1):
            if step < chunks:

                @pl.when(has_outer)
                def _():
                    up_inner(step)

            if 0 <= step - 2 * lag < chunks:

                @pl.when(is_mid)
                def _():
                    down(step - 2 * lag)

    def ring_down(turn):
        @pl.when(is_mid)
        def _():
            run_all(down, *of_turns(turn, turn + 1))

    def ends_down(first, last):
        @pl.when(jnp.logical_not(is_mid))
        def _():
            run_all(down, *of_turns(first, last))

    def first_send(src, part_):
        span = pl.ds(part_ * (half // 2), half // 2)
        return remote(
            src.at[0, span],
            got_gu_x.at[0, span],
            core_sem.at[3 * part_],
            core_sem.at[6 + part_],
            sibling,
        )

    def core_send(array, src):
        dst = got_gu_x.at[array] if array < 2 else got_dn_x
        return remote(src, dst, core_sem.at[array], core_sem.at[3 + array], sibling)

    load_wo = local(wo_hbm, w_buf, late_sem.at[3])

    load_mid = local(mid_hbm, mid_ref, late_sem.at[0])

    def feed_grads(
        g_v, g_own, dgate_v, dup_v, wide_t, near_t, inner_t, far_gu, far_dn, inner_v, wd_v, stage_v
    ):
        loads = [
            local(src, dst, load_sem.at[i])
            for i, (src, dst) in enumerate(
                (
                    (n2_t_hbm.at[far_half], wide_t),
                    (dgate_hbm, dgate_v),
                    (dup_hbm, dup_v),
                    (inner_t_hbm, inner_t),
                    (g_hbm, g_v),
                )
            )
        ]
        load_near = local(n2_t_hbm.at[near_half], near_t, late_sem.at[1])
        load_own = local(g_hbm.at[s_id], g_own, late_sem.at[2])
        loads[0].start()
        loads[1].start()
        load_near.start()
        for load in loads[2:]:
            load.start()
        load_own.start()
        load_mid.start()
        load_wo.start()
        load_inner = local(inner_hbm, inner_v, late_sem.at[4])
        load_wd = local(wd_hbm, wd_v, late_sem.at[5])
        load_inner.start()
        load_wd.start()
        env.barrier([sibling] + peers + mates)
        for k in range(1, shards):
            back_copy(k).start()

        def flat(ref):
            return ref[...].reshape(tokens, ref.shape[2])

        loads[0].wait()
        loads[1].wait()
        split_at = half // 2
        for part_ in range(2):
            span = pl.ds(part_ * split_at, split_at)
            far_gu[0, span, :] = nn(wide_t[span, :], flat(dgate_v)).astype(BF)
            first_send(far_gu, part_).start()
            if part_ == 0:
                load_near.wait()
            own_gu[0, span, :] = nn(near_t[span, :], flat(dgate_v)).astype(BF)
            first_send(far_gu, part_).wait()
            ends_up(2 * part_, 2 * part_ + 2)
        loads[2].wait()
        far_gu[1] = nn(wide_t[...], flat(dup_v)).astype(BF)
        core_send(1, far_gu.at[1]).start()
        own_gu[1] = nn(near_t[...], flat(dup_v)).astype(BF)
        core_send(1, far_gu.at[1]).wait()
        ends_up(4, 8)
        loads[3].wait()
        loads[4].wait()
        far_dn[...] = nn(inner_t[...], g_v[:, :, far_half].reshape(tokens, half)).astype(BF)
        core_send(2, far_dn).start()
        own_dn[...] = nn(inner_t[...], g_v[:, :, near_half].reshape(tokens, half)).astype(BF)
        ring(0)
        core_send(2, far_dn).wait()
        load_inner.wait()
        load_wd.wait()

        def part_keep(k):
            return local(stage_v.at[k % 2], parts_hbm.at[k], late_sem.at[6 + k % 2])

        def project(k, carry):
            @pl.when(k >= 2)
            def _():
                part_keep(k - 2).wait()

            stage_v[k % 2] = nn(inner_v[k], wd_v[...]).astype(BF)
            part_keep(k).start()
            return carry

        lax.fori_loop(0, shards, project, 0)
        for k in range(shards - 2, shards):
            part_keep(k).wait()
        ring(1)
        own_back = local(back_hbm.at[s_id], g_v.at[0], load_sem.at[shards - 1])
        own_back.start()
        stage = []
        for k in range(1, shards):
            if k == shards - 1:
                ring(2)
            back_copy(k).wait()
            stage.append(local(b_zone.at[k - 1], g_v.at[k], load_sem.at[k - 1]))
            stage[-1].start()
        own_back.wait()
        total = g_v[0].astype(F32)
        for k in range(1, shards):
            stage[k - 1].wait()
            total = total + g_v[k].astype(F32)
        load_mid.wait()
        load_own.wait()
        hidden = mid_ref[...]
        scale = lax.rsqrt(jnp.mean(hidden * hidden, -1, keepdims=True) + EPSILON)
        scaled = total * gains_ref[1:2, :]
        gn_own[1:2, :] = jnp.sum(total * hidden * scale, 0, keepdims=True)
        gm[...] = (
            g_own[...].astype(F32)
            + scale * scaled
            - hidden * (scale * scale * scale) * jnp.mean(scaled * hidden, -1, keepdims=True)
        )

    v = pltpu.VMEM
    pl.run_scoped(
        feed_grads,
        v((shards, rows, width), BF),
        v((rows, width), BF),
        v((shards, rows, feed), BF),
        v((shards, rows, feed), BF),
        v((half, tokens), BF),
        v((half, tokens), BF),
        v((feed, tokens), BF),
        v((2, half, feed), BF),
        v((feed, half), BF),
        v((shards, rows, feed), BF),
        v((feed, width), BF),
        v((2, rows, width), BF),
    )

    def attention(
        wkv_buf,
        pt_buf,
        kv_buf,
        dproj,
        dop,
        delta,
        dkv,
        dq,
        dkv_own,
        g_buf,
        attn_ref,
        attn_t_ref,
        qp_ref,
        n1_t_ref,
        x_ref,
    ):
        load_wkv = local(wkv_hbm, wkv_buf, late_sem.at[0])
        load_wq = local(wq_hbm, w_buf, late_sem.at[3])
        early = [
            local(src, dst, late_sem.at[4 + i])
            for i, (src, dst) in enumerate(
                (
                    (attn_hbm, attn_ref),
                    (attn_t_hbm, attn_t_ref),
                    (qp_hbm, qp_ref),
                    (n1_t_hbm, n1_t_ref),
                    (x_hbm, x_ref),
                )
            )
        ]
        for load in early:
            load.start()
        load_wkv.start()
        total_steps = 2 * HK * blocks

        def pt_copy(step, slot):
            pair, block = step // blocks, step % blocks
            span = pl.ds(pl.multiple_of(block * 1024, 1024), 1024)
            return local(pt_hbm.at[pair, span], pt_buf.at[slot], pt_sem.at[slot])

        def kv_copy(step, slot):
            pair, block = step // blocks, step % blocks
            span = pl.ds(pl.multiple_of(block * 1024, 1024), 1024)
            return local(kv_hbm.at[pair, span], kv_buf.at[slot], kv_sem.at[slot])

        pt_copy(0, 0).start()
        kv_copy(0, 0).start()

        def core_part(grad, box, slot):
            far = pl.ds(pl.multiple_of((1 - c_id) * own_rows, 16), own_rows)
            return remote(grad.at[:, far, :], box, g_core.at[slot], g_core.at[3 + slot], sibling)

        def scatter_part(grad, box, zone, slot):
            core_part(grad, box, slot).wait()
            near = pl.ds(pl.multiple_of(c_id * own_rows, 16), own_rows)

            def body(s, carry):
                add_rows(box.at[s], [grad.at[s, near], box.at[s]], own_rows, slab)
                return carry

            lax.fori_loop(0, shards, body, 0)
            for k in range(1, shards):
                scatter_copy(box, zone, slot, k).start()

        def scatter_copy(box, zone, slot, k):
            return remote(
                box.at[peer_of(s_id, shards, k, False)],
                zone.at[k - 1],
                g_send.at[slot],
                g_recv.at[slot],
                peers[k - 1],
            )

        def gather_part(box, zone, slot):
            remote(zone, zone, g_send.at[slot], g_recv.at[slot], peers[0]).wait()
            add_rows(
                box.at[s_id],
                [box.at[s_id]] + [zone.at[k] for k in range(shards - 1)],
                own_rows,
                slab,
            )

        def line_up(mine, came, total, slot, count, group):
            @pl.when(has_outer)
            def _():
                remote(mine, came, a_up.at[group], a_r.at[slot], inner_to).wait_recv()
                add_rows(mine, [mine, came], count, slab if mine.dtype == BF else 8)

            @pl.when(is_mid)
            def _():
                remote(mine, total, a_up.at[group], a_t.at[slot], inner_to).start()

            @pl.when(jnp.logical_not(is_mid))
            def _():
                remote(mine, came, a_up.at[group], a_r.at[slot], inner_to).start()

        def line_down(mine, total, slot, count, group, ready, outs):
            remote(mine, total, a_up.at[group], a_t.at[slot], inner_to).wait_recv()

            @pl.when(is_mid)
            def _():
                add_rows(total, [mine, total], count, slab if mine.dtype == BF else 8)

            @pl.when(has_outer)
            def _():
                remote(total, total, a_down.at[group], a_t.at[slot], outer_to).start()

            if ready is not None:
                ready()
            for src, near, far, box in outs:
                if far is not None:
                    remote(src, near, a_sib_send.at[box], a_sib_recv.at[box], sibling).start()
                local(src, near, a_local.at[box]).start()

        def line_settle(mine, total, group, outs):
            remote(mine, total, a_up.at[group], a_t.at[0], inner_to).wait_send()

            @pl.when(has_outer)
            def _():
                remote(total, total, a_down.at[group], a_t.at[0], outer_to).wait_send()

            for src, near, far, box in outs:
                if far is not None:
                    remote(src, far, a_sib_send.at[box], a_sib_recv.at[box], sibling).wait()
                local(src, near, a_local.at[box]).wait()

        lane = lanes_of(128)
        dproj[...] = gm[...].astype(BF)
        load_wo.wait()
        early[0].wait()

        def spread(head, carry):
            block = nt(
                dproj[...], w_buf[pl.ds(pl.multiple_of(head * 256, 256), 256), :]
            ).astype(BF)
            for seq in range(2):
                for two in range(2):
                    piece = block[
                        seq * 128 : seq * 128 + 128, two * 128 : two * 128 + 128
                    ].astype(F32)
                    place = seq * HK + head
                    first = jnp.where(lane >= 64, pltpu.roll(piece, 64, 1), 0.0)
                    dop[place, pl.ds(two * 256, 128), :] = first.astype(BF)
                    dop[place, pl.ds(two * 256 + 128, 128), :] = jnp.where(
                        lane >= 64, piece, 0.0
                    ).astype(BF)
                    value = attn_ref[
                        pl.ds(seq * 128, 128),
                        pl.ds(pl.multiple_of(head * 256 + two * 128, 128), 128),
                    ].astype(F32)
                    product = jnp.transpose(piece * value)
                    delta[place, :, pl.ds(two * 256, 128)] = jnp.sum(
                        product[:64], 0, keepdims=True
                    )
                    delta[place, :, pl.ds(two * 256 + 128, 128)] = jnp.sum(
                        product[64:], 0, keepdims=True
                    )
            return carry

        lax.fori_loop(0, HK, spread, 0)
        load_wq.start()
        ring(3)

        def weight_grad(left, right, grad, count):
            def body(s, carry):
                grad[s] = nn(
                    left[pl.ds(pl.multiple_of(s * part, 16), part), :], right[...]
                ).astype(BF)
                return carry

            lax.fori_loop(0, count, body, 0)

        early[1].wait()
        weight_grad(attn_t_ref, dproj, g_buf, shards)
        for load in early[2:]:
            load.wait()
        core_part(g_buf, o_x, 0).start()
        cosine, sine = cos_ref, sin_ref

        def attend(step, carry):
            slot = lax.rem(step, 2)
            pair, block = step // blocks, step % blocks

            @pl.when(step + 1 < total_steps)
            def _():
                pt_copy(step + 1, 1 - slot).start()
                kv_copy(step + 1, 1 - slot).start()

            pt_copy(step, slot).wait()
            kv_copy(step, slot).wait()
            keyval = kv_buf[slot]
            soft = pt_buf[slot]
            grad_soft = nt(keyval, dop[pair])
            score = (soft.astype(F32) * (grad_soft - delta[pair])).astype(BF)
            both = (nn(score, qp_ref[pair]) + nn(soft, dop[pair])).astype(BF)
            for sub in range(8):
                dkv[pair, block * 4 + sub // 2, sub % 2] = both[sub * 128 : sub * 128 + 128]
            query = tn(keyval, score)[:64] * (1.0 / math.sqrt(HD))
            seq, head = pair // HK, pair % HK
            for two in range(2):
                piece = jnp.transpose(
                    jnp.concatenate(
                        [
                            query[:, two * 256 : two * 256 + 128],
                            query[:, two * 256 + 128 : two * 256 + 256],
                        ],
                        0,
                    )
                )
                where = (
                    pl.ds(pl.multiple_of(seq * 128, 128), 128),
                    pl.ds(pl.multiple_of(head * 256 + two * 128, 128), 128),
                )
                if blocks == 1:
                    cos = cosine[where[0], :]
                    sin = sine[where[0], :]
                    dq[where] = (piece * cos - swap_halves(piece, lane) * sin).astype(BF)
                else:
                    dq[where] = jnp.where(
                        block == 0, piece, dq[where].astype(F32) + piece
                    ).astype(dq.dtype)
            return carry

        def dkv_core_copy(seq):
            return remote(
                dkv.at[pl.ds(seq * HK, HK), :, 1 - c_id],
                dkv_x.at[pl.ds(seq * HK, HK)],
                dkv_core.at[seq],
                dkv_core.at[2 + seq],
                sibling,
            )

        def dkv_copy(seq, k):
            return remote(
                dkv_x.at[pl.ds(seq * HK, HK), lax.rem(l_id + k, line)],
                dkv_z.at[seq, k - 1],
                dkv_send.at[seq, k - 1],
                dkv_recv.at[seq, k - 1],
                mates[k - 1],
            )

        def dkv_scatter(seq):
            dkv_core_copy(seq).wait()

            def body(index, carry):
                head, place = seq * HK + index // line, index % line
                dkv_x[head, place] = (
                    dkv_x[head, place].astype(F32) + dkv[head, place, c_id].astype(F32)
                ).astype(BF)
                return carry

            lax.fori_loop(0, HK * line, body, 0)
            if not hops:
                for k in range(1, line):
                    dkv_copy(seq, k).start()
                return

            @pl.when(l_id == 0)
            def _():
                for dest in range(line - 1, 0, -1):
                    dkv_hop(seq, 0, dest).start()

            @pl.when(l_id == line - 1)
            def _():
                for dest in range(line - 1):
                    dkv_hop(seq, 1, dest).start()

        def dkv_hop(seq, way, dest):
            to = (s_id, lax.rem(l_id + (1 if way == 0 else line - 1), line), c_id)
            return remote(
                dkv_x.at[pl.ds(seq * HK, HK), dest],
                dkv_z.at[seq, way, dest],
                dkv_send.at[seq, 0],
                dkv_recv.at[seq, way * line + dest],
                to,
            )

        def dkv_hops(seq):
            if not hops:
                return
            low = l_id < line // 2
            for first in (True, False):
                for step in range(1, line):
                    for way, dest in ((0, line - step), (1, step - 1)):
                        ahead = (
                            (l_id > 0) & (l_id < dest)
                            if way == 0
                            else (l_id < line - 1) & (l_id > dest)
                        )
                        turn_now = low if first == (way == 0) else jnp.logical_not(low)

                        @pl.when(ahead & turn_now)
                        def _():
                            dkv_hop(seq, way, dest).wait_recv()
                            dkv_take(seq, way, dest)
                            dkv_hop(seq, way, dest).start()

        def dkv_take(seq, way, dest):
            def body(head, carry):
                dkv_x[seq * HK + head, dest] = (
                    dkv_x[seq * HK + head, dest].astype(F32)
                    + dkv_z[seq, way, dest, head].astype(F32)
                ).astype(BF)
                return carry

            lax.fori_loop(0, HK, body, 0)

        def dkv_arrive(seq):
            if not hops:
                for k in range(1, line):
                    dkv_copy(seq, k).wait()
                return
            sent = dkv_x.at[pl.ds(seq * HK, HK), pl.ds(0, line - 1)]
            remote(sent, sent, dkv_send.at[seq, 0], dkv_recv.at[seq, 0], mates[0]).wait_send()
            for dest in range(line):

                @pl.when((l_id == dest) & (l_id > 0))
                def _():
                    dkv_hop(seq, 0, dest).wait_recv()

                @pl.when((l_id == dest) & (l_id < line - 1))
                def _():
                    dkv_hop(seq, 1, dest).wait_recv()

        def dkv_parts(seq, head, total):
            if not hops:
                for k in range(line - 1):
                    total = total + dkv_z[seq, k, head].astype(F32)
                return total
            left = jnp.where(l_id > 0, dkv_z[seq, 0, l_id, head].astype(F32), 0.0)
            right = jnp.where(l_id < line - 1, dkv_z[seq, 1, l_id, head].astype(F32), 0.0)
            return total + left + right

        def dkv_gather(seq):
            dkv_arrive(seq)
            cos = jnp.where(lane < 64, cosine[pl.ds(seq * 128, 128), :], 1.0)
            sin = jnp.where(lane < 64, sine[pl.ds(seq * 128, 128), :], 0.0)
            for head in range(HK):
                total = dkv_x[seq * HK + head, l_id].astype(F32)
                total = dkv_parts(seq, head, total)
                dkv_own[pl.ds(seq * 128, 128), pl.ds(head * 128, 128)] = (
                    total * cos - swap_halves(total, lane) * sin
                ).astype(BF)

        near = c_id * own_rows
        far = (1 - c_id) * own_rows
        pieces = 5

        def rows_at(out, start, first, count):
            return out.at[pl.ds(pl.multiple_of(start + first, 16), count)]

        def jobs_of(box, came, total, group, outs_of):
            count = own_rows // pieces
            result = []
            for piece in range(pieces):
                span = pl.ds(piece * count, count)
                ready, outs = outs_of(total, piece * count, count)
                result.append(
                    (box.at[s_id, span], came.at[span], total.at[span], group * pieces + piece)
                    + (count, group, ready, outs)
                )
            return result

        def plain(out, box):
            def outs_of(total, first, count):
                return None, [
                    (
                        total.at[pl.ds(first, count)],
                        rows_at(out, near, first, count),
                        rows_at(out, far, first, count),
                        box,
                    )
                ]

            return outs_of

        def unpacked(total, first, count):
            span = pl.ds(first, count)

            def ready():
                value = total[span, :].astype(F32)
                for half_, start in ((0, 0), (1, HD)):
                    k_nat[half_, span, :] = jnp.concatenate(
                        [
                            value[:, head * 128 + start : head * 128 + start + HD]
                            for head in range(HK)
                        ],
                        1,
                    ).astype(BF)

            outs = [
                (
                    k_nat.at[half_, span],
                    rows_at(out, near, first, count),
                    rows_at(out, far, first, count),
                    2 + half_,
                )
                for half_, out in ((0, out_wk), (1, out_wv))
            ]
            return ready, outs

        def own_gain():
            value = gn_t[...]
            chosen = value[:, 0:part]
            for s in range(1, shards):
                chosen = jnp.where(s_id == s, value[:, s * part : (s + 1) * part], chosen)
            gn_out[...] = chosen

        o_jobs = jobs_of(o_x, o_r, o_t, 0, plain(out_wo, 0))
        q_jobs = jobs_of(q_x, q_r, q_t, 1, plain(out_wq, 1))
        k_jobs = jobs_of(k_x, k_r, k_t, 2, unpacked)
        gain_job = [
            (gn_x, gn_r, gn_t, 3 * pieces, 8, 3, own_gain, [(gn_out, out_gain, None, 4)])
        ]
        jobs = o_jobs + q_jobs + gain_job + k_jobs

        def first_up(some):
            @pl.when(jnp.logical_not(has_outer))
            def _():
                for job in some:
                    line_up(*job[:6])

        def job_up(job):
            @pl.when(has_outer)
            def _():
                line_up(*job[:6])

        def job_down(job):
            mine, _, total, slot, count, group, ready, outs = job
            line_down(mine, total, slot, count, group, ready, outs)

        lax.fori_loop(0, 2 * blocks, attend, 0)
        ring(4)
        scatter_part(g_buf, o_x, o_z, 0)
        lax.fori_loop(2 * blocks, HK * blocks, attend, 0)
        dkv_core_copy(0).start()
        ring(5)
        lax.fori_loop(HK * blocks, (HK + 2) * blocks, attend, 0)
        dkv_scatter(0)
        lax.fori_loop((HK + 2) * blocks, total_steps, attend, 0)
        dkv_core_copy(1).start()
        if blocks > 1:
            for two in range(width // 128):
                for seq in range(2):
                    where = (pl.ds(seq * 128, 128), pl.ds(two * 128, 128))
                    piece = dq[where].astype(F32)
                    cos = cosine[where[0], :]
                    sin = sine[where[0], :]
                    dq[where] = (piece * cos - swap_halves(piece, lane) * sin).astype(dq.dtype)
        ring(6)
        weight_grad(n1_t_ref, dq, g_buf, shards)
        core_part(g_buf, q_x, 1).start()
        dkv_scatter(1)
        ends_up(8, turns)
        ring(7)
        ring_down(6)
        dkv_hops(0)
        scatter_part(g_buf, q_x, q_z, 1)
        gather_part(o_x, o_z, 0)
        first_up(o_jobs)
        dkv_hops(1)
        ring_down(7)
        load_wq.wait()
        load_wkv.wait()
        back = nt(dq[...], w_buf[...])
        ends_down(0, 3)
        ring(8, 16)
        dkv_gather(0)
        dkv_gather(1)
        g_kv = g_buf.at[:, :, pl.ds(0, 2 * HK * HD)]
        weight_grad(n1_t_ref, dkv_own, g_kv, shards)
        core_part(g_kv, k_x, 2).start()
        back = back + nt(dkv_own[...], wkv_buf[...])
        scatter_part(g_kv, k_x, k_z, 2)
        ring(9, 1)
        hidden = x_ref[...].astype(F32)
        scale = lax.rsqrt(jnp.mean(hidden * hidden, -1, keepdims=True) + EPSILON)
        scaled = back * gains_ref[0:1, :]
        gn_own[0:1, :] = jnp.sum(back * hidden * scale, 0, keepdims=True)
        gn_own[2:8, :] = jnp.zeros((6, width), F32)
        gain_core = remote(gn_own, gn_x, g_core.at[6], g_core.at[7], sibling)
        gain_core.start()
        x_ref[...] = (
            gm[...]
            + scale * scaled
            - hidden * (scale * scale * scale) * jnp.mean(scaled * hidden, -1, keepdims=True)
        ).astype(BF)
        keep_dx = local(x_ref, out_dx, late_sem.at[1])
        keep_dx.start()
        gain_core.wait()
        gn_own[...] = gn_own[...] + gn_x[...]

        def gain_copy(k):
            return remote(
                gn_own, gn_z.at[k - 1], g_send.at[3], g_recv.at[3], peers[k - 1]
            )

        for k in range(1, shards):
            gain_copy(k).start()
        for k in range(1, shards):
            part_copy(k).start()

        def gather_gain():
            remote(gn_z, gn_z, g_send.at[3], g_recv.at[3], peers[0]).wait()
            total = gn_own[...]
            for k in range(shards - 1):
                total = total + gn_z[k]
            gn_x[...] = total

        @pl.when(jnp.logical_not(has_outer))
        def _():
            gather_part(q_x, q_z, 1)
            for job in q_jobs:
                line_up(*job[:6])
            gather_gain()
            gather_part(k_x, k_z, 2)
            for job in gain_job + k_jobs:
                line_up(*job[:6])

        @pl.when(has_outer)
        def _():
            ring(10, 1)
            ring(11, 1)

        ends_down(3, 8)
        def finish_result():
            remote(p_zone, p_zone, p_send.at[0], p_recv.at[0], peers[0]).wait()
            result = mid_ref[...]
            for first in range(0, shards, 4):
                stage = [
                    local(
                        parts_hbm.at[s_id] if k == 0 else p_zone.at[k - 1],
                        w_buf.at[pl.ds((k - first) * rows, rows)],
                        load_sem.at[k - first],
                    )
                    for k in range(first, min(shards, first + 4))
                ]
                for copy in stage:
                    copy.start()
                for k, copy in enumerate(stage):
                    copy.wait()
                    result = result + w_buf[k * rows : (k + 1) * rows, :].astype(F32)
            dproj[...] = result.astype(BF)
            local(dproj, out_result, late_sem.at[2]).start()

        todo = list(jobs)
        done = []

        def next_up():
            done.append(todo.pop(0))
            job_up(done[-1])

        def last_chunk(index):
            @pl.when(is_mid)
            def _():
                down(index)

        next_up()
        next_up()
        last_chunk(2 * turns - 2)
        next_up()
        last_chunk(2 * turns - 1)
        next_up()

        @pl.when(has_outer)
        def _():
            gather_part(q_x, q_z, 1)
            gather_gain()
            gather_part(k_x, k_z, 2)

        ends_down(8, turns)

        @pl.when(jnp.logical_not(has_outer))
        def _():
            finish_result()

        while todo:
            next_up()
            job_down(done.pop(0))
        for job in done:
            job_down(job)

        @pl.when(has_outer)
        def _():
            finish_result()

        whole = [
            (o_x.at[s_id], o_t, [(o_t, out_wo, 0)]),
            (q_x.at[s_id], q_t, [(q_t, out_wq, 1)]),
            (k_x.at[s_id], k_t, [(k_nat.at[0], out_wk, 2), (k_nat.at[1], out_wv, 3)]),
        ]
        for group, (mine, total, outs) in enumerate(whole):
            line_settle(
                mine,
                total,
                group,
                [
                    (src, rows_at(out, near, 0, own_rows), rows_at(out, far, 0, own_rows), box)
                    for src, out, box in outs
                ],
            )
        line_settle(gn_x, gn_t, 3, [(gn_out, out_gain, None, 4)])
        keep_dx.wait()
        local(dproj, out_result, late_sem.at[2]).wait()

    pl.run_scoped(
        attention,
        v((width, 2 * HK * HD), BF),
        v((2, 1024, 512), BF),
        v((2, 1024, 128), BF),
        v((rows, width), BF),
        v((2 * HK, 512, 128), BF),
        v((2 * HK, 1, 512), F32),
        v((2 * HK, line, 2, 128, 128), BF),
        v((rows, width), BF if blocks == 1 else F32),
        v((rows, 2 * HK * HD), BF),
        v((shards, part, width), BF),
        v((rows, width), BF),
        v((width, rows), BF),
        v((2 * HK, 512, 128), BF),
        v((width, rows), BF),
        v((rows, width), BF),
    )

    for array in range(3):
        settle(array)


def backward_call(shards, line, *arrays):
    x, kv, gate = arrays[7], arrays[-1], arrays[15]
    rows, width = x.shape
    keys = kv.shape[1]
    feed = gate.shape[2]
    part = width // shards
    own_rows = part // 2
    kv_width = 2 * HK * HD
    sizes = (shards, line, keys, rows, width, feed)
    dma = pltpu.SemaphoreType.DMA
    v = pltpu.VMEM
    vm = pl.BlockSpec(memory_space=pltpu.VMEM)
    hbm = pl.BlockSpec(memory_space=pltpu.HBM)
    half = width // 2
    shape = jax.ShapeDtypeStruct

    def boxes(cols):
        return [
            v((shards, own_rows, cols), BF),
            v((shards - 1, own_rows, cols), BF),
            v((own_rows, cols), BF),
            v((own_rows, cols), BF),
        ]

    scratch = [
        v((width, width), BF),
        v((rows, width), F32),
        v((rows, width), F32),
        v((2 * HK, line, 128, 128), BF),
        v((2, 2, 4, HK, 128, 128) if line == 4 else (2, line - 1, HK, 128, 128), BF),
        *[v((2, half, feed), BF) for _ in range(4)],
        *[v((feed, half), BF) for _ in range(4)],
        *boxes(width),
        *boxes(width),
        *boxes(kv_width),
        v((8, width), F32),
        v((8, width), F32),
        v((shards - 1, 8, width), F32),
        v((8, width), F32),
        v((8, width), F32),
        v((2, own_rows, HK * HD), BF),
        v((8, part), F32),
        dma((max(6, shards),)),
        dma((2,)),
        dma((2,)),
        dma((8,)),
        dma((3,)),
        dma((24,)),
        dma((24,)),
        *[dma((3,)) for _ in range(4)],
        dma((4,)),
        dma((2, 1 if line == 4 else line)),
        dma((2, 2 * line)),
        dma((8,)),
        dma((4,)),
        dma((4,)),
        dma((4,)),
        dma((16,)),
        dma((16,)),
        dma((4,)),
        dma((4,)),
        dma((4,)),
        dma((5,)),
        dma((1,)),
        dma((1,)),
        dma((shards - 1,)),
        dma((shards - 1,)),
        dma((9,)),
    ]
    return pl.pallas_call(
        lambda *refs: backward_kernel(sizes, *refs),
        out_shape=(
            shape((width, feed), BF),
            shape((width, feed), BF),
            shape((feed, width), BF),
            shape((part, width), BF),
            shape((part, width), BF),
            shape((part, HK * HD), BF),
            shape((part, HK * HD), BF),
            shape((8, part), F32),
            shape((rows, width), BF),
            shape((rows, width), BF),
            shape((shards, rows, width), BF),
            shape((shards - 1, rows, width), BF),
            shape((shards - 1, rows, width), BF),
        ),
        in_specs=[vm] * 3 + [hbm] * 19,
        out_specs=tuple([hbm] * 13),
        scratch_shapes=scratch,
        compiler_params=pltpu.CompilerParams(
            collective_id=3, has_side_effects=True, vmem_limit_bytes=VMEM_LIMIT
        ),
        name="backward",
    )(*arrays)


def per_device(
    tokens,
    cotangent,
    positions,
    lengths,
    attn_gain,
    w_query,
    w_key,
    w_value,
    w_out,
    mlp_gain,
    w_gate,
    w_up,
    w_down,
):
    seqs, stretch, width = tokens.shape
    shards, line = lax.axis_size("shard"), lax.axis_size("line")
    rows = seqs * stretch
    frequency = ROPE_BASE ** (-np.arange(HD // 2, dtype=np.float32) * 2.0 / HD)
    frequency = np.tile(frequency, 4)[None].astype(np.float32)
    x = tokens.reshape(rows, width)
    (
        gains,
        cos_wide,
        sin_wide,
        wq_all,
        wkv_all,
        out_all,
        packed_kv,
        soft,
        grad_all,
        attn,
        attn_t,
        norm_t,
        packed_q,
        middle,
        inner,
        back,
        norm_all_t,
        inner_t,
        grad_gate,
        grad_up,
    ) = front_call(
        shards,
        line,
        positions,
        lengths,
        frequency,
        attn_gain,
        mlp_gain,
        w_key,
        w_value,
        x,
        cotangent.reshape(rows, width),
        w_query,
        w_out,
        w_gate,
        w_up,
        w_down,
    )
    (
        sum_gate,
        sum_up,
        sum_down,
        sum_out,
        sum_query,
        sum_key,
        sum_value,
        sum_gain,
        grad_input,
        result,
        _,
        _,
        _,
    ) = backward_call(
        shards,
        line,
        gains,
        cos_wide,
        sin_wide,
        attn,
        attn_t,
        packed_q,
        norm_t,
        x,
        middle,
        inner,
        w_down,
        back,
        norm_all_t,
        grad_all,
        inner_t,
        grad_gate,
        grad_up,
        out_all,
        wq_all,
        wkv_all,
        soft,
        packed_kv.reshape(seqs * HK, -1, 128),
    )
    arrays = [sum_gate, sum_up, sum_down, sum_query, sum_out, sum_key, sum_value]
    arrays = widen_call(sum_gain, arrays + [grad_input, result], [F32] * 7 + [BF] * 2)
    sum_gate, sum_up, sum_down, sum_query, sum_out, sum_key, sum_value = arrays[:7]
    grad_input, result, gain_one, gain_two = arrays[7:]
    return (
        result.reshape(seqs, stretch, width),
        grad_input.reshape(seqs, stretch, width),
        gain_one,
        sum_query,
        sum_key,
        sum_value,
        sum_out,
        gain_two,
        sum_gate,
        sum_up,
        sum_down,
    )


def solution(mesh):
    shards, ctx = mesh.devices.shape
    inner = Mesh(mesh.devices.reshape(shards, ctx // 2, 2), ("shard", "line", "core"))
    where = ("line", "core")
    return jax.shard_map(
        per_device,
        mesh=inner,
        in_specs=(
            P("shard", where, None),
            P("shard", where, None),
            P("shard", None),
            P("shard"),
            P("shard"),
            P("shard", None),
            P("shard", None),
            P("shard", None),
            P("shard", None),
            P("shard"),
            P(None, "shard"),
            P(None, "shard"),
            P("shard", None),
        ),
        out_specs=(
            P("shard", where, None),
            P("shard", where, None),
            P("shard"),
            P("shard", None),
            P("shard", None),
            P("shard", None),
            P("shard", None),
            P("shard"),
            P(None, "shard"),
            P(None, "shard"),
            P("shard", None),
        ),
        check_vma=False,
    )
```

```python
import math

import jax
import jax.numpy as jnp
import numpy as np
from jax import lax
from jax.experimental import pallas as pl
from jax.experimental.pallas import tpu as pltpu
from jax.sharding import Mesh
from jax.sharding import PartitionSpec as P

HQ = 20
HK = 5
HD = 64
GROUP = HQ // HK
EPSILON = 1e-05
NEGATIVE = -1e30
ROPE_BASE = 10000.0
BF = jnp.bfloat16
F32 = jnp.float32
BY_MESH = pl.DeviceIdType.MESH
VMEM_LIMIT = 67043328


def nn(a, b):
    return lax.dot_general(a, b, (((1,), (0,)), ((), ())), preferred_element_type=F32)


def nt(a, b):
    return lax.dot_general(a, b, (((1,), (1,)), ((), ())), preferred_element_type=F32)


def tn(a, b):
    return lax.dot_general(a, b, (((0,), (0,)), ((), ())), preferred_element_type=F32)


def lanes_of(rows):
    return lax.broadcasted_iota(jnp.int32, (rows, 128), 1)


def swap_halves(block, lane):
    left = pltpu.roll(block, 96, 1)
    right = pltpu.roll(block, 32, 1)
    return jnp.where(lane % 64 < 32, left, right)


def peer_of(s_id, shards, k, back):
    if shards == 4:
        if isinstance(k, int):
            return [s_id, s_id + 1 - 2 * (s_id % 2), (s_id + 2) % 4, 3 - s_id][k]
        return jnp.where(
            k == 0,
            s_id,
            jnp.where(
                k == 1, s_id + 1 - 2 * (s_id % 2), jnp.where(k == 2, (s_id + 2) % 4, 3 - s_id)
            ),
        )
    return (s_id + (shards - k if back else k)) % shards


class Spread:
    def __init__(self, env, block, source, sems, shared, size):
        self.env, self.block, self.source, self.shared = env, block, source, shared
        self.size = size
        self.send, self.recv, self.sib_send, self.sib_recv = sems
        self.relay = env.shards == 4

    def copy(self, k):
        env = self.env
        return env.remote(
            self.source,
            self.block(env.s_id, env.c_id, 0, 2),
            self.send.at[0],
            self.recv.at[k],
            env.peer(k),
        )

    def passing(self, k):
        env = self.env
        piece = self.block(env.origin(k), env.c_id, k - 1, 1)
        return env.remote(
            piece, piece, self.send.at[0], self.recv.at[2 + k], env.peer(3 - k)
        )

    def direct(self):
        return range(1, 3 if self.relay else self.env.shards)

    def start(self):
        for k in self.direct():
            self.copy(k).start()

    def sib_copy(self, k):
        piece = self.block(self.env.origin(k), self.env.c_id, 0, 2)
        return self.env.remote(
            piece, piece, self.sib_send.at[0], self.sib_recv.at[k], self.env.sibling
        )

    def forward(self):
        for k in self.direct():
            self.copy(k).wait_recv()
            if self.relay:
                self.passing(k).start()
            if self.shared:
                self.sib_copy(k).start()

    def collect(self):
        if self.relay:
            for k in (1, 2):
                self.passing(k).wait_recv()
            if self.shared:
                self.sib_copy(3).start()

    def finish(self):
        if self.shared:
            for k in range(1, self.env.shards):
                self.sib_copy(k).wait_recv()

    def settle(self):
        env = self.env
        piece = self.size(env.shards - 1)
        env.remote(piece, piece, self.send.at[0], self.recv.at[0], env.peer(1)).wait_send()
        if self.shared:
            env.remote(
                piece, piece, self.sib_send.at[0], self.sib_recv.at[0], env.sibling
            ).wait_send()


class Env:
    def __init__(self, shards, line):
        self.shards, self.line = shards, line
        self.s_id = lax.axis_index("shard")
        self.l_id = lax.axis_index("line")
        self.c_id = lax.axis_index("core")
        self.sibling = (self.s_id, self.l_id, 1 - self.c_id)

    def remote(self, src, dst, send, recv, to):
        return pltpu.make_async_remote_copy(
            src, dst, send, recv, device_id=to, device_id_type=BY_MESH
        )

    def peer(self, k):
        return (peer_of(self.s_id, self.shards, k, False), self.l_id, self.c_id)

    def origin(self, k):
        return peer_of(self.s_id, self.shards, k, True)

    def mate(self, k):
        return (self.s_id, lax.rem(self.l_id + k, self.line), self.c_id)

    def greet(self, others):
        barrier = pltpu.get_barrier_semaphore()
        for other in others:
            pl.semaphore_signal(barrier, inc=1, device_id=other, device_id_type=BY_MESH)

    def meet(self, others):
        pl.semaphore_wait(pltpu.get_barrier_semaphore(), len(others))

    def barrier(self, others):
        self.greet(others)
        self.meet(others)


def front_kernel(
    sizes,
    positions_ref,
    lengths_ref,
    freq_ref,
    gain_one_ref,
    gain_two_ref,
    wk_ref,
    wv_ref,
    x_hbm,
    g_hbm,
    wq_ref,
    wo_ref,
    wg_hbm,
    wu_hbm,
    wd_hbm,
    out_gains,
    cos_ref,
    sin_ref,
    out_wq,
    out_wkv,
    out_wo,
    out_kv,
    out_pt,
    out_g,
    keep_attn,
    keep_attn_t,
    keep_n1_t,
    keep_qp,
    keep_mid,
    out_inner,
    out_back,
    out_n2_t,
    out_inner_t,
    out_dgate,
    out_dup,
    wq_all,
    wkv_all,
    wo_all,
    kv_all,
    n2_all,
    g_all,
    wg,
    wu,
    wd,
    out_attn,
    out_attn_t,
    out_n1_t,
    out_qp,
    out_mid,
    norm,
    x_ref,
    bias_ref,
    pt_stage,
    gains_ref,
    gain_zone,
    gain_send,
    gain_recv,
    wq_s,
    wq_r,
    wq_ss,
    wq_sr,
    wkv_s,
    wkv_r,
    wkv_ss,
    wkv_sr,
    wo_s,
    wo_r,
    wo_ss,
    wo_sr,
    g_s,
    g_r,
    n2_send,
    n2_recv,
    kv_send,
    kv_recv,
    kv_sib_send,
    kv_sib_recv,
    pt_sem,
    in_sem,
    load_sem,
    keep_sem,
    part_sem,
    back_sem,
    out_sem,
):
    shards, line, keys, rows, width, feed = sizes
    env = Env(shards, line)
    s_id, l_id, c_id = env.s_id, env.l_id, env.c_id
    part = width // shards
    hp = part // 2
    quarter = hp // 2
    blocks = keys // 1024
    load_g = pltpu.make_async_copy(g_hbm, g_all.at[s_id], in_sem.at[0])
    load_g.start()
    loads = [
        pltpu.make_async_copy(src, dst, load_sem.at[i])
        for i, (src, dst) in enumerate(((wg_hbm, wg), (wu_hbm, wu), (wd_hbm, wd)))
    ]
    for head in range(HK):
        both = jnp.concatenate(
            [ref[:, head * HD : head * HD + HD].astype(F32) for ref in (wk_ref, wv_ref)], 1
        )
        wkv_all[pl.ds(pl.multiple_of(s_id * part, 16), part), head * 128 : head * 128 + 128] = (
            both.astype(BF)
        )
    gains_ref[0:1, :] = gain_one_ref[...].astype(F32).reshape(1, part)
    gains_ref[1:2, :] = gain_two_ref[...].astype(F32).reshape(1, part)
    gains_ref[2:8, :] = jnp.zeros((6, part), F32)
    env.barrier(
        [env.sibling]
        + [env.peer(k) for k in range(1, shards)]
        + [env.mate(k) for k in range(1, line)]
    )

    def tokens_of(ref):
        def block(s, core, first, count):
            return ref.at[s, pl.ds(first * (rows // 2), count * (rows // 2))]

        return block

    def first_tokens(ref):
        return lambda count: ref.at[pl.ds(0, count)]

    def first_rows(ref):
        return lambda count: ref.at[pl.ds(0, count * hp)]

    grad_gather = Spread(
        env,
        tokens_of(g_all),
        g_all.at[s_id],
        (g_s, g_r, None, None),
        False,
        first_tokens(g_all),
    )
    n2_gather = Spread(
        env,
        tokens_of(n2_all),
        n2_all.at[s_id],
        (n2_send, n2_recv, None, None),
        False,
        first_tokens(n2_all),
    )

    def rows_of(ref):
        def block(s, core, first, count):
            start = s * part + core * hp + first * quarter
            return ref.at[pl.ds(pl.multiple_of(start, 16), count * quarter)]

        return block


    mine = pl.ds(pl.multiple_of(c_id * hp, 16), hp)
    own = pl.ds(pl.multiple_of(s_id * part, 16), part)
    kv_mine = pl.ds(pl.multiple_of(s_id * part + c_id * hp, 16), hp)
    kv_gather = Spread(
        env,
        rows_of(wkv_all),
        wkv_all.at[kv_mine],
        (wkv_s, wkv_r, wkv_ss, wkv_sr),
        True,
        first_rows(wkv_all),
    )
    q_gather = Spread(
        env,
        rows_of(wq_all),
        wq_ref.at[mine],
        (wq_s, wq_r, wq_ss, wq_sr),
        True,
        first_rows(wq_all),
    )
    o_gather = Spread(
        env,
        rows_of(wo_all),
        wo_ref.at[mine],
        (wo_s, wo_r, wo_ss, wo_sr),
        True,
        first_rows(wo_all),
    )
    outs = [
        pltpu.make_async_copy(src, dst, keep_sem.at[i])
        for i, (src, dst) in enumerate(
            (
                (wkv_all, out_wkv),
                (wq_all, out_wq),
                (kv_all, out_kv),
                (wo_all, out_wo),
                (out_attn, keep_attn),
                (out_attn_t, keep_attn_t),
                (out_n1_t, keep_n1_t),
                (out_qp, keep_qp),
                (out_mid, keep_mid),
            )
        )
    ]

    def attention_part():
        load_x = pltpu.make_async_copy(x_hbm, x_ref, in_sem.at[3])
        load_x.start()
        def gain_copy(k):
            return env.remote(
                gains_ref, gain_zone.at[s_id], gain_send.at[k], gain_recv.at[k], env.peer(k)
            )

        for k in range(1, shards):
            gain_copy(k).start()
        kv_gather.start()
        locals_ = [
            pltpu.make_async_copy(wq_ref, wq_all.at[own], in_sem.at[1]),
            pltpu.make_async_copy(wo_ref, wo_all.at[own], in_sem.at[2]),
        ]
        for copy in locals_:
            copy.start()
        gain_zone[s_id] = gains_ref[...]
        lane = lanes_of(128)
        place = pl.ds(pl.multiple_of((l_id * 2 + c_id) * 128, 128), 128)
        spots = positions_ref[:, place].astype(F32)
        good = [
            jnp.where(positions_ref[seq : seq + 1, place] < lengths_ref[seq], 1.0, 0.0).astype(F32)
            for seq in range(2)
        ]
        info = jnp.transpose(jnp.concatenate([spots] + good + [jnp.zeros((4, 128), F32)], 0))
        for seq in range(2):
            angle = info[:, seq : seq + 1] * freq_ref[...]
            cos_ref[seq * 128 : seq * 128 + 128, :] = jnp.cos(angle)
            sine = jnp.sin(angle)
            sin_ref[seq * 128 : seq * 128 + 128, :] = jnp.where(lane % 64 < 32, -sine, sine)
        load_x.wait()
        hidden = x_ref[...].astype(F32)
        scale = lax.rsqrt(jnp.mean(hidden * hidden, -1, keepdims=True) + EPSILON)
        for k in range(1, shards):
            gain_copy(k).wait()
        out_gains[...] = jnp.concatenate([gain_zone[s] for s in range(shards)], 1)
        norm[...] = (hidden * scale * out_gains[0:1, :]).astype(BF)
        kv_gather.forward()
        q_gather.start()
        for copy in locals_:
            copy.wait()
        kv_gather.collect()
        kv_gather.finish()

        spot = l_id * 2 + c_id

        def make_kv(head, carry):
            block = nn(norm[...], wkv_all[:, pl.ds(pl.multiple_of(head * 128, 128), 128)])
            for seq in range(2):
                piece = block[seq * 128 : seq * 128 + 128]
                cos = jnp.where(lane < 64, cos_ref[pl.ds(seq * 128, 128), :], 1.0)
                sin = jnp.where(lane < 64, sin_ref[pl.ds(seq * 128, 128), :], 0.0)
                kv_all[seq * HK + head, spot] = (piece * cos + swap_halves(piece, lane) * sin).astype(
                    BF
                )
            return carry

        lax.fori_loop(0, HK, make_kv, 0)

        def kv_slice(seq, l, c):
            return kv_all.at[pl.ds(seq * HK, HK), l * 2 + c]

        def kv_move(seq, way, src):
            piece = kv_slice(seq, src, c_id)
            to = (s_id, lax.rem(l_id + (1 if way == 0 else line - 1), line), c_id)
            return env.remote(
                piece, piece, kv_send.at[seq, way * line + src], kv_recv.at[seq, src], to
            )

        def kv_sib(seq, src):
            piece = kv_slice(seq, src, c_id)
            return env.remote(
                piece, piece, kv_sib_send.at[seq], kv_sib_recv.at[seq], env.sibling
            )

        def kv_onward(seq, way, src):
            @pl.when((l_id < line - 1) if way == 0 else (l_id > 0))
            def _():
                kv_move(seq, way, src).start()

        def kv_start(seq):
            for way in range(2):
                kv_onward(seq, way, l_id)
            kv_sib(seq, l_id).start()

        def kv_step(seq, far):
            for way in range(2):
                src = l_id - far if way == 0 else l_id + far

                @pl.when((src >= 0) & (src < line))
                def _():
                    kv_move(seq, way, src).wait_recv()
                    kv_onward(seq, way, src)
                    kv_sib(seq, src).start()

        def kv_finish(seq):
            piece = kv_all.at[pl.ds(seq * HK, HK), pl.ds(0, line)]
            env.remote(
                piece, piece, kv_sib_send.at[seq], kv_sib_recv.at[seq], env.sibling
            ).wait()

        def kv_settle(seq):
            for src in range(line):

                @pl.when((l_id < line - 1) & (src <= l_id))
                def _():
                    kv_move(seq, 0, src).wait_send()

                @pl.when((l_id > 0) & (src >= l_id))
                def _():
                    kv_move(seq, 1, src).wait_send()

        kv_start(0)
        for load in loads:
            load.start()
        load_g.wait()
        for seq in range(2):
            rows_ = pl.ds(seq * 128, 128)
            g_all[s_id, rows_, :] = (
                g_all[s_id, rows_, :].astype(F32) * info[:, 2 + seq : 3 + seq]
            ).astype(BF)
            for group in range(keys // 1024):
                some = jnp.concatenate(
                    [
                        positions_ref[seq : seq + 1, (group * 8 + t) * 128 : (group * 8 + t + 1) * 128]
                        for t in range(8)
                    ],
                    0,
                )
                some = jnp.where(some < lengths_ref[seq], some, 1 << 24)
                key_at = jnp.transpose(some.astype(F32))
                for t in range(8):
                    first = (group * 8 + t) * 128
                    bias_ref[seq, first : first + 128, :] = jnp.where(
                        key_at[:, t : t + 1] <= spots[seq : seq + 1, :], 0.0, NEGATIVE
                    )
        for tile in range(width // 128):
            piece = norm[:, tile * 128 : tile * 128 + 128].astype(F32)
            out_n1_t[tile * 128 : tile * 128 + 128, :] = jnp.transpose(piece).astype(BF)
        q_gather.forward()
        o_gather.start()
        kv_step(0, 1)
        if line == 2:
            kv_start(1)
        else:
            kv_step(0, 2)
            kv_start(1)
        q_gather.collect()
        q_gather.finish()

        def make_q(head, carry):
            block = nn(norm[...], wq_all[:, pl.ds(pl.multiple_of(head * 256, 256), 256)])
            for seq in range(2):
                cos = cos_ref[pl.ds(seq * 128, 128), :]
                sin = sin_ref[pl.ds(seq * 128, 128), :]
                for two in range(2):
                    piece = block[seq * 128 : seq * 128 + 128, two * 128 : two * 128 + 128]
                    piece = piece * cos + swap_halves(piece, lane) * sin
                    piece = piece.astype(BF).astype(F32) * (1.0 / math.sqrt(HD))
                    pair = seq * HK + head
                    out_qp[pair, pl.ds(two * 256, 128), :] = jnp.where(lane < 64, piece, 0.0).astype(
                        BF
                    )
                    out_qp[pair, pl.ds(two * 256 + 128, 128), :] = jnp.where(
                        lane < 64, pltpu.roll(piece, 64, 1), 0.0
                    ).astype(BF)
            return carry

        lax.fori_loop(0, HK, make_q, 0)

        def pt_copy(pair, block, slot):
            span = pl.ds(pl.multiple_of(block * 1024, 1024), 1024)
            return pltpu.make_async_copy(pt_stage.at[slot], out_pt.at[pair, span], pt_sem.at[slot])

        def keys_of(pair, block):
            if blocks == 1:
                return kv_all[pair].reshape(1024, 128)
            return kv_all[pair, pl.ds(block * 8, 8)].reshape(1024, 128)

        def scores(pair, block):
            span = pl.ds(pl.multiple_of(block * 1024, 1024), 1024)
            bias = bias_ref[pair // HK, span, :]
            return nt(keys_of(pair, block), out_qp[pair]) + jnp.concatenate([bias] * GROUP, 1)

        def attend(pair, carry):
            if blocks == 1:
                slot = lax.rem(pair, 2)

                @pl.when(pair >= 2)
                def _():
                    pt_copy(pair - 2, 0, slot).wait()

                value = scores(pair, 0)
                top = jnp.max(value, 0, keepdims=True)
                weight = jnp.exp(value - top)
                inverse = 1.0 / jnp.sum(weight, 0, keepdims=True)
                soft = (weight * inverse).astype(BF)
                pt_stage[slot] = soft
                pt_copy(pair, 0, slot).start()
                mixed = tn(keys_of(pair, 0), soft)[HD:]
            else:

                def first(block, state):
                    top, total = state
                    value = scores(pair, block)
                    new = jnp.maximum(top, jnp.max(value, 0, keepdims=True))
                    total = total * jnp.exp(top - new) + jnp.sum(
                        jnp.exp(value - new), 0, keepdims=True
                    )
                    return new, total

                top, total = lax.fori_loop(
                    0,
                    blocks,
                    first,
                    (jnp.full((1, 512), NEGATIVE, F32), jnp.zeros((1, 512), F32)),
                )
                inverse = 1.0 / total

                def second(block, mixed):
                    pt_stage[0] = (jnp.exp(scores(pair, block) - top) * inverse).astype(BF)
                    copy = pt_copy(pair, block, 0)
                    copy.start()
                    mixed = mixed + tn(keys_of(pair, block), pt_stage[0])[HD:]
                    copy.wait()
                    return mixed

                mixed = lax.fori_loop(0, blocks, second, jnp.zeros((HD, 512), F32))
            seq, head = pair // HK, pair % HK
            for two in range(2):
                both = jnp.concatenate(
                    [
                        mixed[:, two * 256 : two * 256 + 128],
                        mixed[:, two * 256 + 128 : two * 256 + 256],
                    ],
                    0,
                )
                tokens_ = pl.ds(pl.multiple_of(seq * 128, 128), 128)
                cols = pl.ds(pl.multiple_of(head * 256 + two * 128, 128), 128)
                out_attn_t[cols, tokens_] = both.astype(BF)
                out_attn[tokens_, cols] = jnp.transpose(both).astype(BF)
            return carry

        for far in range(3, line):
            kv_step(0, far)
        o_gather.forward()
        grad_gather.start()
        kv_step(1, 1)
        kv_finish(0)
        lax.fori_loop(0, 2, attend, 0)
        if line > 2:
            kv_step(1, 2)
        lax.fori_loop(2, HK, attend, 0)
        for far in range(3, line):
            kv_step(1, far)
        o_gather.collect()
        kv_finish(1)
        lax.fori_loop(HK, 2 * HK, attend, 0)
        o_gather.finish()

        def project(tile, carry):
            cols = pl.ds(pl.multiple_of(tile * 256, 256), 256)
            out_mid[:, cols] = x_ref[:, cols].astype(F32) + nn(out_attn[...], wo_all[:, cols])
            return carry

        lax.fori_loop(0, width // 256, project, 0)
        middle = out_mid[...]
        scale_two = lax.rsqrt(jnp.mean(middle * middle, -1, keepdims=True) + EPSILON)
        n2_all[s_id] = (middle * scale_two * out_gains[1:2, :]).astype(BF)
        n2_gather.start()
        grad_gather.forward()
        for copy in outs:
            copy.start()
        if blocks == 1:
            pt_copy(2 * HK - 2, 0, 0).wait()
            pt_copy(2 * HK - 1, 0, 1).wait()

        def finish():
            for gather in (kv_gather, q_gather, o_gather):
                gather.settle()
            kv_settle(0)
            kv_settle(1)
            for copy in outs:
                copy.wait()

        finishing.append(finish)

    v = pltpu.VMEM
    finishing = []
    attention_part()

    def feed_part(inner, dgate, dup, stage, grads, n2_t, inner_t):
        def back_copy(k, slot):
            return pltpu.make_async_copy(
                stage.at[slot], out_back.at[peer_of(s_id, shards, k, True)], back_sem.at[slot]
            )

        def outs(k):
            source = peer_of(s_id, shards, k, True)
            cols = pl.ds(pl.multiple_of(source * rows, 128), rows)
            return [
                pltpu.make_async_copy(n2_t.at[k], out_n2_t.at[:, cols], out_sem.at[0]),
                pltpu.make_async_copy(inner_t.at[k], out_inner_t.at[:, cols], out_sem.at[1]),
                pltpu.make_async_copy(dgate.at[source], out_dgate.at[source], out_sem.at[2]),
                pltpu.make_async_copy(dup.at[source], out_dup.at[source], out_sem.at[3]),
                pltpu.make_async_copy(g_all.at[source], out_g.at[source], out_sem.at[4]),
                pltpu.make_async_copy(inner.at[source], out_inner.at[source], out_sem.at[5]),
            ]

        def block(k, carry):
            source = peer_of(s_id, shards, k, True)
            slot = lax.rem(k, 2)
            if n2_gather.relay:

                @pl.when(k == 0)
                def _():
                    loads[2].wait()

                @pl.when(k == 3)
                def _():
                    grad_gather.collect()

                def grad_of(other, carry):
                    grads[other] = nt(g_all[peer_of(s_id, shards, other, True)], wd[...])
                    return carry

                first = jnp.where(k == 0, 0, jnp.where(k == 1, 1, 3))
                last = jnp.where(k == 0, 1, jnp.where(k == 3, 4, 3))
                lax.fori_loop(first, last, grad_of, 0)

                @pl.when(k == 1)
                def _():
                    n2_gather.forward()

                @pl.when(k == 3)
                def _():
                    n2_gather.collect()

            else:

                @pl.when(k == 0)
                def _():
                    loads[2].wait()

                @pl.when(k > 0)
                def _():
                    n2_gather.copy(k).wait_recv()

                grads[0] = nt(g_all[source], wd[...])

            normed = n2_all[source]
            n2_t[k] = jnp.transpose(normed)
            copies = outs(k)
            copies[0].start()
            copies[4].start()
            gate, upper = nn(normed, wg[...]), nn(normed, wu[...])
            grad_inner = grads[k if n2_gather.relay else 0]
            sig = 1.0 / (1.0 + jnp.exp(-gate))
            act = gate * sig
            inner[source] = (act * upper).astype(BF)
            dgate[source] = (grad_inner * upper * sig * (1.0 + gate * (1.0 - sig))).astype(BF)
            dup[source] = (grad_inner * act).astype(BF)
            for index in (2, 3, 5):
                copies[index].start()
            inner_t[k] = jnp.transpose(inner[source])
            copies[1].start()

            @pl.when(k >= 2)
            def _():
                back_copy(k - 2, slot).wait()

            stage[slot] = (nt(dgate[source], wg[...]) + nt(dup[source], wu[...])).astype(BF)
            back_copy(k, slot).start()
            return carry

        loads[0].wait()
        loads[1].wait()
        lax.fori_loop(0, shards, block, 0)
        whole = ((g_all, out_g), (inner, out_inner), (dgate, out_dgate), (dup, out_dup))
        for index, (src, dst) in zip((4, 5, 2, 3), whole):
            pltpu.make_async_copy(src, dst, out_sem.at[index]).wait()
        pltpu.make_async_copy(out_n2_t, out_n2_t, out_sem.at[0]).wait()
        pltpu.make_async_copy(out_inner_t, out_inner_t, out_sem.at[1]).wait()
        n2_gather.settle()
        grad_gather.settle()
        for last in (2, 1):
            back_copy(shards - last, (shards - last) % 2).wait()

    pl.run_scoped(
        feed_part,
        v((shards, rows, feed), BF),
        v((shards, rows, feed), BF),
        v((shards, rows, feed), BF),
        v((2, rows, width), BF),
        v((shards if shards == 4 else 1, rows, feed), F32),
        v((shards, width, rows), BF),
        v((shards, feed, rows), BF),
    )
    finishing[0]()


def front_call(shards, line, *arrays):
    positions, x, w_gate = arrays[0], arrays[7], arrays[11]
    rows, width = x.shape
    keys = positions.shape[1]
    feed = w_gate.shape[1]
    kv_width = 2 * HK * HD
    dma = pltpu.SemaphoreType.DMA
    v = pltpu.VMEM
    vm = pl.BlockSpec(memory_space=pltpu.VMEM)
    sm = pl.BlockSpec(memory_space=pltpu.SMEM)
    hbm = pl.BlockSpec(memory_space=pltpu.HBM)
    part = width // shards
    shape = jax.ShapeDtypeStruct
    hops = max(5, shards)
    return pl.pallas_call(
        lambda *refs: front_kernel((shards, line, keys, rows, width, feed), *refs),
        out_shape=(
            shape((8, width), F32),
            shape((rows, 128), F32),
            shape((rows, 128), F32),
            shape((width, width), BF),
            shape((width, kv_width), BF),
            shape((width, width), BF),
            shape((2 * HK, 2 * line, 128, 128), BF),
            shape((2 * HK, keys, 512), BF),
            shape((shards, rows, width), BF),
            shape((rows, width), BF),
            shape((width, rows), BF),
            shape((width, rows), BF),
            shape((2 * HK, 512, 128), BF),
            shape((rows, width), F32),
            shape((shards, rows, feed), BF),
            shape((shards, rows, width), BF),
            shape((width, shards * rows), BF),
            shape((feed, shards * rows), BF),
            shape((shards, rows, feed), BF),
            shape((shards, rows, feed), BF),
        ),
        in_specs=[vm, sm, vm, vm, vm, vm, vm] + [hbm] * 7,
        out_specs=(*[vm] * 3, *[hbm] * 17),
        scratch_shapes=[
            v((width, width), BF),
            v((width, kv_width), BF),
            v((width, width), BF),
            v((2 * HK, 2 * line, 128, 128), BF),
            v((shards, rows, width), BF),
            v((shards, rows, width), BF),
            v((width, feed), BF),
            v((width, feed), BF),
            v((feed, width), BF),
            v((rows, width), BF),
            v((width, rows), BF),
            v((width, rows), BF),
            v((2 * HK, 512, 128), BF),
            v((rows, width), F32),
            v((rows, width), BF),
            v((rows, width), BF),
            v((2, keys, 128), F32),
            v((2, 1024, 512), BF),
            v((8, part), F32),
            v((shards, 8, part), F32),
            dma((shards,)),
            dma((shards,)),
            *[dma((n,)) for n in (1, hops, 1, shards) * 3],
            *[dma((n,)) for n in (1, hops) * 2],
            dma((2, 2 * line)),
            dma((2, line)),
            dma((2,)),
            dma((2,)),
            dma((2,)),
            dma((4,)),
            dma((3,)),
            dma((9,)),
            dma((2,)),
            dma((2,)),
            dma((6,)),
        ],
        compiler_params=pltpu.CompilerParams(
            collective_id=1, has_side_effects=True, vmem_limit_bytes=VMEM_LIMIT
        ),
        name="front",
    )(*arrays)


def widen_kernel(count, gain_ref, *refs):
    src, dst = refs[:count], refs[count : 2 * count]
    out_one, out_two = refs[2 * count : 2 * count + 2]
    refs = refs[2 * count + 2 :]
    narrow, wide = refs[:count], refs[count : 2 * count]
    load_sem, store_sem = refs[2 * count :]
    out_one[...] = gain_ref[0:1, :].reshape(out_one.shape)
    out_two[...] = gain_ref[1:2, :].reshape(out_two.shape)
    for i in range(count):
        pltpu.make_async_copy(src[i], narrow[i], load_sem.at[i]).start()

    def piece(i, part, parts):
        rows = narrow[i].shape[0] // parts
        span = pl.ds(part * rows, rows)
        held = wide[i] if dst[i].dtype == F32 else narrow[i]
        return span, pltpu.make_async_copy(held.at[span], dst[i].at[span], store_sem.at[i])

    for i in range(count):
        pltpu.make_async_copy(src[i], narrow[i], load_sem.at[i]).wait()
        for part in range(4):
            span, copy = piece(i, part, 4)
            if dst[i].dtype == F32:
                wide[i][span, :] = narrow[i][span, :].astype(F32)
            copy.start()
    for i in range(count):
        piece(i, 0, 1)[1].wait()


def widen_call(gains, arrays, types):
    v = pltpu.VMEM
    hbm = pl.BlockSpec(memory_space=pltpu.HBM)
    vm = pl.BlockSpec(memory_space=pltpu.VMEM)
    count = len(arrays)
    return pl.pallas_call(
        lambda *refs: widen_kernel(count, *refs),
        out_shape=tuple(jax.ShapeDtypeStruct(a.shape, t) for a, t in zip(arrays, types))
        + (jax.ShapeDtypeStruct(gains.shape[1:], F32),) * 2,
        in_specs=[vm] + [hbm] * count,
        out_specs=tuple([hbm] * count) + (vm, vm),
        scratch_shapes=[
            *[v(a.shape, a.dtype) for a in arrays],
            *[v(a.shape if t == F32 else (16, 128), F32) for a, t in zip(arrays, types)],
            pltpu.SemaphoreType.DMA((count,)),
            pltpu.SemaphoreType.DMA((count,)),
        ],
        compiler_params=pltpu.CompilerParams(vmem_limit_bytes=VMEM_LIMIT),
        name="widen",
    )(gains, *arrays)


def add_rows(target, parts, rows, step):
    def body(index, carry):
        span = pl.ds(pl.multiple_of(index * step, step), step)
        total = parts[0][span, :].astype(F32)
        for part in parts[1:]:
            total = total + part[span, :].astype(F32)
        target[span, :] = total.astype(target.dtype)
        return carry

    lax.fori_loop(0, rows // step, body, 0)


def backward_kernel(
    sizes,
    gains_ref,
    cos_ref,
    sin_ref,
    attn_hbm,
    attn_t_hbm,
    qp_hbm,
    n1_t_hbm,
    x_hbm,
    mid_hbm,
    inner_hbm,
    wd_hbm,
    back_hbm,
    n2_t_hbm,
    g_hbm,
    inner_t_hbm,
    dgate_hbm,
    dup_hbm,
    wo_hbm,
    wq_hbm,
    wkv_hbm,
    pt_hbm,
    kv_hbm,
    out_gate,
    out_up,
    out_dn,
    out_wo,
    out_wq,
    out_wk,
    out_wv,
    out_gain,
    out_dx,
    out_result,
    parts_hbm,
    p_zone,
    b_zone,
    w_buf,
    gm,
    mid_ref,
    dkv_x,
    dkv_z,
    own_gu,
    got_gu_x,
    got_gu_r,
    got_gu_t,
    own_dn,
    got_dn_x,
    got_dn_r,
    got_dn_t,
    o_x,
    o_z,
    o_r,
    o_t,
    q_x,
    q_z,
    q_r,
    q_t,
    k_x,
    k_z,
    k_r,
    k_t,
    gn_own,
    gn_x,
    gn_z,
    gn_r,
    gn_t,
    k_nat,
    gn_out,
    load_sem,
    pt_sem,
    kv_sem,
    core_sem,
    first_sem,
    up_send,
    r_recv,
    t_recv,
    down_send,
    sib_send,
    sib_recv,
    local_sem,
    dkv_core,
    dkv_send,
    dkv_recv,
    g_core,
    g_send,
    g_recv,
    a_up,
    a_r,
    a_t,
    a_down,
    a_sib_send,
    a_sib_recv,
    a_local,
    p_send,
    p_recv,
    b_send,
    b_recv,
    late_sem,
):
    shards, line, keys, rows, width, feed = sizes
    env = Env(shards, line)
    s_id, l_id, c_id = env.s_id, env.l_id, env.c_id
    sibling, remote = env.sibling, env.remote
    toward = jnp.where(l_id < line // 2, 1, -1)
    inner_to = (s_id, l_id + toward, c_id)
    has_outer = (l_id > 0) & (l_id < line - 1)
    is_mid = (l_id == line // 2 - 1) | (l_id == line // 2)
    outer_to = (s_id, jnp.where(has_outer, l_id - toward, l_id + toward), c_id)
    peers = [env.peer(k) for k in range(1, shards)]
    mates = [env.mate(k) for k in range(1, line)]
    env.greet([sibling] + peers + mates)
    half = width // 2
    wide_pieces = 8
    down_pieces = 8 if feed % 128 == 0 else 4
    chunks = 2 * wide_pieces + down_pieces
    turns = 12
    slab = 16
    part = width // shards
    own_rows = part // 2
    blocks = keys // 1024
    tokens = shards * rows
    hops = line == 4
    near_half = pl.ds(pl.multiple_of(c_id * half, 128), half)
    far_half = pl.ds(pl.multiple_of((1 - c_id) * half, 128), half)

    def back_copy(k):
        return remote(
            back_hbm.at[peer_of(s_id, shards, k, False)],
            b_zone.at[k - 1],
            b_send.at[k - 1],
            b_recv.at[k - 1],
            peers[k - 1],
        )

    def part_copy(k):
        return remote(
            parts_hbm.at[peer_of(s_id, shards, k, False)],
            p_zone.at[k - 1],
            p_send.at[0],
            p_recv.at[0],
            peers[k - 1],
        )

    def local(src, dst, sem):
        return pltpu.make_async_copy(src, dst, sem)

    def views(index, where):
        if where != "dn":
            rows_ = half // wide_pieces
            array, piece = (0 if where == "gate" else 1), index % wide_pieces
            array_of = out_gate if where == "gate" else out_up
            span = pl.ds(pl.multiple_of(piece * rows_, 16), rows_)
            bufs = [ref.at[array, span] for ref in (own_gu, got_gu_x, got_gu_r, got_gu_t)]

            def out(core):
                start = core * half + piece * rows_
                return array_of.at[pl.ds(pl.multiple_of(start, 16), rows_)]

            return rows_, bufs, out, array
        rows_ = feed // down_pieces
        span = pl.ds(pl.multiple_of((index - 2 * wide_pieces) * rows_, 16), rows_)
        bufs = [ref.at[span] for ref in (own_dn, got_dn_x, got_dn_r, got_dn_t)]

        def out(core):
            return out_dn.at[span, pl.ds(pl.multiple_of(core * half, 128), half)]

        return rows_, bufs, out, 2

    def split(action):
        def run(index):
            if isinstance(index, int):
                if 0 <= index < chunks:
                    action(index, ("gate", "up", "dn")[min(2, index // wide_pieces)])
                return
            for number, where in enumerate(("gate", "up", "dn")):

                @pl.when(jnp.minimum(index // wide_pieces, 2) == number)
                def _():
                    action(index, where)

        return run

    def up_end(index, where):
        count, (mine, extra, came, total), _, array = views(index, where)
        add_rows(mine, [mine, extra], count, slab)
        send_up(index, mine, came, total, array)

    def up_inner(index, where):
        count, (mine, extra, came, total), _, array = views(index, where)
        remote(mine, came, up_send.at[array], r_recv.at[index], inner_to).wait_recv()
        add_rows(mine, [mine, extra, came], count, slab)
        send_up(index, mine, came, total, array)

    def send_up(index, mine, came, total, array):
        @pl.when(is_mid)
        def _():
            remote(mine, total, up_send.at[array], t_recv.at[index], inner_to).start()

        @pl.when(jnp.logical_not(is_mid))
        def _():
            remote(mine, came, up_send.at[array], r_recv.at[index], inner_to).start()

    def down(index, where):
        count, (mine, _, _, total), out, array = views(index, where)
        remote(mine, total, up_send.at[array], t_recv.at[index], inner_to).wait_recv()

        @pl.when(is_mid)
        def _():
            add_rows(total, [mine, total], count, slab)

        @pl.when(has_outer)
        def _():
            remote(total, total, down_send.at[array], t_recv.at[index], outer_to).start()

        remote(total, out(c_id), sib_send.at[array], sib_recv.at[array], sibling).start()
        local(total, out(c_id), local_sem.at[array]).start()

    def settle(array):
        if array < 2:
            mine, total = own_gu.at[array], got_gu_t.at[array]
            out_of = (out_gate, out_up)[array]
            outs = [
                out_of.at[pl.ds(pl.multiple_of(core * half, 16), half)]
                for core in (c_id, 1 - c_id)
            ]
        else:
            mine, total = own_dn, got_dn_t
            outs = [
                out_dn.at[:, pl.ds(pl.multiple_of(core * half, 128), half)]
                for core in (c_id, 1 - c_id)
            ]
        remote(mine, total, up_send.at[array], t_recv.at[0], inner_to).wait_send()

        @pl.when(has_outer)
        def _():
            remote(total, total, down_send.at[array], t_recv.at[0], outer_to).wait_send()

        remote(total, outs[1], sib_send.at[array], sib_recv.at[array], sibling).wait()
        local(total, outs[0], local_sem.at[array]).wait()

    up_end, up_inner, down = [split(f) for f in (up_end, up_inner, down)]

    def of_turns(first, last):
        return min(2 * first, chunks), min(2 * last, chunks)

    def run_all(action, first, last):
        def body(index, carry):
            action(index)
            return carry

        lax.fori_loop(first, last, body, 0)

    def ends_up(first, last):
        @pl.when(jnp.logical_not(has_outer))
        def _():
            run_all(up_end, *of_turns(first, last))

    def ring(turn, lag=2):
        for step in (2 * turn, 2 * turn + 1):
            if step < chunks:

                @pl.when(has_outer)
                def _():
                    up_inner(step)

            if 0 <= step - 2 * lag < chunks:

                @pl.when(is_mid)
                def _():
                    down(step - 2 * lag)

    def ring_down(turn):
        @pl.when(is_mid)
        def _():
            run_all(down, *of_turns(turn, turn + 1))

    def ends_down(first, last):
        @pl.when(jnp.logical_not(is_mid))
        def _():
            run_all(down, *of_turns(first, last))

    def quarter_span(part_):
        return pl.ds(pl.multiple_of(part_ * (half // 4), 16), half // 4)

    def first_send(src, part_):
        span = quarter_span(part_)
        return remote(
            src.at[0, span],
            got_gu_x.at[0, span],
            first_sem.at[part_],
            first_sem.at[4 + part_],
            sibling,
        )

    def core_send(array, src):
        dst = got_gu_x.at[array] if array < 2 else got_dn_x
        return remote(src, dst, core_sem.at[array], core_sem.at[3 + array], sibling)

    load_wo = local(wo_hbm, w_buf, late_sem.at[3])

    load_mid = local(mid_hbm, mid_ref, late_sem.at[0])

    def feed_grads(
        g_v, g_own, dgate_v, dup_v, wide_t, near_t, inner_t, far_gu, far_dn, inner_v, wd_v, stage_v
    ):
        loads = [
            local(src, dst, load_sem.at[i])
            for i, (src, dst) in enumerate(
                (
                    (n2_t_hbm.at[far_half], wide_t),
                    (dgate_hbm, dgate_v),
                    (dup_hbm, dup_v),
                    (inner_t_hbm, inner_t),
                    (g_hbm, g_v),
                )
            )
        ]
        load_near = local(n2_t_hbm.at[near_half], near_t, late_sem.at[1])
        load_own = local(g_hbm.at[s_id], g_own, late_sem.at[2])
        loads[0].start()
        loads[1].start()
        load_near.start()
        for load in loads[2:]:
            load.start()
        load_own.start()
        load_mid.start()
        load_wo.start()
        load_inner = local(inner_hbm, inner_v, late_sem.at[4])
        load_wd = local(wd_hbm, wd_v, late_sem.at[5])
        load_inner.start()
        load_wd.start()

        def flat(ref):
            return ref[...].reshape(tokens, ref.shape[2])

        loads[0].wait()
        loads[1].wait()

        def quarter(part_, carry):
            span = quarter_span(part_)
            far_gu[0, span, :] = nn(wide_t[span, :], flat(dgate_v)).astype(BF)

            @pl.when(part_ == 0)
            def _():
                env.meet([sibling] + peers + mates)

            first_send(far_gu, part_).start()

            @pl.when(part_ == 0)
            def _():
                for k in range(1, shards):
                    back_copy(k).start()
                load_near.wait()

            own_gu[0, span, :] = nn(near_t[span, :], flat(dgate_v)).astype(BF)
            first_send(far_gu, part_).wait()

            @pl.when(jnp.logical_not(has_outer))
            def _():
                run_all(up_end, part_ * wide_pieces // 4, (part_ + 1) * wide_pieces // 4)

            return carry

        lax.fori_loop(0, 4, quarter, 0)
        loads[2].wait()
        far_gu[1] = nn(wide_t[...], flat(dup_v)).astype(BF)
        core_send(1, far_gu.at[1]).start()
        own_gu[1] = nn(near_t[...], flat(dup_v)).astype(BF)
        core_send(1, far_gu.at[1]).wait()
        ends_up(4, 8)
        loads[3].wait()
        loads[4].wait()
        far_dn[...] = nn(inner_t[...], g_v[:, :, far_half].reshape(tokens, half)).astype(BF)
        core_send(2, far_dn).start()
        own_dn[...] = nn(inner_t[...], g_v[:, :, near_half].reshape(tokens, half)).astype(BF)
        ring(0)
        core_send(2, far_dn).wait()
        load_inner.wait()
        load_wd.wait()

        def part_keep(k):
            return local(stage_v.at[k % 2], parts_hbm.at[k], late_sem.at[6 + k % 2])

        def project(k, carry):
            @pl.when(k >= 2)
            def _():
                part_keep(k - 2).wait()

            stage_v[k % 2] = nn(inner_v[k], wd_v[...]).astype(BF)
            part_keep(k).start()
            return carry

        lax.fori_loop(0, shards, project, 0)
        for k in range(shards - 2, shards):
            part_keep(k).wait()
        ring(1)
        own_back = local(back_hbm.at[s_id], g_v.at[0], load_sem.at[shards - 1])
        own_back.start()
        stage = []
        for k in range(1, shards):
            if k == shards - 1:
                ring(2)
            back_copy(k).wait()
            stage.append(local(b_zone.at[k - 1], g_v.at[k], load_sem.at[k - 1]))
            stage[-1].start()
        own_back.wait()
        total = g_v[0].astype(F32)
        for k in range(1, shards):
            stage[k - 1].wait()
            total = total + g_v[k].astype(F32)
        load_mid.wait()
        load_own.wait()
        hidden = mid_ref[...]
        scale = lax.rsqrt(jnp.mean(hidden * hidden, -1, keepdims=True) + EPSILON)
        scaled = total * gains_ref[1:2, :]
        gn_own[1:2, :] = jnp.sum(total * hidden * scale, 0, keepdims=True)
        gm[...] = (
            g_own[...].astype(F32)
            + scale * scaled
            - hidden * (scale * scale * scale) * jnp.mean(scaled * hidden, -1, keepdims=True)
        )

    v = pltpu.VMEM
    pl.run_scoped(
        feed_grads,
        v((shards, rows, width), BF),
        v((rows, width), BF),
        v((shards, rows, feed), BF),
        v((shards, rows, feed), BF),
        v((half, tokens), BF),
        v((half, tokens), BF),
        v((feed, tokens), BF),
        v((2, half, feed), BF),
        v((feed, half), BF),
        v((shards, rows, feed), BF),
        v((feed, width), BF),
        v((2, rows, width), BF),
    )

    def attention(
        wkv_buf,
        pt_buf,
        kv_buf,
        dproj,
        dop,
        delta,
        dkv,
        dq,
        dkv_own,
        g_buf,
        attn_ref,
        attn_t_ref,
        qp_ref,
        n1_t_ref,
        x_ref,
    ):
        load_wkv = local(wkv_hbm, wkv_buf, late_sem.at[0])
        load_wq = local(wq_hbm, w_buf, late_sem.at[3])
        early = [
            local(src, dst, late_sem.at[4 + i])
            for i, (src, dst) in enumerate(
                (
                    (attn_hbm, attn_ref),
                    (attn_t_hbm, attn_t_ref),
                    (qp_hbm, qp_ref),
                    (n1_t_hbm, n1_t_ref),
                    (x_hbm, x_ref),
                )
            )
        ]
        for load in early:
            load.start()
        load_wkv.start()
        total_steps = 2 * HK * blocks

        def pt_copy(step, slot):
            pair, block = step // blocks, step % blocks
            span = pl.ds(pl.multiple_of(block * 1024, 1024), 1024)
            return local(pt_hbm.at[pair, span], pt_buf.at[slot], pt_sem.at[slot])

        def kv_copy(step, slot):
            pair, block = step // blocks, step % blocks
            span = pl.ds(pl.multiple_of(block * 1024, 1024), 1024)
            return local(kv_hbm.at[pair, span], kv_buf.at[slot], kv_sem.at[slot])

        pt_copy(0, 0).start()
        kv_copy(0, 0).start()

        def core_part(grad, box, slot):
            far = pl.ds(pl.multiple_of((1 - c_id) * own_rows, 16), own_rows)
            return remote(grad.at[:, far, :], box, g_core.at[slot], g_core.at[3 + slot], sibling)

        def scatter_part(grad, box, zone, slot):
            core_part(grad, box, slot).wait()
            near = pl.ds(pl.multiple_of(c_id * own_rows, 16), own_rows)

            def body(s, carry):
                add_rows(box.at[s], [grad.at[s, near], box.at[s]], own_rows, slab)
                return carry

            lax.fori_loop(0, shards, body, 0)
            for k in range(1, shards):
                scatter_copy(box, zone, slot, k).start()

        def scatter_copy(box, zone, slot, k):
            return remote(
                box.at[peer_of(s_id, shards, k, False)],
                zone.at[k - 1],
                g_send.at[slot],
                g_recv.at[slot],
                peers[k - 1],
            )

        def gather_part(box, zone, slot):
            remote(zone, zone, g_send.at[slot], g_recv.at[slot], peers[0]).wait()
            add_rows(
                box.at[s_id],
                [box.at[s_id]] + [zone.at[k] for k in range(shards - 1)],
                own_rows,
                slab,
            )

        def line_up(mine, came, total, slot, count, group):
            @pl.when(has_outer)
            def _():
                remote(mine, came, a_up.at[group], a_r.at[slot], inner_to).wait_recv()
                add_rows(mine, [mine, came], count, slab if mine.dtype == BF else 2)

            @pl.when(is_mid)
            def _():
                remote(mine, total, a_up.at[group], a_t.at[slot], inner_to).start()

            @pl.when(jnp.logical_not(is_mid))
            def _():
                remote(mine, came, a_up.at[group], a_r.at[slot], inner_to).start()

        def line_down(mine, total, slot, count, group, ready, outs):
            remote(mine, total, a_up.at[group], a_t.at[slot], inner_to).wait_recv()

            @pl.when(is_mid)
            def _():
                add_rows(total, [mine, total], count, slab if mine.dtype == BF else 2)

            @pl.when(has_outer)
            def _():
                remote(total, total, a_down.at[group], a_t.at[slot], outer_to).start()

            if ready is not None:
                ready()
            for src, near, far, box in outs:
                if far is not None:
                    remote(src, near, a_sib_send.at[box], a_sib_recv.at[box], sibling).start()
                local(src, near, a_local.at[box]).start()

        def line_settle(mine, total, group, outs):
            remote(mine, total, a_up.at[group], a_t.at[0], inner_to).wait_send()

            @pl.when(has_outer)
            def _():
                remote(total, total, a_down.at[group], a_t.at[0], outer_to).wait_send()

            for src, near, far, box in outs:
                if far is not None:
                    remote(src, far, a_sib_send.at[box], a_sib_recv.at[box], sibling).wait()
                local(src, near, a_local.at[box]).wait()

        lane = lanes_of(128)
        dproj[...] = gm[...].astype(BF)
        load_wo.wait()
        early[0].wait()

        def spread(head, carry):
            block = nt(
                dproj[...], w_buf[pl.ds(pl.multiple_of(head * 256, 256), 256), :]
            ).astype(BF)
            for seq in range(2):
                for two in range(2):
                    piece = block[
                        seq * 128 : seq * 128 + 128, two * 128 : two * 128 + 128
                    ].astype(F32)
                    place = seq * HK + head
                    first = jnp.where(lane >= 64, pltpu.roll(piece, 64, 1), 0.0)
                    dop[place, pl.ds(two * 256, 128), :] = first.astype(BF)
                    dop[place, pl.ds(two * 256 + 128, 128), :] = jnp.where(
                        lane >= 64, piece, 0.0
                    ).astype(BF)
                    value = attn_ref[
                        pl.ds(seq * 128, 128),
                        pl.ds(pl.multiple_of(head * 256 + two * 128, 128), 128),
                    ].astype(F32)
                    product = jnp.transpose(piece * value)
                    delta[place, :, pl.ds(two * 256, 128)] = jnp.sum(
                        product[:64], 0, keepdims=True
                    )
                    delta[place, :, pl.ds(two * 256 + 128, 128)] = jnp.sum(
                        product[64:], 0, keepdims=True
                    )
            return carry

        lax.fori_loop(0, HK, spread, 0)
        load_wq.start()
        ring(3)

        def weight_grad(left, right, grad, count):
            def body(s, carry):
                grad[s] = nn(
                    left[pl.ds(pl.multiple_of(s * part, 16), part), :], right[...]
                ).astype(BF)
                return carry

            lax.fori_loop(0, count, body, 0)

        early[1].wait()
        weight_grad(attn_t_ref, dproj, g_buf, shards)
        for load in early[2:]:
            load.wait()
        core_part(g_buf, o_x, 0).start()
        cosine, sine = cos_ref, sin_ref

        def attend(step, carry):
            slot = lax.rem(step, 2)
            pair, block = step // blocks, step % blocks

            @pl.when(step + 1 < total_steps)
            def _():
                pt_copy(step + 1, 1 - slot).start()
                kv_copy(step + 1, 1 - slot).start()

            pt_copy(step, slot).wait()
            kv_copy(step, slot).wait()
            keyval = kv_buf[slot]
            soft = pt_buf[slot]
            grad_soft = nt(keyval, dop[pair])
            score = (soft.astype(F32) * (grad_soft - delta[pair])).astype(BF)
            both = (nn(score, qp_ref[pair]) + nn(soft, dop[pair])).astype(BF)
            for sub in range(8):
                dkv[pair, block * 4 + sub // 2, sub % 2] = both[sub * 128 : sub * 128 + 128]
            query = tn(keyval, score)[:64] * (1.0 / math.sqrt(HD))
            seq, head = pair // HK, pair % HK
            for two in range(2):
                piece = jnp.transpose(
                    jnp.concatenate(
                        [
                            query[:, two * 256 : two * 256 + 128],
                            query[:, two * 256 + 128 : two * 256 + 256],
                        ],
                        0,
                    )
                )
                where = (
                    pl.ds(pl.multiple_of(seq * 128, 128), 128),
                    pl.ds(pl.multiple_of(head * 256 + two * 128, 128), 128),
                )
                if blocks == 1:
                    cos = cosine[where[0], :]
                    sin = sine[where[0], :]
                    dq[where] = (piece * cos - swap_halves(piece, lane) * sin).astype(BF)
                else:
                    dq[where] = jnp.where(
                        block == 0, piece, dq[where].astype(F32) + piece
                    ).astype(dq.dtype)
            return carry

        def dkv_core_copy(seq):
            return remote(
                dkv.at[pl.ds(seq * HK, HK), :, 1 - c_id],
                dkv_x.at[pl.ds(seq * HK, HK)],
                dkv_core.at[seq],
                dkv_core.at[2 + seq],
                sibling,
            )

        def dkv_copy(seq, k):
            return remote(
                dkv_x.at[pl.ds(seq * HK, HK), lax.rem(l_id + k, line)],
                dkv_z.at[seq, k - 1],
                dkv_send.at[seq, k - 1],
                dkv_recv.at[seq, k - 1],
                mates[k - 1],
            )

        def dkv_scatter(seq):
            dkv_core_copy(seq).wait()

            def body(index, carry):
                head, place = seq * HK + index // line, index % line
                dkv_x[head, place] = (
                    dkv_x[head, place].astype(F32) + dkv[head, place, c_id].astype(F32)
                ).astype(BF)
                return carry

            lax.fori_loop(0, HK * line, body, 0)
            if not hops:
                for k in range(1, line):
                    dkv_copy(seq, k).start()
                return

            @pl.when(l_id == 0)
            def _():
                for dest in range(line - 1, 0, -1):
                    dkv_hop(seq, 0, dest).start()

            @pl.when(l_id == line - 1)
            def _():
                for dest in range(line - 1):
                    dkv_hop(seq, 1, dest).start()

        def dkv_hop(seq, way, dest):
            to = (s_id, lax.rem(l_id + (1 if way == 0 else line - 1), line), c_id)
            return remote(
                dkv_x.at[pl.ds(seq * HK, HK), dest],
                dkv_z.at[seq, way, dest],
                dkv_send.at[seq, 0],
                dkv_recv.at[seq, way * line + dest],
                to,
            )

        def dkv_hops(seq, outward):
            if not hops:
                return
            low = l_id < line // 2
            for step in range(1, line):
                for way, dest in ((0, line - step), (1, step - 1)):
                    ahead = (
                        (l_id > 0) & (l_id < dest)
                        if way == 0
                        else (l_id < line - 1) & (l_id > dest)
                    )
                    turn_now = jnp.logical_not(low) if outward == (way == 0) else low

                    @pl.when(ahead & turn_now)
                    def _():
                        dkv_hop(seq, way, dest).wait_recv()
                        dkv_take(seq, way, dest)
                        dkv_hop(seq, way, dest).start()

        def dkv_take(seq, way, dest):
            def body(head, carry):
                dkv_x[seq * HK + head, dest] = (
                    dkv_x[seq * HK + head, dest].astype(F32)
                    + dkv_z[seq, way, dest, head].astype(F32)
                ).astype(BF)
                return carry

            lax.fori_loop(0, HK, body, 0)

        def dkv_arrive(seq):
            if not hops:
                for k in range(1, line):
                    dkv_copy(seq, k).wait()
                return
            sent = dkv_x.at[pl.ds(seq * HK, HK), pl.ds(0, line - 1)]
            remote(sent, sent, dkv_send.at[seq, 0], dkv_recv.at[seq, 0], mates[0]).wait_send()
            for dest in range(line):

                @pl.when((l_id == dest) & (l_id > 0))
                def _():
                    dkv_hop(seq, 0, dest).wait_recv()

                @pl.when((l_id == dest) & (l_id < line - 1))
                def _():
                    dkv_hop(seq, 1, dest).wait_recv()

        def dkv_parts(seq, head, total):
            if not hops:
                for k in range(line - 1):
                    total = total + dkv_z[seq, k, head].astype(F32)
                return total
            left = jnp.where(l_id > 0, dkv_z[seq, 0, l_id, head].astype(F32), 0.0)
            right = jnp.where(l_id < line - 1, dkv_z[seq, 1, l_id, head].astype(F32), 0.0)
            return total + left + right

        def dkv_gather(seq):
            dkv_arrive(seq)
            cos = jnp.where(lane < 64, cosine[pl.ds(seq * 128, 128), :], 1.0)
            sin = jnp.where(lane < 64, sine[pl.ds(seq * 128, 128), :], 0.0)
            for head in range(HK):
                total = dkv_x[seq * HK + head, l_id].astype(F32)
                total = dkv_parts(seq, head, total)
                dkv_own[pl.ds(seq * 128, 128), pl.ds(head * 128, 128)] = (
                    total * cos - swap_halves(total, lane) * sin
                ).astype(BF)

        near = c_id * own_rows
        far = (1 - c_id) * own_rows
        pieces = 5

        def rows_at(out, start, first, count):
            return out.at[pl.ds(pl.multiple_of(start + first, 16), count)]

        def jobs_of(box, came, total, group, outs_of):
            count = own_rows // pieces
            result = []
            for piece in range(pieces):
                span = pl.ds(piece * count, count)
                ready, outs = outs_of(total, piece * count, count)
                result.append(
                    (box.at[s_id, span], came.at[span], total.at[span], group * pieces + piece)
                    + (count, group, ready, outs)
                )
            return result

        def plain(out, box):
            def outs_of(total, first, count):
                return None, [
                    (
                        total.at[pl.ds(first, count)],
                        rows_at(out, near, first, count),
                        rows_at(out, far, first, count),
                        box,
                    )
                ]

            return outs_of

        def unpacked(total, first, count):
            span = pl.ds(first, count)

            def ready():
                value = total[span, :].astype(F32)
                for half_, start in ((0, 0), (1, HD)):
                    k_nat[half_, span, :] = jnp.concatenate(
                        [
                            value[:, head * 128 + start : head * 128 + start + HD]
                            for head in range(HK)
                        ],
                        1,
                    ).astype(BF)

            outs = [
                (
                    k_nat.at[half_, span],
                    rows_at(out, near, first, count),
                    rows_at(out, far, first, count),
                    2 + half_,
                )
                for half_, out in ((0, out_wk), (1, out_wv))
            ]
            return ready, outs

        def own_gain():
            value = gn_t[...]
            chosen = value[:, 0:part]
            for s in range(1, shards):
                chosen = jnp.where(s_id == s, value[:, s * part : (s + 1) * part], chosen)
            gn_out[...] = chosen

        o_jobs = jobs_of(o_x, o_r, o_t, 0, plain(out_wo, 0))
        q_jobs = jobs_of(q_x, q_r, q_t, 1, plain(out_wq, 1))
        k_jobs = jobs_of(k_x, k_r, k_t, 2, unpacked)
        gain_job = [
            (gn_x, gn_r, gn_t, 3 * pieces, 2, 3, own_gain, [(gn_out, out_gain, None, 4)])
        ]
        jobs = o_jobs + q_jobs + gain_job + k_jobs

        def first_up(some):
            @pl.when(jnp.logical_not(has_outer))
            def _():
                for job in some:
                    line_up(*job[:6])

        def job_up(job):
            @pl.when(has_outer)
            def _():
                line_up(*job[:6])

        def job_down(job):
            mine, _, total, slot, count, group, ready, outs = job
            line_down(mine, total, slot, count, group, ready, outs)

        lax.fori_loop(0, 2 * blocks, attend, 0)
        ring(4)
        scatter_part(g_buf, o_x, o_z, 0)
        lax.fori_loop(2 * blocks, HK * blocks, attend, 0)
        dkv_core_copy(0).start()
        ring(5)
        lax.fori_loop(HK * blocks, (HK + 2) * blocks, attend, 0)
        dkv_scatter(0)
        lax.fori_loop((HK + 2) * blocks, total_steps, attend, 0)
        dkv_core_copy(1).start()
        if blocks > 1:
            for two in range(width // 128):
                for seq in range(2):
                    where = (pl.ds(seq * 128, 128), pl.ds(two * 128, 128))
                    piece = dq[where].astype(F32)
                    cos = cosine[where[0], :]
                    sin = sine[where[0], :]
                    dq[where] = (piece * cos - swap_halves(piece, lane) * sin).astype(dq.dtype)
        ring(6)
        weight_grad(n1_t_ref, dq, g_buf, shards)
        core_part(g_buf, q_x, 1).start()
        dkv_scatter(1)
        ends_up(8, turns)
        ring(7, 16)
        dkv_hops(0, False)
        scatter_part(g_buf, q_x, q_z, 1)
        ring_down(5)
        ring_down(6)
        dkv_hops(1, False)
        gather_part(o_x, o_z, 0)
        first_up(o_jobs)
        dkv_hops(0, True)
        dkv_hops(1, True)
        ring_down(7)
        load_wq.wait()
        load_wkv.wait()
        back = nt(dq[...], w_buf[...])
        ends_down(0, 3)
        ring(8, 16)
        dkv_gather(0)
        dkv_gather(1)
        g_kv = g_buf.at[:, :, pl.ds(0, 2 * HK * HD)]
        weight_grad(n1_t_ref, dkv_own, g_kv, shards)
        core_part(g_kv, k_x, 2).start()
        back = back + nt(dkv_own[...], wkv_buf[...])
        scatter_part(g_kv, k_x, k_z, 2)
        ring(9, 1)
        hidden = x_ref[...].astype(F32)
        scale = lax.rsqrt(jnp.mean(hidden * hidden, -1, keepdims=True) + EPSILON)
        scaled = back * gains_ref[0:1, :]
        gn_own[0:1, :] = jnp.sum(back * hidden * scale, 0, keepdims=True)
        gain_core = remote(gn_own, gn_x, g_core.at[6], g_core.at[7], sibling)
        gain_core.start()
        x_ref[...] = (
            gm[...]
            + scale * scaled
            - hidden * (scale * scale * scale) * jnp.mean(scaled * hidden, -1, keepdims=True)
        ).astype(BF)
        keep_dx = local(x_ref, out_dx, late_sem.at[1])
        keep_dx.start()
        gain_core.wait()
        gn_own[...] = gn_own[...] + gn_x[...]

        def gain_copy(k):
            return remote(
                gn_own, gn_z.at[k - 1], g_send.at[3], g_recv.at[3], peers[k - 1]
            )

        for k in range(1, shards):
            gain_copy(k).start()
        for k in range(1, shards):
            part_copy(k).start()

        def gather_gain():
            remote(gn_z, gn_z, g_send.at[3], g_recv.at[3], peers[0]).wait()
            total = gn_own[...]
            for k in range(shards - 1):
                total = total + gn_z[k]
            gn_x[...] = total

        @pl.when(jnp.logical_not(has_outer))
        def _():
            gather_part(q_x, q_z, 1)
            for job in q_jobs:
                line_up(*job[:6])
            gather_gain()
            gather_part(k_x, k_z, 2)
            for job in gain_job + k_jobs:
                line_up(*job[:6])

        @pl.when(has_outer)
        def _():
            ring(10, 1)
            ring(11, 1)

        ends_down(3, 8)
        def finish_result():
            remote(p_zone, p_zone, p_send.at[0], p_recv.at[0], peers[0]).wait()
            result = mid_ref[...]
            for first in range(0, shards, 4):
                stage = [
                    local(
                        parts_hbm.at[s_id] if k == 0 else p_zone.at[k - 1],
                        w_buf.at[pl.ds((k - first) * rows, rows)],
                        load_sem.at[k - first],
                    )
                    for k in range(first, min(shards, first + 4))
                ]
                for copy in stage:
                    copy.start()
                for k, copy in enumerate(stage):
                    copy.wait()
                    result = result + w_buf[k * rows : (k + 1) * rows, :].astype(F32)
            dproj[...] = result.astype(BF)
            local(dproj, out_result, late_sem.at[2]).start()

        todo = list(jobs)
        done = []

        def next_up():
            done.append(todo.pop(0))
            job_up(done[-1])

        def last_chunk(index):
            @pl.when(is_mid)
            def _():
                down(index)

        next_up()
        next_up()
        last_chunk(2 * turns - 2)
        next_up()
        last_chunk(2 * turns - 1)
        next_up()

        @pl.when(has_outer)
        def _():
            gather_part(q_x, q_z, 1)
            gather_gain()
            gather_part(k_x, k_z, 2)

        ends_down(8, turns)

        @pl.when(jnp.logical_not(has_outer))
        def _():
            finish_result()

        while todo:
            next_up()
            job_down(done.pop(0))
        for job in done:
            job_down(job)

        @pl.when(has_outer)
        def _():
            finish_result()

        whole = [
            (o_x.at[s_id], o_t, [(o_t, out_wo, 0)]),
            (q_x.at[s_id], q_t, [(q_t, out_wq, 1)]),
            (k_x.at[s_id], k_t, [(k_nat.at[0], out_wk, 2), (k_nat.at[1], out_wv, 3)]),
        ]
        for group, (mine, total, outs) in enumerate(whole):
            line_settle(
                mine,
                total,
                group,
                [
                    (src, rows_at(out, near, 0, own_rows), rows_at(out, far, 0, own_rows), box)
                    for src, out, box in outs
                ],
            )
        line_settle(gn_x, gn_t, 3, [(gn_out, out_gain, None, 4)])
        keep_dx.wait()
        local(dproj, out_result, late_sem.at[2]).wait()

    pl.run_scoped(
        attention,
        v((width, 2 * HK * HD), BF),
        v((2, 1024, 512), BF),
        v((2, 1024, 128), BF),
        v((rows, width), BF),
        v((2 * HK, 512, 128), BF),
        v((2 * HK, 1, 512), F32),
        v((2 * HK, line, 2, 128, 128), BF),
        v((rows, width), BF if blocks == 1 else F32),
        v((rows, 2 * HK * HD), BF),
        v((shards, part, width), BF),
        v((rows, width), BF),
        v((width, rows), BF),
        v((2 * HK, 512, 128), BF),
        v((width, rows), BF),
        v((rows, width), BF),
    )

    for array in range(3):
        settle(array)


def backward_call(shards, line, *arrays):
    x, kv, gate = arrays[7], arrays[-1], arrays[15]
    rows, width = x.shape
    keys = kv.shape[1]
    feed = gate.shape[2]
    part = width // shards
    own_rows = part // 2
    kv_width = 2 * HK * HD
    sizes = (shards, line, keys, rows, width, feed)
    dma = pltpu.SemaphoreType.DMA
    v = pltpu.VMEM
    vm = pl.BlockSpec(memory_space=pltpu.VMEM)
    hbm = pl.BlockSpec(memory_space=pltpu.HBM)
    half = width // 2
    shape = jax.ShapeDtypeStruct

    def boxes(cols):
        return [
            v((shards, own_rows, cols), BF),
            v((shards - 1, own_rows, cols), BF),
            v((own_rows, cols), BF),
            v((own_rows, cols), BF),
        ]

    scratch = [
        v((width, width), BF),
        v((rows, width), F32),
        v((rows, width), F32),
        v((2 * HK, line, 128, 128), BF),
        v((2, 2, 4, HK, 128, 128) if line == 4 else (2, line - 1, HK, 128, 128), BF),
        *[v((2, half, feed), BF) for _ in range(4)],
        *[v((feed, half), BF) for _ in range(4)],
        *boxes(width),
        *boxes(width),
        *boxes(kv_width),
        v((2, width), F32),
        v((2, width), F32),
        v((shards - 1, 2, width), F32),
        v((2, width), F32),
        v((2, width), F32),
        v((2, own_rows, HK * HD), BF),
        v((2, part), F32),
        dma((max(6, shards),)),
        dma((2,)),
        dma((2,)),
        dma((6,)),
        dma((8,)),
        dma((3,)),
        dma((24,)),
        dma((24,)),
        *[dma((3,)) for _ in range(4)],
        dma((4,)),
        dma((2, 1 if line == 4 else line)),
        dma((2, 2 * line)),
        dma((8,)),
        dma((4,)),
        dma((4,)),
        dma((4,)),
        dma((16,)),
        dma((16,)),
        dma((4,)),
        dma((4,)),
        dma((4,)),
        dma((5,)),
        dma((1,)),
        dma((1,)),
        dma((shards - 1,)),
        dma((shards - 1,)),
        dma((9,)),
    ]
    return pl.pallas_call(
        lambda *refs: backward_kernel(sizes, *refs),
        out_shape=(
            shape((width, feed), BF),
            shape((width, feed), BF),
            shape((feed, width), BF),
            shape((part, width), BF),
            shape((part, width), BF),
            shape((part, HK * HD), BF),
            shape((part, HK * HD), BF),
            shape((2, part), F32),
            shape((rows, width), BF),
            shape((rows, width), BF),
            shape((shards, rows, width), BF),
            shape((shards - 1, rows, width), BF),
            shape((shards - 1, rows, width), BF),
        ),
        in_specs=[vm] * 3 + [hbm] * 19,
        out_specs=tuple([hbm] * 13),
        scratch_shapes=scratch,
        compiler_params=pltpu.CompilerParams(
            collective_id=3, has_side_effects=True, vmem_limit_bytes=VMEM_LIMIT
        ),
        name="backward",
    )(*arrays)


def per_device(
    tokens,
    cotangent,
    positions,
    lengths,
    attn_gain,
    w_query,
    w_key,
    w_value,
    w_out,
    mlp_gain,
    w_gate,
    w_up,
    w_down,
):
    seqs, stretch, width = tokens.shape
    shards, line = lax.axis_size("shard"), lax.axis_size("line")
    rows = seqs * stretch
    frequency = ROPE_BASE ** (-np.arange(HD // 2, dtype=np.float32) * 2.0 / HD)
    frequency = np.tile(frequency, 4)[None].astype(np.float32)
    x = tokens.reshape(rows, width)
    (
        gains,
        cos_wide,
        sin_wide,
        wq_all,
        wkv_all,
        out_all,
        packed_kv,
        soft,
        grad_all,
        attn,
        attn_t,
        norm_t,
        packed_q,
        middle,
        inner,
        back,
        norm_all_t,
        inner_t,
        grad_gate,
        grad_up,
    ) = front_call(
        shards,
        line,
        positions,
        lengths,
        frequency,
        attn_gain,
        mlp_gain,
        w_key,
        w_value,
        x,
        cotangent.reshape(rows, width),
        w_query,
        w_out,
        w_gate,
        w_up,
        w_down,
    )
    (
        sum_gate,
        sum_up,
        sum_down,
        sum_out,
        sum_query,
        sum_key,
        sum_value,
        sum_gain,
        grad_input,
        result,
        _,
        _,
        _,
    ) = backward_call(
        shards,
        line,
        gains,
        cos_wide,
        sin_wide,
        attn,
        attn_t,
        packed_q,
        norm_t,
        x,
        middle,
        inner,
        w_down,
        back,
        norm_all_t,
        grad_all,
        inner_t,
        grad_gate,
        grad_up,
        out_all,
        wq_all,
        wkv_all,
        soft,
        packed_kv.reshape(seqs * HK, -1, 128),
    )
    arrays = [sum_gate, sum_up, sum_down, sum_query, sum_out, sum_key, sum_value]
    arrays = widen_call(sum_gain, arrays + [grad_input, result], [F32] * 7 + [BF] * 2)
    sum_gate, sum_up, sum_down, sum_query, sum_out, sum_key, sum_value = arrays[:7]
    grad_input, result, gain_one, gain_two = arrays[7:]
    return (
        result.reshape(seqs, stretch, width),
        grad_input.reshape(seqs, stretch, width),
        gain_one,
        sum_query,
        sum_key,
        sum_value,
        sum_out,
        gain_two,
        sum_gate,
        sum_up,
        sum_down,
    )


def solution(mesh):
    shards, ctx = mesh.devices.shape
    inner = Mesh(mesh.devices.reshape(shards, ctx // 2, 2), ("shard", "line", "core"))
    where = ("line", "core")
    return jax.shard_map(
        per_device,
        mesh=inner,
        in_specs=(
            P("shard", where, None),
            P("shard", where, None),
            P("shard", None),
            P("shard"),
            P("shard"),
            P("shard", None),
            P("shard", None),
            P("shard", None),
            P("shard", None),
            P("shard"),
            P(None, "shard"),
            P(None, "shard"),
            P("shard", None),
        ),
        out_specs=(
            P("shard", where, None),
            P("shard", where, None),
            P("shard"),
            P("shard", None),
            P("shard", None),
            P("shard", None),
            P("shard", None),
            P("shard"),
            P(None, "shard"),
            P(None, "shard"),
            P("shard", None),
        ),
        check_vma=False,
    )
```

```python
import math

import jax
import jax.numpy as jnp
import numpy as np
from jax import lax
from jax.experimental import pallas as pl
from jax.experimental.pallas import tpu as pltpu
from jax.sharding import Mesh
from jax.sharding import PartitionSpec as P

HQ = 20
HK = 5
HD = 64
GROUP = HQ // HK
EPSILON = 1e-05
NEGATIVE = -1e30
ROPE_BASE = 10000.0
BF = jnp.bfloat16
F32 = jnp.float32
BY_MESH = pl.DeviceIdType.MESH
VMEM_LIMIT = 67043328


def nn(a, b):
    return lax.dot_general(a, b, (((1,), (0,)), ((), ())), preferred_element_type=F32)


def nt(a, b):
    return lax.dot_general(a, b, (((1,), (1,)), ((), ())), preferred_element_type=F32)


def tn(a, b):
    return lax.dot_general(a, b, (((0,), (0,)), ((), ())), preferred_element_type=F32)


def lanes_of(rows):
    return lax.broadcasted_iota(jnp.int32, (rows, 128), 1)


def swap_halves(block, lane):
    left = pltpu.roll(block, 96, 1)
    right = pltpu.roll(block, 32, 1)
    return jnp.where(lane % 64 < 32, left, right)


def peer_of(s_id, shards, k, back):
    if shards == 4:
        if isinstance(k, int):
            return [s_id, s_id + 1 - 2 * (s_id % 2), (s_id + 2) % 4, 3 - s_id][k]
        return jnp.where(
            k == 0,
            s_id,
            jnp.where(
                k == 1, s_id + 1 - 2 * (s_id % 2), jnp.where(k == 2, (s_id + 2) % 4, 3 - s_id)
            ),
        )
    return (s_id + (shards - k if back else k)) % shards


class Spread:
    def __init__(self, env, block, source, sems, shared, size):
        self.env, self.block, self.source, self.shared = env, block, source, shared
        self.size = size
        self.send, self.recv, self.sib_send, self.sib_recv = sems
        self.relay = env.shards == 4

    def copy(self, k):
        env = self.env
        return env.remote(
            self.source,
            self.block(env.s_id, env.c_id, 0, 2),
            self.send.at[0],
            self.recv.at[k],
            env.peer(k),
        )

    def passing(self, k):
        env = self.env
        piece = self.block(env.origin(k), env.c_id, k - 1, 1)
        return env.remote(
            piece, piece, self.send.at[0], self.recv.at[2 + k], env.peer(3 - k)
        )

    def direct(self):
        return range(1, 3 if self.relay else self.env.shards)

    def start(self):
        for k in self.direct():
            self.copy(k).start()

    def sib_copy(self, k):
        piece = self.block(self.env.origin(k), self.env.c_id, 0, 2)
        return self.env.remote(
            piece, piece, self.sib_send.at[0], self.sib_recv.at[k], self.env.sibling
        )

    def forward(self):
        for k in self.direct():
            self.copy(k).wait_recv()
            if self.relay:
                self.passing(k).start()
            if self.shared:
                self.sib_copy(k).start()

    def collect(self):
        if self.relay:
            for k in (1, 2):
                self.passing(k).wait_recv()
            if self.shared:
                self.sib_copy(3).start()

    def finish(self):
        if self.shared:
            for k in range(1, self.env.shards):
                self.sib_copy(k).wait_recv()

    def settle(self):
        env = self.env
        piece = self.size(env.shards - 1)
        env.remote(piece, piece, self.send.at[0], self.recv.at[0], env.peer(1)).wait_send()
        if self.shared:
            env.remote(
                piece, piece, self.sib_send.at[0], self.sib_recv.at[0], env.sibling
            ).wait_send()


class Env:
    def __init__(self, shards, line):
        self.shards, self.line = shards, line
        self.s_id = lax.axis_index("shard")
        self.l_id = lax.axis_index("line")
        self.c_id = lax.axis_index("core")
        self.sibling = (self.s_id, self.l_id, 1 - self.c_id)

    def remote(self, src, dst, send, recv, to):
        return pltpu.make_async_remote_copy(
            src, dst, send, recv, device_id=to, device_id_type=BY_MESH
        )

    def peer(self, k):
        return (peer_of(self.s_id, self.shards, k, False), self.l_id, self.c_id)

    def origin(self, k):
        return peer_of(self.s_id, self.shards, k, True)

    def mate(self, k):
        return (self.s_id, lax.rem(self.l_id + k, self.line), self.c_id)

    def greet(self, others):
        barrier = pltpu.get_barrier_semaphore()
        for other in others:
            pl.semaphore_signal(barrier, inc=1, device_id=other, device_id_type=BY_MESH)

    def meet(self, others):
        pl.semaphore_wait(pltpu.get_barrier_semaphore(), len(others))

    def barrier(self, others):
        self.greet(others)
        self.meet(others)


def front_kernel(
    sizes,
    positions_ref,
    lengths_ref,
    freq_ref,
    gain_one_ref,
    gain_two_ref,
    wk_ref,
    wv_ref,
    x_hbm,
    g_hbm,
    wq_ref,
    wo_ref,
    wg_hbm,
    wu_hbm,
    wd_hbm,
    out_gains,
    cos_ref,
    sin_ref,
    out_wq,
    out_wkv,
    out_wo,
    out_kv,
    out_pt,
    out_g,
    keep_attn,
    keep_attn_t,
    keep_n1_t,
    keep_qp,
    keep_mid,
    out_inner,
    out_back,
    out_n2_t,
    out_inner_t,
    out_dgate,
    out_dup,
    wq_all,
    wkv_all,
    wo_all,
    kv_all,
    n2_all,
    g_all,
    wg,
    wu,
    wd,
    out_attn,
    out_attn_t,
    out_n1_t,
    out_qp,
    out_mid,
    norm,
    x_ref,
    bias_ref,
    pt_stage,
    gains_ref,
    gain_zone,
    gain_send,
    gain_recv,
    wq_s,
    wq_r,
    wq_ss,
    wq_sr,
    wkv_s,
    wkv_r,
    wkv_ss,
    wkv_sr,
    wo_s,
    wo_r,
    wo_ss,
    wo_sr,
    g_s,
    g_r,
    n2_send,
    n2_recv,
    kv_send,
    kv_recv,
    kv_sib_send,
    kv_sib_recv,
    pt_sem,
    in_sem,
    load_sem,
    keep_sem,
    part_sem,
    back_sem,
    out_sem,
):
    shards, line, keys, rows, width, feed = sizes
    env = Env(shards, line)
    s_id, l_id, c_id = env.s_id, env.l_id, env.c_id
    part = width // shards
    hp = part // 2
    quarter = hp // 2
    blocks = keys // 1024
    load_g = pltpu.make_async_copy(g_hbm, g_all.at[s_id], in_sem.at[0])
    load_g.start()
    loads = [
        pltpu.make_async_copy(src, dst, load_sem.at[i])
        for i, (src, dst) in enumerate(((wg_hbm, wg), (wu_hbm, wu), (wd_hbm, wd)))
    ]
    for head in range(HK):
        both = jnp.concatenate(
            [ref[:, head * HD : head * HD + HD].astype(F32) for ref in (wk_ref, wv_ref)], 1
        )
        wkv_all[pl.ds(pl.multiple_of(s_id * part, 16), part), head * 128 : head * 128 + 128] = (
            both.astype(BF)
        )
    gains_ref[0:1, :] = gain_one_ref[...].astype(F32).reshape(1, part)
    gains_ref[1:2, :] = gain_two_ref[...].astype(F32).reshape(1, part)
    gains_ref[2:8, :] = jnp.zeros((6, part), F32)
    env.barrier(
        [env.sibling]
        + [env.peer(k) for k in range(1, shards)]
        + [env.mate(k) for k in range(1, line)]
    )

    def tokens_of(ref):
        def block(s, core, first, count):
            return ref.at[s, pl.ds(first * (rows // 2), count * (rows // 2))]

        return block

    def first_tokens(ref):
        return lambda count: ref.at[pl.ds(0, count)]

    def first_rows(ref):
        return lambda count: ref.at[pl.ds(0, count * hp)]

    grad_gather = Spread(
        env,
        tokens_of(g_all),
        g_all.at[s_id],
        (g_s, g_r, None, None),
        False,
        first_tokens(g_all),
    )
    n2_gather = Spread(
        env,
        tokens_of(n2_all),
        n2_all.at[s_id],
        (n2_send, n2_recv, None, None),
        False,
        first_tokens(n2_all),
    )

    def rows_of(ref):
        def block(s, core, first, count):
            start = s * part + core * hp + first * quarter
            return ref.at[pl.ds(pl.multiple_of(start, 16), count * quarter)]

        return block


    mine = pl.ds(pl.multiple_of(c_id * hp, 16), hp)
    own = pl.ds(pl.multiple_of(s_id * part, 16), part)
    kv_mine = pl.ds(pl.multiple_of(s_id * part + c_id * hp, 16), hp)
    kv_gather = Spread(
        env,
        rows_of(wkv_all),
        wkv_all.at[kv_mine],
        (wkv_s, wkv_r, wkv_ss, wkv_sr),
        True,
        first_rows(wkv_all),
    )
    q_gather = Spread(
        env,
        rows_of(wq_all),
        wq_ref.at[mine],
        (wq_s, wq_r, wq_ss, wq_sr),
        True,
        first_rows(wq_all),
    )
    o_gather = Spread(
        env,
        rows_of(wo_all),
        wo_ref.at[mine],
        (wo_s, wo_r, wo_ss, wo_sr),
        True,
        first_rows(wo_all),
    )
    outs = [
        pltpu.make_async_copy(src, dst, keep_sem.at[i])
        for i, (src, dst) in enumerate(
            (
                (wkv_all, out_wkv),
                (wq_all, out_wq),
                (kv_all, out_kv),
                (wo_all, out_wo),
                (out_attn, keep_attn),
                (out_attn_t, keep_attn_t),
                (out_n1_t, keep_n1_t),
                (out_qp, keep_qp),
                (out_mid, keep_mid),
            )
        )
    ]

    def attention_part():
        load_x = pltpu.make_async_copy(x_hbm, x_ref, in_sem.at[3])
        load_x.start()
        def gain_copy(k):
            return env.remote(
                gains_ref, gain_zone.at[s_id], gain_send.at[k], gain_recv.at[k], env.peer(k)
            )

        for k in range(1, shards):
            gain_copy(k).start()
        kv_gather.start()
        locals_ = [
            pltpu.make_async_copy(wq_ref, wq_all.at[own], in_sem.at[1]),
            pltpu.make_async_copy(wo_ref, wo_all.at[own], in_sem.at[2]),
        ]
        for copy in locals_:
            copy.start()
        gain_zone[s_id] = gains_ref[...]
        lane = lanes_of(128)
        place = pl.ds(pl.multiple_of((l_id * 2 + c_id) * 128, 128), 128)
        spots = positions_ref[:, place].astype(F32)
        good = [
            jnp.where(positions_ref[seq : seq + 1, place] < lengths_ref[seq], 1.0, 0.0).astype(F32)
            for seq in range(2)
        ]
        info = jnp.transpose(jnp.concatenate([spots] + good + [jnp.zeros((4, 128), F32)], 0))
        for seq in range(2):
            angle = info[:, seq : seq + 1] * freq_ref[...]
            cos_ref[seq * 128 : seq * 128 + 128, :] = jnp.cos(angle)
            sine = jnp.sin(angle)
            sin_ref[seq * 128 : seq * 128 + 128, :] = jnp.where(lane % 64 < 32, -sine, sine)
        load_x.wait()
        hidden = x_ref[...].astype(F32)
        scale = lax.rsqrt(jnp.mean(hidden * hidden, -1, keepdims=True) + EPSILON)
        for k in range(1, shards):
            gain_copy(k).wait()
        out_gains[...] = jnp.concatenate([gain_zone[s] for s in range(shards)], 1)
        norm[...] = (hidden * scale * out_gains[0:1, :]).astype(BF)
        kv_gather.forward()
        q_gather.start()
        for copy in locals_:
            copy.wait()
        kv_gather.collect()
        kv_gather.finish()

        spot = l_id * 2 + c_id

        def make_kv(head, carry):
            block = nn(norm[...], wkv_all[:, pl.ds(pl.multiple_of(head * 128, 128), 128)])
            for seq in range(2):
                piece = block[seq * 128 : seq * 128 + 128]
                cos = jnp.where(lane < 64, cos_ref[pl.ds(seq * 128, 128), :], 1.0)
                sin = jnp.where(lane < 64, sin_ref[pl.ds(seq * 128, 128), :], 0.0)
                kv_all[seq * HK + head, spot] = (piece * cos + swap_halves(piece, lane) * sin).astype(
                    BF
                )
            return carry

        lax.fori_loop(0, HK, make_kv, 0)

        def kv_slice(seq, l, c):
            return kv_all.at[pl.ds(seq * HK, HK), l * 2 + c]

        def kv_move(seq, way, src):
            piece = kv_slice(seq, src, c_id)
            to = (s_id, lax.rem(l_id + (1 if way == 0 else line - 1), line), c_id)
            return env.remote(
                piece, piece, kv_send.at[seq, way * line + src], kv_recv.at[seq, src], to
            )

        def kv_sib(seq, src):
            piece = kv_slice(seq, src, c_id)
            return env.remote(
                piece, piece, kv_sib_send.at[seq], kv_sib_recv.at[seq], env.sibling
            )

        def kv_onward(seq, way, src):
            @pl.when((l_id < line - 1) if way == 0 else (l_id > 0))
            def _():
                kv_move(seq, way, src).start()

        def kv_start(seq):
            for way in range(2):
                kv_onward(seq, way, l_id)
            kv_sib(seq, l_id).start()

        def kv_step(seq, far):
            for way in range(2):
                src = l_id - far if way == 0 else l_id + far

                @pl.when((src >= 0) & (src < line))
                def _():
                    kv_move(seq, way, src).wait_recv()
                    kv_onward(seq, way, src)
                    kv_sib(seq, src).start()

        def kv_finish(seq):
            piece = kv_all.at[pl.ds(seq * HK, HK), pl.ds(0, line)]
            env.remote(
                piece, piece, kv_sib_send.at[seq], kv_sib_recv.at[seq], env.sibling
            ).wait()

        def kv_settle(seq):
            for src in range(line):

                @pl.when((l_id < line - 1) & (src <= l_id))
                def _():
                    kv_move(seq, 0, src).wait_send()

                @pl.when((l_id > 0) & (src >= l_id))
                def _():
                    kv_move(seq, 1, src).wait_send()

        kv_start(0)
        for load in loads:
            load.start()
        load_g.wait()
        for seq in range(2):
            rows_ = pl.ds(seq * 128, 128)
            g_all[s_id, rows_, :] = (
                g_all[s_id, rows_, :].astype(F32) * info[:, 2 + seq : 3 + seq]
            ).astype(BF)
            for group in range(keys // 1024):
                some = jnp.concatenate(
                    [
                        positions_ref[seq : seq + 1, (group * 8 + t) * 128 : (group * 8 + t + 1) * 128]
                        for t in range(8)
                    ],
                    0,
                )
                some = jnp.where(some < lengths_ref[seq], some, 1 << 24)
                key_at = jnp.transpose(some.astype(F32))
                for t in range(8):
                    first = (group * 8 + t) * 128
                    bias_ref[seq, first : first + 128, :] = jnp.where(
                        key_at[:, t : t + 1] <= spots[seq : seq + 1, :], 0.0, NEGATIVE
                    )
        for tile in range(width // 128):
            piece = norm[:, tile * 128 : tile * 128 + 128].astype(F32)
            out_n1_t[tile * 128 : tile * 128 + 128, :] = jnp.transpose(piece).astype(BF)
        q_gather.forward()
        o_gather.start()
        kv_step(0, 1)
        if line == 2:
            kv_start(1)
        else:
            kv_step(0, 2)
            kv_start(1)
        q_gather.collect()
        q_gather.finish()

        def make_q(head, carry):
            block = nn(norm[...], wq_all[:, pl.ds(pl.multiple_of(head * 256, 256), 256)])
            for seq in range(2):
                cos = cos_ref[pl.ds(seq * 128, 128), :]
                sin = sin_ref[pl.ds(seq * 128, 128), :]
                for two in range(2):
                    piece = block[seq * 128 : seq * 128 + 128, two * 128 : two * 128 + 128]
                    piece = piece * cos + swap_halves(piece, lane) * sin
                    piece = piece.astype(BF).astype(F32) * (1.0 / math.sqrt(HD))
                    pair = seq * HK + head
                    out_qp[pair, pl.ds(two * 256, 128), :] = jnp.where(lane < 64, piece, 0.0).astype(
                        BF
                    )
                    out_qp[pair, pl.ds(two * 256 + 128, 128), :] = jnp.where(
                        lane < 64, pltpu.roll(piece, 64, 1), 0.0
                    ).astype(BF)
            return carry

        lax.fori_loop(0, HK, make_q, 0)

        def pt_copy(pair, block, slot):
            span = pl.ds(pl.multiple_of(block * 1024, 1024), 1024)
            return pltpu.make_async_copy(pt_stage.at[slot], out_pt.at[pair, span], pt_sem.at[slot])

        def keys_of(pair, block):
            if blocks == 1:
                return kv_all[pair].reshape(1024, 128)
            return kv_all[pair, pl.ds(block * 8, 8)].reshape(1024, 128)

        def scores(pair, block):
            span = pl.ds(pl.multiple_of(block * 1024, 1024), 1024)
            bias = bias_ref[pair // HK, span, :]
            return nt(keys_of(pair, block), out_qp[pair]) + jnp.concatenate([bias] * GROUP, 1)

        def attend(pair, carry):
            if blocks == 1:
                slot = lax.rem(pair, 2)

                @pl.when(pair >= 2)
                def _():
                    pt_copy(pair - 2, 0, slot).wait()

                value = scores(pair, 0)
                top = jnp.max(value, 0, keepdims=True)
                weight = jnp.exp(value - top)
                inverse = 1.0 / jnp.sum(weight, 0, keepdims=True)
                soft = (weight * inverse).astype(BF)
                pt_stage[slot] = soft
                pt_copy(pair, 0, slot).start()
                mixed = tn(keys_of(pair, 0), soft)[HD:]
            else:

                def first(block, state):
                    top, total = state
                    value = scores(pair, block)
                    new = jnp.maximum(top, jnp.max(value, 0, keepdims=True))
                    total = total * jnp.exp(top - new) + jnp.sum(
                        jnp.exp(value - new), 0, keepdims=True
                    )
                    return new, total

                top, total = lax.fori_loop(
                    0,
                    blocks,
                    first,
                    (jnp.full((1, 512), NEGATIVE, F32), jnp.zeros((1, 512), F32)),
                )
                inverse = 1.0 / total

                def second(block, mixed):
                    pt_stage[0] = (jnp.exp(scores(pair, block) - top) * inverse).astype(BF)
                    copy = pt_copy(pair, block, 0)
                    copy.start()
                    mixed = mixed + tn(keys_of(pair, block), pt_stage[0])[HD:]
                    copy.wait()
                    return mixed

                mixed = lax.fori_loop(0, blocks, second, jnp.zeros((HD, 512), F32))
            seq, head = pair // HK, pair % HK
            for two in range(2):
                both = jnp.concatenate(
                    [
                        mixed[:, two * 256 : two * 256 + 128],
                        mixed[:, two * 256 + 128 : two * 256 + 256],
                    ],
                    0,
                )
                tokens_ = pl.ds(pl.multiple_of(seq * 128, 128), 128)
                cols = pl.ds(pl.multiple_of(head * 256 + two * 128, 128), 128)
                out_attn_t[cols, tokens_] = both.astype(BF)
                out_attn[tokens_, cols] = jnp.transpose(both).astype(BF)
            return carry

        for far in range(3, line):
            kv_step(0, far)
        o_gather.forward()
        grad_gather.start()
        kv_step(1, 1)
        kv_finish(0)
        lax.fori_loop(0, 2, attend, 0)
        if line > 2:
            kv_step(1, 2)
        lax.fori_loop(2, HK, attend, 0)
        for far in range(3, line):
            kv_step(1, far)
        o_gather.collect()
        kv_finish(1)
        lax.fori_loop(HK, 2 * HK, attend, 0)
        o_gather.finish()

        def project(tile, carry):
            cols = pl.ds(pl.multiple_of(tile * 256, 256), 256)
            out_mid[:, cols] = x_ref[:, cols].astype(F32) + nn(out_attn[...], wo_all[:, cols])
            return carry

        lax.fori_loop(0, width // 256, project, 0)
        middle = out_mid[...]
        scale_two = lax.rsqrt(jnp.mean(middle * middle, -1, keepdims=True) + EPSILON)
        n2_all[s_id] = (middle * scale_two * out_gains[1:2, :]).astype(BF)
        n2_gather.start()
        grad_gather.forward()
        for copy in outs:
            copy.start()
        if blocks == 1:
            pt_copy(2 * HK - 2, 0, 0).wait()
            pt_copy(2 * HK - 1, 0, 1).wait()

        def finish():
            for gather in (kv_gather, q_gather, o_gather):
                gather.settle()
            kv_settle(0)
            kv_settle(1)
            for copy in outs:
                copy.wait()

        finishing.append(finish)

    v = pltpu.VMEM
    finishing = []
    attention_part()

    def feed_part(inner, dgate, dup, stage, grads, n2_t, inner_t):
        def back_copy(k, slot):
            return pltpu.make_async_copy(
                stage.at[slot], out_back.at[peer_of(s_id, shards, k, True)], back_sem.at[slot]
            )

        def outs(k):
            source = peer_of(s_id, shards, k, True)
            cols = pl.ds(pl.multiple_of(source * rows, 128), rows)
            return [
                pltpu.make_async_copy(n2_t.at[k], out_n2_t.at[:, cols], out_sem.at[0]),
                pltpu.make_async_copy(inner_t.at[k], out_inner_t.at[:, cols], out_sem.at[1]),
                pltpu.make_async_copy(dgate.at[source], out_dgate.at[source], out_sem.at[2]),
                pltpu.make_async_copy(dup.at[source], out_dup.at[source], out_sem.at[3]),
                pltpu.make_async_copy(g_all.at[source], out_g.at[source], out_sem.at[4]),
                pltpu.make_async_copy(inner.at[source], out_inner.at[source], out_sem.at[5]),
            ]

        def block(k, carry):
            source = peer_of(s_id, shards, k, True)
            slot = lax.rem(k, 2)
            if n2_gather.relay:

                @pl.when(k == 0)
                def _():
                    loads[2].wait()

                @pl.when(k == 3)
                def _():
                    grad_gather.collect()

                def grad_of(other, carry):
                    grads[other] = nt(g_all[peer_of(s_id, shards, other, True)], wd[...])
                    return carry

                first = jnp.where(k == 0, 0, jnp.where(k == 1, 1, 3))
                last = jnp.where(k == 0, 1, jnp.where(k == 3, 4, 3))
                lax.fori_loop(first, last, grad_of, 0)

                @pl.when(k == 1)
                def _():
                    n2_gather.forward()

                @pl.when(k == 3)
                def _():
                    n2_gather.collect()

            else:

                @pl.when(k == 0)
                def _():
                    loads[2].wait()

                @pl.when(k > 0)
                def _():
                    n2_gather.copy(k).wait_recv()

                grads[0] = nt(g_all[source], wd[...])

            normed = n2_all[source]
            n2_t[k] = jnp.transpose(normed)
            copies = outs(k)
            copies[0].start()
            copies[4].start()
            gate, upper = nn(normed, wg[...]), nn(normed, wu[...])
            grad_inner = grads[k if n2_gather.relay else 0]
            sig = 1.0 / (1.0 + jnp.exp(-gate))
            act = gate * sig
            inner[source] = (act * upper).astype(BF)
            dgate[source] = (grad_inner * upper * sig * (1.0 + gate * (1.0 - sig))).astype(BF)
            dup[source] = (grad_inner * act).astype(BF)
            for index in (2, 3, 5):
                copies[index].start()
            inner_t[k] = jnp.transpose(inner[source])
            copies[1].start()

            @pl.when(k >= 2)
            def _():
                back_copy(k - 2, slot).wait()

            stage[slot] = (nt(dgate[source], wg[...]) + nt(dup[source], wu[...])).astype(BF)
            back_copy(k, slot).start()
            return carry

        loads[0].wait()
        loads[1].wait()
        lax.fori_loop(0, shards, block, 0)
        whole = ((g_all, out_g), (inner, out_inner), (dgate, out_dgate), (dup, out_dup))
        for index, (src, dst) in zip((4, 5, 2, 3), whole):
            pltpu.make_async_copy(src, dst, out_sem.at[index]).wait()
        pltpu.make_async_copy(out_n2_t, out_n2_t, out_sem.at[0]).wait()
        pltpu.make_async_copy(out_inner_t, out_inner_t, out_sem.at[1]).wait()
        n2_gather.settle()
        grad_gather.settle()
        for last in (2, 1):
            back_copy(shards - last, (shards - last) % 2).wait()

    pl.run_scoped(
        feed_part,
        v((shards, rows, feed), BF),
        v((shards, rows, feed), BF),
        v((shards, rows, feed), BF),
        v((2, rows, width), BF),
        v((shards if shards == 4 else 1, rows, feed), F32),
        v((shards, width, rows), BF),
        v((shards, feed, rows), BF),
    )
    finishing[0]()


def front_call(shards, line, *arrays):
    positions, x, w_gate = arrays[0], arrays[7], arrays[11]
    rows, width = x.shape
    keys = positions.shape[1]
    feed = w_gate.shape[1]
    kv_width = 2 * HK * HD
    dma = pltpu.SemaphoreType.DMA
    v = pltpu.VMEM
    vm = pl.BlockSpec(memory_space=pltpu.VMEM)
    sm = pl.BlockSpec(memory_space=pltpu.SMEM)
    hbm = pl.BlockSpec(memory_space=pltpu.HBM)
    part = width // shards
    shape = jax.ShapeDtypeStruct
    hops = max(5, shards)
    return pl.pallas_call(
        lambda *refs: front_kernel((shards, line, keys, rows, width, feed), *refs),
        out_shape=(
            shape((8, width), F32),
            shape((rows, 128), F32),
            shape((rows, 128), F32),
            shape((width, width), BF),
            shape((width, kv_width), BF),
            shape((width, width), BF),
            shape((2 * HK, 2 * line, 128, 128), BF),
            shape((2 * HK, keys, 512), BF),
            shape((shards, rows, width), BF),
            shape((rows, width), BF),
            shape((width, rows), BF),
            shape((width, rows), BF),
            shape((2 * HK, 512, 128), BF),
            shape((rows, width), F32),
            shape((shards, rows, feed), BF),
            shape((shards, rows, width), BF),
            shape((width, shards * rows), BF),
            shape((feed, shards * rows), BF),
            shape((shards, rows, feed), BF),
            shape((shards, rows, feed), BF),
        ),
        in_specs=[vm, sm, vm, vm, vm, vm, vm] + [hbm] * 7,
        out_specs=(*[vm] * 3, *[hbm] * 17),
        scratch_shapes=[
            v((width, width), BF),
            v((width, kv_width), BF),
            v((width, width), BF),
            v((2 * HK, 2 * line, 128, 128), BF),
            v((shards, rows, width), BF),
            v((shards, rows, width), BF),
            v((width, feed), BF),
            v((width, feed), BF),
            v((feed, width), BF),
            v((rows, width), BF),
            v((width, rows), BF),
            v((width, rows), BF),
            v((2 * HK, 512, 128), BF),
            v((rows, width), F32),
            v((rows, width), BF),
            v((rows, width), BF),
            v((2, keys, 128), F32),
            v((2, 1024, 512), BF),
            v((8, part), F32),
            v((shards, 8, part), F32),
            dma((shards,)),
            dma((shards,)),
            *[dma((n,)) for n in (1, hops, 1, shards) * 3],
            *[dma((n,)) for n in (1, hops) * 2],
            dma((2, 2 * line)),
            dma((2, line)),
            dma((2,)),
            dma((2,)),
            dma((2,)),
            dma((4,)),
            dma((3,)),
            dma((9,)),
            dma((2,)),
            dma((2,)),
            dma((6,)),
        ],
        compiler_params=pltpu.CompilerParams(
            collective_id=1, has_side_effects=True, vmem_limit_bytes=VMEM_LIMIT
        ),
        name="front",
    )(*arrays)


def widen_kernel(count, gain_ref, *refs):
    src, dst = refs[:count], refs[count : 2 * count]
    out_one, out_two = refs[2 * count : 2 * count + 2]
    refs = refs[2 * count + 2 :]
    narrow, wide = refs[:count], refs[count : 2 * count]
    load_sem, store_sem = refs[2 * count :]
    out_one[...] = gain_ref[0:1, :].reshape(out_one.shape)
    out_two[...] = gain_ref[1:2, :].reshape(out_two.shape)
    for i in range(count):
        pltpu.make_async_copy(src[i], narrow[i], load_sem.at[i]).start()

    def piece(i, part, parts):
        rows = narrow[i].shape[0] // parts
        span = pl.ds(part * rows, rows)
        held = wide[i] if dst[i].dtype == F32 else narrow[i]
        return span, pltpu.make_async_copy(held.at[span], dst[i].at[span], store_sem.at[i])

    for i in range(count):
        pltpu.make_async_copy(src[i], narrow[i], load_sem.at[i]).wait()
        for part in range(2):
            span, copy = piece(i, part, 2)
            if dst[i].dtype == F32:
                wide[i][span, :] = narrow[i][span, :].astype(F32)
            copy.start()
    for i in range(count):
        piece(i, 0, 1)[1].wait()


def widen_call(gains, arrays, types):
    v = pltpu.VMEM
    hbm = pl.BlockSpec(memory_space=pltpu.HBM)
    vm = pl.BlockSpec(memory_space=pltpu.VMEM)
    count = len(arrays)
    return pl.pallas_call(
        lambda *refs: widen_kernel(count, *refs),
        out_shape=tuple(jax.ShapeDtypeStruct(a.shape, t) for a, t in zip(arrays, types))
        + (jax.ShapeDtypeStruct(gains.shape[1:], F32),) * 2,
        in_specs=[vm] + [hbm] * count,
        out_specs=tuple([hbm] * count) + (vm, vm),
        scratch_shapes=[
            *[v(a.shape, a.dtype) for a in arrays],
            *[v(a.shape if t == F32 else (16, 128), F32) for a, t in zip(arrays, types)],
            pltpu.SemaphoreType.DMA((count,)),
            pltpu.SemaphoreType.DMA((count,)),
        ],
        compiler_params=pltpu.CompilerParams(vmem_limit_bytes=VMEM_LIMIT),
        name="widen",
    )(gains, *arrays)


def add_rows(target, parts, rows, step):
    def body(index, carry):
        span = pl.ds(pl.multiple_of(index * step, step), step)
        total = parts[0][span, :].astype(F32)
        for part in parts[1:]:
            total = total + part[span, :].astype(F32)
        target[span, :] = total.astype(target.dtype)
        return carry

    lax.fori_loop(0, rows // step, body, 0)


def backward_kernel(
    sizes,
    gains_ref,
    cos_ref,
    sin_ref,
    attn_hbm,
    attn_t_hbm,
    qp_hbm,
    n1_t_hbm,
    x_hbm,
    mid_hbm,
    inner_hbm,
    wd_hbm,
    back_hbm,
    n2_t_hbm,
    g_hbm,
    inner_t_hbm,
    dgate_hbm,
    dup_hbm,
    wo_hbm,
    wq_hbm,
    wkv_hbm,
    pt_hbm,
    kv_hbm,
    out_gate,
    out_up,
    out_dn,
    out_wo,
    out_wq,
    out_wk,
    out_wv,
    out_gain,
    out_dx,
    out_result,
    parts_hbm,
    p_zone,
    b_zone,
    w_buf,
    gm,
    mid_ref,
    dkv_x,
    dkv_z,
    own_gu,
    got_gu_x,
    got_gu_r,
    got_gu_t,
    own_dn,
    got_dn_x,
    got_dn_r,
    got_dn_t,
    o_x,
    o_z,
    o_r,
    o_t,
    q_x,
    q_z,
    q_r,
    q_t,
    k_x,
    k_z,
    k_r,
    k_t,
    gn_own,
    gn_x,
    gn_z,
    gn_r,
    gn_t,
    k_nat,
    gn_out,
    load_sem,
    pt_sem,
    kv_sem,
    core_sem,
    first_sem,
    up_send,
    r_recv,
    t_recv,
    down_send,
    sib_send,
    sib_recv,
    local_sem,
    dkv_core,
    dkv_send,
    dkv_recv,
    g_core,
    g_send,
    g_recv,
    a_up,
    a_r,
    a_t,
    a_down,
    a_sib_send,
    a_sib_recv,
    a_local,
    p_send,
    p_recv,
    b_send,
    b_recv,
    late_sem,
):
    shards, line, keys, rows, width, feed = sizes
    env = Env(shards, line)
    s_id, l_id, c_id = env.s_id, env.l_id, env.c_id
    sibling, remote = env.sibling, env.remote
    toward = jnp.where(l_id < line // 2, 1, -1)
    inner_to = (s_id, l_id + toward, c_id)
    has_outer = (l_id > 0) & (l_id < line - 1)
    is_mid = (l_id == line // 2 - 1) | (l_id == line // 2)
    outer_to = (s_id, jnp.where(has_outer, l_id - toward, l_id + toward), c_id)
    peers = [env.peer(k) for k in range(1, shards)]
    mates = [env.mate(k) for k in range(1, line)]
    env.greet([sibling] + peers + mates)
    half = width // 2
    wide_pieces = 8
    down_pieces = 8 if feed % 128 == 0 else 4
    chunks = 2 * wide_pieces + down_pieces
    turns = 12
    slab = 16
    part = width // shards
    own_rows = part // 2
    blocks = keys // 1024
    tokens = shards * rows
    hops = line == 4
    near_half = pl.ds(pl.multiple_of(c_id * half, 128), half)
    far_half = pl.ds(pl.multiple_of((1 - c_id) * half, 128), half)

    def back_copy(k):
        return remote(
            back_hbm.at[peer_of(s_id, shards, k, False)],
            b_zone.at[k - 1],
            b_send.at[k - 1],
            b_recv.at[k - 1],
            peers[k - 1],
        )

    def part_copy(k):
        return remote(
            parts_hbm.at[peer_of(s_id, shards, k, False)],
            p_zone.at[k - 1],
            p_send.at[0],
            p_recv.at[0],
            peers[k - 1],
        )

    def local(src, dst, sem):
        return pltpu.make_async_copy(src, dst, sem)

    def views(index, where):
        if where != "dn":
            rows_ = half // wide_pieces
            array, piece = (0 if where == "gate" else 1), index % wide_pieces
            array_of = out_gate if where == "gate" else out_up
            span = pl.ds(pl.multiple_of(piece * rows_, 16), rows_)
            bufs = [ref.at[array, span] for ref in (own_gu, got_gu_x, got_gu_r, got_gu_t)]

            def out(core):
                start = core * half + piece * rows_
                return array_of.at[pl.ds(pl.multiple_of(start, 16), rows_)]

            return rows_, bufs, out, array
        rows_ = feed // down_pieces
        span = pl.ds(pl.multiple_of((index - 2 * wide_pieces) * rows_, 16), rows_)
        bufs = [ref.at[span] for ref in (own_dn, got_dn_x, got_dn_r, got_dn_t)]

        def out(core):
            return out_dn.at[span, pl.ds(pl.multiple_of(core * half, 128), half)]

        return rows_, bufs, out, 2

    def split(action):
        def run(index):
            if isinstance(index, int):
                if 0 <= index < chunks:
                    action(index, ("gate", "up", "dn")[min(2, index // wide_pieces)])
                return
            for number, where in enumerate(("gate", "up", "dn")):

                @pl.when(jnp.minimum(index // wide_pieces, 2) == number)
                def _():
                    action(index, where)

        return run

    def up_end(index, where):
        count, (mine, extra, came, total), _, array = views(index, where)
        add_rows(mine, [mine, extra], count, slab)
        send_up(index, mine, came, total, array)

    def up_inner(index, where):
        count, (mine, extra, came, total), _, array = views(index, where)
        remote(mine, came, up_send.at[array], r_recv.at[index], inner_to).wait_recv()
        add_rows(mine, [mine, extra, came], count, slab)
        send_up(index, mine, came, total, array)

    def send_up(index, mine, came, total, array):
        @pl.when(is_mid)
        def _():
            remote(mine, total, up_send.at[array], t_recv.at[index], inner_to).start()

        @pl.when(jnp.logical_not(is_mid))
        def _():
            remote(mine, came, up_send.at[array], r_recv.at[index], inner_to).start()

    def down(index, where):
        count, (mine, _, _, total), out, array = views(index, where)
        remote(mine, total, up_send.at[array], t_recv.at[index], inner_to).wait_recv()

        @pl.when(is_mid)
        def _():
            add_rows(total, [mine, total], count, slab)

        @pl.when(has_outer)
        def _():
            remote(total, total, down_send.at[array], t_recv.at[index], outer_to).start()

        remote(total, out(c_id), sib_send.at[array], sib_recv.at[array], sibling).start()
        local(total, out(c_id), local_sem.at[array]).start()

    def settle(array):
        if array < 2:
            mine, total = own_gu.at[array], got_gu_t.at[array]
            out_of = (out_gate, out_up)[array]
            outs = [
                out_of.at[pl.ds(pl.multiple_of(core * half, 16), half)]
                for core in (c_id, 1 - c_id)
            ]
        else:
            mine, total = own_dn, got_dn_t
            outs = [
                out_dn.at[:, pl.ds(pl.multiple_of(core * half, 128), half)]
                for core in (c_id, 1 - c_id)
            ]
        remote(mine, total, up_send.at[array], t_recv.at[0], inner_to).wait_send()

        @pl.when(has_outer)
        def _():
            remote(total, total, down_send.at[array], t_recv.at[0], outer_to).wait_send()

        remote(total, outs[1], sib_send.at[array], sib_recv.at[array], sibling).wait()
        local(total, outs[0], local_sem.at[array]).wait()

    up_end, up_inner, down = [split(f) for f in (up_end, up_inner, down)]

    def of_turns(first, last):
        return min(2 * first, chunks), min(2 * last, chunks)

    def run_all(action, first, last):
        def body(index, carry):
            action(index)
            return carry

        lax.fori_loop(first, last, body, 0)

    def ends_up(first, last):
        @pl.when(jnp.logical_not(has_outer))
        def _():
            run_all(up_end, *of_turns(first, last))

    def ring(turn, lag=2):
        for step in (2 * turn, 2 * turn + 1):
            if step < chunks:

                @pl.when(has_outer)
                def _():
                    up_inner(step)

            if 0 <= step - 2 * lag < chunks:

                @pl.when(is_mid)
                def _():
                    down(step - 2 * lag)

    def ring_down(turn):
        @pl.when(is_mid)
        def _():
            run_all(down, *of_turns(turn, turn + 1))

    def ends_down(first, last):
        @pl.when(jnp.logical_not(is_mid))
        def _():
            run_all(down, *of_turns(first, last))

    def quarter_span(part_):
        return pl.ds(pl.multiple_of(part_ * (half // 4), 16), half // 4)

    def first_send(src, part_):
        span = quarter_span(part_)
        return remote(
            src.at[0, span],
            got_gu_x.at[0, span],
            first_sem.at[part_],
            first_sem.at[4 + part_],
            sibling,
        )

    def core_send(array, src):
        dst = got_gu_x.at[array] if array < 2 else got_dn_x
        return remote(src, dst, core_sem.at[array], core_sem.at[3 + array], sibling)

    load_wo = local(wo_hbm, w_buf, late_sem.at[3])

    load_mid = local(mid_hbm, mid_ref, late_sem.at[0])

    def feed_grads(
        g_v, g_own, dgate_v, dup_v, wide_t, near_t, inner_t, far_gu, far_dn, inner_v, wd_v, stage_v
    ):
        loads = [
            local(src, dst, load_sem.at[i])
            for i, (src, dst) in enumerate(
                (
                    (n2_t_hbm.at[far_half], wide_t),
                    (dgate_hbm, dgate_v),
                    (dup_hbm, dup_v),
                    (inner_t_hbm, inner_t),
                    (g_hbm, g_v),
                )
            )
        ]
        load_near = local(n2_t_hbm.at[near_half], near_t, late_sem.at[1])
        load_own = local(g_hbm.at[s_id], g_own, late_sem.at[2])
        loads[0].start()
        loads[1].start()
        load_near.start()
        for load in loads[2:]:
            load.start()
        load_own.start()
        load_mid.start()
        load_wo.start()
        load_inner = local(inner_hbm, inner_v, late_sem.at[4])
        load_wd = local(wd_hbm, wd_v, late_sem.at[5])
        load_inner.start()
        load_wd.start()

        def flat(ref):
            return ref[...].reshape(tokens, ref.shape[2])

        loads[0].wait()
        loads[1].wait()

        def quarter(part_, carry):
            span = quarter_span(part_)
            far_gu[0, span, :] = nn(wide_t[span, :], flat(dgate_v)).astype(BF)

            @pl.when(part_ == 0)
            def _():
                env.meet([sibling] + peers + mates)

            first_send(far_gu, part_).start()

            @pl.when(part_ == 0)
            def _():
                for k in range(1, shards):
                    back_copy(k).start()
                load_near.wait()

            own_gu[0, span, :] = nn(near_t[span, :], flat(dgate_v)).astype(BF)
            first_send(far_gu, part_).wait()

            @pl.when(jnp.logical_not(has_outer))
            def _():
                run_all(up_end, part_ * wide_pieces // 4, (part_ + 1) * wide_pieces // 4)

            return carry

        lax.fori_loop(0, 4, quarter, 0)
        loads[2].wait()
        far_gu[1] = nn(wide_t[...], flat(dup_v)).astype(BF)
        core_send(1, far_gu.at[1]).start()
        own_gu[1] = nn(near_t[...], flat(dup_v)).astype(BF)
        core_send(1, far_gu.at[1]).wait()
        ends_up(4, 8)
        loads[3].wait()
        loads[4].wait()
        far_dn[...] = nn(inner_t[...], g_v[:, :, far_half].reshape(tokens, half)).astype(BF)
        core_send(2, far_dn).start()
        own_dn[...] = nn(inner_t[...], g_v[:, :, near_half].reshape(tokens, half)).astype(BF)
        ring(0)
        core_send(2, far_dn).wait()
        load_inner.wait()
        load_wd.wait()

        def part_keep(k):
            return local(stage_v.at[k % 2], parts_hbm.at[k], late_sem.at[6 + k % 2])

        def project(k, carry):
            @pl.when(k >= 2)
            def _():
                part_keep(k - 2).wait()

            stage_v[k % 2] = nn(inner_v[k], wd_v[...]).astype(BF)
            part_keep(k).start()
            return carry

        lax.fori_loop(0, shards, project, 0)
        for k in range(shards - 2, shards):
            part_keep(k).wait()
        ring(1)
        own_back = local(back_hbm.at[s_id], g_v.at[0], load_sem.at[shards - 1])
        own_back.start()
        stage = []
        for k in range(1, shards):
            if k == shards - 1:
                ring(2)
            back_copy(k).wait()
            stage.append(local(b_zone.at[k - 1], g_v.at[k], load_sem.at[k - 1]))
            stage[-1].start()
        own_back.wait()
        total = g_v[0].astype(F32)
        for k in range(1, shards):
            stage[k - 1].wait()
            total = total + g_v[k].astype(F32)
        load_mid.wait()
        load_own.wait()
        hidden = mid_ref[...]
        scale = lax.rsqrt(jnp.mean(hidden * hidden, -1, keepdims=True) + EPSILON)
        scaled = total * gains_ref[1:2, :]
        gn_own[1:2, :] = jnp.sum(total * hidden * scale, 0, keepdims=True)
        gm[...] = (
            g_own[...].astype(F32)
            + scale * scaled
            - hidden * (scale * scale * scale) * jnp.mean(scaled * hidden, -1, keepdims=True)
        )

    v = pltpu.VMEM
    pl.run_scoped(
        feed_grads,
        v((shards, rows, width), BF),
        v((rows, width), BF),
        v((shards, rows, feed), BF),
        v((shards, rows, feed), BF),
        v((half, tokens), BF),
        v((half, tokens), BF),
        v((feed, tokens), BF),
        v((2, half, feed), BF),
        v((feed, half), BF),
        v((shards, rows, feed), BF),
        v((feed, width), BF),
        v((2, rows, width), BF),
    )

    def attention(
        wkv_buf,
        pt_buf,
        kv_buf,
        dproj,
        dop,
        delta,
        dkv,
        dq,
        dkv_own,
        g_buf,
        attn_ref,
        attn_t_ref,
        qp_ref,
        n1_t_ref,
        x_ref,
    ):
        load_wkv = local(wkv_hbm, wkv_buf, late_sem.at[0])
        load_wq = local(wq_hbm, w_buf, late_sem.at[3])
        early = [
            local(src, dst, late_sem.at[4 + i])
            for i, (src, dst) in enumerate(
                (
                    (attn_hbm, attn_ref),
                    (attn_t_hbm, attn_t_ref),
                    (qp_hbm, qp_ref),
                    (n1_t_hbm, n1_t_ref),
                    (x_hbm, x_ref),
                )
            )
        ]
        for load in early:
            load.start()
        load_wkv.start()
        total_steps = 2 * HK * blocks

        def pt_copy(step, slot):
            pair, block = step // blocks, step % blocks
            span = pl.ds(pl.multiple_of(block * 1024, 1024), 1024)
            return local(pt_hbm.at[pair, span], pt_buf.at[slot], pt_sem.at[slot])

        def kv_copy(step, slot):
            pair, block = step // blocks, step % blocks
            span = pl.ds(pl.multiple_of(block * 1024, 1024), 1024)
            return local(kv_hbm.at[pair, span], kv_buf.at[slot], kv_sem.at[slot])

        pt_copy(0, 0).start()
        kv_copy(0, 0).start()

        def core_part(grad, box, slot):
            far = pl.ds(pl.multiple_of((1 - c_id) * own_rows, 16), own_rows)
            return remote(grad.at[:, far, :], box, g_core.at[slot], g_core.at[3 + slot], sibling)

        def scatter_part(grad, box, zone, slot):
            core_part(grad, box, slot).wait()
            near = pl.ds(pl.multiple_of(c_id * own_rows, 16), own_rows)

            def body(s, carry):
                add_rows(box.at[s], [grad.at[s, near], box.at[s]], own_rows, slab)
                return carry

            lax.fori_loop(0, shards, body, 0)
            for k in range(1, shards):
                scatter_copy(box, zone, slot, k).start()

        def scatter_copy(box, zone, slot, k):
            return remote(
                box.at[peer_of(s_id, shards, k, False)],
                zone.at[k - 1],
                g_send.at[slot],
                g_recv.at[slot],
                peers[k - 1],
            )

        def gather_part(box, zone, slot):
            remote(zone, zone, g_send.at[slot], g_recv.at[slot], peers[0]).wait()
            add_rows(
                box.at[s_id],
                [box.at[s_id]] + [zone.at[k] for k in range(shards - 1)],
                own_rows,
                slab,
            )

        def line_up(mine, came, total, slot, count, group):
            @pl.when(has_outer)
            def _():
                remote(mine, came, a_up.at[group], a_r.at[slot], inner_to).wait_recv()
                add_rows(mine, [mine, came], count, slab if mine.dtype == BF else 2)

            @pl.when(is_mid)
            def _():
                remote(mine, total, a_up.at[group], a_t.at[slot], inner_to).start()

            @pl.when(jnp.logical_not(is_mid))
            def _():
                remote(mine, came, a_up.at[group], a_r.at[slot], inner_to).start()

        def line_down(mine, total, slot, count, group, ready, outs):
            remote(mine, total, a_up.at[group], a_t.at[slot], inner_to).wait_recv()

            @pl.when(is_mid)
            def _():
                add_rows(total, [mine, total], count, slab if mine.dtype == BF else 2)

            @pl.when(has_outer)
            def _():
                remote(total, total, a_down.at[group], a_t.at[slot], outer_to).start()

            if ready is not None:
                ready()
            for src, near, far, box in outs:
                if far is not None:
                    remote(src, near, a_sib_send.at[box], a_sib_recv.at[box], sibling).start()
                local(src, near, a_local.at[box]).start()

        def line_settle(mine, total, group, outs):
            remote(mine, total, a_up.at[group], a_t.at[0], inner_to).wait_send()

            @pl.when(has_outer)
            def _():
                remote(total, total, a_down.at[group], a_t.at[0], outer_to).wait_send()

            for src, near, far, box in outs:
                if far is not None:
                    remote(src, far, a_sib_send.at[box], a_sib_recv.at[box], sibling).wait()
                local(src, near, a_local.at[box]).wait()

        lane = lanes_of(128)
        dproj[...] = gm[...].astype(BF)
        load_wo.wait()
        early[0].wait()

        def spread(head, carry):
            block = nt(
                dproj[...], w_buf[pl.ds(pl.multiple_of(head * 256, 256), 256), :]
            ).astype(BF)
            for seq in range(2):
                for two in range(2):
                    piece = block[
                        seq * 128 : seq * 128 + 128, two * 128 : two * 128 + 128
                    ].astype(F32)
                    place = seq * HK + head
                    first = jnp.where(lane >= 64, pltpu.roll(piece, 64, 1), 0.0)
                    dop[place, pl.ds(two * 256, 128), :] = first.astype(BF)
                    dop[place, pl.ds(two * 256 + 128, 128), :] = jnp.where(
                        lane >= 64, piece, 0.0
                    ).astype(BF)
                    value = attn_ref[
                        pl.ds(seq * 128, 128),
                        pl.ds(pl.multiple_of(head * 256 + two * 128, 128), 128),
                    ].astype(F32)
                    product = jnp.transpose(piece * value)
                    delta[place, :, pl.ds(two * 256, 128)] = jnp.sum(
                        product[:64], 0, keepdims=True
                    )
                    delta[place, :, pl.ds(two * 256 + 128, 128)] = jnp.sum(
                        product[64:], 0, keepdims=True
                    )
            return carry

        lax.fori_loop(0, HK, spread, 0)
        load_wq.start()
        ring(3)

        def weight_grad(left, right, grad, count):
            def body(s, carry):
                grad[s] = nn(
                    left[pl.ds(pl.multiple_of(s * part, 16), part), :], right[...]
                ).astype(BF)
                return carry

            lax.fori_loop(0, count, body, 0)

        early[1].wait()
        weight_grad(attn_t_ref, dproj, g_buf, shards)
        for load in early[2:]:
            load.wait()
        core_part(g_buf, o_x, 0).start()
        cosine, sine = cos_ref, sin_ref

        def attend(step, carry):
            slot = lax.rem(step, 2)
            pair, block = step // blocks, step % blocks

            @pl.when(step + 1 < total_steps)
            def _():
                pt_copy(step + 1, 1 - slot).start()
                kv_copy(step + 1, 1 - slot).start()

            pt_copy(step, slot).wait()
            kv_copy(step, slot).wait()
            keyval = kv_buf[slot]
            soft = pt_buf[slot]
            grad_soft = nt(keyval, dop[pair])
            score = (soft.astype(F32) * (grad_soft - delta[pair])).astype(BF)
            both = (nn(score, qp_ref[pair]) + nn(soft, dop[pair])).astype(BF)
            for sub in range(8):
                dkv[pair, block * 4 + sub // 2, sub % 2] = both[sub * 128 : sub * 128 + 128]
            query = tn(keyval, score)[:64] * (1.0 / math.sqrt(HD))
            seq, head = pair // HK, pair % HK
            for two in range(2):
                piece = jnp.transpose(
                    jnp.concatenate(
                        [
                            query[:, two * 256 : two * 256 + 128],
                            query[:, two * 256 + 128 : two * 256 + 256],
                        ],
                        0,
                    )
                )
                where = (
                    pl.ds(pl.multiple_of(seq * 128, 128), 128),
                    pl.ds(pl.multiple_of(head * 256 + two * 128, 128), 128),
                )
                if blocks == 1:
                    cos = cosine[where[0], :]
                    sin = sine[where[0], :]
                    dq[where] = (piece * cos - swap_halves(piece, lane) * sin).astype(BF)
                else:
                    dq[where] = jnp.where(
                        block == 0, piece, dq[where].astype(F32) + piece
                    ).astype(dq.dtype)
            return carry

        def dkv_core_copy(seq):
            return remote(
                dkv.at[pl.ds(seq * HK, HK), :, 1 - c_id],
                dkv_x.at[pl.ds(seq * HK, HK)],
                dkv_core.at[seq],
                dkv_core.at[2 + seq],
                sibling,
            )

        def dkv_copy(seq, k):
            return remote(
                dkv_x.at[pl.ds(seq * HK, HK), lax.rem(l_id + k, line)],
                dkv_z.at[seq, k - 1],
                dkv_send.at[seq, k - 1],
                dkv_recv.at[seq, k - 1],
                mates[k - 1],
            )

        def dkv_scatter(seq):
            dkv_core_copy(seq).wait()

            def body(index, carry):
                head, place = seq * HK + index // line, index % line
                dkv_x[head, place] = (
                    dkv_x[head, place].astype(F32) + dkv[head, place, c_id].astype(F32)
                ).astype(BF)
                return carry

            lax.fori_loop(0, HK * line, body, 0)
            if not hops:
                for k in range(1, line):
                    dkv_copy(seq, k).start()
                return

            @pl.when(l_id == 0)
            def _():
                for dest in range(line - 1, 0, -1):
                    dkv_hop(seq, 0, dest).start()

            @pl.when(l_id == line - 1)
            def _():
                for dest in range(line - 1):
                    dkv_hop(seq, 1, dest).start()

        def dkv_hop(seq, way, dest):
            to = (s_id, lax.rem(l_id + (1 if way == 0 else line - 1), line), c_id)
            return remote(
                dkv_x.at[pl.ds(seq * HK, HK), dest],
                dkv_z.at[seq, way, dest],
                dkv_send.at[seq, 0],
                dkv_recv.at[seq, way * line + dest],
                to,
            )

        def dkv_hops(seq, outward):
            if not hops:
                return
            low = l_id < line // 2
            for step in range(1, line):
                for way, dest in ((0, line - step), (1, step - 1)):
                    ahead = (
                        (l_id > 0) & (l_id < dest)
                        if way == 0
                        else (l_id < line - 1) & (l_id > dest)
                    )
                    turn_now = jnp.logical_not(low) if outward == (way == 0) else low

                    @pl.when(ahead & turn_now)
                    def _():
                        dkv_hop(seq, way, dest).wait_recv()
                        dkv_take(seq, way, dest)
                        dkv_hop(seq, way, dest).start()

        def dkv_take(seq, way, dest):
            def body(head, carry):
                dkv_x[seq * HK + head, dest] = (
                    dkv_x[seq * HK + head, dest].astype(F32)
                    + dkv_z[seq, way, dest, head].astype(F32)
                ).astype(BF)
                return carry

            lax.fori_loop(0, HK, body, 0)

        def dkv_arrive(seq):
            if not hops:
                for k in range(1, line):
                    dkv_copy(seq, k).wait()
                return
            sent = dkv_x.at[pl.ds(seq * HK, HK), pl.ds(0, line - 1)]
            remote(sent, sent, dkv_send.at[seq, 0], dkv_recv.at[seq, 0], mates[0]).wait_send()
            for dest in range(line):

                @pl.when((l_id == dest) & (l_id > 0))
                def _():
                    dkv_hop(seq, 0, dest).wait_recv()

                @pl.when((l_id == dest) & (l_id < line - 1))
                def _():
                    dkv_hop(seq, 1, dest).wait_recv()

        def dkv_parts(seq, head, total):
            if not hops:
                for k in range(line - 1):
                    total = total + dkv_z[seq, k, head].astype(F32)
                return total
            left = jnp.where(l_id > 0, dkv_z[seq, 0, l_id, head].astype(F32), 0.0)
            right = jnp.where(l_id < line - 1, dkv_z[seq, 1, l_id, head].astype(F32), 0.0)
            return total + left + right

        def dkv_gather(seq):
            dkv_arrive(seq)
            cos = jnp.where(lane < 64, cosine[pl.ds(seq * 128, 128), :], 1.0)
            sin = jnp.where(lane < 64, sine[pl.ds(seq * 128, 128), :], 0.0)
            for head in range(HK):
                total = dkv_x[seq * HK + head, l_id].astype(F32)
                total = dkv_parts(seq, head, total)
                dkv_own[pl.ds(seq * 128, 128), pl.ds(head * 128, 128)] = (
                    total * cos - swap_halves(total, lane) * sin
                ).astype(BF)

        near = c_id * own_rows
        far = (1 - c_id) * own_rows
        pieces = 5

        def rows_at(out, start, first, count):
            return out.at[pl.ds(pl.multiple_of(start + first, 16), count)]

        def jobs_of(box, came, total, group, outs_of):
            count = own_rows // pieces
            result = []
            for piece in range(pieces):
                span = pl.ds(piece * count, count)
                ready, outs = outs_of(total, piece * count, count)
                result.append(
                    (box.at[s_id, span], came.at[span], total.at[span], group * pieces + piece)
                    + (count, group, ready, outs)
                )
            return result

        def plain(out, box):
            def outs_of(total, first, count):
                return None, [
                    (
                        total.at[pl.ds(first, count)],
                        rows_at(out, near, first, count),
                        rows_at(out, far, first, count),
                        box,
                    )
                ]

            return outs_of

        def unpacked(total, first, count):
            span = pl.ds(first, count)

            def ready():
                value = total[span, :].astype(F32)
                for half_, start in ((0, 0), (1, HD)):
                    k_nat[half_, span, :] = jnp.concatenate(
                        [
                            value[:, head * 128 + start : head * 128 + start + HD]
                            for head in range(HK)
                        ],
                        1,
                    ).astype(BF)

            outs = [
                (
                    k_nat.at[half_, span],
                    rows_at(out, near, first, count),
                    rows_at(out, far, first, count),
                    2 + half_,
                )
                for half_, out in ((0, out_wk), (1, out_wv))
            ]
            return ready, outs

        def own_gain():
            value = gn_t[...]
            chosen = value[:, 0:part]
            for s in range(1, shards):
                chosen = jnp.where(s_id == s, value[:, s * part : (s + 1) * part], chosen)
            gn_out[...] = chosen

        o_jobs = jobs_of(o_x, o_r, o_t, 0, plain(out_wo, 0))
        q_jobs = jobs_of(q_x, q_r, q_t, 1, plain(out_wq, 1))
        k_jobs = jobs_of(k_x, k_r, k_t, 2, unpacked)
        gain_job = [
            (gn_x, gn_r, gn_t, 3 * pieces, 2, 3, own_gain, [(gn_out, out_gain, None, 4)])
        ]
        jobs = o_jobs + q_jobs + gain_job + k_jobs

        def first_up(some):
            @pl.when(jnp.logical_not(has_outer))
            def _():
                for job in some:
                    line_up(*job[:6])

        def job_up(job):
            @pl.when(has_outer)
            def _():
                line_up(*job[:6])

        def job_down(job):
            mine, _, total, slot, count, group, ready, outs = job
            line_down(mine, total, slot, count, group, ready, outs)

        lax.fori_loop(0, 2 * blocks, attend, 0)
        ring(4)
        scatter_part(g_buf, o_x, o_z, 0)
        lax.fori_loop(2 * blocks, HK * blocks, attend, 0)
        dkv_core_copy(0).start()
        ring(5)
        lax.fori_loop(HK * blocks, (HK + 2) * blocks, attend, 0)
        dkv_scatter(0)
        lax.fori_loop((HK + 2) * blocks, total_steps, attend, 0)
        dkv_core_copy(1).start()
        if blocks > 1:
            for two in range(width // 128):
                for seq in range(2):
                    where = (pl.ds(seq * 128, 128), pl.ds(two * 128, 128))
                    piece = dq[where].astype(F32)
                    cos = cosine[where[0], :]
                    sin = sine[where[0], :]
                    dq[where] = (piece * cos - swap_halves(piece, lane) * sin).astype(dq.dtype)
        ring(6)
        weight_grad(n1_t_ref, dq, g_buf, shards)
        core_part(g_buf, q_x, 1).start()
        dkv_scatter(1)
        ends_up(8, turns)
        ring(7, 16)
        dkv_hops(0, False)
        scatter_part(g_buf, q_x, q_z, 1)
        ring_down(5)
        ring_down(6)
        dkv_hops(1, False)
        gather_part(o_x, o_z, 0)
        first_up(o_jobs)
        dkv_hops(0, True)
        dkv_hops(1, True)
        ring_down(7)
        load_wq.wait()
        load_wkv.wait()
        back = nt(dq[...], w_buf[...])
        ends_down(0, 3)
        ring(8, 16)
        dkv_gather(0)
        dkv_gather(1)
        g_kv = g_buf.at[:, :, pl.ds(0, 2 * HK * HD)]
        weight_grad(n1_t_ref, dkv_own, g_kv, shards)
        core_part(g_kv, k_x, 2).start()
        back = back + nt(dkv_own[...], wkv_buf[...])
        scatter_part(g_kv, k_x, k_z, 2)
        ring(9, 1)
        hidden = x_ref[...].astype(F32)
        scale = lax.rsqrt(jnp.mean(hidden * hidden, -1, keepdims=True) + EPSILON)
        scaled = back * gains_ref[0:1, :]
        gn_own[0:1, :] = jnp.sum(back * hidden * scale, 0, keepdims=True)
        gain_core = remote(gn_own, gn_x, g_core.at[6], g_core.at[7], sibling)
        gain_core.start()
        x_ref[...] = (
            gm[...]
            + scale * scaled
            - hidden * (scale * scale * scale) * jnp.mean(scaled * hidden, -1, keepdims=True)
        ).astype(BF)
        keep_dx = local(x_ref, out_dx, late_sem.at[1])
        keep_dx.start()
        gain_core.wait()
        gn_own[...] = gn_own[...] + gn_x[...]

        def gain_copy(k):
            return remote(
                gn_own, gn_z.at[k - 1], g_send.at[3], g_recv.at[3], peers[k - 1]
            )

        for k in range(1, shards):
            gain_copy(k).start()
        for k in range(1, shards):
            part_copy(k).start()

        def gather_gain():
            remote(gn_z, gn_z, g_send.at[3], g_recv.at[3], peers[0]).wait()
            total = gn_own[...]
            for k in range(shards - 1):
                total = total + gn_z[k]
            gn_x[...] = total

        @pl.when(jnp.logical_not(has_outer))
        def _():
            gather_part(q_x, q_z, 1)
            for job in q_jobs:
                line_up(*job[:6])
            gather_gain()
            gather_part(k_x, k_z, 2)
            for job in gain_job + k_jobs:
                line_up(*job[:6])

        @pl.when(has_outer)
        def _():
            ring(10, 1)
            ring(11, 1)

        ends_down(3, 8)
        def finish_result():
            remote(p_zone, p_zone, p_send.at[0], p_recv.at[0], peers[0]).wait()
            result = mid_ref[...]
            for first in range(0, shards, 4):
                stage = [
                    local(
                        parts_hbm.at[s_id] if k == 0 else p_zone.at[k - 1],
                        w_buf.at[pl.ds((k - first) * rows, rows)],
                        load_sem.at[k - first],
                    )
                    for k in range(first, min(shards, first + 4))
                ]
                for copy in stage:
                    copy.start()
                for k, copy in enumerate(stage):
                    copy.wait()
                    result = result + w_buf[k * rows : (k + 1) * rows, :].astype(F32)
            dproj[...] = result.astype(BF)
            local(dproj, out_result, late_sem.at[2]).start()

        todo = list(jobs)
        done = []

        def next_up():
            done.append(todo.pop(0))
            job_up(done[-1])

        def last_chunk(index):
            @pl.when(is_mid)
            def _():
                down(index)

        next_up()
        next_up()
        last_chunk(2 * turns - 2)
        next_up()
        last_chunk(2 * turns - 1)
        next_up()

        @pl.when(has_outer)
        def _():
            gather_part(q_x, q_z, 1)
            gather_gain()
            gather_part(k_x, k_z, 2)

        ends_down(8, turns)

        @pl.when(jnp.logical_not(has_outer))
        def _():
            finish_result()

        while todo:
            next_up()
            job_down(done.pop(0))
        for job in done:
            job_down(job)

        @pl.when(has_outer)
        def _():
            finish_result()

        whole = [
            (o_x.at[s_id], o_t, [(o_t, out_wo, 0)]),
            (q_x.at[s_id], q_t, [(q_t, out_wq, 1)]),
            (k_x.at[s_id], k_t, [(k_nat.at[0], out_wk, 2), (k_nat.at[1], out_wv, 3)]),
        ]
        for group, (mine, total, outs) in enumerate(whole):
            line_settle(
                mine,
                total,
                group,
                [
                    (src, rows_at(out, near, 0, own_rows), rows_at(out, far, 0, own_rows), box)
                    for src, out, box in outs
                ],
            )
        line_settle(gn_x, gn_t, 3, [(gn_out, out_gain, None, 4)])
        keep_dx.wait()
        local(dproj, out_result, late_sem.at[2]).wait()

    pl.run_scoped(
        attention,
        v((width, 2 * HK * HD), BF),
        v((2, 1024, 512), BF),
        v((2, 1024, 128), BF),
        v((rows, width), BF),
        v((2 * HK, 512, 128), BF),
        v((2 * HK, 1, 512), F32),
        v((2 * HK, line, 2, 128, 128), BF),
        v((rows, width), BF if blocks == 1 else F32),
        v((rows, 2 * HK * HD), BF),
        v((shards, part, width), BF),
        v((rows, width), BF),
        v((width, rows), BF),
        v((2 * HK, 512, 128), BF),
        v((width, rows), BF),
        v((rows, width), BF),
    )

    for array in range(3):
        settle(array)


def backward_call(shards, line, *arrays):
    x, kv, gate = arrays[7], arrays[-1], arrays[15]
    rows, width = x.shape
    keys = kv.shape[1]
    feed = gate.shape[2]
    part = width // shards
    own_rows = part // 2
    kv_width = 2 * HK * HD
    sizes = (shards, line, keys, rows, width, feed)
    dma = pltpu.SemaphoreType.DMA
    v = pltpu.VMEM
    vm = pl.BlockSpec(memory_space=pltpu.VMEM)
    hbm = pl.BlockSpec(memory_space=pltpu.HBM)
    half = width // 2
    shape = jax.ShapeDtypeStruct

    def boxes(cols):
        return [
            v((shards, own_rows, cols), BF),
            v((shards - 1, own_rows, cols), BF),
            v((own_rows, cols), BF),
            v((own_rows, cols), BF),
        ]

    scratch = [
        v((width, width), BF),
        v((rows, width), F32),
        v((rows, width), F32),
        v((2 * HK, line, 128, 128), BF),
        v((2, 2, 4, HK, 128, 128) if line == 4 else (2, line - 1, HK, 128, 128), BF),
        *[v((2, half, feed), BF) for _ in range(4)],
        *[v((feed, half), BF) for _ in range(4)],
        *boxes(width),
        *boxes(width),
        *boxes(kv_width),
        v((2, width), F32),
        v((2, width), F32),
        v((shards - 1, 2, width), F32),
        v((2, width), F32),
        v((2, width), F32),
        v((2, own_rows, HK * HD), BF),
        v((2, part), F32),
        dma((max(6, shards),)),
        dma((2,)),
        dma((2,)),
        dma((6,)),
        dma((8,)),
        dma((3,)),
        dma((24,)),
        dma((24,)),
        *[dma((3,)) for _ in range(4)],
        dma((4,)),
        dma((2, 1 if line == 4 else line)),
        dma((2, 2 * line)),
        dma((8,)),
        dma((4,)),
        dma((4,)),
        dma((4,)),
        dma((16,)),
        dma((16,)),
        dma((4,)),
        dma((4,)),
        dma((4,)),
        dma((5,)),
        dma((1,)),
        dma((1,)),
        dma((shards - 1,)),
        dma((shards - 1,)),
        dma((9,)),
    ]
    return pl.pallas_call(
        lambda *refs: backward_kernel(sizes, *refs),
        out_shape=(
            shape((width, feed), BF),
            shape((width, feed), BF),
            shape((feed, width), BF),
            shape((part, width), BF),
            shape((part, width), BF),
            shape((part, HK * HD), BF),
            shape((part, HK * HD), BF),
            shape((2, part), F32),
            shape((rows, width), BF),
            shape((rows, width), BF),
            shape((shards, rows, width), BF),
            shape((shards - 1, rows, width), BF),
            shape((shards - 1, rows, width), BF),
        ),
        in_specs=[vm] * 3 + [hbm] * 19,
        out_specs=tuple([hbm] * 13),
        scratch_shapes=scratch,
        compiler_params=pltpu.CompilerParams(
            collective_id=3,
            has_side_effects=True,
            vmem_limit_bytes=VMEM_LIMIT,
        ),
        name="backward",
    )(*arrays)


def per_device(
    tokens,
    cotangent,
    positions,
    lengths,
    attn_gain,
    w_query,
    w_key,
    w_value,
    w_out,
    mlp_gain,
    w_gate,
    w_up,
    w_down,
):
    seqs, stretch, width = tokens.shape
    shards, line = lax.axis_size("shard"), lax.axis_size("line")
    rows = seqs * stretch
    frequency = ROPE_BASE ** (-np.arange(HD // 2, dtype=np.float32) * 2.0 / HD)
    frequency = np.tile(frequency, 4)[None].astype(np.float32)
    x = tokens.reshape(rows, width)
    (
        gains,
        cos_wide,
        sin_wide,
        wq_all,
        wkv_all,
        out_all,
        packed_kv,
        soft,
        grad_all,
        attn,
        attn_t,
        norm_t,
        packed_q,
        middle,
        inner,
        back,
        norm_all_t,
        inner_t,
        grad_gate,
        grad_up,
    ) = front_call(
        shards,
        line,
        positions,
        lengths,
        frequency,
        attn_gain,
        mlp_gain,
        w_key,
        w_value,
        x,
        cotangent.reshape(rows, width),
        w_query,
        w_out,
        w_gate,
        w_up,
        w_down,
    )
    (
        sum_gate,
        sum_up,
        sum_down,
        sum_out,
        sum_query,
        sum_key,
        sum_value,
        sum_gain,
        grad_input,
        result,
        _,
        _,
        _,
    ) = backward_call(
        shards,
        line,
        gains,
        cos_wide,
        sin_wide,
        attn,
        attn_t,
        packed_q,
        norm_t,
        x,
        middle,
        inner,
        w_down,
        back,
        norm_all_t,
        grad_all,
        inner_t,
        grad_gate,
        grad_up,
        out_all,
        wq_all,
        wkv_all,
        soft,
        packed_kv.reshape(seqs * HK, -1, 128),
    )
    arrays = [sum_gate, sum_up, sum_down, sum_query, sum_out, sum_key, sum_value]
    arrays = widen_call(sum_gain, arrays + [grad_input, result], [F32] * 7 + [BF] * 2)
    sum_gate, sum_up, sum_down, sum_query, sum_out, sum_key, sum_value = arrays[:7]
    grad_input, result, gain_one, gain_two = arrays[7:]
    return (
        result.reshape(seqs, stretch, width),
        grad_input.reshape(seqs, stretch, width),
        gain_one,
        sum_query,
        sum_key,
        sum_value,
        sum_out,
        gain_two,
        sum_gate,
        sum_up,
        sum_down,
    )


def solution(mesh):
    shards, ctx = mesh.devices.shape
    inner = Mesh(mesh.devices.reshape(shards, ctx // 2, 2), ("shard", "line", "core"))
    where = ("line", "core")
    return jax.shard_map(
        per_device,
        mesh=inner,
        in_specs=(
            P("shard", where, None),
            P("shard", where, None),
            P("shard", None),
            P("shard"),
            P("shard"),
            P("shard", None),
            P("shard", None),
            P("shard", None),
            P("shard", None),
            P("shard"),
            P(None, "shard"),
            P(None, "shard"),
            P("shard", None),
        ),
        out_specs=(
            P("shard", where, None),
            P("shard", where, None),
            P("shard"),
            P("shard", None),
            P("shard", None),
            P("shard", None),
            P("shard", None),
            P("shard"),
            P(None, "shard"),
            P(None, "shard"),
            P("shard", None),
        ),
        check_vma=False,
    )
```
